32 devices in a mesh: grp: 2 (over x), spec: 16 (over z, y, core).
Axes of the slice: x: 2, y: 2, z: 4, core: 2. Of those that a mesh axis runs over, the one named last changes fastest.
Arguments:
- spectrum: float32 [3072, 1536], P(('grp', 'spec')), parts along dimension 0, may hold values from 0.05 to 5
- sea_mask: int32 [1536], replicated, may hold values from 0 to 1, as said below
- wind_speed: float32 [3072], P('grp'), parts along dimension 0, may hold values from 0.3 to 3
- wind_angle: float32 [3072], P('grp'), parts along dimension 0, may hold values from -3.140625 to 3.140625
Outputs:
- new_spectrum: float32 [3072, 1536], P(('grp', 'spec')), parts along dimension 0
- wave_height: float32 [3072], P(('grp', 'spec')), parts along dimension 0
- mean_height: float32 [2], P('grp'), parts along dimension 0
The draws below stay inside these ranges and needn't reach their ends.
There are 2 independent parts, one for each index of `grp`. The reference program is written for one: setup_inputs(seed, part) draws one part's arguments, and reference() takes and returns one part's arrays. A program takes and returns all parts, laid end to end along the dimension named above; an argument that names none is the same for every part. Nothing has to cross between parts.
Inputs may be any that keep to these rules, and one draw needn't show every extreme that they name: `sea_mask`: exactly 1024 cells are sea.
All inputs are finite; a program needn't handle non-finite values.
Results may differ from the reference program's by a relative error of at most 0.00002.
Values sent between devices are 32-bit elements; how exact they have to be, the bound alone decides.
A program may use at most 64 MiB of HBM per device.

```python
import math
import jax
import jax.numpy as jnp
from jax import lax

NF = 48
ND = 32
NLON = 384
ADV_STEPS = 2
PTS_DEV = 96
BINS = 1536
CELLS = 1536
NLAT = 4
SEA = 1024
N_SPEC = 16


def draw_sea_mask(key, part):
    coarse_key, fine_key = jax.random.split(jax.random.fold_in(key, 17))
    block_rows = (NLAT + 7) // 8
    block_cols = (NLON + 7) // 8
    coarse = jax.random.randint(coarse_key, (block_rows, block_cols), 0, 64)
    fine = jax.random.randint(fine_key, (NLAT, NLON), 0, 16)
    row_ids = jnp.arange(NLAT, dtype=jnp.int32) // 8
    col_ids = jnp.arange(NLON, dtype=jnp.int32) // 8
    spread = coarse[row_ids][:, col_ids] * 16 + fine
    scores = spread.reshape(-1) * CELLS + jnp.arange(CELLS, dtype=jnp.int32)
    order = jnp.argsort(scores, stable=True)
    chosen = order[:SEA]
    return jnp.zeros((CELLS,), jnp.int32).at[chosen].set(1)


def levels(stream_key, shape, cuts, least, top_value):
    def one(position, blocks):
        draws = jax.random.uniform(jax.random.fold_in(jax.random.fold_in(stream_key, 6), position), (blocks,), jnp.float32, least / len(cuts), top_value / len(cuts))
        return jnp.repeat(jnp.exp(draws), shape[position] // blocks).reshape((-1,) + (1,) * (len(shape) - position - 1))

    factor_of = one(*cuts[0])
    for cut in cuts[1:]:
        factor_of = factor_of * one(*cut)
    return factor_of


def setup_inputs(seed: int = 0, part: int = 0) -> dict:
    key_of = jax.random.split(jax.random.key(seed), 5)
    part_splits = jax.random.split(jax.random.fold_in(key_of[4], part), 5)
    spectrum = jnp.clip(jnp.exp(math.log(5.0) - 4.6051702 * jax.random.uniform(part_splits[0], (BINS, CELLS), jnp.float32) ** levels(part_splits[0], (BINS, CELLS), ((0, 16),), -0.2, 0.2)), 0.05, 5.0)
    sea_mask = draw_sea_mask(jax.random.fold_in(key_of[4], 71), part)
    wind_speed = jnp.clip(jnp.exp(jax.random.uniform(part_splits[2], (CELLS,), jnp.float32, math.log(0.3), math.log(3.0))), 0.3, 3.0)
    wind_angle = jnp.clip(jax.random.uniform(part_splits[3], (CELLS,), jnp.float32, -3.140625, 3.140625), -3.140625, 3.140625)
    return {"spectrum": spectrum, "sea_mask": sea_mask, "wind_speed": wind_speed, "wind_angle": wind_angle}


def upwind_step(energy, courant_x, courant_y, sea_grid):
    west_cell = jnp.roll(energy, 1, axis=2)
    east_cell = jnp.roll(energy, -1, axis=2)
    edge_row = jnp.zeros_like(energy[:, :1])
    south_cell = jnp.concatenate([edge_row, energy[:, :-1]], axis=1)
    north_cell = jnp.concatenate([energy[:, 1:], edge_row], axis=1)
    updated = energy - jnp.maximum(courant_x, 0.0) * (energy - west_cell) - jnp.minimum(courant_x, 0.0) * (east_cell - energy) - jnp.maximum(courant_y, 0.0) * (energy - south_cell) - jnp.minimum(courant_y, 0.0) * (north_cell - energy)
    return updated * sea_grid

def courant_numbers(freq_index, dir_index, lat_count, dir_count):
    speed = 0.2 * jnp.exp(-math.log(1.1) * freq_index)
    heading = 2.0 * math.pi * (dir_index + 0.5) / dir_count
    rows = jnp.arange(lat_count, dtype=jnp.float32)
    latitude = (-75.0 + 150.0 * (rows + 0.5) / lat_count) * (math.pi / 180.0)
    courant_x = (speed * jnp.cos(heading))[:, None, None] / jnp.cos(latitude)[None, :, None]
    courant_y = (speed * jnp.sin(heading))[:, None, None]
    return (courant_x, courant_y)

def shift_freq(values, amount):
    if amount > 0:
        filler = jnp.zeros_like(values[:amount])
        return jnp.concatenate([filler, values[:-amount]], axis=0)
    filler = jnp.zeros_like(values[:-amount])
    return jnp.concatenate([values[-amount:], filler], axis=0)

def source_terms(energy, speed, angle):
    freq_count = energy.shape[0]
    dir_count = energy.shape[1]
    freq_ids = jnp.arange(freq_count, dtype=jnp.float32)
    frequency = jnp.exp(math.log(1.1) * (freq_ids - freq_count // 2))[:, None, None]
    heading = (2.0 * math.pi * (jnp.arange(dir_count, dtype=jnp.float32) + 0.5) / dir_count)[None, :, None]
    energy_mean = lax.optimization_barrier(jnp.mean(energy, axis=(0, 1)))
    moment_one = lax.optimization_barrier(jnp.mean(frequency * energy, axis=(0, 1)))
    mean_freq = moment_one / (energy_mean + 1e-06)
    steepness = energy_mean * mean_freq * mean_freq
    breaking = steepness * steepness / (1.0 + steepness * steepness)
    wind_gain = 0.05 * frequency * jnp.maximum(0.0, speed[None, None, :] * frequency * jnp.cos(heading - angle[None, None, :]) - 1.0)
    damping = 0.03 * frequency * breaking[None, None, :]
    valid = ((freq_ids >= 3) & (freq_ids <= freq_count - 3)).astype(jnp.float32)[:, None, None]
    interaction = jnp.zeros_like(energy)
    for mirror in (1, -1):
        plus_bins = shift_freq(jnp.roll(energy, -mirror, axis=1), -2)
        minus_bins = shift_freq(jnp.roll(energy, 3 * mirror, axis=1), 3)
        transfer_rate = 0.001 * valid * (energy * energy * (plus_bins + minus_bins) - 2.0 * energy * plus_bins * minus_bins)
        interaction = interaction - 2.0 * transfer_rate
        interaction = interaction + jnp.roll(shift_freq(transfer_rate, 2), mirror, axis=1)
        interaction = interaction + jnp.roll(shift_freq(transfer_rate, -3), -3 * mirror, axis=1)
    updated = energy + (wind_gain - damping) * energy + interaction
    raw_height = 4.0 * jnp.sqrt(lax.optimization_barrier(jnp.mean(updated, axis=(0, 1))) + 1e-06)
    return (updated, raw_height)

def reference(spectrum, sea_mask, wind_speed, wind_angle):
    sea_float = sea_mask.astype(jnp.float32)
    sea_grid = sea_float.reshape(1, NLAT, NLON)
    bands = (spectrum * sea_float[None, :]).reshape(NF, ND, NLAT, NLON)

    def advect_band(inputs):
        band, freq_value = inputs
        dir_index = jnp.arange(ND, dtype=jnp.float32)
        freq_index = jnp.zeros((ND,), jnp.float32) + freq_value
        courant_x, courant_y = courant_numbers(freq_index, dir_index, NLAT, ND)
        for substep in range(ADV_STEPS):
            band = upwind_step(band, courant_x, courant_y, sea_grid)
        return band
    advected = lax.map(advect_band, (bands, jnp.arange(NF, dtype=jnp.float32)))
    blocks = jnp.moveaxis(advected.reshape(NF, ND, N_SPEC, PTS_DEV), 2, 0)
    speed_blocks = wind_speed.reshape(N_SPEC, PTS_DEV)
    angle_blocks = wind_angle.reshape(N_SPEC, PTS_DEV)

    def block_sources(inputs):
        return source_terms(inputs[0], inputs[1], inputs[2])
    updated, raw_height = lax.map(block_sources, (blocks, speed_blocks, angle_blocks))
    new_spectrum = jnp.moveaxis(updated, 0, 2).reshape(NF * ND, CELLS)
    wave_height = sea_float * raw_height.reshape(CELLS)
    mean_height = (jnp.sum(wave_height) / SEA).reshape(1)
    return (new_spectrum, wave_height, mean_height)
```

```python
import functools
import math

import jax
import jax.numpy as jnp
from jax import lax
from jax.experimental import pallas as pl
from jax.experimental.pallas import tpu as pltpu
from jax.sharding import PartitionSpec as P

NF = 48
ND = 32
NLON = 384
ADV_STEPS = 2
SEA_DEV = 64


def upwind_step(energy, courant_x, courant_y, sea_grid):
    west_cell = jnp.roll(energy, 1, axis=2)
    east_cell = jnp.roll(energy, -1, axis=2)
    edge_row = jnp.zeros_like(energy[:, :1])
    south_cell = jnp.concatenate([edge_row, energy[:, :-1]], axis=1)
    north_cell = jnp.concatenate([energy[:, 1:], edge_row], axis=1)
    updated = (
        energy
        - jnp.maximum(courant_x, 0.0) * (energy - west_cell)
        - jnp.minimum(courant_x, 0.0) * (east_cell - energy)
        - jnp.maximum(courant_y, 0.0) * (energy - south_cell)
        - jnp.minimum(courant_y, 0.0) * (north_cell - energy)
    )
    return updated * sea_grid


def courant_numbers(freq_index, dir_index, lat_count, dir_count):
    speed = 0.2 * jnp.exp(-math.log(1.1) * freq_index)
    heading = 2.0 * math.pi * (dir_index + 0.5) / dir_count
    rows = jnp.arange(lat_count, dtype=jnp.float32)
    latitude = (-75.0 + 150.0 * (rows + 0.5) / lat_count) * (math.pi / 180.0)
    courant_x = (speed * jnp.cos(heading))[:, None, None] / jnp.cos(latitude)[None, :, None]
    courant_y = (speed * jnp.sin(heading))[:, None, None]
    return (courant_x, courant_y)


def shift_freq(values, amount):
    if amount > 0:
        filler = jnp.zeros_like(values[:amount])
        return jnp.concatenate([filler, values[:-amount]], axis=0)
    filler = jnp.zeros_like(values[:-amount])
    return jnp.concatenate([values[-amount:], filler], axis=0)


def source_terms(energy, speed, angle):
    freq_count = energy.shape[0]
    dir_count = energy.shape[1]
    freq_ids = jnp.arange(freq_count, dtype=jnp.float32)
    frequency = jnp.exp(math.log(1.1) * (freq_ids - freq_count // 2))[:, None, None]
    heading = (2.0 * math.pi * (jnp.arange(dir_count, dtype=jnp.float32) + 0.5) / dir_count)[
        None, :, None
    ]
    energy_mean = jnp.mean(energy, axis=(0, 1))
    moment_one = jnp.mean(frequency * energy, axis=(0, 1))
    mean_freq = moment_one / (energy_mean + 1e-06)
    steepness = energy_mean * mean_freq * mean_freq
    breaking = steepness * steepness / (1.0 + steepness * steepness)
    wind_gain = (
        0.05
        * frequency
        * jnp.maximum(
            0.0, speed[None, None, :] * frequency * jnp.cos(heading - angle[None, None, :]) - 1.0
        )
    )
    damping = 0.03 * frequency * breaking[None, None, :]
    valid = ((freq_ids >= 3) & (freq_ids <= freq_count - 3)).astype(jnp.float32)[:, None, None]
    interaction = jnp.zeros_like(energy)
    for mirror in (1, -1):
        plus_bins = shift_freq(jnp.roll(energy, -mirror, axis=1), -2)
        minus_bins = shift_freq(jnp.roll(energy, 3 * mirror, axis=1), 3)
        transfer_rate = (
            0.001
            * valid
            * (energy * energy * (plus_bins + minus_bins) - 2.0 * energy * plus_bins * minus_bins)
        )
        interaction = interaction - 2.0 * transfer_rate
        interaction = interaction + jnp.roll(shift_freq(transfer_rate, 2), mirror, axis=1)
        interaction = interaction + jnp.roll(shift_freq(transfer_rate, -3), -3 * mirror, axis=1)
    updated = energy + (wind_gain - damping) * energy + interaction
    raw_height = 4.0 * jnp.sqrt(jnp.mean(updated, axis=(0, 1)) + 1e-06)
    return (updated, raw_height)


def local(spectrum, sea_mask, wind_speed, wind_angle):
    count = lax.axis_size("spec")
    position = lax.axis_index("spec")
    bins_dev = spectrum.shape[0]
    cells = spectrum.shape[1]
    points = cells // count
    lat_count = cells // NLON
    sea_float = sea_mask.astype(jnp.float32)
    bin_ids = position * bins_dev + jnp.arange(bins_dev, dtype=jnp.int32)
    freq_index = (bin_ids // ND).astype(jnp.float32)
    dir_index = (bin_ids % ND).astype(jnp.float32)
    courant_x, courant_y = courant_numbers(freq_index, dir_index, lat_count, ND)
    sea_grid = sea_float.reshape(1, lat_count, NLON)
    energy = (spectrum * sea_float[None, :]).reshape(bins_dev, lat_count, NLON)
    for substep in range(ADV_STEPS):
        energy = upwind_step(energy, courant_x, courant_y, sea_grid)
    advected = energy.reshape(bins_dev, cells)
    outgoing = advected.reshape(bins_dev, count, points)
    arrived = lax.all_to_all(outgoing, "spec", split_axis=1, concat_axis=0, tiled=True)
    start = position * points
    speed_own = lax.dynamic_slice_in_dim(wind_speed, start, points)
    angle_own = lax.dynamic_slice_in_dim(wind_angle, start, points)
    sea_own = lax.dynamic_slice_in_dim(sea_float, start, points)
    updated, raw_height = source_terms(arrived.reshape(NF, ND, points), speed_own, angle_own)
    wave_height = sea_own * raw_height
    own_total = jnp.zeros((count, 1), jnp.float32) + jnp.sum(wave_height)
    returned, totals = (
        lax.all_to_all(
            updated.reshape(NF * ND, 1, points), "spec", split_axis=0, concat_axis=1, tiled=True
        ),
        lax.all_to_all(own_total, "spec", split_axis=0, concat_axis=1, tiled=True),
    )
    new_spectrum = returned.reshape(bins_dev, cells)
    height_sum = jnp.sum(totals)
    mean_height = (height_sum / (SEA_DEV * count)).reshape(1)
    return (new_spectrum, wave_height, mean_height)


HALO = 5
LANES = 128
WIDE = 256
LAND = 4096.0


def group_size(count, bins_dev, cells):
    size = 4
    if count % size or bins_dev % ND or cells % (size * LANES) or cells % NLON:
        return 0
    if NLON % LANES or bins_dev // ND * size < 2 * HALO or cells % count:
        return 0
    sea = SEA_DEV * count
    if sea > min(cells, LAND) or sea % (size * LANES) or sea % WIDE or cells % WIDE:
        return 0
    if (cells - sea) % WIDE:
        return 0
    return size


def split_bf16(values):
    high = values.astype(jnp.bfloat16)
    left = values - high.astype(jnp.float32)
    mid = left.astype(jnp.bfloat16)
    low = (left - mid.astype(jnp.float32)).astype(jnp.bfloat16)
    return high, mid, low


def rows_of(parts, height, width):
    ids = lax.broadcasted_iota(jnp.int32, (height, width), 0)
    out = jnp.zeros((height, width), jnp.float32)
    for i, part in enumerate(parts):
        out = jnp.where(ids == i, jnp.broadcast_to(part.astype(jnp.float32), (height, width)), out)
    return out.astype(jnp.bfloat16)


def fused_kernel(
    count, group, sea_in, wind_in, angle_in, spec_ref, out_ref, height_ref, spread_ref,
    sea_raw, wind_raw, angle_raw, aux_ref, aux_sem,
    raw, moved, split, pick, wsplit, adv, held, done, mom_out, mom_in, wind, acc, sum_out, sum_in,
    load_sem, held_sem, y_sem, up_sem, down_sem, mom_send, mom_recv,
    ret_send, ret_recv, sum_send, sum_recv,
):
    f32, bf16 = jnp.float32, jnp.bfloat16
    freq_dev, _, sea_cells = adv.shape
    cells = moved.shape[1]
    freq_group = freq_dev * group
    width = sea_cells // group
    zones = count // group
    lat_count = cells // NLON
    sides = group // 2
    parts = width // LANES
    blocks = sea_cells // LANES
    cell_tiles = cells // LANES
    reach = cells - sea_cells + LANES
    me = lax.axis_index("spec")
    zone, rank = me // group, me % group
    side, core = rank // 2, rank % 2

    def remote(src, dst, send, recv, target):
        return pltpu.make_async_remote_copy(
            src_ref=src, dst_ref=dst, send_sem=send, recv_sem=recv,
            device_id={"spec": target}, device_id_type=pl.DeviceIdType.MESH,
        )

    barrier = pltpu.get_barrier_semaphore()
    for step in range(1, count):
        pl.semaphore_signal(
            barrier, inc=1, device_id={"spec": (me + step) % count},
            device_id_type=pl.DeviceIdType.MESH,
        )
    loads = [
        pltpu.make_async_copy(
            spec_ref.at[pl.ds(f * ND, ND)], raw.at[pl.ds(f * ND, ND)], load_sem.at[f]
        )
        for f in range(freq_dev)
    ]
    small = [
        pltpu.make_async_copy(sea_in, sea_raw, aux_sem.at[0]),
        pltpu.make_async_copy(wind_in, wind_raw, aux_sem.at[1]),
        pltpu.make_async_copy(angle_in, angle_raw, aux_sem.at[2]),
    ]
    for load in small[:1] + loads + small[1:]:
        load.start()

    @pl.when(zone == 0)
    def _():
        held[0:HALO] = jnp.zeros((HALO, ND, width), f32)

    @pl.when(zone == zones - 1)
    def _():
        held[HALO + freq_group :] = jnp.zeros((HALO, ND, width), f32)

    def block_of(index, t):
        return t * group + index

    def tile_of(index, t):
        return pl.ds(pl.multiple_of(block_of(index, t) * LANES, LANES), LANES)

    def lanes_of(t):
        return pl.ds(t * LANES, LANES)

    offsets = [(dy, dc) for dy in range(sides) for dc in range(2)]

    def rank_of(offset):
        return (side + offset[0]) % sides * 2 + (core + offset[1]) % 2

    def y_copy(f, i, t):
        peer = rank_of(offsets[i])
        slot = HALO + rank * freq_dev + f
        return remote(
            adv.at[f, :, tile_of(peer, t)], held.at[slot, :, lanes_of(t)],
            y_sem.at[i - 1, f, t], held_sem.at[slot, t], zone * group + peer,
        )

    order = list(range(2, group)) + [1]

    dirs = lax.broadcasted_iota(jnp.int32, (ND, LANES), 0).astype(f32)
    heading = 2.0 * math.pi * (dirs + 0.5) / ND
    cos_h, sin_h = jnp.cos(heading), jnp.sin(heading)
    log_step = math.log(1.1)
    lats = [math.radians(-75.0 + 150.0 * (r + 0.5) / lat_count) for r in range(lat_count)]

    square_rows = lax.broadcasted_iota(jnp.int32, (LANES, LANES), 0)
    square_cols = lax.broadcasted_iota(jnp.int32, (LANES, LANES), 1)
    lane_ids = square_cols.astype(f32)
    ones = jnp.ones((LANES, LANES), bf16)

    small[0].wait()
    aux_ref[...] = sea_raw[...].astype(f32).reshape(1, cells)
    sea = [aux_ref[0:1, r * NLON : (r + 1) * NLON] for r in range(lat_count)]
    mask = [aux_ref[0:1, i * LANES : (i + 1) * LANES] for i in range(cell_tiles)]
    before = [jnp.zeros((1, 1), f32)]
    for i in range(cell_tiles):
        before.append(before[i] + jnp.sum(mask[i], axis=1, keepdims=True))
    for i in range(cell_tiles):
        tri = jnp.where(
            square_cols < square_rows,
            mask[i],
            jnp.where(square_cols == square_rows, LAND * (1.0 - mask[i]), 0.0),
        )
        within = jnp.dot(tri.astype(bf16), ones, preferred_element_type=f32)
        place = within + before[i]
        for b in range(blocks):
            if b <= i and (i - b) * LANES < reach:
                hit = jnp.where(place == lane_ids + float(b * LANES), 1.0, 0.0)
                pick[b, (i - b) * LANES : (i - b + 1) * LANES, :] = hit.astype(bf16)

    quarter = ND // 4
    tiles = NLON // LANES
    mom_out[...] = jnp.zeros_like(mom_out)

    def picked(values, b):
        cols = pl.ds(pl.multiple_of(b * LANES, LANES), reach)
        return jnp.dot(values[:, cols], pick[b], preferred_element_type=f32)

    for f in range(freq_dev):
        loads[f].wait()
        freq = (me * freq_dev + f).astype(f32)
        speed = 0.2 * jnp.exp(jnp.full((quarter, LANES), -log_step, f32) * freq)
        omega = jnp.exp(jnp.full((1, LANES), log_step, f32) * (freq - NF // 2))
        for q in range(4):
            east, north = q in (0, 3), q in (0, 1)
            rows = slice(f * ND + q * quarter, f * ND + (q + 1) * quarter)
            part = slice(q * quarter, (q + 1) * quarter)
            cx0 = speed * jnp.abs(cos_h[part])
            cy = jnp.concatenate([speed * jnp.abs(sin_h[part])] * tiles, axis=1)
            cx = [jnp.concatenate([cx0 * (1.0 / math.cos(a))] * tiles, axis=1) for a in lats]
            energy = [raw[rows, r * NLON : (r + 1) * NLON] * sea[r] for r in range(lat_count)]
            for _ in range(ADV_STEPS):
                fresh = []
                for r in range(lat_count):
                    e = energy[r]
                    side_x = pltpu.roll(e, 1 if east else NLON - 1, 1)
                    other = r - 1 if north else r + 1
                    side_y = energy[other] if 0 <= other < lat_count else 0.0
                    fresh.append((e - cx[r] * (e - side_x) - cy * (e - side_y)) * sea[r])
                energy = fresh
            for r in range(lat_count):
                moved[rows, r * NLON : (r + 1) * NLON] = energy[r]
        for i, piece in enumerate(split_bf16(moved[f * ND : (f + 1) * ND])):
            split[f, i * ND : (i + 1) * ND, :] = piece
        if f == 0:
            pl.semaphore_wait(barrier, count - 1)
        for t in range(parts):
            for i in order + [0]:
                peer = rank_of(offsets[i])
                got = picked(split.at[f], block_of(peer, t))
                got = got[:ND] + got[ND : 2 * ND] + got[2 * ND :]
                if i:
                    adv[f, :, tile_of(peer, t)] = got
                    if t == 0:
                        y_copy(f, i, t).start()
                else:
                    held[HALO + rank * freq_dev + f, :, lanes_of(t)] = got
                total = jnp.sum(got, axis=0, keepdims=True)
                mom_out[0:1, tile_of(peer, t)] += total
                mom_out[1:2, tile_of(peer, t)] += omega * total

    for step in range(1, count):
        target = (me + step) % count
        for t in range(parts):
            remote(
                mom_out.at[:, tile_of(target % group, t)], mom_in.at[me, :, lanes_of(t)],
                mom_send.at[step - 1, t], mom_recv.at[me, t], target,
            ).start()
    for t in range(parts):
        mom_in[me, :, lanes_of(t)] = mom_out[:, tile_of(rank, t)]
    for t in range(1, parts):
        for f in range(freq_dev):
            for i in order:
                y_copy(f, i, t).start()

    small[1].wait()
    small[2].wait()
    speed_all = wind_raw[...].reshape(1, cells)
    angle_all = angle_raw[...].reshape(1, cells)
    wsplit[...] = rows_of(
        split_bf16(speed_all * jnp.cos(angle_all)) + split_bf16(speed_all * jnp.sin(angle_all)),
        2 * quarter, cells,
    )
    for t in range(parts):
        own = picked(wsplit, block_of(rank, t))
        along = own[0:1] + own[1:2] + own[2:3]
        across = own[3:4] + own[4:5] + own[5:6]
        wind[:, t * LANES : (t + 1) * LANES] = cos_h * along + sin_h * across

    tri_up = jnp.where(square_rows < square_cols, 1.0, 0.0).astype(bf16)
    ranks = jnp.dot(
        rows_of(mask, 2 * quarter, LANES), tri_up, preferred_element_type=f32
    )
    places = [
        jnp.where(mask[i] > 0.0, ranks[i : i + 1] + before[i], LAND) for i in range(cell_tiles)
    ]
    wide_rows = lax.broadcasted_iota(jnp.int32, (WIDE, LANES), 0).astype(f32)
    for j in range(cells // WIDE):
        for u in range(sea_cells // WIDE):
            if u * WIDE < (j + 1) * WIDE and (u + 1) * WIDE > j * WIDE - (cells - sea_cells):
                for h in range(WIDE // LANES):
                    i = j * (WIDE // LANES) + h
                    hit = jnp.where(wide_rows + float(u * WIDE) == places[i], 1.0, 0.0)
                    spread_ref[
                        u * WIDE : (u + 1) * WIDE, i * LANES : (i + 1) * LANES
                    ] = hit.astype(bf16)

    def up_copy(slot, t):
        return remote(
            held.at[HALO + slot, :, lanes_of(t)],
            held.at[HALO + slot - freq_group, :, lanes_of(t)],
            up_sem.at[slot - (freq_group - HALO), t],
            held_sem.at[HALO + slot - freq_group, t],
            (zone + 1) % zones * group + rank,
        )

    def down_copy(slot, t):
        return remote(
            held.at[HALO + slot, :, lanes_of(t)],
            held.at[HALO + slot + freq_group, :, lanes_of(t)],
            down_sem.at[slot, t],
            held_sem.at[HALO + slot + freq_group, t],
            (zone + zones - 1) % zones * group + rank,
        )

    def arrive(index, t):
        block = held.at[index, :, lanes_of(t)]
        remote(
            block, block, up_sem.at[0, t], held_sem.at[index, t], (me + 1) % count
        ).wait_recv()

    def arrive_group(dy, t):
        for f in range(freq_dev):
            for dc in range(2):
                slot = rank_of((dy, dc)) * freq_dev + f
                if (dy, dc) != (0, 0):
                    arrive(HALO + slot, t)

                @pl.when((slot >= freq_group - HALO) & (zone < zones - 1))
                def _():
                    up_copy(slot, t).start()

                @pl.when((slot < HALO) & (zone > 0))
                def _():
                    down_copy(slot, t).start()

    for t in range(parts):
        arrive_group(0, t)
    for dy in range(1, sides):
        arrive_group(dy, 0)

    for step in range(1, count):
        source = (me + step) % count
        for t in range(parts):
            block = mom_in.at[source, :, lanes_of(t)]
            remote(
                block, block, mom_send.at[0, t], mom_recv.at[source, t], source
            ).wait_recv()
    total = jnp.sum(mom_in[...], axis=0) * (1.0 / (NF * ND))
    energy_mean, moment_one = total[0:1], total[1:2]
    mean_freq = moment_one / (energy_mean + 1e-06)
    steepness = energy_mean * mean_freq * mean_freq
    breaking = steepness * steepness / (1.0 + steepness * steepness)

    acc[...] = jnp.zeros_like(acc)
    ascending = side > 0

    def arrive_halo(at_top, t):
        @pl.when(jnp.where(at_top, zone < zones - 1, zone > 0))
        def _():
            for i in range(HALO):
                arrive(jnp.where(at_top, HALO + freq_group + i, i), t)

    def ret_copy(owner, t):
        return remote(
            done.at[pl.ds(owner * freq_dev, freq_dev), :, lanes_of(t)],
            out_ref.at[:, :, tile_of(rank, t)],
            ret_send.at[owner, t], ret_recv.at[rank, t], zone * group + owner,
        )

    def sources(t, begin, end):
        lanes = slice(t * LANES, (t + 1) * LANES)

        def source_step(i, carry):
            k = jnp.where(ascending, i, freq_group - 1 - i)
            freq = zone * freq_group + k

            def scale(index, factor):
                return jnp.where((index >= 3) & (index <= NF - 3), factor, 0.0).astype(f32)

            w_own = scale(freq, -0.002)
            w_low, w_high = scale(freq - 2, 0.001), scale(freq + 3, 0.001)
            omega = jnp.exp(
                jnp.full((1, LANES), log_step, f32) * (freq.astype(f32) - NF // 2)
            )

            def slab(shift):
                return held[HALO + k + shift, :, lanes]

            def turn(values, amount):
                return pltpu.roll(values, amount % ND, 0)

            def rate(a, p, m):
                return a * (a * (p + m) - 2.0 * (p * m))

            own = slab(0)
            p2, m3, m2, m5, p3, p5 = (slab(shift) for shift in (2, -3, -2, -5, 3, 5))
            near = rate(own, turn(p2, -1), turn(m3, 3)) + rate(own, turn(p2, 1), turn(m3, -3))
            low = rate(turn(m2, 1), own, turn(m5, 4)) + rate(turn(m2, -1), own, turn(m5, -4))
            high = rate(turn(p3, -3), turn(p5, -4), own) + rate(turn(p3, 3), turn(p5, 4), own)
            interaction = w_own * near + w_low * low + w_high * high
            gain = (0.05 * omega) * jnp.maximum(0.0, wind[:, lanes] * omega - 1.0)
            damping = (0.03 * omega) * breaking[:, lanes]
            fresh = own + (gain - damping) * own + interaction
            done[k, :, lanes] = fresh
            acc[:, lanes] += fresh
            return carry

        lax.fori_loop(begin, end, source_step, 0)

    half = freq_group // 2
    near_side = rank_of((0, 1))

    def first_half(t):
        arrive_halo(jnp.logical_not(ascending), t)
        sources(t, 0, half)
        for dy in range(1, sides):
            for dc in range(2):
                ret_copy(rank_of((dy, dc)), t).start()

    def second_half(t):
        arrive_halo(ascending, t)
        sources(t, half, freq_group)
        ret_copy(near_side, t).start()
        out_ref[:, :, tile_of(rank, t)] = done[
            pl.ds(rank * freq_dev, freq_dev), :, lanes_of(t)
        ]

    first_half(0)
    for t in range(1, parts):
        for dy in range(1, sides):
            arrive_group(dy, t)
        first_half(t)
        second_half(t - 1)
    second_half(parts - 1)

    sum_out[...] = jnp.sum(acc[...], axis=0, keepdims=True)

    def sum_copy(step):
        return remote(
            sum_out, sum_in.at[me], sum_send.at[step - 1], sum_recv.at[me], (me + step) % count
        )

    for step in range(1, count):
        sum_copy(step).start()
    sum_in[me] = sum_out[...]
    for step in range(1, count):
        source = (me + step) % count
        remote(
            sum_out, sum_in.at[source], sum_send.at[0], sum_recv.at[source], source
        ).wait_recv()

    for g in range(group):
        mass = sum_in[g]
        for other in range(1, zones):
            mass = mass + sum_in[other * group + g]
        height = 4.0 * jnp.sqrt(mass * (1.0 / (NF * ND)) + 1e-06)
        for t in range(parts):
            height_ref[0:1, block_of(g, t) * LANES : (block_of(g, t) + 1) * LANES] = height[
                :, t * LANES : (t + 1) * LANES
            ]

    for t in range(parts):
        for i in range(1, group):
            peer = rank_of(offsets[i])
            remote(
                done.at[pl.ds(0, freq_dev), :, lanes_of(t)], out_ref.at[:, :, tile_of(peer, t)],
                ret_send.at[peer, t], ret_recv.at[peer, t], zone * group + peer,
            ).wait_recv()
            for f in range(freq_dev):
                y_copy(f, i, t).wait_send()
            ret_copy(peer, t).wait_send()
    for step in range(1, count):
        for t in range(parts):
            remote(
                mom_out.at[:, tile_of(0, t)], mom_in.at[me, :, lanes_of(t)],
                mom_send.at[step - 1, t], mom_recv.at[me, t], (me + step) % count,
            ).wait_send()
        sum_copy(step).wait_send()

    @pl.when(zone < zones - 1)
    def _():
        for t in range(parts):
            for slot in range(freq_group - HALO, freq_group):
                up_copy(slot, t).wait_send()

    @pl.when(zone > 0)
    def _():
        for t in range(parts):
            for slot in range(HALO):
                down_copy(slot, t).wait_send()


def store_kernel(
    count, new_in, height_in, spread_in, new_out, wave_ref, mean_ref, split, full, tall, sem
):
    rows, cells = full.shape
    sea_cells = height_in.shape[1]
    land = cells - sea_cells
    f32 = jnp.float32
    me = lax.axis_index("spec")
    height = height_in[...]
    mean_ref[...] = jnp.sum(height, axis=1, keepdims=True) * (1.0 / sea_cells)
    for i, piece in enumerate(split_bf16(new_in[...].reshape(rows, sea_cells))):
        split[i * rows : (i + 1) * rows, :] = piece
    split[3 * rows :, :] = rows_of(split_bf16(height), split.shape[0] - 3 * rows, sea_cells)
    copies = []
    for j in range(cells // WIDE):
        low, high = max(0, j * WIDE - land), min(sea_cells, (j + 1) * WIDE)
        cols = slice(j * WIDE, (j + 1) * WIDE)
        got = jnp.dot(
            split[:, low:high], spread_in[low:high, cols], preferred_element_type=f32
        )
        full[:, cols] = got[:rows] + got[rows : 2 * rows] + got[2 * rows : 3 * rows]
        tall[:, cols] = got[3 * rows : 3 * rows + 1] + got[3 * rows + 1 : 3 * rows + 2] + (
            got[3 * rows + 2 : 3 * rows + 3]
        )
        copy = pltpu.make_async_copy(full.at[:, cols], new_out.at[:, cols], sem.at[j])
        copy.start()
        copies.append(copy)
    points = cells // count
    row = LANES * points // math.gcd(LANES, points)
    per_row = row // points
    mine = tall[:, pl.ds(pl.multiple_of(me // per_row * row, LANES), row)]
    shift = (me % per_row) * points
    turned = pltpu.roll(jnp.broadcast_to(mine, (8, row)), (row - shift) % row, 1)
    wave_ref[...] = turned[0, :points]
    for copy in copies:
        copy.wait()


def fused_local(spectrum, sea_mask, wind_speed, wind_angle):
    count = lax.axis_size("spec")
    bins_dev, cells = spectrum.shape
    group = group_size(count, bins_dev, cells)
    freq_dev = bins_dev // ND
    freq_group = freq_dev * group
    sea_cells = SEA_DEV * count
    width = sea_cells // group
    points = cells // count
    parts = width // LANES
    blocks = sea_cells // LANES
    reach = cells - sea_cells + LANES
    tail = 16
    f32, bf16 = jnp.float32, jnp.bfloat16
    dma = pltpu.SemaphoreType.DMA
    vmem = pl.BlockSpec(memory_space=pltpu.VMEM)
    handed = pl.pallas_call(
        functools.partial(fused_kernel, count, group),
        out_shape=(
            pltpu.VMEM((freq_dev, ND, sea_cells), f32),
            pltpu.VMEM((1, sea_cells), f32),
            pltpu.VMEM((sea_cells, cells), bf16),
        ),
        in_specs=[pl.BlockSpec(memory_space=pl.ANY)] * 4,
        out_specs=(vmem,) * 3,
        scratch_shapes=[
            pltpu.VMEM((cells,), jnp.int32),
            pltpu.VMEM((cells,), f32),
            pltpu.VMEM((cells,), f32),
            pltpu.VMEM((1, cells), f32),
            dma((3,)),
            pltpu.VMEM((bins_dev, cells), f32),
            pltpu.VMEM((bins_dev, cells), f32),
            pltpu.VMEM((freq_dev, 3 * ND, cells), bf16),
            pltpu.VMEM((blocks, reach, LANES), bf16),
            pltpu.VMEM((ND // 2, cells), bf16),
            pltpu.VMEM((freq_dev, ND, sea_cells), f32),
            pltpu.VMEM((freq_group + 2 * HALO, ND, width), f32),
            pltpu.VMEM((freq_group, ND, width), f32),
            pltpu.VMEM((2, sea_cells), f32),
            pltpu.VMEM((count, 2, width), f32),
            pltpu.VMEM((ND, width), f32),
            pltpu.VMEM((ND, width), f32),
            pltpu.VMEM((1, width), f32),
            pltpu.VMEM((count, 1, width), f32),
            dma((freq_dev,)),
            dma((freq_group + 2 * HALO, parts)),
            dma((group - 1, freq_dev, parts)),
            dma((HALO, parts)),
            dma((HALO, parts)),
            dma((count - 1, parts)),
            dma((count, parts)),
            dma((group, parts)),
            dma((group, parts)),
            dma((count - 1,)),
            dma((count,)),
        ],
        compiler_params=pltpu.CompilerParams(collective_id=0, has_side_effects=True),
    )(sea_mask, wind_speed, wind_angle, spectrum)
    out, wave, mean = pl.pallas_call(
        functools.partial(store_kernel, count),
        out_shape=(
            pltpu.HBM((bins_dev, cells), f32),
            jax.ShapeDtypeStruct((points,), f32),
            jax.ShapeDtypeStruct((1, 1), f32),
        ),
        in_specs=[vmem] * 3,
        out_specs=(pl.BlockSpec(memory_space=pltpu.HBM), vmem, vmem),
        scratch_shapes=[
            pltpu.VMEM((3 * bins_dev + tail, sea_cells), bf16),
            pltpu.VMEM((bins_dev, cells), f32),
            pltpu.VMEM((1, cells), f32),
            dma((cells // WIDE,)),
        ],
    )(*[pltpu.with_memory_space_constraint(piece, pltpu.VMEM) for piece in handed])
    return (out, wave, mean.reshape(1))


def solution(mesh):
    in_specs = (P(("grp", "spec"), None), P(), P("grp"), P("grp"))
    out_specs = (P(("grp", "spec"), None), P(("grp", "spec")), P("grp"))

    def body(spectrum, sea_mask, wind_speed, wind_angle):
        fits = group_size(mesh.shape["spec"], *spectrum.shape)
        plan = fused_local if fits else local
        return plan(spectrum, sea_mask, wind_speed, wind_angle)

    return jax.shard_map(body, mesh=mesh, in_specs=in_specs, out_specs=out_specs, check_vma=False)
```

```python
import functools
import math

import jax
import jax.numpy as jnp
from jax import lax
from jax.experimental import pallas as pl
from jax.experimental.pallas import tpu as pltpu
from jax.sharding import PartitionSpec as P

NF = 48
ND = 32
NLON = 384
ADV_STEPS = 2
SEA_DEV = 64


def upwind_step(energy, courant_x, courant_y, sea_grid):
    west_cell = jnp.roll(energy, 1, axis=2)
    east_cell = jnp.roll(energy, -1, axis=2)
    edge_row = jnp.zeros_like(energy[:, :1])
    south_cell = jnp.concatenate([edge_row, energy[:, :-1]], axis=1)
    north_cell = jnp.concatenate([energy[:, 1:], edge_row], axis=1)
    updated = (
        energy
        - jnp.maximum(courant_x, 0.0) * (energy - west_cell)
        - jnp.minimum(courant_x, 0.0) * (east_cell - energy)
        - jnp.maximum(courant_y, 0.0) * (energy - south_cell)
        - jnp.minimum(courant_y, 0.0) * (north_cell - energy)
    )
    return updated * sea_grid


def courant_numbers(freq_index, dir_index, lat_count, dir_count):
    speed = 0.2 * jnp.exp(-math.log(1.1) * freq_index)
    heading = 2.0 * math.pi * (dir_index + 0.5) / dir_count
    rows = jnp.arange(lat_count, dtype=jnp.float32)
    latitude = (-75.0 + 150.0 * (rows + 0.5) / lat_count) * (math.pi / 180.0)
    courant_x = (speed * jnp.cos(heading))[:, None, None] / jnp.cos(latitude)[None, :, None]
    courant_y = (speed * jnp.sin(heading))[:, None, None]
    return (courant_x, courant_y)


def shift_freq(values, amount):
    if amount > 0:
        filler = jnp.zeros_like(values[:amount])
        return jnp.concatenate([filler, values[:-amount]], axis=0)
    filler = jnp.zeros_like(values[:-amount])
    return jnp.concatenate([values[-amount:], filler], axis=0)


def source_terms(energy, speed, angle):
    freq_count = energy.shape[0]
    dir_count = energy.shape[1]
    freq_ids = jnp.arange(freq_count, dtype=jnp.float32)
    frequency = jnp.exp(math.log(1.1) * (freq_ids - freq_count // 2))[:, None, None]
    heading = (2.0 * math.pi * (jnp.arange(dir_count, dtype=jnp.float32) + 0.5) / dir_count)[
        None, :, None
    ]
    energy_mean = jnp.mean(energy, axis=(0, 1))
    moment_one = jnp.mean(frequency * energy, axis=(0, 1))
    mean_freq = moment_one / (energy_mean + 1e-06)
    steepness = energy_mean * mean_freq * mean_freq
    breaking = steepness * steepness / (1.0 + steepness * steepness)
    wind_gain = (
        0.05
        * frequency
        * jnp.maximum(
            0.0, speed[None, None, :] * frequency * jnp.cos(heading - angle[None, None, :]) - 1.0
        )
    )
    damping = 0.03 * frequency * breaking[None, None, :]
    valid = ((freq_ids >= 3) & (freq_ids <= freq_count - 3)).astype(jnp.float32)[:, None, None]
    interaction = jnp.zeros_like(energy)
    for mirror in (1, -1):
        plus_bins = shift_freq(jnp.roll(energy, -mirror, axis=1), -2)
        minus_bins = shift_freq(jnp.roll(energy, 3 * mirror, axis=1), 3)
        transfer_rate = (
            0.001
            * valid
            * (energy * energy * (plus_bins + minus_bins) - 2.0 * energy * plus_bins * minus_bins)
        )
        interaction = interaction - 2.0 * transfer_rate
        interaction = interaction + jnp.roll(shift_freq(transfer_rate, 2), mirror, axis=1)
        interaction = interaction + jnp.roll(shift_freq(transfer_rate, -3), -3 * mirror, axis=1)
    updated = energy + (wind_gain - damping) * energy + interaction
    raw_height = 4.0 * jnp.sqrt(jnp.mean(updated, axis=(0, 1)) + 1e-06)
    return (updated, raw_height)


def local(spectrum, sea_mask, wind_speed, wind_angle):
    count = lax.axis_size("spec")
    position = lax.axis_index("spec")
    bins_dev = spectrum.shape[0]
    cells = spectrum.shape[1]
    points = cells // count
    lat_count = cells // NLON
    sea_float = sea_mask.astype(jnp.float32)
    bin_ids = position * bins_dev + jnp.arange(bins_dev, dtype=jnp.int32)
    freq_index = (bin_ids // ND).astype(jnp.float32)
    dir_index = (bin_ids % ND).astype(jnp.float32)
    courant_x, courant_y = courant_numbers(freq_index, dir_index, lat_count, ND)
    sea_grid = sea_float.reshape(1, lat_count, NLON)
    energy = (spectrum * sea_float[None, :]).reshape(bins_dev, lat_count, NLON)
    for substep in range(ADV_STEPS):
        energy = upwind_step(energy, courant_x, courant_y, sea_grid)
    advected = energy.reshape(bins_dev, cells)
    outgoing = advected.reshape(bins_dev, count, points)
    arrived = lax.all_to_all(outgoing, "spec", split_axis=1, concat_axis=0, tiled=True)
    start = position * points
    speed_own = lax.dynamic_slice_in_dim(wind_speed, start, points)
    angle_own = lax.dynamic_slice_in_dim(wind_angle, start, points)
    sea_own = lax.dynamic_slice_in_dim(sea_float, start, points)
    updated, raw_height = source_terms(arrived.reshape(NF, ND, points), speed_own, angle_own)
    wave_height = sea_own * raw_height
    own_total = jnp.zeros((count, 1), jnp.float32) + jnp.sum(wave_height)
    returned, totals = (
        lax.all_to_all(
            updated.reshape(NF * ND, 1, points), "spec", split_axis=0, concat_axis=1, tiled=True
        ),
        lax.all_to_all(own_total, "spec", split_axis=0, concat_axis=1, tiled=True),
    )
    new_spectrum = returned.reshape(bins_dev, cells)
    height_sum = jnp.sum(totals)
    mean_height = (height_sum / (SEA_DEV * count)).reshape(1)
    return (new_spectrum, wave_height, mean_height)


HALO = 5
LANES = 128
WIDE = 256
LAND = 4096.0


def group_size(count, bins_dev, cells):
    size = 4
    if count % size or bins_dev % ND or cells % (size * LANES) or cells % NLON:
        return 0
    if NLON % LANES or bins_dev // ND * size < 2 * HALO or cells % count:
        return 0
    sea = SEA_DEV * count
    if sea > min(cells, LAND) or sea % (size * LANES) or sea % WIDE or cells % WIDE:
        return 0
    if (cells - sea) % WIDE:
        return 0
    return size


def split_bf16(values):
    high = values.astype(jnp.bfloat16)
    left = values - high.astype(jnp.float32)
    mid = left.astype(jnp.bfloat16)
    low = (left - mid.astype(jnp.float32)).astype(jnp.bfloat16)
    return high, mid, low


def rows_of(parts, height, width):
    ids = lax.broadcasted_iota(jnp.int32, (height, width), 0)
    out = jnp.zeros((height, width), jnp.float32)
    for i, part in enumerate(parts):
        out = jnp.where(ids == i, jnp.broadcast_to(part.astype(jnp.float32), (height, width)), out)
    return out.astype(jnp.bfloat16)


def fused_kernel(
    count, group, sea_in, wind_in, angle_in, spec_ref, full_ref, height_ref, spread_ref,
    sea_raw, wind_raw, angle_raw, aux_ref, aux_sem,
    raw, moved, split, pick, wsplit, adv, held, done, back, mom_out, mom_in, wind, acc,
    sum_out, sum_in, damp_out, damp_in,
    load_sem, held_sem, halo_sem, y_sem, z_sem, mom_send, mom_recv,
    ret_send, ret_recv, sum_send, sum_recv, damp_send, damp_recv,
):
    f32, bf16 = jnp.float32, jnp.bfloat16
    freq_dev, _, sea_cells = adv.shape
    bins_dev, cells = moved.shape
    freq_group = freq_dev * group
    width = sea_cells // group
    zones = count // group
    lat_count = cells // NLON
    sides = group // 2
    parts = width // LANES
    cell_tiles = cells // LANES
    land = cells - sea_cells
    reach = land + WIDE
    me = lax.axis_index("spec")
    zone, rank = me // group, me % group
    side, core = rank // 2, rank % 2

    def remote(src, dst, send, recv, target):
        return pltpu.make_async_remote_copy(
            src_ref=src, dst_ref=dst, send_sem=send, recv_sem=recv,
            device_id={"spec": target}, device_id_type=pl.DeviceIdType.MESH,
        )

    loads = [
        pltpu.make_async_copy(
            spec_ref.at[pl.ds(f * ND, ND)], raw.at[pl.ds(f * ND, ND)], load_sem.at[f]
        )
        for f in range(freq_dev)
    ]
    small = [
        pltpu.make_async_copy(sea_in, sea_raw, aux_sem.at[0]),
        pltpu.make_async_copy(wind_in, wind_raw, aux_sem.at[1]),
        pltpu.make_async_copy(angle_in, angle_raw, aux_sem.at[2]),
    ]
    for load in small[:1] + loads + small[1:]:
        load.start()
    barrier = pltpu.get_barrier_semaphore()
    for step in range(1, count):
        pl.semaphore_signal(
            barrier, inc=1, device_id={"spec": (me + step) % count},
            device_id_type=pl.DeviceIdType.MESH,
        )

    @pl.when(zone == 0)
    def _():
        held[0:HALO] = jnp.zeros((HALO, ND, width), f32)

    @pl.when(zone == zones - 1)
    def _():
        held[HALO + freq_group :] = jnp.zeros((HALO, ND, width), f32)

    def block_of(index, t):
        return t * group + index

    def tile_of(index, t):
        return pl.ds(pl.multiple_of(block_of(index, t) * LANES, LANES), LANES)

    def lanes_of(t):
        return pl.ds(t * LANES, LANES)

    offsets = [(dy, dc) for dy in range(sides) for dc in range(2)]

    def rank_of(offset):
        return (side + offset[0]) % sides * 2 + (core + offset[1]) % 2

    def y_copy(f, i, t):
        peer = rank_of(offsets[i])
        slot = HALO + rank * freq_dev + f
        return remote(
            adv.at[f, :, tile_of(peer, t)], held.at[slot, :, lanes_of(t)],
            y_sem, held_sem.at[slot, t], zone * group + peer,
        )

    dirs = lax.broadcasted_iota(jnp.int32, (ND, LANES), 0).astype(f32)
    heading = 2.0 * math.pi * (dirs + 0.5) / ND
    cos_h, sin_h = jnp.cos(heading), jnp.sin(heading)
    log_step = math.log(1.1)
    lats = [math.radians(-75.0 + 150.0 * (r + 0.5) / lat_count) for r in range(lat_count)]

    def omega_of(freq, shape):
        return jnp.exp(jnp.full(shape, log_step, f32) * (freq.astype(f32) - NF // 2))

    square_rows = lax.broadcasted_iota(jnp.int32, (LANES, LANES), 0)
    square_cols = lax.broadcasted_iota(jnp.int32, (LANES, LANES), 1)
    lane_ids = square_cols.astype(f32)
    ones = jnp.ones((LANES, LANES), bf16)

    small[0].wait()
    aux_ref[...] = sea_raw[...].astype(f32).reshape(1, cells)
    sea = [aux_ref[0:1, r * NLON : (r + 1) * NLON] for r in range(lat_count)]
    mask = [aux_ref[0:1, i * LANES : (i + 1) * LANES] for i in range(cell_tiles)]
    before = [jnp.zeros((1, 1), f32)]
    for i in range(cell_tiles):
        before.append(before[i] + jnp.sum(mask[i], axis=1, keepdims=True))
    for i in range(cell_tiles):
        tri = jnp.where(
            square_cols < square_rows,
            mask[i],
            jnp.where(square_cols == square_rows, LAND * (1.0 - mask[i]), 0.0),
        )
        within = jnp.dot(tri.astype(bf16), ones, preferred_element_type=f32)
        place = within + before[i]
        for p in range(sea_cells // WIDE):
            row = i * LANES - p * WIDE
            if 0 <= row < reach:
                for h in range(WIDE // LANES):
                    first = float(p * WIDE + h * LANES)
                    hit = jnp.where(place == lane_ids + first, 1.0, 0.0)
                    pick[p, row : row + LANES, h * LANES : (h + 1) * LANES] = hit.astype(bf16)

    quarter = ND // 4
    tiles = NLON // LANES
    for f in range(freq_dev):
        loads[f].wait()
        freq = (me * freq_dev + f).astype(f32)
        speed = 0.2 * jnp.exp(jnp.full((quarter, LANES), -log_step, f32) * freq)
        for q in range(4):
            east, north = q in (0, 3), q in (0, 1)
            rows = slice(f * ND + q * quarter, f * ND + (q + 1) * quarter)
            part = slice(q * quarter, (q + 1) * quarter)
            cx0 = speed * jnp.abs(cos_h[part])
            cy = jnp.concatenate([speed * jnp.abs(sin_h[part])] * tiles, axis=1)
            cx = [jnp.concatenate([cx0 * (1.0 / math.cos(a))] * tiles, axis=1) for a in lats]
            energy = [raw[rows, r * NLON : (r + 1) * NLON] * sea[r] for r in range(lat_count)]
            for _ in range(ADV_STEPS):
                fresh = []
                for r in range(lat_count):
                    e = energy[r]
                    side_x = pltpu.roll(e, 1 if east else NLON - 1, 1)
                    other = r - 1 if north else r + 1
                    side_y = energy[other] if 0 <= other < lat_count else 0.0
                    fresh.append((e - cx[r] * (e - side_x) - cy * (e - side_y)) * sea[r])
                energy = fresh
            for r in range(lat_count):
                moved[rows, r * NLON : (r + 1) * NLON] = energy[r]
        rows = slice(f * ND, (f + 1) * ND)
        for i, piece in enumerate(split_bf16(moved[rows])):
            split[i * bins_dev + f * ND : i * bins_dev + (f + 1) * ND, :] = piece

    pl.semaphore_wait(barrier, count - 1)

    def packed(values, pair):
        cols = pl.ds(pl.multiple_of(pair * WIDE, LANES), reach)
        return jnp.dot(values[:, cols], pick[pair], preferred_element_type=f32)

    for t in range(parts):
        for dy in list(range(1, sides)) + [0]:
            pair = t * sides + (side + dy) % sides
            got = packed(split, pair)
            got = got[:bins_dev] + got[bins_dev : 2 * bins_dev] + got[2 * bins_dev :]
            cols = pl.ds(pl.multiple_of(pair * WIDE, LANES), WIDE)
            mass, moment = None, None
            for f in range(freq_dev):
                piece = got[f * ND : (f + 1) * ND]
                adv[f, :, cols] = piece
                total = jnp.sum(piece, axis=0, keepdims=True)
                scaled = omega_of(me * freq_dev + f, (1, WIDE)) * total
                mass = total if f == 0 else mass + total
                moment = scaled if f == 0 else moment + scaled
            for f in range(freq_dev):
                for dc in ((0, 1) if dy else (1,)):
                    y_copy(f, dy * 2 + dc, t).start()
            if dy == 0:
                for f in range(freq_dev):
                    held[HALO + rank * freq_dev + f, :, lanes_of(t)] = adv[
                        f, :, tile_of(rank, t)
                    ]
            here = pl.ds(pl.multiple_of((side + dy) % sides * WIDE, LANES), WIDE)
            mom_out[t, 0:1, here] = mass
            mom_out[t, 1:2, here] = moment

    def cols_of(index):
        return pl.ds(pl.multiple_of(index * LANES, LANES), LANES)

    for step in range(1, count):
        target = (me + step) % count
        remote(
            mom_out.at[:, :, cols_of(target % group)], mom_in.at[me],
            mom_send, mom_recv, target,
        ).start()
    mom_in[me] = mom_out[:, :, cols_of(rank)]

    small[1].wait()
    small[2].wait()
    speed_all = wind_raw[...].reshape(1, cells)
    angle_all = angle_raw[...].reshape(1, cells)
    wsplit[...] = rows_of(
        split_bf16(speed_all * jnp.cos(angle_all)) + split_bf16(speed_all * jnp.sin(angle_all)),
        2 * quarter, cells,
    )
    for t in range(parts):
        own = packed(wsplit, t * sides + side)
        own = jnp.where(core == 0, own[:, :LANES], own[:, LANES:])
        along = own[0:1] + own[1:2] + own[2:3]
        across = own[3:4] + own[4:5] + own[5:6]
        wind[:, t * LANES : (t + 1) * LANES] = cos_h * along + sin_h * across

    def up_copy(slot, t):
        return remote(
            held.at[HALO + slot, :, lanes_of(t)],
            held.at[HALO + slot - freq_group, :, lanes_of(t)],
            z_sem.at[0], halo_sem.at[0, t], (zone + 1) % zones * group + rank,
        )

    def down_copy(slot, t):
        return remote(
            held.at[HALO + slot, :, lanes_of(t)],
            held.at[HALO + slot + freq_group, :, lanes_of(t)],
            z_sem.at[1], halo_sem.at[1, t], (zone + zones - 1) % zones * group + rank,
        )

    def arrive(index, t):
        block = held.at[index, :, lanes_of(t)]
        remote(block, block, y_sem, held_sem.at[index, t], (me + 1) % count).wait_recv()

    def arrive_group(dy, t):
        for f in range(freq_dev):
            for dc in range(2):
                slot = rank_of((dy, dc)) * freq_dev + f
                if (dy, dc) != (0, 0):
                    arrive(HALO + slot, t)

                @pl.when((slot >= freq_group - HALO) & (zone < zones - 1))
                def _():
                    up_copy(slot, t).start()

                @pl.when((slot < HALO) & (zone > 0))
                def _():
                    down_copy(slot, t).start()

    for t in range(parts):
        arrive_group(0, t)

    tri_up = jnp.where(square_rows < square_cols, 1.0, 0.0).astype(bf16)
    ranks = jnp.dot(
        rows_of(mask, 2 * quarter, LANES), tri_up, preferred_element_type=f32
    )
    places = [
        jnp.where(mask[i] > 0.0, ranks[i : i + 1] + before[i], LAND) for i in range(cell_tiles)
    ]
    wide_rows = lax.broadcasted_iota(jnp.int32, (WIDE, LANES), 0).astype(f32)
    for u in range(sea_cells // WIDE):
        for i in range(cell_tiles):
            if u * WIDE < (i + 1) * LANES + LANES and (u + 1) * WIDE + LANES > i * LANES - land:
                hit = jnp.where(wide_rows + float(u * WIDE) == places[i], 1.0, 0.0)
                spread_ref[u * WIDE : (u + 1) * WIDE, i * LANES : (i + 1) * LANES] = hit.astype(
                    bf16
                )
            else:
                spread_ref[u * WIDE : (u + 1) * WIDE, i * LANES : (i + 1) * LANES] = jnp.zeros(
                    (WIDE, LANES), bf16
                )

    for dy in range(1, sides):
        arrive_group(dy, 0)

    acc[...] = jnp.zeros_like(acc)
    ascending = side > 0

    def arrive_halo(at_top, t):
        block = held.at[0:HALO, :, lanes_of(t)]

        @pl.when(jnp.where(at_top, zone < zones - 1, zone > 0))
        def _():
            way = jnp.where(at_top, 1, 0)
            remote(
                block, block, z_sem.at[0], halo_sem.at[way, t], (me + 1) % count
            ).wait_recv()

    def ret_copy(owner, t):
        return remote(
            done.at[pl.ds(owner * freq_dev, freq_dev), :, lanes_of(t)],
            back.at[:, :, tile_of(rank, t)],
            ret_send, ret_recv.at[t], zone * group + owner,
        )

    def sources(t, begin, end):
        lanes = slice(t * LANES, (t + 1) * LANES)

        def source_step(i, carry):
            k = jnp.where(ascending, i, freq_group - 1 - i)
            freq = zone * freq_group + k

            def scale(index, factor):
                return jnp.where((index >= 3) & (index <= NF - 3), factor, 0.0).astype(f32)

            w_own = scale(freq, -0.002)
            w_low, w_high = scale(freq - 2, 0.001), scale(freq + 3, 0.001)
            omega = omega_of(freq, (1, LANES))

            def slab(shift):
                return held[HALO + k + shift, :, lanes]

            def turn(values, amount):
                return pltpu.roll(values, amount % ND, 0)

            def rate(a, p, m):
                return a * (a * (p + m) - 2.0 * (p * m))

            own = slab(0)
            p2, m3, m2, m5, p3, p5 = (slab(shift) for shift in (2, -3, -2, -5, 3, 5))
            near = rate(own, turn(p2, -1), turn(m3, 3)) + rate(own, turn(p2, 1), turn(m3, -3))
            low = rate(turn(m2, 1), own, turn(m5, 4)) + rate(turn(m2, -1), own, turn(m5, -4))
            high = rate(turn(p3, -3), turn(p5, -4), own) + rate(turn(p3, 3), turn(p5, 4), own)
            interaction = w_own * near + w_low * low + w_high * high
            gain = (0.05 * omega) * jnp.maximum(0.0, wind[:, lanes] * omega - 1.0)
            fresh = own + gain * own + interaction
            done[k, :, lanes] = fresh
            acc[:, lanes] += fresh
            return carry

        lax.fori_loop(begin, end, source_step, 0)

    half = freq_group // 2
    near_side = rank_of((0, 1))

    def first_half(t):
        arrive_halo(jnp.logical_not(ascending), t)
        sources(t, 0, half)
        for dy in range(1, sides):
            for dc in range(2):
                ret_copy(rank_of((dy, dc)), t).start()

    def second_half(t):
        arrive_halo(ascending, t)
        sources(t, half, freq_group)
        ret_copy(near_side, t).start()
        back[:, :, tile_of(rank, t)] = done[
            pl.ds(rank * freq_dev, freq_dev), :, lanes_of(t)
        ]

    def zone_copy(dst_rank, src, dst, send, recv):
        return remote(src, dst, send, recv, zone * group + dst_rank)

    def damping_terms():
        others = mom_in.at[0 : count - 1]
        remote(others, others, mom_send, mom_recv, (me + 1) % count).wait_recv()
        total = jnp.sum(mom_in[...], axis=0) * (1.0 / (NF * ND))
        for t in range(parts):
            energy_mean, moment_one = total[t, 0:1], total[t, 1:2]
            mean_freq = moment_one / (energy_mean + 1e-06)
            steepness = energy_mean * mean_freq * mean_freq
            breaking = steepness * steepness / (1.0 + steepness * steepness)
            damp_out[t, 0:1] = 0.03 * breaking
            damp_out[t, 1:2] = 0.03 * breaking * moment_one
        for i in range(1, group):
            zone_copy(
                rank_of(offsets[i]), damp_out, damp_in.at[rank], damp_send, damp_recv
            ).start()
        damp_in[rank] = damp_out[...]

    first_half(0)
    for t in range(1, parts):
        for dy in range(1, sides):
            arrive_group(dy, t)
        first_half(t)
        if t == parts - 1:
            damping_terms()
        second_half(t - 1)
    second_half(parts - 1)

    sum_out[...] = jnp.sum(acc[...], axis=0, keepdims=True)
    for step in range(1, count):
        remote(sum_out, sum_in.at[me], sum_send, sum_recv, (me + step) % count).start()
    sum_in[me] = sum_out[...]

    others = damp_in.at[0 : group - 1]
    remote(others, others, damp_send, damp_recv, (me + 1) % count).wait_recv()
    for t in range(parts):
        block = done.at[0 : (group - 1) * freq_dev, :, lanes_of(t)]
        remote(block, block, ret_send, ret_recv.at[t], (me + 1) % count).wait_recv()
    for f in range(freq_dev):
        omega = omega_of(me * freq_dev + f, (1, LANES))
        for t in range(parts):
            for g in range(group):
                cols = slice(block_of(g, t) * LANES, (block_of(g, t) + 1) * LANES)
                value = back[f, :, cols] - (omega * damp_in[g, t, 0:1]) * adv[f, :, cols]
                for i, piece in enumerate(split_bf16(value)):
                    split[
                        i * bins_dev + f * ND : i * bins_dev + (f + 1) * ND, cols
                    ] = piece
    for j in range(cells // WIDE):
        low, high = max(0, j * WIDE - land), min(sea_cells, (j + 1) * WIDE)
        cols = slice(j * WIDE, (j + 1) * WIDE)
        got = jnp.dot(
            split[:, low:high], spread_ref[low:high, cols], preferred_element_type=f32
        )
        full_ref[:, cols] = got[:bins_dev] + got[bins_dev : 2 * bins_dev] + got[2 * bins_dev :]

    block = held.at[0 : (group - 1) * freq_dev]
    remote(block, block, y_sem, held_sem.at[0, 0], (me + 1) % count).wait_send()
    remote(block, block, ret_send, ret_recv.at[0], (me + 1) % count).wait_send()
    others = mom_in.at[0 : count - 1]
    remote(others, others, mom_send, mom_recv, (me + 1) % count).wait_send()
    others = damp_in.at[0 : group - 1]
    remote(others, others, damp_send, damp_recv, (me + 1) % count).wait_send()
    block = held.at[0:HALO]

    @pl.when(zone < zones - 1)
    def _():
        remote(block, block, z_sem.at[0], halo_sem.at[0, 0], (me + 1) % count).wait_send()

    @pl.when(zone > 0)
    def _():
        remote(block, block, z_sem.at[1], halo_sem.at[0, 0], (me + 1) % count).wait_send()

    others = sum_in.at[0 : count - 1]
    remote(others, others, sum_send, sum_recv, (me + 1) % count).wait()
    for g in range(group):
        mass = sum_in[g]
        for other in range(1, zones):
            mass = mass + sum_in[other * group + g]
        for t in range(parts):
            mean = mass[:, t * LANES : (t + 1) * LANES] * (1.0 / (NF * ND)) - damp_in[g, t, 1:2]
            cols = slice(block_of(g, t) * LANES, (block_of(g, t) + 1) * LANES)
            height_ref[0:1, cols] = 4.0 * jnp.sqrt(mean + 1e-06)


def store_kernel(
    count, full_in, height_in, spread_in, new_out, wave_ref, mean_ref, sem
):
    cells = full_in.shape[1]
    sea_cells = height_in.shape[1]
    copy = pltpu.make_async_copy(full_in, new_out, sem)
    copy.start()
    me = lax.axis_index("spec")
    height = height_in[...]
    mean_ref[...] = jnp.sum(height, axis=1, keepdims=True) * (1.0 / sea_cells)
    points = cells // count
    start = jnp.minimum(me * points // LANES * LANES, cells - WIDE)
    window = spread_in[:, pl.ds(pl.multiple_of(start, LANES), WIDE)]
    got = jnp.dot(
        rows_of(split_bf16(height), ND // 2, sea_cells), window,
        preferred_element_type=jnp.float32,
    )
    wave = got[0:1] + got[1:2] + got[2:3]
    shift = me * points - start
    turned = pltpu.roll(jnp.broadcast_to(wave, (8, WIDE)), (WIDE - shift) % WIDE, 1)
    wave_ref[...] = turned[0, :points]
    copy.wait()


def fused_local(spectrum, sea_mask, wind_speed, wind_angle):
    count = lax.axis_size("spec")
    bins_dev, cells = spectrum.shape
    group = group_size(count, bins_dev, cells)
    freq_dev = bins_dev // ND
    freq_group = freq_dev * group
    sea_cells = SEA_DEV * count
    width = sea_cells // group
    points = cells // count
    parts = width // LANES
    reach = cells - sea_cells + WIDE
    f32, bf16 = jnp.float32, jnp.bfloat16
    dma = pltpu.SemaphoreType.DMA
    vmem = pl.BlockSpec(memory_space=pltpu.VMEM)
    handed = pl.pallas_call(
        functools.partial(fused_kernel, count, group),
        out_shape=(
            pltpu.VMEM((bins_dev, cells), f32),
            pltpu.VMEM((1, sea_cells), f32),
            pltpu.VMEM((sea_cells, cells), bf16),
        ),
        in_specs=[pl.BlockSpec(memory_space=pl.ANY)] * 4,
        out_specs=(vmem,) * 3,
        scratch_shapes=[
            pltpu.VMEM((cells,), jnp.int32),
            pltpu.VMEM((cells,), f32),
            pltpu.VMEM((cells,), f32),
            pltpu.VMEM((1, cells), f32),
            dma((3,)),
            pltpu.VMEM((bins_dev, cells), f32),
            pltpu.VMEM((bins_dev, cells), f32),
            pltpu.VMEM((3 * bins_dev, cells), bf16),
            pltpu.VMEM((sea_cells // WIDE, reach, WIDE), bf16),
            pltpu.VMEM((ND // 2, cells), bf16),
            pltpu.VMEM((freq_dev, ND, sea_cells), f32),
            pltpu.VMEM((freq_group + 2 * HALO, ND, width), f32),
            pltpu.VMEM((freq_group, ND, width), f32),
            pltpu.VMEM((freq_dev, ND, sea_cells), f32),
            pltpu.VMEM((parts, 2, group * LANES), f32),
            pltpu.VMEM((count, parts, 2, LANES), f32),
            pltpu.VMEM((ND, width), f32),
            pltpu.VMEM((ND, width), f32),
            pltpu.VMEM((1, width), f32),
            pltpu.VMEM((count, 1, width), f32),
            pltpu.VMEM((parts, 2, LANES), f32),
            pltpu.VMEM((group, parts, 2, LANES), f32),
            dma((freq_dev,)),
            dma((freq_group + 2 * HALO, parts)),
            dma((2, parts)),
            dma,
            dma((2,)),
            dma,
            dma,
            dma,
            dma((parts,)),
            dma,
            dma,
            dma,
            dma,
        ],
        compiler_params=pltpu.CompilerParams(
            collective_id=0, has_side_effects=True, vmem_limit_bytes=32 * 2**20
        ),
    )(sea_mask, wind_speed, wind_angle, spectrum)
    out, wave, mean = pl.pallas_call(
        functools.partial(store_kernel, count),
        out_shape=(
            pltpu.HBM((bins_dev, cells), f32),
            jax.ShapeDtypeStruct((points,), f32),
            jax.ShapeDtypeStruct((1, 1), f32),
        ),
        in_specs=[vmem] * 3,
        out_specs=(pl.BlockSpec(memory_space=pltpu.HBM), vmem, vmem),
        scratch_shapes=[dma],
        compiler_params=pltpu.CompilerParams(vmem_limit_bytes=16 * 2**20),
    )(*[pltpu.with_memory_space_constraint(piece, pltpu.VMEM) for piece in handed])
    return (out, wave, mean.reshape(1))


def solution(mesh):
    in_specs = (P(("grp", "spec"), None), P(), P("grp"), P("grp"))
    out_specs = (P(("grp", "spec"), None), P(("grp", "spec")), P("grp"))

    def body(spectrum, sea_mask, wind_speed, wind_angle):
        fits = group_size(mesh.shape["spec"], *spectrum.shape)
        plan = fused_local if fits else local
        return plan(spectrum, sea_mask, wind_speed, wind_angle)

    return jax.shard_map(body, mesh=mesh, in_specs=in_specs, out_specs=out_specs, check_vma=False)
```

```python
import functools
import math

import jax
import jax.numpy as jnp
from jax import lax
from jax.experimental import pallas as pl
from jax.experimental.pallas import tpu as pltpu
from jax.sharding import PartitionSpec as P

NF = 48
ND = 32
NLON = 384
ADV_STEPS = 2
SEA_DEV = 64


def upwind_step(energy, courant_x, courant_y, sea_grid):
    west_cell = jnp.roll(energy, 1, axis=2)
    east_cell = jnp.roll(energy, -1, axis=2)
    edge_row = jnp.zeros_like(energy[:, :1])
    south_cell = jnp.concatenate([edge_row, energy[:, :-1]], axis=1)
    north_cell = jnp.concatenate([energy[:, 1:], edge_row], axis=1)
    updated = (
        energy
        - jnp.maximum(courant_x, 0.0) * (energy - west_cell)
        - jnp.minimum(courant_x, 0.0) * (east_cell - energy)
        - jnp.maximum(courant_y, 0.0) * (energy - south_cell)
        - jnp.minimum(courant_y, 0.0) * (north_cell - energy)
    )
    return updated * sea_grid


def courant_numbers(freq_index, dir_index, lat_count, dir_count):
    speed = 0.2 * jnp.exp(-math.log(1.1) * freq_index)
    heading = 2.0 * math.pi * (dir_index + 0.5) / dir_count
    rows = jnp.arange(lat_count, dtype=jnp.float32)
    latitude = (-75.0 + 150.0 * (rows + 0.5) / lat_count) * (math.pi / 180.0)
    courant_x = (speed * jnp.cos(heading))[:, None, None] / jnp.cos(latitude)[None, :, None]
    courant_y = (speed * jnp.sin(heading))[:, None, None]
    return (courant_x, courant_y)


def shift_freq(values, amount):
    if amount > 0:
        filler = jnp.zeros_like(values[:amount])
        return jnp.concatenate([filler, values[:-amount]], axis=0)
    filler = jnp.zeros_like(values[:-amount])
    return jnp.concatenate([values[-amount:], filler], axis=0)


def source_terms(energy, speed, angle):
    freq_count = energy.shape[0]
    dir_count = energy.shape[1]
    freq_ids = jnp.arange(freq_count, dtype=jnp.float32)
    frequency = jnp.exp(math.log(1.1) * (freq_ids - freq_count // 2))[:, None, None]
    heading = (2.0 * math.pi * (jnp.arange(dir_count, dtype=jnp.float32) + 0.5) / dir_count)[
        None, :, None
    ]
    energy_mean = jnp.mean(energy, axis=(0, 1))
    moment_one = jnp.mean(frequency * energy, axis=(0, 1))
    mean_freq = moment_one / (energy_mean + 1e-06)
    steepness = energy_mean * mean_freq * mean_freq
    breaking = steepness * steepness / (1.0 + steepness * steepness)
    wind_gain = (
        0.05
        * frequency
        * jnp.maximum(
            0.0, speed[None, None, :] * frequency * jnp.cos(heading - angle[None, None, :]) - 1.0
        )
    )
    damping = 0.03 * frequency * breaking[None, None, :]
    valid = ((freq_ids >= 3) & (freq_ids <= freq_count - 3)).astype(jnp.float32)[:, None, None]
    interaction = jnp.zeros_like(energy)
    for mirror in (1, -1):
        plus_bins = shift_freq(jnp.roll(energy, -mirror, axis=1), -2)
        minus_bins = shift_freq(jnp.roll(energy, 3 * mirror, axis=1), 3)
        transfer_rate = (
            0.001
            * valid
            * (energy * energy * (plus_bins + minus_bins) - 2.0 * energy * plus_bins * minus_bins)
        )
        interaction = interaction - 2.0 * transfer_rate
        interaction = interaction + jnp.roll(shift_freq(transfer_rate, 2), mirror, axis=1)
        interaction = interaction + jnp.roll(shift_freq(transfer_rate, -3), -3 * mirror, axis=1)
    updated = energy + (wind_gain - damping) * energy + interaction
    raw_height = 4.0 * jnp.sqrt(jnp.mean(updated, axis=(0, 1)) + 1e-06)
    return (updated, raw_height)


def local(spectrum, sea_mask, wind_speed, wind_angle):
    count = lax.axis_size("spec")
    position = lax.axis_index("spec")
    bins_dev = spectrum.shape[0]
    cells = spectrum.shape[1]
    points = cells // count
    lat_count = cells // NLON
    sea_float = sea_mask.astype(jnp.float32)
    bin_ids = position * bins_dev + jnp.arange(bins_dev, dtype=jnp.int32)
    freq_index = (bin_ids // ND).astype(jnp.float32)
    dir_index = (bin_ids % ND).astype(jnp.float32)
    courant_x, courant_y = courant_numbers(freq_index, dir_index, lat_count, ND)
    sea_grid = sea_float.reshape(1, lat_count, NLON)
    energy = (spectrum * sea_float[None, :]).reshape(bins_dev, lat_count, NLON)
    for substep in range(ADV_STEPS):
        energy = upwind_step(energy, courant_x, courant_y, sea_grid)
    advected = energy.reshape(bins_dev, cells)
    outgoing = advected.reshape(bins_dev, count, points)
    arrived = lax.all_to_all(outgoing, "spec", split_axis=1, concat_axis=0, tiled=True)
    start = position * points
    speed_own = lax.dynamic_slice_in_dim(wind_speed, start, points)
    angle_own = lax.dynamic_slice_in_dim(wind_angle, start, points)
    sea_own = lax.dynamic_slice_in_dim(sea_float, start, points)
    updated, raw_height = source_terms(arrived.reshape(NF, ND, points), speed_own, angle_own)
    wave_height = sea_own * raw_height
    own_total = jnp.zeros((count, 1), jnp.float32) + jnp.sum(wave_height)
    returned, totals = (
        lax.all_to_all(
            updated.reshape(NF * ND, 1, points), "spec", split_axis=0, concat_axis=1, tiled=True
        ),
        lax.all_to_all(own_total, "spec", split_axis=0, concat_axis=1, tiled=True),
    )
    new_spectrum = returned.reshape(bins_dev, cells)
    height_sum = jnp.sum(totals)
    mean_height = (height_sum / (SEA_DEV * count)).reshape(1)
    return (new_spectrum, wave_height, mean_height)


HALO = 5
LANES = 128
WIDE = 256
LAND = 4096.0


def group_size(count, bins_dev, cells):
    size = 4
    if count % size or bins_dev % ND or cells % (size * LANES) or cells % NLON:
        return 0
    if NLON % LANES or bins_dev // ND * size < 2 * HALO or cells % count:
        return 0
    sea = SEA_DEV * count
    if sea > min(cells, LAND) or sea % (size * LANES) or sea % WIDE or cells % WIDE:
        return 0
    if (cells - sea) % WIDE:
        return 0
    return size


def split_bf16(values):
    high = values.astype(jnp.bfloat16)
    left = values - high.astype(jnp.float32)
    mid = left.astype(jnp.bfloat16)
    low = (left - mid.astype(jnp.float32)).astype(jnp.bfloat16)
    return high, mid, low


def rows_of(parts, height, width):
    ids = lax.broadcasted_iota(jnp.int32, (height, width), 0)
    out = jnp.zeros((height, width), jnp.float32)
    for i, part in enumerate(parts):
        out = jnp.where(ids == i, jnp.broadcast_to(part.astype(jnp.float32), (height, width)), out)
    return out.astype(jnp.bfloat16)


def window_start(count, me, cells):
    return jnp.minimum(me * (cells // count) // LANES * LANES, cells - WIDE)


def fused_kernel(
    count, group, sea_in, wind_in, angle_in, spec_ref, full_ref, height_ref, window_ref,
    sea_raw, wind_raw, angle_raw, aux_ref, place_ref, spread_ref, aux_sem,
    raw, moved, split, pick, wsplit, adv, held, done, back, mom_out, mom_in, wind, acc,
    sum_out, sum_in, damp_out, damp_in,
    load_sem, held_sem, halo_sem, y_sem, z_sem, mom_send, mom_recv,
    ret_send, ret_recv, sum_send, sum_recv, damp_send, damp_recv,
):
    f32, bf16 = jnp.float32, jnp.bfloat16
    freq_dev, _, sea_cells = adv.shape
    bins_dev, cells = moved.shape
    freq_group = freq_dev * group
    width = sea_cells // group
    zones = count // group
    lat_count = cells // NLON
    sides = group // 2
    parts = width // LANES
    cell_tiles = cells // LANES
    land = cells - sea_cells
    reach = land + WIDE
    me = lax.axis_index("spec")
    zone, rank = me // group, me % group
    side, core = rank // 2, rank % 2

    def remote(src, dst, send, recv, target):
        return pltpu.make_async_remote_copy(
            src_ref=src, dst_ref=dst, send_sem=send, recv_sem=recv,
            device_id={"spec": target}, device_id_type=pl.DeviceIdType.MESH,
        )

    loads = [
        pltpu.make_async_copy(
            spec_ref.at[pl.ds(f * ND, ND)], raw.at[pl.ds(f * ND, ND)], load_sem.at[f]
        )
        for f in range(freq_dev)
    ]
    small = [
        pltpu.make_async_copy(sea_in, sea_raw, aux_sem.at[0]),
        pltpu.make_async_copy(wind_in, wind_raw, aux_sem.at[1]),
        pltpu.make_async_copy(angle_in, angle_raw, aux_sem.at[2]),
    ]
    for load in small[:1] + loads + small[1:]:
        load.start()
    barrier = pltpu.get_barrier_semaphore()
    for step in range(1, count):
        pl.semaphore_signal(
            barrier, inc=1, device_id={"spec": (me + step) % count},
            device_id_type=pl.DeviceIdType.MESH,
        )

    @pl.when(zone == 0)
    def _():
        held[0:HALO] = jnp.zeros((HALO, ND, width), f32)

    @pl.when(zone == zones - 1)
    def _():
        held[HALO + freq_group :] = jnp.zeros((HALO, ND, width), f32)

    def block_of(index, t):
        return t * group + index

    def tile_of(index, t):
        return pl.ds(pl.multiple_of(block_of(index, t) * LANES, LANES), LANES)

    def lanes_of(t):
        return pl.ds(t * LANES, LANES)

    offsets = [(dy, dc) for dy in range(sides) for dc in range(2)]

    def rank_of(offset):
        return (side + offset[0]) % sides * 2 + (core + offset[1]) % 2

    def y_copy(f, i, t):
        peer = rank_of(offsets[i])
        slot = HALO + rank * freq_dev + f
        return remote(
            adv.at[f, :, tile_of(peer, t)], held.at[slot, :, lanes_of(t)],
            y_sem, held_sem.at[slot, t], zone * group + peer,
        )

    dirs = lax.broadcasted_iota(jnp.int32, (ND, LANES), 0).astype(f32)
    heading = 2.0 * math.pi * (dirs + 0.5) / ND
    cos_h, sin_h = jnp.cos(heading), jnp.sin(heading)
    log_step = math.log(1.1)
    lats = [math.radians(-75.0 + 150.0 * (r + 0.5) / lat_count) for r in range(lat_count)]

    def omega_of(freq, shape):
        return jnp.exp(jnp.full(shape, log_step, f32) * (freq.astype(f32) - NF // 2))

    square_rows = lax.broadcasted_iota(jnp.int32, (LANES, LANES), 0)
    square_cols = lax.broadcasted_iota(jnp.int32, (LANES, LANES), 1)
    lane_ids = square_cols.astype(f32)
    ones = jnp.ones((LANES, LANES), bf16)

    small[0].wait()
    aux_ref[...] = sea_raw[...].astype(f32).reshape(1, cells)
    sea = [aux_ref[0:1, r * NLON : (r + 1) * NLON] for r in range(lat_count)]
    mask = [aux_ref[0:1, i * LANES : (i + 1) * LANES] for i in range(cell_tiles)]
    before = [jnp.zeros((1, 1), f32)]
    for i in range(cell_tiles):
        before.append(before[i] + jnp.sum(mask[i], axis=1, keepdims=True))
    for i in range(cell_tiles):
        tri = jnp.where(
            square_cols < square_rows,
            mask[i],
            jnp.where(square_cols == square_rows, LAND * (1.0 - mask[i]), 0.0),
        )
        within = jnp.dot(tri.astype(bf16), ones, preferred_element_type=f32)
        place = within + before[i]
        for p in range(sea_cells // WIDE):
            row = i * LANES - p * WIDE
            if 0 <= row < reach:
                for h in range(WIDE // LANES):
                    first = float(p * WIDE + h * LANES)
                    hit = jnp.where(place == lane_ids + first, 1.0, 0.0)
                    pick[p, row : row + LANES, h * LANES : (h + 1) * LANES] = hit.astype(bf16)

    quarter = ND // 4
    tiles = NLON // LANES
    for f in range(freq_dev):
        loads[f].wait()
        freq = (me * freq_dev + f).astype(f32)
        speed = 0.2 * jnp.exp(jnp.full((quarter, LANES), -log_step, f32) * freq)
        for q in range(4):
            east, north = q in (0, 3), q in (0, 1)
            rows = slice(f * ND + q * quarter, f * ND + (q + 1) * quarter)
            part = slice(q * quarter, (q + 1) * quarter)
            cx0 = speed * jnp.abs(cos_h[part])
            cy = jnp.concatenate([speed * jnp.abs(sin_h[part])] * tiles, axis=1)
            cx = [jnp.concatenate([cx0 * (1.0 / math.cos(a))] * tiles, axis=1) for a in lats]
            energy = [raw[rows, r * NLON : (r + 1) * NLON] * sea[r] for r in range(lat_count)]
            for _ in range(ADV_STEPS):
                fresh = []
                for r in range(lat_count):
                    e = energy[r]
                    side_x = pltpu.roll(e, 1 if east else NLON - 1, 1)
                    other = r - 1 if north else r + 1
                    side_y = energy[other] if 0 <= other < lat_count else 0.0
                    fresh.append((e - cx[r] * (e - side_x) - cy * (e - side_y)) * sea[r])
                energy = fresh
            for r in range(lat_count):
                moved[rows, r * NLON : (r + 1) * NLON] = energy[r]
        rows = slice(f * ND, (f + 1) * ND)
        for i, piece in enumerate(split_bf16(moved[rows])):
            split[i * bins_dev + f * ND : i * bins_dev + (f + 1) * ND, :] = piece

    pl.semaphore_wait(barrier, count - 1)

    def packed(values, pair):
        cols = pl.ds(pl.multiple_of(pair * WIDE, LANES), reach)
        return jnp.dot(values[:, cols], pick[pair], preferred_element_type=f32)

    for t in range(parts):
        for dy in list(range(1, sides)) + [0]:
            pair = t * sides + (side + dy) % sides
            got = packed(split, pair)
            got = got[:bins_dev] + got[bins_dev : 2 * bins_dev] + got[2 * bins_dev :]
            cols = pl.ds(pl.multiple_of(pair * WIDE, LANES), WIDE)
            mass, moment = None, None
            for f in range(freq_dev):
                piece = got[f * ND : (f + 1) * ND]
                adv[f, :, cols] = piece
                total = jnp.sum(piece, axis=0, keepdims=True)
                scaled = omega_of(me * freq_dev + f, (1, WIDE)) * total
                mass = total if f == 0 else mass + total
                moment = scaled if f == 0 else moment + scaled
            for f in range(freq_dev):
                for dc in ((0, 1) if dy else (1,)):
                    y_copy(f, dy * 2 + dc, t).start()
            if dy == 0:
                for f in range(freq_dev):
                    held[HALO + rank * freq_dev + f, :, lanes_of(t)] = adv[
                        f, :, tile_of(rank, t)
                    ]
            here = pl.ds(pl.multiple_of((side + dy) % sides * WIDE, LANES), WIDE)
            mom_out[t, 0:1, here] = mass
            mom_out[t, 1:2, here] = moment

    def cols_of(index):
        return pl.ds(pl.multiple_of(index * LANES, LANES), LANES)

    for step in range(1, count):
        target = (me + step) % count
        remote(
            mom_out.at[:, :, cols_of(target % group)], mom_in.at[me],
            mom_send, mom_recv, target,
        ).start()
    mom_in[me] = mom_out[:, :, cols_of(rank)]

    small[1].wait()
    small[2].wait()
    speed_all = wind_raw[...].reshape(1, cells)
    angle_all = angle_raw[...].reshape(1, cells)
    wsplit[...] = rows_of(
        split_bf16(speed_all * jnp.cos(angle_all)) + split_bf16(speed_all * jnp.sin(angle_all)),
        2 * quarter, cells,
    )
    for t in range(parts):
        own = packed(wsplit, t * sides + side)
        own = jnp.where(core == 0, own[:, :LANES], own[:, LANES:])
        along = own[0:1] + own[1:2] + own[2:3]
        across = own[3:4] + own[4:5] + own[5:6]
        wind[:, t * LANES : (t + 1) * LANES] = cos_h * along + sin_h * across

    def up_copy(slot, t):
        return remote(
            held.at[HALO + slot, :, lanes_of(t)],
            held.at[HALO + slot - freq_group, :, lanes_of(t)],
            z_sem.at[0], halo_sem.at[0, t], (zone + 1) % zones * group + rank,
        )

    def down_copy(slot, t):
        return remote(
            held.at[HALO + slot, :, lanes_of(t)],
            held.at[HALO + slot + freq_group, :, lanes_of(t)],
            z_sem.at[1], halo_sem.at[1, t], (zone + zones - 1) % zones * group + rank,
        )

    def arrive(index, t):
        block = held.at[index, :, lanes_of(t)]
        remote(block, block, y_sem, held_sem.at[index, t], (me + 1) % count).wait_recv()

    def arrive_group(dy, t):
        for f in range(freq_dev):
            for dc in range(2):
                slot = rank_of((dy, dc)) * freq_dev + f
                if (dy, dc) != (0, 0):
                    arrive(HALO + slot, t)

                @pl.when((slot >= freq_group - HALO) & (zone < zones - 1))
                def _():
                    up_copy(slot, t).start()

                @pl.when((slot < HALO) & (zone > 0))
                def _():
                    down_copy(slot, t).start()

    for t in range(parts):
        arrive_group(0, t)

    tri_up = jnp.where(square_rows < square_cols, 1.0, 0.0).astype(bf16)
    ranks = jnp.dot(
        rows_of(mask, 2 * quarter, LANES), tri_up, preferred_element_type=f32
    )
    places = [
        jnp.where(mask[i] > 0.0, ranks[i : i + 1] + before[i], LAND) for i in range(cell_tiles)
    ]
    for i in range(cell_tiles):
        place_ref[0:1, i * LANES : (i + 1) * LANES] = places[i]
    start = window_start(count, me, cells)
    mine = place_ref[0:1, pl.ds(pl.multiple_of(start, LANES), WIDE)]
    sea_rows = lax.broadcasted_iota(jnp.int32, (sea_cells, WIDE), 0).astype(f32)
    window_ref[...] = jnp.where(sea_rows == mine, 1.0, 0.0).astype(bf16)
    wide_rows = lax.broadcasted_iota(jnp.int32, (WIDE, LANES), 0).astype(f32)
    for u in range(sea_cells // WIDE):
        for i in range(cell_tiles):
            if u * WIDE < (i + 1) * LANES + LANES and (u + 1) * WIDE + LANES > i * LANES - land:
                hit = jnp.where(wide_rows + float(u * WIDE) == places[i], 1.0, 0.0)
                spread_ref[u * WIDE : (u + 1) * WIDE, i * LANES : (i + 1) * LANES] = hit.astype(
                    bf16
                )
            else:
                spread_ref[u * WIDE : (u + 1) * WIDE, i * LANES : (i + 1) * LANES] = jnp.zeros(
                    (WIDE, LANES), bf16
                )

    for dy in range(1, sides):
        arrive_group(dy, 0)

    acc[...] = jnp.zeros_like(acc)
    ascending = side > 0

    def arrive_halo(at_top, t):
        block = held.at[0:HALO, :, lanes_of(t)]

        @pl.when(jnp.where(at_top, zone < zones - 1, zone > 0))
        def _():
            way = jnp.where(at_top, 1, 0)
            remote(
                block, block, z_sem.at[0], halo_sem.at[way, t], (me + 1) % count
            ).wait_recv()

    def ret_copy(owner, t):
        return remote(
            done.at[pl.ds(owner * freq_dev, freq_dev), :, lanes_of(t)],
            back.at[:, :, tile_of(rank, t)],
            ret_send, ret_recv.at[t], zone * group + owner,
        )

    def sources(t, begin, end):
        lanes = slice(t * LANES, (t + 1) * LANES)

        def source_step(i, carry):
            k = jnp.where(ascending, i, freq_group - 1 - i)
            freq = zone * freq_group + k

            def scale(index, factor):
                return jnp.where((index >= 3) & (index <= NF - 3), factor, 0.0).astype(f32)

            w_own = scale(freq, -0.002)
            w_low, w_high = scale(freq - 2, 0.001), scale(freq + 3, 0.001)
            omega = omega_of(freq, (1, LANES))

            def slab(shift):
                return held[HALO + k + shift, :, lanes]

            def turn(values, amount):
                return pltpu.roll(values, amount % ND, 0)

            def rate(a, p, m):
                return a * (a * (p + m) - 2.0 * (p * m))

            own = slab(0)
            p2, m3, m2, m5, p3, p5 = (slab(shift) for shift in (2, -3, -2, -5, 3, 5))
            near = rate(own, turn(p2, -1), turn(m3, 3)) + rate(own, turn(p2, 1), turn(m3, -3))
            low = rate(turn(m2, 1), own, turn(m5, 4)) + rate(turn(m2, -1), own, turn(m5, -4))
            high = rate(turn(p3, -3), turn(p5, -4), own) + rate(turn(p3, 3), turn(p5, 4), own)
            interaction = w_own * near + w_low * low + w_high * high
            gain = (0.05 * omega) * jnp.maximum(0.0, wind[:, lanes] * omega - 1.0)
            fresh = own + gain * own + interaction
            done[k, :, lanes] = fresh
            acc[:, lanes] += fresh
            return carry

        lax.fori_loop(begin, end, source_step, 0)

    half = freq_group // 2
    near_side = rank_of((0, 1))

    def first_half(t):
        arrive_halo(jnp.logical_not(ascending), t)
        sources(t, 0, half)
        for dy in range(1, sides):
            for dc in range(2):
                ret_copy(rank_of((dy, dc)), t).start()

    def second_half(t):
        arrive_halo(ascending, t)
        sources(t, half, freq_group)
        ret_copy(near_side, t).start()
        back[:, :, tile_of(rank, t)] = done[
            pl.ds(rank * freq_dev, freq_dev), :, lanes_of(t)
        ]

    def zone_copy(dst_rank, src, dst, send, recv):
        return remote(src, dst, send, recv, zone * group + dst_rank)

    def damping_terms():
        others = mom_in.at[0 : count - 1]
        remote(others, others, mom_send, mom_recv, (me + 1) % count).wait_recv()
        total = jnp.sum(mom_in[...], axis=0) * (1.0 / (NF * ND))
        for t in range(parts):
            energy_mean, moment_one = total[t, 0:1], total[t, 1:2]
            mean_freq = moment_one / (energy_mean + 1e-06)
            steepness = energy_mean * mean_freq * mean_freq
            breaking = steepness * steepness / (1.0 + steepness * steepness)
            damp_out[t, 0:1] = 0.03 * breaking
            damp_out[t, 1:2] = 0.03 * breaking * moment_one
        for i in range(1, group):
            zone_copy(
                rank_of(offsets[i]), damp_out, damp_in.at[rank], damp_send, damp_recv
            ).start()
        damp_in[rank] = damp_out[...]

    first_half(0)
    for t in range(1, parts):
        for dy in range(1, sides):
            arrive_group(dy, t)
        first_half(t)
        if t == parts - 1:
            damping_terms()
        second_half(t - 1)
    second_half(parts - 1)

    sum_out[...] = jnp.sum(acc[...], axis=0, keepdims=True)
    for step in range(1, count):
        remote(sum_out, sum_in.at[me], sum_send, sum_recv, (me + step) % count).start()
    sum_in[me] = sum_out[...]

    others = damp_in.at[0 : group - 1]
    remote(others, others, damp_send, damp_recv, (me + 1) % count).wait_recv()
    for t in range(parts):
        block = done.at[0 : (group - 1) * freq_dev, :, lanes_of(t)]
        remote(block, block, ret_send, ret_recv.at[t], (me + 1) % count).wait_recv()
    for f in range(freq_dev):
        omega = omega_of(me * freq_dev + f, (1, LANES))
        for t in range(parts):
            for g in range(group):
                cols = slice(block_of(g, t) * LANES, (block_of(g, t) + 1) * LANES)
                value = back[f, :, cols] - (omega * damp_in[g, t, 0:1]) * adv[f, :, cols]
                for i, piece in enumerate(split_bf16(value)):
                    split[
                        i * bins_dev + f * ND : i * bins_dev + (f + 1) * ND, cols
                    ] = piece
    for j in range(cells // WIDE):
        low, high = max(0, j * WIDE - land), min(sea_cells, (j + 1) * WIDE)
        cols = slice(j * WIDE, (j + 1) * WIDE)
        got = jnp.dot(
            split[:, low:high], spread_ref[low:high, cols], preferred_element_type=f32
        )
        full_ref[:, cols] = got[:bins_dev] + got[bins_dev : 2 * bins_dev] + got[2 * bins_dev :]

    block = held.at[0 : (group - 1) * freq_dev]
    remote(block, block, y_sem, held_sem.at[0, 0], (me + 1) % count).wait_send()
    remote(block, block, ret_send, ret_recv.at[0], (me + 1) % count).wait_send()
    others = mom_in.at[0 : count - 1]
    remote(others, others, mom_send, mom_recv, (me + 1) % count).wait_send()
    others = damp_in.at[0 : group - 1]
    remote(others, others, damp_send, damp_recv, (me + 1) % count).wait_send()
    block = held.at[0:HALO]

    @pl.when(zone < zones - 1)
    def _():
        remote(block, block, z_sem.at[0], halo_sem.at[0, 0], (me + 1) % count).wait_send()

    @pl.when(zone > 0)
    def _():
        remote(block, block, z_sem.at[1], halo_sem.at[0, 0], (me + 1) % count).wait_send()

    others = sum_in.at[0 : count - 1]
    remote(others, others, sum_send, sum_recv, (me + 1) % count).wait()
    for g in range(group):
        mass = sum_in[g]
        for other in range(1, zones):
            mass = mass + sum_in[other * group + g]
        for t in range(parts):
            mean = mass[:, t * LANES : (t + 1) * LANES] * (1.0 / (NF * ND)) - damp_in[g, t, 1:2]
            cols = slice(block_of(g, t) * LANES, (block_of(g, t) + 1) * LANES)
            height_ref[0:1, cols] = 4.0 * jnp.sqrt(mean + 1e-06)


def store_kernel(
    count, full_in, height_in, window_in, new_out, wave_ref, mean_ref, sem
):
    cells = full_in.shape[1]
    sea_cells = height_in.shape[1]
    copy = pltpu.make_async_copy(full_in, new_out, sem)
    copy.start()
    me = lax.axis_index("spec")
    height = height_in[...]
    mean_ref[...] = jnp.sum(height, axis=1, keepdims=True) * (1.0 / sea_cells)
    points = cells // count
    start = window_start(count, me, cells)
    got = jnp.dot(
        rows_of(split_bf16(height), ND // 2, sea_cells), window_in[...],
        preferred_element_type=jnp.float32,
    )
    wave = got[0:1] + got[1:2] + got[2:3]
    shift = me * points - start
    turned = pltpu.roll(jnp.broadcast_to(wave, (8, WIDE)), (WIDE - shift) % WIDE, 1)
    wave_ref[...] = turned[0, :points]
    copy.wait()


def fused_local(spectrum, sea_mask, wind_speed, wind_angle):
    count = lax.axis_size("spec")
    bins_dev, cells = spectrum.shape
    group = group_size(count, bins_dev, cells)
    freq_dev = bins_dev // ND
    freq_group = freq_dev * group
    sea_cells = SEA_DEV * count
    width = sea_cells // group
    points = cells // count
    parts = width // LANES
    reach = cells - sea_cells + WIDE
    f32, bf16 = jnp.float32, jnp.bfloat16
    dma = pltpu.SemaphoreType.DMA
    vmem = pl.BlockSpec(memory_space=pltpu.VMEM)
    handed = pl.pallas_call(
        functools.partial(fused_kernel, count, group),
        out_shape=(
            pltpu.VMEM((bins_dev, cells), f32),
            pltpu.VMEM((1, sea_cells), f32),
            pltpu.VMEM((sea_cells, WIDE), bf16),
        ),
        in_specs=[pl.BlockSpec(memory_space=pl.ANY)] * 4,
        out_specs=(vmem,) * 3,
        scratch_shapes=[
            pltpu.VMEM((cells,), jnp.int32),
            pltpu.VMEM((cells,), f32),
            pltpu.VMEM((cells,), f32),
            pltpu.VMEM((1, cells), f32),
            pltpu.VMEM((1, cells), f32),
            pltpu.VMEM((sea_cells, cells), bf16),
            dma((3,)),
            pltpu.VMEM((bins_dev, cells), f32),
            pltpu.VMEM((bins_dev, cells), f32),
            pltpu.VMEM((3 * bins_dev, cells), bf16),
            pltpu.VMEM((sea_cells // WIDE, reach, WIDE), bf16),
            pltpu.VMEM((ND // 2, cells), bf16),
            pltpu.VMEM((freq_dev, ND, sea_cells), f32),
            pltpu.VMEM((freq_group + 2 * HALO, ND, width), f32),
            pltpu.VMEM((freq_group, ND, width), f32),
            pltpu.VMEM((freq_dev, ND, sea_cells), f32),
            pltpu.VMEM((parts, 2, group * LANES), f32),
            pltpu.VMEM((count, parts, 2, LANES), f32),
            pltpu.VMEM((ND, width), f32),
            pltpu.VMEM((ND, width), f32),
            pltpu.VMEM((1, width), f32),
            pltpu.VMEM((count, 1, width), f32),
            pltpu.VMEM((parts, 2, LANES), f32),
            pltpu.VMEM((group, parts, 2, LANES), f32),
            dma((freq_dev,)),
            dma((freq_group + 2 * HALO, parts)),
            dma((2, parts)),
            dma,
            dma((2,)),
            dma,
            dma,
            dma,
            dma((parts,)),
            dma,
            dma,
            dma,
            dma,
        ],
        compiler_params=pltpu.CompilerParams(collective_id=0, has_side_effects=True),
    )(sea_mask, wind_speed, wind_angle, spectrum)
    out, wave, mean = pl.pallas_call(
        functools.partial(store_kernel, count),
        out_shape=(
            pltpu.HBM((bins_dev, cells), f32),
            jax.ShapeDtypeStruct((points,), f32),
            jax.ShapeDtypeStruct((1, 1), f32),
        ),
        in_specs=[vmem] * 3,
        out_specs=(pl.BlockSpec(memory_space=pltpu.HBM), vmem, vmem),
        scratch_shapes=[dma],
    )(*[pltpu.with_memory_space_constraint(piece, pltpu.VMEM) for piece in handed])
    return (out, wave, mean.reshape(1))


def solution(mesh):
    in_specs = (P(("grp", "spec"), None), P(), P("grp"), P("grp"))
    out_specs = (P(("grp", "spec"), None), P(("grp", "spec")), P("grp"))

    def body(spectrum, sea_mask, wind_speed, wind_angle):
        fits = group_size(mesh.shape["spec"], *spectrum.shape)
        plan = fused_local if fits else local
        return plan(spectrum, sea_mask, wind_speed, wind_angle)

    return jax.shard_map(body, mesh=mesh, in_specs=in_specs, out_specs=out_specs, check_vma=False)
```

```python
import functools
import math

import jax
import jax.numpy as jnp
from jax import lax
from jax.experimental import pallas as pl
from jax.experimental.pallas import tpu as pltpu
from jax.sharding import PartitionSpec as P

NF = 48
ND = 32
NLON = 384
ADV_STEPS = 2
SEA_DEV = 64


def upwind_step(energy, courant_x, courant_y, sea_grid):
    west_cell = jnp.roll(energy, 1, axis=2)
    east_cell = jnp.roll(energy, -1, axis=2)
    edge_row = jnp.zeros_like(energy[:, :1])
    south_cell = jnp.concatenate([edge_row, energy[:, :-1]], axis=1)
    north_cell = jnp.concatenate([energy[:, 1:], edge_row], axis=1)
    updated = (
        energy
        - jnp.maximum(courant_x, 0.0) * (energy - west_cell)
        - jnp.minimum(courant_x, 0.0) * (east_cell - energy)
        - jnp.maximum(courant_y, 0.0) * (energy - south_cell)
        - jnp.minimum(courant_y, 0.0) * (north_cell - energy)
    )
    return updated * sea_grid


def courant_numbers(freq_index, dir_index, lat_count, dir_count):
    speed = 0.2 * jnp.exp(-math.log(1.1) * freq_index)
    heading = 2.0 * math.pi * (dir_index + 0.5) / dir_count
    rows = jnp.arange(lat_count, dtype=jnp.float32)
    latitude = (-75.0 + 150.0 * (rows + 0.5) / lat_count) * (math.pi / 180.0)
    courant_x = (speed * jnp.cos(heading))[:, None, None] / jnp.cos(latitude)[None, :, None]
    courant_y = (speed * jnp.sin(heading))[:, None, None]
    return (courant_x, courant_y)


def shift_freq(values, amount):
    if amount > 0:
        filler = jnp.zeros_like(values[:amount])
        return jnp.concatenate([filler, values[:-amount]], axis=0)
    filler = jnp.zeros_like(values[:-amount])
    return jnp.concatenate([values[-amount:], filler], axis=0)


def source_terms(energy, speed, angle):
    freq_count = energy.shape[0]
    dir_count = energy.shape[1]
    freq_ids = jnp.arange(freq_count, dtype=jnp.float32)
    frequency = jnp.exp(math.log(1.1) * (freq_ids - freq_count // 2))[:, None, None]
    heading = (2.0 * math.pi * (jnp.arange(dir_count, dtype=jnp.float32) + 0.5) / dir_count)[
        None, :, None
    ]
    energy_mean = jnp.mean(energy, axis=(0, 1))
    moment_one = jnp.mean(frequency * energy, axis=(0, 1))
    mean_freq = moment_one / (energy_mean + 1e-06)
    steepness = energy_mean * mean_freq * mean_freq
    breaking = steepness * steepness / (1.0 + steepness * steepness)
    wind_gain = (
        0.05
        * frequency
        * jnp.maximum(
            0.0, speed[None, None, :] * frequency * jnp.cos(heading - angle[None, None, :]) - 1.0
        )
    )
    damping = 0.03 * frequency * breaking[None, None, :]
    valid = ((freq_ids >= 3) & (freq_ids <= freq_count - 3)).astype(jnp.float32)[:, None, None]
    interaction = jnp.zeros_like(energy)
    for mirror in (1, -1):
        plus_bins = shift_freq(jnp.roll(energy, -mirror, axis=1), -2)
        minus_bins = shift_freq(jnp.roll(energy, 3 * mirror, axis=1), 3)
        transfer_rate = (
            0.001
            * valid
            * (energy * energy * (plus_bins + minus_bins) - 2.0 * energy * plus_bins * minus_bins)
        )
        interaction = interaction - 2.0 * transfer_rate
        interaction = interaction + jnp.roll(shift_freq(transfer_rate, 2), mirror, axis=1)
        interaction = interaction + jnp.roll(shift_freq(transfer_rate, -3), -3 * mirror, axis=1)
    updated = energy + (wind_gain - damping) * energy + interaction
    raw_height = 4.0 * jnp.sqrt(jnp.mean(updated, axis=(0, 1)) + 1e-06)
    return (updated, raw_height)


def local(spectrum, sea_mask, wind_speed, wind_angle):
    count = lax.axis_size("spec")
    position = lax.axis_index("spec")
    bins_dev = spectrum.shape[0]
    cells = spectrum.shape[1]
    points = cells // count
    lat_count = cells // NLON
    sea_float = sea_mask.astype(jnp.float32)
    bin_ids = position * bins_dev + jnp.arange(bins_dev, dtype=jnp.int32)
    freq_index = (bin_ids // ND).astype(jnp.float32)
    dir_index = (bin_ids % ND).astype(jnp.float32)
    courant_x, courant_y = courant_numbers(freq_index, dir_index, lat_count, ND)
    sea_grid = sea_float.reshape(1, lat_count, NLON)
    energy = (spectrum * sea_float[None, :]).reshape(bins_dev, lat_count, NLON)
    for substep in range(ADV_STEPS):
        energy = upwind_step(energy, courant_x, courant_y, sea_grid)
    advected = energy.reshape(bins_dev, cells)
    outgoing = advected.reshape(bins_dev, count, points)
    arrived = lax.all_to_all(outgoing, "spec", split_axis=1, concat_axis=0, tiled=True)
    start = position * points
    speed_own = lax.dynamic_slice_in_dim(wind_speed, start, points)
    angle_own = lax.dynamic_slice_in_dim(wind_angle, start, points)
    sea_own = lax.dynamic_slice_in_dim(sea_float, start, points)
    updated, raw_height = source_terms(arrived.reshape(NF, ND, points), speed_own, angle_own)
    wave_height = sea_own * raw_height
    own_total = jnp.zeros((count, 1), jnp.float32) + jnp.sum(wave_height)
    returned, totals = (
        lax.all_to_all(
            updated.reshape(NF * ND, 1, points), "spec", split_axis=0, concat_axis=1, tiled=True
        ),
        lax.all_to_all(own_total, "spec", split_axis=0, concat_axis=1, tiled=True),
    )
    new_spectrum = returned.reshape(bins_dev, cells)
    height_sum = jnp.sum(totals)
    mean_height = (height_sum / (SEA_DEV * count)).reshape(1)
    return (new_spectrum, wave_height, mean_height)


HALO = 5
LANES = 128
WIDE = 256
LAND = 4096.0


def group_size(count, bins_dev, cells):
    size = 4
    if count % size or bins_dev % ND or cells % (size * LANES) or cells % NLON:
        return 0
    if NLON % LANES or bins_dev // ND * size < 2 * HALO or cells % count:
        return 0
    sea = SEA_DEV * count
    if sea > min(cells, LAND) or sea % (size * LANES) or sea % WIDE or cells % WIDE:
        return 0
    if (cells - sea) % WIDE:
        return 0
    return size


def split_bf16(values):
    high = values.astype(jnp.bfloat16)
    left = values - high.astype(jnp.float32)
    mid = left.astype(jnp.bfloat16)
    low = (left - mid.astype(jnp.float32)).astype(jnp.bfloat16)
    return high, mid, low


def rows_of(parts, height, width):
    ids = lax.broadcasted_iota(jnp.int32, (height, width), 0)
    out = jnp.zeros((height, width), jnp.float32)
    for i, part in enumerate(parts):
        out = jnp.where(ids == i, jnp.broadcast_to(part.astype(jnp.float32), (height, width)), out)
    return out.astype(jnp.bfloat16)


def window_start(count, me, cells):
    return jnp.minimum(me * (cells // count) // LANES * LANES, cells - WIDE)


def fused_kernel(
    count, group, sea_in, wind_in, angle_in, spec_ref, full_ref, height_ref, window_ref,
    sea_raw, wind_raw, angle_raw, aux_ref, place_ref, spread_ref, aux_sem,
    raw, moved, split, wsplit, adv, held, done, back, mom_out, mom_in, wind, acc,
    sum_out, sum_in, damp_out, damp_in,
    load_sem, held_sem, halo_sem, y_sem, z_sem, chain_sem, mom_send, mom_recv,
    ret_send, ret_recv, sum_send, sum_recv, damp_send, damp_recv,
):
    f32, bf16 = jnp.float32, jnp.bfloat16
    freq_dev, _, sea_cells = adv.shape
    bins_dev, cells = moved.shape
    freq_group = freq_dev * group
    width = sea_cells // group
    zones = count // group
    lat_count = cells // NLON
    sides = group // 2
    parts = width // LANES
    cell_tiles = cells // LANES
    land = cells - sea_cells
    reach = land + WIDE
    me = lax.axis_index("spec")
    zone, rank = me // group, me % group
    side, core = rank // 2, rank % 2

    def remote(src, dst, send, recv, target):
        return pltpu.make_async_remote_copy(
            src_ref=src, dst_ref=dst, send_sem=send, recv_sem=recv,
            device_id={"spec": target}, device_id_type=pl.DeviceIdType.MESH,
        )

    loads = [
        pltpu.make_async_copy(
            spec_ref.at[pl.ds(f * ND, ND)], raw.at[pl.ds(f * ND, ND)], load_sem.at[f]
        )
        for f in range(freq_dev)
    ]
    small = [
        pltpu.make_async_copy(sea_in, sea_raw, aux_sem.at[0]),
        pltpu.make_async_copy(wind_in, wind_raw, aux_sem.at[1]),
        pltpu.make_async_copy(angle_in, angle_raw, aux_sem.at[2]),
    ]
    for load in small[:1] + loads + small[1:]:
        load.start()
    barrier = pltpu.get_barrier_semaphore()

    def signal(semaphore, target):
        pl.semaphore_signal(
            semaphore, inc=1, device_id={"spec": target}, device_id_type=pl.DeviceIdType.MESH
        )

    for step in range(1, group):
        signal(barrier, zone * group + (rank + step) % group)

    @pl.when(zone > 0)
    def _():
        signal(barrier, me - group)

    @pl.when(zone < zones - 1)
    def _():
        signal(barrier, me + group)

    @pl.when(zone == 0)
    def _():
        held[0:HALO] = jnp.zeros((HALO, ND, width), f32)

    @pl.when(zone == zones - 1)
    def _():
        held[HALO + freq_group :] = jnp.zeros((HALO, ND, width), f32)

    def block_of(index, t):
        return t * group + index

    def tile_of(index, t):
        return pl.ds(pl.multiple_of(block_of(index, t) * LANES, LANES), LANES)

    def lanes_of(t):
        return pl.ds(t * LANES, LANES)

    offsets = [(dy, dc) for dy in range(sides) for dc in range(2)]

    def rank_of(offset):
        return (side + offset[0]) % sides * 2 + (core + offset[1]) % 2

    def y_copy(f, peer, t):
        return remote(
            adv.at[f, :, tile_of(peer, t)],
            held.at[HALO + rank * freq_dev + f, :, lanes_of(t)],
            y_sem, held_sem.at[rank, f, t], zone * group + peer,
        )

    dirs = lax.broadcasted_iota(jnp.int32, (ND, LANES), 0).astype(f32)
    heading = 2.0 * math.pi * (dirs + 0.5) / ND
    cos_h, sin_h = jnp.cos(heading), jnp.sin(heading)
    log_step = math.log(1.1)
    lats = [math.radians(-75.0 + 150.0 * (r + 0.5) / lat_count) for r in range(lat_count)]

    def omega_of(freq, shape):
        return jnp.exp(jnp.full(shape, log_step, f32) * (freq.astype(f32) - NF // 2))

    square_rows = lax.broadcasted_iota(jnp.int32, (LANES, LANES), 0)
    square_cols = lax.broadcasted_iota(jnp.int32, (LANES, LANES), 1)
    small[0].wait()
    aux_ref[...] = sea_raw[...].astype(f32).reshape(1, cells)
    sea = [aux_ref[0:1, r * NLON : (r + 1) * NLON] for r in range(lat_count)]
    mask = [aux_ref[0:1, i * LANES : (i + 1) * LANES] for i in range(cell_tiles)]
    tri_up = jnp.where(square_rows < square_cols, 1.0, 0.0).astype(bf16)
    ranks = jnp.dot(rows_of(mask, ND // 2, LANES), tri_up, preferred_element_type=f32)
    before = jnp.zeros((1, 1), f32)
    for i in range(cell_tiles):
        place_ref[0:1, i * LANES : (i + 1) * LANES] = jnp.where(
            mask[i] > 0.0, ranks[i : i + 1] + before, LAND
        )
        before = before + jnp.sum(mask[i], axis=1, keepdims=True)
    pair_rows = lax.broadcasted_iota(jnp.int32, (WIDE, reach), 0).astype(f32)

    def build(pair):
        cols = pl.ds(pl.multiple_of(pair * WIDE, LANES), reach)
        first = (pair * WIDE).astype(f32)
        hit = jnp.where(place_ref[0:1, cols] - first == pair_rows, 1.0, 0.0)
        spread_ref[pl.ds(pl.multiple_of(pair * WIDE, LANES), WIDE), cols] = hit.astype(bf16)

    def packed(values, pair):
        cols = pl.ds(pl.multiple_of(pair * WIDE, LANES), reach)
        return lax.dot_general(
            values[:, cols],
            spread_ref[pl.ds(pl.multiple_of(pair * WIDE, LANES), WIDE), cols],
            (((1,), (1,)), ((), ())), preferred_element_type=f32,
        )

    quarter = ND // 4
    tiles = NLON // LANES
    def advect(f):
        loads[f].wait()
        freq = (me * freq_dev + f).astype(f32)
        speed = 0.2 * jnp.exp(jnp.full((quarter, LANES), -log_step, f32) * freq)
        for q in range(4):
            east, north = q in (0, 3), q in (0, 1)
            rows = slice(f * ND + q * quarter, f * ND + (q + 1) * quarter)
            part = slice(q * quarter, (q + 1) * quarter)
            cx0 = speed * jnp.abs(cos_h[part])
            cy = jnp.concatenate([speed * jnp.abs(sin_h[part])] * tiles, axis=1)
            cx = [jnp.concatenate([cx0 * (1.0 / math.cos(a))] * tiles, axis=1) for a in lats]
            energy = [raw[rows, r * NLON : (r + 1) * NLON] * sea[r] for r in range(lat_count)]
            for _ in range(ADV_STEPS):
                fresh = []
                for r in range(lat_count):
                    e = energy[r]
                    side_x = pltpu.roll(e, 1 if east else NLON - 1, 1)
                    other = r - 1 if north else r + 1
                    side_y = energy[other] if 0 <= other < lat_count else 0.0
                    fresh.append((e - cx[r] * (e - side_x) - cy * (e - side_y)) * sea[r])
                energy = fresh
            for r in range(lat_count):
                moved[rows, r * NLON : (r + 1) * NLON] = energy[r]
        for i, piece in enumerate(split_bf16(moved[f * ND : (f + 1) * ND])):
            split[(3 * f + i) * ND : (3 * f + i + 1) * ND, :] = piece

    def cols_of(index):
        return pl.ds(pl.multiple_of(index * LANES, LANES), LANES)

    def side_of(dy):
        return (side + dy) % sides

    def pack(t, dy, begin, end):
        pair = t * sides + side_of(dy)
        got = packed(split.at[begin * 3 * ND : end * 3 * ND], pair)
        cols = pl.ds(pl.multiple_of(pair * WIDE, LANES), WIDE)
        here = pl.ds(pl.multiple_of(side_of(dy) * WIDE, LANES), WIDE)
        mass, moment = None, None
        for f in range(begin, end):
            base = (f - begin) * 3 * ND
            piece = got[base : base + ND] + got[base + ND : base + 2 * ND] + (
                got[base + 2 * ND : base + 3 * ND]
            )
            adv[f, :, cols] = piece
            total = jnp.sum(piece, axis=0, keepdims=True)
            scaled = omega_of(me * freq_dev + f, (1, WIDE)) * total
            mass = total if mass is None else mass + total
            moment = scaled if moment is None else moment + scaled
        if begin:
            mass, moment = mass + mom_out[t, 0:1, here], moment + mom_out[t, 1:2, here]
        mom_out[t, 0:1, here] = mass
        mom_out[t, 1:2, here] = moment

    def send_far(t, dy, begin, end):
        for c in range(2):
            for f in range(begin, end):
                y_copy(f, side_of(dy) * 2 + c, t).start()

    def up_copy(slot, t):
        return remote(
            held.at[HALO + slot, :, lanes_of(t)],
            held.at[HALO + slot - freq_group, :, lanes_of(t)],
            z_sem.at[0], halo_sem.at[0, t], (zone + 1) % zones * group + rank,
        )

    def down_copy(slot, t):
        return remote(
            held.at[HALO + slot, :, lanes_of(t)],
            held.at[HALO + slot + freq_group, :, lanes_of(t)],
            z_sem.at[1], halo_sem.at[1, t], (zone + zones - 1) % zones * group + rank,
        )

    def forward(slot, t):
        @pl.when((slot >= freq_group - HALO) & (zone < zones - 1))
        def _():
            up_copy(slot, t).start()

        @pl.when((slot < HALO) & (zone > 0))
        def _():
            down_copy(slot, t).start()

    def send_near(t):
        for f in range(freq_dev):
            y_copy(f, rank_of((0, 1)), t).start()
            held[HALO + rank * freq_dev + f, :, lanes_of(t)] = adv[f, :, tile_of(rank, t)]
        for f in range(freq_dev):
            forward(rank * freq_dev + f, t)

    def arrive_group(dy, t):
        for f in range(freq_dev):
            for dc in range(2):
                if (dy, dc) != (0, 0):
                    source = rank_of((dy, dc))
                    slot = source * freq_dev + f
                    block = held.at[HALO + slot, :, lanes_of(t)]
                    remote(
                        block, block, y_sem, held_sem.at[source, f, t], (me + 1) % count
                    ).wait_recv()
                    forward(slot, t)

    far = list(range(1, sides))
    for dy in far:
        build(side_of(dy))
    advect(0)
    for dy in far:
        pack(0, dy, 0, 1)
    advect(1)
    pl.semaphore_wait(
        barrier, group - 1 + jnp.where(zone > 0, 1, 0) + jnp.where(zone < zones - 1, 1, 0)
    )
    for dy in far:
        send_far(0, dy, 0, 1)

    @pl.when(zone == 0)
    def _():
        signal(chain_sem.at[0], (me + group) % count)

    @pl.when(zone == zones - 1)
    def _():
        signal(chain_sem.at[1], (me + count - group) % count)

    for f in range(2, freq_dev):
        advect(f)
    for dy in far:
        pack(0, dy, 1, freq_dev)
        send_far(0, dy, 1, freq_dev)
    build(side)
    pack(0, 0, 0, freq_dev)
    send_near(0)
    for t in range(1, parts):
        for dy in far:
            build(t * sides + side_of(dy))
            pack(t, dy, 0, freq_dev)
            send_far(t, dy, 0, freq_dev)
        build(t * sides + side)
        pack(t, 0, 0, freq_dev)
        send_near(t)

    def relay(level):
        @pl.when(zone == level)
        def _():
            pl.semaphore_wait(chain_sem.at[0], 1)

            @pl.when(zone < zones - 1)
            def _():
                signal(chain_sem.at[0], (me + group) % count)

        @pl.when(zone == zones - 1 - level)
        def _():
            pl.semaphore_wait(chain_sem.at[1], 1)

            @pl.when(zone > 0)
            def _():
                signal(chain_sem.at[1], (me + count - group) % count)

    relay(1)
    small[1].wait()
    small[2].wait()
    speed_all = wind_raw[...].reshape(1, cells)
    angle_all = angle_raw[...].reshape(1, cells)
    wsplit[...] = rows_of(
        split_bf16(speed_all * jnp.cos(angle_all)) + split_bf16(speed_all * jnp.sin(angle_all)),
        2 * quarter, cells,
    )
    for t in range(parts):
        own = packed(wsplit, t * sides + side)
        own = jnp.where(core == 0, own[:, :LANES], own[:, LANES:])
        along = own[0:1] + own[1:2] + own[2:3]
        across = own[3:4] + own[4:5] + own[5:6]
        wind[:, t * LANES : (t + 1) * LANES] = cos_h * along + sin_h * across

    for t in range(parts):
        arrive_group(0, t)
    for level in range(2, zones):
        relay(level)
    for step in range(1, count):
        target = (me + step) % count
        remote(
            mom_out.at[:, :, cols_of(target % group)], mom_in.at[me],
            mom_send, mom_recv, target,
        ).start()
    mom_in[me] = mom_out[:, :, cols_of(rank)]
    start = window_start(count, me, cells)
    mine = place_ref[0:1, pl.ds(pl.multiple_of(start, LANES), WIDE)]
    sea_rows = lax.broadcasted_iota(jnp.int32, (sea_cells, WIDE), 0).astype(f32)
    window_ref[...] = jnp.where(sea_rows == mine, 1.0, 0.0).astype(bf16)
    for dy in far:
        arrive_group(dy, 0)

    acc[...] = jnp.zeros_like(acc)
    ascending = side > 0

    def arrive_halo(at_top, t):
        block = held.at[0:HALO, :, lanes_of(t)]

        @pl.when(jnp.where(at_top, zone < zones - 1, zone > 0))
        def _():
            way = jnp.where(at_top, 1, 0)
            remote(
                block, block, z_sem.at[0], halo_sem.at[way, t], (me + 1) % count
            ).wait_recv()

    def ret_copy(owner, t):
        return remote(
            done.at[pl.ds(owner * freq_dev, freq_dev), :, lanes_of(t)],
            back.at[:, :, tile_of(rank, t)],
            ret_send, ret_recv.at[t], zone * group + owner,
        )

    def sources(t, begin, end):
        lanes = slice(t * LANES, (t + 1) * LANES)

        def source_step(i, carry):
            k = jnp.where(ascending, i, freq_group - 1 - i)
            freq = zone * freq_group + k

            def scale(index, factor):
                return jnp.where((index >= 3) & (index <= NF - 3), factor, 0.0).astype(f32)

            w_own = scale(freq, -0.002)
            w_low, w_high = scale(freq - 2, 0.001), scale(freq + 3, 0.001)
            omega = omega_of(freq, (1, LANES))

            def slab(shift):
                return held[HALO + k + shift, :, lanes]

            def turn(values, amount):
                return pltpu.roll(values, amount % ND, 0)

            def rate(a, p, m):
                return a * (a * (p + m) - 2.0 * (p * m))

            own = slab(0)
            p2, m3, m2, m5, p3, p5 = (slab(shift) for shift in (2, -3, -2, -5, 3, 5))
            near = rate(own, turn(p2, -1), turn(m3, 3)) + rate(own, turn(p2, 1), turn(m3, -3))
            low = rate(turn(m2, 1), own, turn(m5, 4)) + rate(turn(m2, -1), own, turn(m5, -4))
            high = rate(turn(p3, -3), turn(p5, -4), own) + rate(turn(p3, 3), turn(p5, 4), own)
            interaction = w_own * near + w_low * low + w_high * high
            gain = (0.05 * omega) * jnp.maximum(0.0, wind[:, lanes] * omega - 1.0)
            fresh = own + gain * own + interaction
            done[k, :, lanes] = fresh
            acc[:, lanes] += fresh
            return carry

        lax.fori_loop(begin, end, source_step, 0)

    half = freq_group // 2
    near_side = rank_of((0, 1))

    def first_half(t):
        arrive_halo(jnp.logical_not(ascending), t)
        sources(t, 0, half)
        for dy in range(1, sides):
            for dc in range(2):
                ret_copy(rank_of((dy, dc)), t).start()

    def second_half(t):
        arrive_halo(ascending, t)
        sources(t, half, freq_group)
        ret_copy(near_side, t).start()
        back[:, :, tile_of(rank, t)] = done[
            pl.ds(rank * freq_dev, freq_dev), :, lanes_of(t)
        ]

    def zone_copy(dst_rank, src, dst, send, recv):
        return remote(src, dst, send, recv, zone * group + dst_rank)

    def damping_terms():
        others = mom_in.at[0 : count - 1]
        remote(others, others, mom_send, mom_recv, (me + 1) % count).wait_recv()
        total = jnp.sum(mom_in[...], axis=0) * (1.0 / (NF * ND))
        for t in range(parts):
            energy_mean, moment_one = total[t, 0:1], total[t, 1:2]
            mean_freq = moment_one / (energy_mean + 1e-06)
            steepness = energy_mean * mean_freq * mean_freq
            breaking = steepness * steepness / (1.0 + steepness * steepness)
            damp_out[t, 0:1] = 0.03 * breaking
            damp_out[t, 1:2] = 0.03 * breaking * moment_one
        for i in range(1, group):
            zone_copy(
                rank_of(offsets[i]), damp_out, damp_in.at[rank], damp_send, damp_recv
            ).start()
        damp_in[rank] = damp_out[...]

    first_half(0)
    for t in range(1, parts):
        for dy in range(1, sides):
            arrive_group(dy, t)
        first_half(t)
        if t == parts - 1:
            damping_terms()
        second_half(t - 1)
    second_half(parts - 1)

    sum_out[...] = jnp.sum(acc[...], axis=0, keepdims=True)
    for step in range(1, count):
        remote(sum_out, sum_in.at[me], sum_send, sum_recv, (me + step) % count).start()
    sum_in[me] = sum_out[...]

    others = damp_in.at[0 : group - 1]
    remote(others, others, damp_send, damp_recv, (me + 1) % count).wait_recv()
    for t in range(parts):
        block = done.at[0 : (group - 1) * freq_dev, :, lanes_of(t)]
        remote(block, block, ret_send, ret_recv.at[t], (me + 1) % count).wait_recv()
    for f in range(freq_dev):
        omega = omega_of(me * freq_dev + f, (1, LANES))
        for t in range(parts):
            for g in range(group):
                cols = slice(block_of(g, t) * LANES, (block_of(g, t) + 1) * LANES)
                value = back[f, :, cols] - (omega * damp_in[g, t, 0:1]) * adv[f, :, cols]
                for i, piece in enumerate(split_bf16(value)):
                    split[(3 * f + i) * ND : (3 * f + i + 1) * ND, cols] = piece
    for j in range(cells // WIDE):
        low, high = max(0, j * WIDE - land), min(sea_cells, (j + 1) * WIDE)
        cols = slice(j * WIDE, (j + 1) * WIDE)
        got = jnp.dot(
            split[:, low:high], spread_ref[low:high, cols], preferred_element_type=f32
        )
        for f in range(freq_dev):
            base = 3 * f * ND
            full_ref[f * ND : (f + 1) * ND, cols] = got[base : base + ND] + (
                got[base + ND : base + 2 * ND]
            ) + got[base + 2 * ND : base + 3 * ND]

    block = held.at[0 : (group - 1) * freq_dev]
    remote(block, block, y_sem, held_sem.at[0, 0, 0], (me + 1) % count).wait_send()
    remote(block, block, ret_send, ret_recv.at[0], (me + 1) % count).wait_send()
    others = mom_in.at[0 : count - 1]
    remote(others, others, mom_send, mom_recv, (me + 1) % count).wait_send()
    others = damp_in.at[0 : group - 1]
    remote(others, others, damp_send, damp_recv, (me + 1) % count).wait_send()
    block = held.at[0:HALO]

    @pl.when(zone < zones - 1)
    def _():
        remote(block, block, z_sem.at[0], halo_sem.at[0, 0], (me + 1) % count).wait_send()

    @pl.when(zone > 0)
    def _():
        remote(block, block, z_sem.at[1], halo_sem.at[0, 0], (me + 1) % count).wait_send()

    others = sum_in.at[0 : count - 1]
    remote(others, others, sum_send, sum_recv, (me + 1) % count).wait()
    for g in range(group):
        mass = sum_in[g]
        for other in range(1, zones):
            mass = mass + sum_in[other * group + g]
        for t in range(parts):
            mean = mass[:, t * LANES : (t + 1) * LANES] * (1.0 / (NF * ND)) - damp_in[g, t, 1:2]
            cols = slice(block_of(g, t) * LANES, (block_of(g, t) + 1) * LANES)
            height_ref[0:1, cols] = 4.0 * jnp.sqrt(mean + 1e-06)


def store_kernel(
    count, full_in, height_in, window_in, new_out, wave_ref, mean_ref, sem
):
    cells = full_in.shape[1]
    sea_cells = height_in.shape[1]
    copy = pltpu.make_async_copy(full_in, new_out, sem)
    copy.start()
    me = lax.axis_index("spec")
    height = height_in[...]
    mean_ref[...] = jnp.sum(height, axis=1, keepdims=True) * (1.0 / sea_cells)
    points = cells // count
    start = window_start(count, me, cells)
    got = jnp.dot(
        rows_of(split_bf16(height), ND // 2, sea_cells), window_in[...],
        preferred_element_type=jnp.float32,
    )
    wave = got[0:1] + got[1:2] + got[2:3]
    shift = me * points - start
    turned = pltpu.roll(jnp.broadcast_to(wave, (8, WIDE)), (WIDE - shift) % WIDE, 1)
    wave_ref[...] = turned[0, :points]
    copy.wait()


def fused_local(spectrum, sea_mask, wind_speed, wind_angle):
    count = lax.axis_size("spec")
    bins_dev, cells = spectrum.shape
    group = group_size(count, bins_dev, cells)
    freq_dev = bins_dev // ND
    freq_group = freq_dev * group
    sea_cells = SEA_DEV * count
    width = sea_cells // group
    points = cells // count
    parts = width // LANES
    f32, bf16 = jnp.float32, jnp.bfloat16
    dma = pltpu.SemaphoreType.DMA
    vmem = pl.BlockSpec(memory_space=pltpu.VMEM)
    handed = pl.pallas_call(
        functools.partial(fused_kernel, count, group),
        out_shape=(
            pltpu.VMEM((bins_dev, cells), f32),
            pltpu.VMEM((1, sea_cells), f32),
            pltpu.VMEM((sea_cells, WIDE), bf16),
        ),
        in_specs=[pl.BlockSpec(memory_space=pl.ANY)] * 4,
        out_specs=(vmem,) * 3,
        scratch_shapes=[
            pltpu.VMEM((cells,), jnp.int32),
            pltpu.VMEM((cells,), f32),
            pltpu.VMEM((cells,), f32),
            pltpu.VMEM((1, cells), f32),
            pltpu.VMEM((1, cells), f32),
            pltpu.VMEM((sea_cells, cells), bf16),
            dma((3,)),
            pltpu.VMEM((bins_dev, cells), f32),
            pltpu.VMEM((bins_dev, cells), f32),
            pltpu.VMEM((3 * bins_dev, cells), bf16),
            pltpu.VMEM((ND // 2, cells), bf16),
            pltpu.VMEM((freq_dev, ND, sea_cells), f32),
            pltpu.VMEM((freq_group + 2 * HALO, ND, width), f32),
            pltpu.VMEM((freq_group, ND, width), f32),
            pltpu.VMEM((freq_dev, ND, sea_cells), f32),
            pltpu.VMEM((parts, 2, group * LANES), f32),
            pltpu.VMEM((count, parts, 2, LANES), f32),
            pltpu.VMEM((ND, width), f32),
            pltpu.VMEM((ND, width), f32),
            pltpu.VMEM((1, width), f32),
            pltpu.VMEM((count, 1, width), f32),
            pltpu.VMEM((parts, 2, LANES), f32),
            pltpu.VMEM((group, parts, 2, LANES), f32),
            dma((freq_dev,)),
            dma((group, freq_dev, parts)),
            dma((2, parts)),
            dma,
            dma((2,)),
            pltpu.SemaphoreType.REGULAR((2,)),
            dma,
            dma,
            dma,
            dma((parts,)),
            dma,
            dma,
            dma,
            dma,
        ],
        compiler_params=pltpu.CompilerParams(collective_id=0, has_side_effects=True),
    )(sea_mask, wind_speed, wind_angle, spectrum)
    out, wave, mean = pl.pallas_call(
        functools.partial(store_kernel, count),
        out_shape=(
            pltpu.HBM((bins_dev, cells), f32),
            jax.ShapeDtypeStruct((points,), f32),
            jax.ShapeDtypeStruct((1, 1), f32),
        ),
        in_specs=[vmem] * 3,
        out_specs=(pl.BlockSpec(memory_space=pltpu.HBM), vmem, vmem),
        scratch_shapes=[dma],
    )(*[pltpu.with_memory_space_constraint(piece, pltpu.VMEM) for piece in handed])
    return (out, wave, mean.reshape(1))


def solution(mesh):
    in_specs = (P(("grp", "spec"), None), P(), P("grp"), P("grp"))
    out_specs = (P(("grp", "spec"), None), P(("grp", "spec")), P("grp"))

    def body(spectrum, sea_mask, wind_speed, wind_angle):
        fits = group_size(mesh.shape["spec"], *spectrum.shape)
        plan = fused_local if fits else local
        return plan(spectrum, sea_mask, wind_speed, wind_angle)

    return jax.shard_map(body, mesh=mesh, in_specs=in_specs, out_specs=out_specs, check_vma=False)
```

```python
import functools
import math

import jax
import jax.numpy as jnp
from jax import lax
from jax.experimental import pallas as pl
from jax.experimental.pallas import tpu as pltpu
from jax.sharding import PartitionSpec as P

NF = 48
ND = 32
NLON = 384
ADV_STEPS = 2
SEA_DEV = 64


def upwind_step(energy, courant_x, courant_y, sea_grid):
    west_cell = jnp.roll(energy, 1, axis=2)
    east_cell = jnp.roll(energy, -1, axis=2)
    edge_row = jnp.zeros_like(energy[:, :1])
    south_cell = jnp.concatenate([edge_row, energy[:, :-1]], axis=1)
    north_cell = jnp.concatenate([energy[:, 1:], edge_row], axis=1)
    updated = (
        energy
        - jnp.maximum(courant_x, 0.0) * (energy - west_cell)
        - jnp.minimum(courant_x, 0.0) * (east_cell - energy)
        - jnp.maximum(courant_y, 0.0) * (energy - south_cell)
        - jnp.minimum(courant_y, 0.0) * (north_cell - energy)
    )
    return updated * sea_grid


def courant_numbers(freq_index, dir_index, lat_count, dir_count):
    speed = 0.2 * jnp.exp(-math.log(1.1) * freq_index)
    heading = 2.0 * math.pi * (dir_index + 0.5) / dir_count
    rows = jnp.arange(lat_count, dtype=jnp.float32)
    latitude = (-75.0 + 150.0 * (rows + 0.5) / lat_count) * (math.pi / 180.0)
    courant_x = (speed * jnp.cos(heading))[:, None, None] / jnp.cos(latitude)[None, :, None]
    courant_y = (speed * jnp.sin(heading))[:, None, None]
    return (courant_x, courant_y)


def shift_freq(values, amount):
    if amount > 0:
        filler = jnp.zeros_like(values[:amount])
        return jnp.concatenate([filler, values[:-amount]], axis=0)
    filler = jnp.zeros_like(values[:-amount])
    return jnp.concatenate([values[-amount:], filler], axis=0)


def source_terms(energy, speed, angle):
    freq_count = energy.shape[0]
    dir_count = energy.shape[1]
    freq_ids = jnp.arange(freq_count, dtype=jnp.float32)
    frequency = jnp.exp(math.log(1.1) * (freq_ids - freq_count // 2))[:, None, None]
    heading = (2.0 * math.pi * (jnp.arange(dir_count, dtype=jnp.float32) + 0.5) / dir_count)[
        None, :, None
    ]
    energy_mean = jnp.mean(energy, axis=(0, 1))
    moment_one = jnp.mean(frequency * energy, axis=(0, 1))
    mean_freq = moment_one / (energy_mean + 1e-06)
    steepness = energy_mean * mean_freq * mean_freq
    breaking = steepness * steepness / (1.0 + steepness * steepness)
    wind_gain = (
        0.05
        * frequency
        * jnp.maximum(
            0.0, speed[None, None, :] * frequency * jnp.cos(heading - angle[None, None, :]) - 1.0
        )
    )
    damping = 0.03 * frequency * breaking[None, None, :]
    valid = ((freq_ids >= 3) & (freq_ids <= freq_count - 3)).astype(jnp.float32)[:, None, None]
    interaction = jnp.zeros_like(energy)
    for mirror in (1, -1):
        plus_bins = shift_freq(jnp.roll(energy, -mirror, axis=1), -2)
        minus_bins = shift_freq(jnp.roll(energy, 3 * mirror, axis=1), 3)
        transfer_rate = (
            0.001
            * valid
            * (energy * energy * (plus_bins + minus_bins) - 2.0 * energy * plus_bins * minus_bins)
        )
        interaction = interaction - 2.0 * transfer_rate
        interaction = interaction + jnp.roll(shift_freq(transfer_rate, 2), mirror, axis=1)
        interaction = interaction + jnp.roll(shift_freq(transfer_rate, -3), -3 * mirror, axis=1)
    updated = energy + (wind_gain - damping) * energy + interaction
    raw_height = 4.0 * jnp.sqrt(jnp.mean(updated, axis=(0, 1)) + 1e-06)
    return (updated, raw_height)


def local(spectrum, sea_mask, wind_speed, wind_angle):
    count = lax.axis_size("spec")
    position = lax.axis_index("spec")
    bins_dev = spectrum.shape[0]
    cells = spectrum.shape[1]
    points = cells // count
    lat_count = cells // NLON
    sea_float = sea_mask.astype(jnp.float32)
    bin_ids = position * bins_dev + jnp.arange(bins_dev, dtype=jnp.int32)
    freq_index = (bin_ids // ND).astype(jnp.float32)
    dir_index = (bin_ids % ND).astype(jnp.float32)
    courant_x, courant_y = courant_numbers(freq_index, dir_index, lat_count, ND)
    sea_grid = sea_float.reshape(1, lat_count, NLON)
    energy = (spectrum * sea_float[None, :]).reshape(bins_dev, lat_count, NLON)
    for substep in range(ADV_STEPS):
        energy = upwind_step(energy, courant_x, courant_y, sea_grid)
    advected = energy.reshape(bins_dev, cells)
    outgoing = advected.reshape(bins_dev, count, points)
    arrived = lax.all_to_all(outgoing, "spec", split_axis=1, concat_axis=0, tiled=True)
    start = position * points
    speed_own = lax.dynamic_slice_in_dim(wind_speed, start, points)
    angle_own = lax.dynamic_slice_in_dim(wind_angle, start, points)
    sea_own = lax.dynamic_slice_in_dim(sea_float, start, points)
    updated, raw_height = source_terms(arrived.reshape(NF, ND, points), speed_own, angle_own)
    wave_height = sea_own * raw_height
    own_total = jnp.zeros((count, 1), jnp.float32) + jnp.sum(wave_height)
    returned, totals = (
        lax.all_to_all(
            updated.reshape(NF * ND, 1, points), "spec", split_axis=0, concat_axis=1, tiled=True
        ),
        lax.all_to_all(own_total, "spec", split_axis=0, concat_axis=1, tiled=True),
    )
    new_spectrum = returned.reshape(bins_dev, cells)
    height_sum = jnp.sum(totals)
    mean_height = (height_sum / (SEA_DEV * count)).reshape(1)
    return (new_spectrum, wave_height, mean_height)


HALO = 5
LANES = 128
WIDE = 256
LAND = 4096.0


def group_size(count, bins_dev, cells):
    size = 4
    if count % size or bins_dev % ND or cells % (size * LANES) or cells % NLON:
        return 0
    if NLON % LANES or bins_dev // ND * size < 2 * HALO or cells % count:
        return 0
    sea = SEA_DEV * count
    if sea > min(cells, LAND) or sea % (size * LANES) or sea % WIDE or cells % WIDE:
        return 0
    if (cells - sea) % WIDE:
        return 0
    return size


def split_bf16(values):
    high = values.astype(jnp.bfloat16)
    left = values - high.astype(jnp.float32)
    mid = left.astype(jnp.bfloat16)
    low = (left - mid.astype(jnp.float32)).astype(jnp.bfloat16)
    return high, mid, low


def rows_of(parts, height, width):
    ids = lax.broadcasted_iota(jnp.int32, (height, width), 0)
    out = jnp.zeros((height, width), jnp.float32)
    for i, part in enumerate(parts):
        out = jnp.where(ids == i, jnp.broadcast_to(part.astype(jnp.float32), (height, width)), out)
    return out.astype(jnp.bfloat16)


def window_start(count, me, cells):
    return jnp.minimum(me * (cells // count) // LANES * LANES, cells - WIDE)


def fused_kernel(
    count, group, sea_in, wind_in, angle_in, spec_ref, full_ref, height_ref, near_ref,
    sea_raw, wind_raw, angle_raw, aux_ref, place_ref, spread_ref, aux_sem,
    raw, moved, split, wsplit, adv, held, done, back, mom_out, mom_in, wind, acc,
    sum_out, sum_in, damp_out, damp_in,
    load_sem, held_sem, halo_sem, y_sem, z_sem, chain_sem, mom_send, mom_recv,
    ret_send, ret_recv, sum_send, sum_recv, damp_send, damp_recv,
):
    f32, bf16 = jnp.float32, jnp.bfloat16
    freq_dev, _, sea_cells = adv.shape
    bins_dev, cells = moved.shape
    freq_group = freq_dev * group
    width = sea_cells // group
    zones = count // group
    lat_count = cells // NLON
    sides = group // 2
    parts = width // LANES
    cell_tiles = cells // LANES
    land = cells - sea_cells
    reach = land + WIDE
    me = lax.axis_index("spec")
    zone, rank = me // group, me % group
    side, core = rank // 2, rank % 2

    def remote(src, dst, send, recv, target):
        return pltpu.make_async_remote_copy(
            src_ref=src, dst_ref=dst, send_sem=send, recv_sem=recv,
            device_id={"spec": target}, device_id_type=pl.DeviceIdType.MESH,
        )

    loads = [
        pltpu.make_async_copy(
            spec_ref.at[pl.ds(f * ND, ND)], raw.at[pl.ds(f * ND, ND)], load_sem.at[f]
        )
        for f in range(freq_dev)
    ]
    small = [
        pltpu.make_async_copy(sea_in, sea_raw, aux_sem.at[0]),
        pltpu.make_async_copy(wind_in, wind_raw, aux_sem.at[1]),
        pltpu.make_async_copy(angle_in, angle_raw, aux_sem.at[2]),
    ]
    for load in small[:1] + loads + small[1:]:
        load.start()
    barrier = pltpu.get_barrier_semaphore()

    def signal(semaphore, target):
        pl.semaphore_signal(
            semaphore, inc=1, device_id={"spec": target}, device_id_type=pl.DeviceIdType.MESH
        )

    for step in range(1, group):
        signal(barrier, zone * group + (rank + step) % group)

    @pl.when(zone > 0)
    def _():
        for c in range(2):
            signal(barrier, (zone - 1) * group + side * 2 + c)

    @pl.when(zone < zones - 1)
    def _():
        for c in range(2):
            signal(barrier, (zone + 1) * group + side * 2 + c)

    @pl.when(zone == 0)
    def _():
        held[0:HALO] = jnp.zeros((HALO, ND, width), f32)

    @pl.when(zone == zones - 1)
    def _():
        held[HALO + freq_group :] = jnp.zeros((HALO, ND, width), f32)

    def block_of(index, t):
        return t * group + index

    def tile_of(index, t):
        return pl.ds(pl.multiple_of(block_of(index, t) * LANES, LANES), LANES)

    def lanes_of(t):
        return pl.ds(t * LANES, LANES)

    offsets = [(dy, dc) for dy in range(sides) for dc in range(2)]

    def rank_of(offset):
        return (side + offset[0]) % sides * 2 + (core + offset[1]) % 2

    def y_copy(f, peer, t):
        return remote(
            adv.at[f, :, tile_of(peer, t)],
            held.at[HALO + rank * freq_dev + f, :, lanes_of(t)],
            y_sem, held_sem.at[rank, f, t], zone * group + peer,
        )

    dirs = lax.broadcasted_iota(jnp.int32, (ND, LANES), 0).astype(f32)
    heading = 2.0 * math.pi * (dirs + 0.5) / ND
    cos_h, sin_h = jnp.cos(heading), jnp.sin(heading)
    log_step = math.log(1.1)
    lats = [math.radians(-75.0 + 150.0 * (r + 0.5) / lat_count) for r in range(lat_count)]

    def omega_of(freq, shape):
        return jnp.exp(jnp.full(shape, log_step, f32) * (freq.astype(f32) - NF // 2))

    square_rows = lax.broadcasted_iota(jnp.int32, (LANES, LANES), 0)
    square_cols = lax.broadcasted_iota(jnp.int32, (LANES, LANES), 1)
    small[0].wait()
    aux_ref[...] = sea_raw[...].astype(f32).reshape(1, cells)
    sea = [aux_ref[0:1, r * NLON : (r + 1) * NLON] for r in range(lat_count)]
    mask = [aux_ref[0:1, i * LANES : (i + 1) * LANES] for i in range(cell_tiles)]
    tri_up = jnp.where(square_rows < square_cols, 1.0, 0.0).astype(bf16)
    ranks = jnp.dot(rows_of(mask, ND // 2, LANES), tri_up, preferred_element_type=f32)
    before = jnp.zeros((1, 1), f32)
    for i in range(cell_tiles):
        place_ref[0:1, i * LANES : (i + 1) * LANES] = jnp.where(
            mask[i] > 0.0, ranks[i : i + 1] + before, LAND
        )
        before = before + jnp.sum(mask[i], axis=1, keepdims=True)
    pair_rows = lax.broadcasted_iota(jnp.int32, (WIDE, reach), 0).astype(f32)

    def build(pair):
        cols = pl.ds(pl.multiple_of(pair * WIDE, LANES), reach)
        first = (pair * WIDE).astype(f32)
        hit = jnp.where(place_ref[0:1, cols] - first == pair_rows, 1.0, 0.0)
        spread_ref[pl.ds(pl.multiple_of(pair * WIDE, LANES), WIDE), cols] = hit.astype(bf16)

    def packed(values, pair):
        cols = pl.ds(pl.multiple_of(pair * WIDE, LANES), reach)
        return lax.dot_general(
            values[:, cols],
            spread_ref[pl.ds(pl.multiple_of(pair * WIDE, LANES), WIDE), cols],
            (((1,), (1,)), ((), ())), preferred_element_type=f32,
        )

    quarter = ND // 4
    tiles = NLON // LANES
    def advect(f):
        loads[f].wait()
        freq = (me * freq_dev + f).astype(f32)
        speed = 0.2 * jnp.exp(jnp.full((quarter, LANES), -log_step, f32) * freq)
        for q in range(4):
            east, north = q in (0, 3), q in (0, 1)
            rows = slice(f * ND + q * quarter, f * ND + (q + 1) * quarter)
            part = slice(q * quarter, (q + 1) * quarter)
            cx0 = speed * jnp.abs(cos_h[part])
            cy = jnp.concatenate([speed * jnp.abs(sin_h[part])] * tiles, axis=1)
            cx = [jnp.concatenate([cx0 * (1.0 / math.cos(a))] * tiles, axis=1) for a in lats]
            energy = [raw[rows, r * NLON : (r + 1) * NLON] * sea[r] for r in range(lat_count)]
            for _ in range(ADV_STEPS):
                fresh = []
                for r in range(lat_count):
                    e = energy[r]
                    side_x = pltpu.roll(e, 1 if east else NLON - 1, 1)
                    other = r - 1 if north else r + 1
                    side_y = energy[other] if 0 <= other < lat_count else 0.0
                    fresh.append((e - cx[r] * (e - side_x) - cy * (e - side_y)) * sea[r])
                energy = fresh
            for r in range(lat_count):
                moved[rows, r * NLON : (r + 1) * NLON] = energy[r]
        for i, piece in enumerate(split_bf16(moved[f * ND : (f + 1) * ND])):
            split[(3 * f + i) * ND : (3 * f + i + 1) * ND, :] = piece

    def cols_of(index):
        return pl.ds(pl.multiple_of(index * LANES, LANES), LANES)

    def side_of(dy):
        return (side + dy) % sides

    def pack(t, dy, begin, end):
        pair = t * sides + side_of(dy)
        got = packed(split.at[begin * 3 * ND : end * 3 * ND], pair)
        cols = pl.ds(pl.multiple_of(pair * WIDE, LANES), WIDE)
        here = pl.ds(pl.multiple_of(side_of(dy) * WIDE, LANES), WIDE)
        mass, moment = None, None
        for f in range(begin, end):
            base = (f - begin) * 3 * ND
            piece = got[base : base + ND] + got[base + ND : base + 2 * ND] + (
                got[base + 2 * ND : base + 3 * ND]
            )
            adv[f, :, cols] = piece
            total = jnp.sum(piece, axis=0, keepdims=True)
            scaled = omega_of(me * freq_dev + f, (1, WIDE)) * total
            mass = total if mass is None else mass + total
            moment = scaled if moment is None else moment + scaled
        if begin:
            mass, moment = mass + mom_out[t, 0:1, here], moment + mom_out[t, 1:2, here]
        mom_out[t, 0:1, here] = mass
        mom_out[t, 1:2, here] = moment

    def send_far(t, dy, begin, end):
        for c in range(2):
            for f in range(begin, end):
                y_copy(f, side_of(dy) * 2 + c, t).start()

    def up_copy(slot, t):
        return remote(
            held.at[HALO + slot, :, lanes_of(t)],
            held.at[HALO + slot - freq_group, :, lanes_of(t)],
            z_sem.at[0], halo_sem.at[0, t], (zone + 1) % zones * group + rank,
        )

    def down_copy(slot, t):
        return remote(
            held.at[HALO + slot, :, lanes_of(t)],
            held.at[HALO + slot + freq_group, :, lanes_of(t)],
            z_sem.at[1], halo_sem.at[1, t], (zone + zones - 1) % zones * group + rank,
        )

    def early_up(f, c, t):
        slot = rank * freq_dev + f
        return remote(
            adv.at[f, :, tile_of(side * 2 + c, t)],
            held.at[HALO + slot - freq_group, :, lanes_of(t)],
            z_sem.at[0], halo_sem.at[0, t], (zone + 1) % zones * group + side * 2 + c,
        )

    def early_down(f, c, t):
        slot = rank * freq_dev + f
        return remote(
            adv.at[f, :, tile_of(side * 2 + c, t)],
            held.at[HALO + slot + freq_group, :, lanes_of(t)],
            z_sem.at[1], halo_sem.at[1, t], (zone + zones - 1) % zones * group + side * 2 + c,
        )

    def goes_up(slot):
        return (slot >= freq_group - HALO) & (zone < zones - 1)

    def goes_down(slot):
        return (slot < HALO) & (zone > 0)

    def forward(slot, t):
        @pl.when(goes_up(slot))
        def _():
            up_copy(slot, t).start()

        @pl.when(goes_down(slot))
        def _():
            down_copy(slot, t).start()

    def send_near(t):
        for f in range(freq_dev):
            y_copy(f, rank_of((0, 1)), t).start()
        for f in range(freq_dev):
            @pl.when(goes_up(rank * freq_dev + f))
            def _():
                for c in range(2):
                    early_up(f, c, t).start()

            @pl.when(goes_down(rank * freq_dev + f))
            def _():
                for c in range(2):
                    early_down(f, c, t).start()

        for f in range(freq_dev):
            held[HALO + rank * freq_dev + f, :, lanes_of(t)] = adv[f, :, tile_of(rank, t)]

    def arrive_group(dy, t):
        for f in range(freq_dev):
            for dc in range(2):
                if (dy, dc) != (0, 0):
                    source = rank_of((dy, dc))
                    slot = source * freq_dev + f
                    block = held.at[HALO + slot, :, lanes_of(t)]
                    remote(
                        block, block, y_sem, held_sem.at[source, f, t], (me + 1) % count
                    ).wait_recv()
                    if dy:
                        forward(slot, t)

    far = list(range(1, sides))
    for dy in far:
        build(side_of(dy))
    advect(0)
    for dy in far:
        pack(0, dy, 0, 1)
    advect(1)
    pl.semaphore_wait(
        barrier, group - 1 + jnp.where(zone > 0, 2, 0) + jnp.where(zone < zones - 1, 2, 0)
    )
    for dy in far:
        send_far(0, dy, 0, 1)

    @pl.when(zone == 0)
    def _():
        signal(chain_sem.at[0], (me + group) % count)

    @pl.when(zone == zones - 1)
    def _():
        signal(chain_sem.at[1], (me + count - group) % count)

    for f in range(2, freq_dev):
        advect(f)
    for dy in far:
        pack(0, dy, 1, freq_dev)
        send_far(0, dy, 1, freq_dev)
    build(side)
    pack(0, 0, 0, freq_dev)
    send_near(0)
    for t in range(1, parts):
        for dy in far:
            build(t * sides + side_of(dy))
            pack(t, dy, 0, freq_dev)
            send_far(t, dy, 0, freq_dev)
        build(t * sides + side)
        pack(t, 0, 0, freq_dev)
        send_near(t)

    def relay(level):
        @pl.when(zone == level)
        def _():
            pl.semaphore_wait(chain_sem.at[0], 1)

            @pl.when(zone < zones - 1)
            def _():
                signal(chain_sem.at[0], (me + group) % count)

        @pl.when(zone == zones - 1 - level)
        def _():
            pl.semaphore_wait(chain_sem.at[1], 1)

            @pl.when(zone > 0)
            def _():
                signal(chain_sem.at[1], (me + count - group) % count)

    relay(1)
    small[1].wait()
    small[2].wait()
    speed_all = wind_raw[...].reshape(1, cells)
    angle_all = angle_raw[...].reshape(1, cells)
    wsplit[...] = rows_of(
        split_bf16(speed_all * jnp.cos(angle_all)) + split_bf16(speed_all * jnp.sin(angle_all)),
        2 * quarter, cells,
    )
    for t in range(parts):
        own = packed(wsplit, t * sides + side)
        own = jnp.where(core == 0, own[:, :LANES], own[:, LANES:])
        along = own[0:1] + own[1:2] + own[2:3]
        across = own[3:4] + own[4:5] + own[5:6]
        wind[:, t * LANES : (t + 1) * LANES] = cos_h * along + sin_h * across

    for t in range(parts):
        arrive_group(0, t)
    for level in range(2, zones):
        relay(level)
    for step in range(1, count):
        target = (me + step) % count
        remote(
            mom_out.at[:, :, cols_of(target % group)], mom_in.at[me],
            mom_send, mom_recv, target,
        ).start()
    mom_in[me] = mom_out[:, :, cols_of(rank)]
    start = window_start(count, me, cells)
    near_ref[...] = place_ref[0:1, pl.ds(pl.multiple_of(start, LANES), WIDE)]
    for dy in far:
        arrive_group(dy, 0)

    acc[...] = jnp.zeros_like(acc)
    ascending = side > 0

    def arrive_halo(at_top, t):
        block = held.at[0:HALO, :, lanes_of(t)]

        @pl.when(jnp.where(at_top, zone < zones - 1, zone > 0))
        def _():
            way = jnp.where(at_top, 1, 0)
            remote(
                block, block, z_sem.at[0], halo_sem.at[way, t], (me + 1) % count
            ).wait_recv()

    def ret_copy(owner, t):
        return remote(
            done.at[pl.ds(owner * freq_dev, freq_dev), :, lanes_of(t)],
            back.at[:, :, tile_of(rank, t)],
            ret_send, ret_recv.at[t], zone * group + owner,
        )

    def sources(t, begin, end):
        lanes = slice(t * LANES, (t + 1) * LANES)

        def source_step(i, carry):
            k = jnp.where(ascending, i, freq_group - 1 - i)
            freq = zone * freq_group + k

            def scale(index, factor):
                return jnp.where((index >= 3) & (index <= NF - 3), factor, 0.0).astype(f32)

            w_own = scale(freq, -0.002)
            w_low, w_high = scale(freq - 2, 0.001), scale(freq + 3, 0.001)
            omega = omega_of(freq, (1, LANES))

            def slab(shift):
                return held[HALO + k + shift, :, lanes]

            def turn(values, amount):
                return pltpu.roll(values, amount % ND, 0)

            def rate(a, p, m):
                return a * (a * (p + m) - 2.0 * (p * m))

            own = slab(0)
            p2, m3, m2, m5, p3, p5 = (slab(shift) for shift in (2, -3, -2, -5, 3, 5))
            near = rate(own, turn(p2, -1), turn(m3, 3)) + rate(own, turn(p2, 1), turn(m3, -3))
            low = rate(turn(m2, 1), own, turn(m5, 4)) + rate(turn(m2, -1), own, turn(m5, -4))
            high = rate(turn(p3, -3), turn(p5, -4), own) + rate(turn(p3, 3), turn(p5, 4), own)
            interaction = w_own * near + w_low * low + w_high * high
            gain = (0.05 * omega) * jnp.maximum(0.0, wind[:, lanes] * omega - 1.0)
            fresh = own + gain * own + interaction
            done[k, :, lanes] = fresh
            acc[:, lanes] += fresh
            return carry

        lax.fori_loop(begin, end, source_step, 0)

    half = freq_group // 2
    near_side = rank_of((0, 1))

    def first_half(t):
        arrive_halo(jnp.logical_not(ascending), t)
        sources(t, 0, half)
        for dy in range(1, sides):
            for dc in range(2):
                ret_copy(rank_of((dy, dc)), t).start()

    def second_half(t):
        arrive_halo(ascending, t)
        sources(t, half, freq_group)
        ret_copy(near_side, t).start()
        back[:, :, tile_of(rank, t)] = done[
            pl.ds(rank * freq_dev, freq_dev), :, lanes_of(t)
        ]

    def zone_copy(dst_rank, src, dst, send, recv):
        return remote(src, dst, send, recv, zone * group + dst_rank)

    def damping_terms():
        others = mom_in.at[0 : count - 1]
        remote(others, others, mom_send, mom_recv, (me + 1) % count).wait_recv()
        total = jnp.sum(mom_in[...], axis=0) * (1.0 / (NF * ND))
        for t in range(parts):
            energy_mean, moment_one = total[t, 0:1], total[t, 1:2]
            mean_freq = moment_one / (energy_mean + 1e-06)
            steepness = energy_mean * mean_freq * mean_freq
            breaking = steepness * steepness / (1.0 + steepness * steepness)
            damp_out[t, 0:1] = 0.03 * breaking
            damp_out[t, 1:2] = 0.03 * breaking * moment_one
        for i in range(1, group):
            zone_copy(
                rank_of(offsets[i]), damp_out, damp_in.at[rank], damp_send, damp_recv
            ).start()
        damp_in[rank] = damp_out[...]

    first_half(0)
    for t in range(1, parts):
        for dy in range(1, sides):
            arrive_group(dy, t)
        first_half(t)
        second_half(t - 1)
    second_half(parts - 1)

    sum_out[...] = jnp.sum(acc[...], axis=0, keepdims=True)
    for step in range(1, count):
        remote(sum_out, sum_in.at[me], sum_send, sum_recv, (me + step) % count).start()
    sum_in[me] = sum_out[...]
    damping_terms()

    others = damp_in.at[0 : group - 1]
    remote(others, others, damp_send, damp_recv, (me + 1) % count).wait_recv()
    for t in range(parts):
        block = done.at[0 : (group - 1) * freq_dev, :, lanes_of(t)]
        remote(block, block, ret_send, ret_recv.at[t], (me + 1) % count).wait_recv()
    for f in range(freq_dev):
        omega = omega_of(me * freq_dev + f, (1, LANES))
        for t in range(parts):
            for g in range(group):
                cols = slice(block_of(g, t) * LANES, (block_of(g, t) + 1) * LANES)
                value = back[f, :, cols] - (omega * damp_in[g, t, 0:1]) * adv[f, :, cols]
                for i, piece in enumerate(split_bf16(value)):
                    split[(3 * f + i) * ND : (3 * f + i + 1) * ND, cols] = piece
    for j in range(cells // WIDE):
        low, high = max(0, j * WIDE - land), min(sea_cells, (j + 1) * WIDE)
        cols = slice(j * WIDE, (j + 1) * WIDE)
        got = jnp.dot(
            split[:, low:high], spread_ref[low:high, cols], preferred_element_type=f32
        )
        for f in range(freq_dev):
            base = 3 * f * ND
            full_ref[f * ND : (f + 1) * ND, cols] = got[base : base + ND] + (
                got[base + ND : base + 2 * ND]
            ) + got[base + 2 * ND : base + 3 * ND]

    block = held.at[0 : (group - 1) * freq_dev]
    remote(block, block, y_sem, held_sem.at[0, 0, 0], (me + 1) % count).wait_send()
    remote(block, block, ret_send, ret_recv.at[0], (me + 1) % count).wait_send()
    others = mom_in.at[0 : count - 1]
    remote(others, others, mom_send, mom_recv, (me + 1) % count).wait_send()
    others = damp_in.at[0 : group - 1]
    remote(others, others, damp_send, damp_recv, (me + 1) % count).wait_send()
    def drain(slots, way):
        block = held.at[0:slots]
        remote(
            block, block, z_sem.at[way], halo_sem.at[0, 0], (me + 1) % count
        ).wait_send()

    for f in range(freq_dev):
        @pl.when(goes_up(rank * freq_dev + f))
        def _():
            drain(2, 0)

        @pl.when(goes_down(rank * freq_dev + f))
        def _():
            drain(2, 1)

    for dy in far:
        for c in range(2):
            for f in range(freq_dev):
                slot = (side_of(dy) * 2 + c) * freq_dev + f

                @pl.when(goes_up(slot))
                def _():
                    drain(1, 0)

                @pl.when(goes_down(slot))
                def _():
                    drain(1, 1)

    others = sum_in.at[0 : count - 1]
    remote(others, others, sum_send, sum_recv, (me + 1) % count).wait()
    for g in range(group):
        mass = sum_in[g]
        for other in range(1, zones):
            mass = mass + sum_in[other * group + g]
        for t in range(parts):
            mean = mass[:, t * LANES : (t + 1) * LANES] * (1.0 / (NF * ND)) - damp_in[g, t, 1:2]
            cols = slice(block_of(g, t) * LANES, (block_of(g, t) + 1) * LANES)
            height_ref[0:1, cols] = 4.0 * jnp.sqrt(mean + 1e-06)


def store_kernel(
    count, full_in, height_in, near_in, new_out, wave_out, mean_out, wave_ref, mean_ref, sem
):
    cells = full_in.shape[1]
    sea_cells = height_in.shape[1]
    copies = [
        pltpu.make_async_copy(full_in, new_out, sem.at[0]),
        pltpu.make_async_copy(wave_ref, wave_out, sem.at[1]),
        pltpu.make_async_copy(mean_ref, mean_out, sem.at[2]),
    ]
    copies[0].start()
    me = lax.axis_index("spec")
    points = cells // count
    shift = me * points - window_start(count, me, cells)
    halves = []
    for h in range(WIDE // LANES):
        place = jnp.broadcast_to(near_in[:, h * LANES : (h + 1) * LANES], (8, LANES))
        place = place.astype(jnp.int32)
        wave = jnp.zeros((8, LANES), jnp.float32)
        for b in range(sea_cells // LANES):
            values = jnp.broadcast_to(height_in[:, b * LANES : (b + 1) * LANES], (8, LANES))
            found = jnp.take_along_axis(values, place % LANES, axis=1)
            wave = jnp.where(place // LANES == b, found, wave)
        halves.append(wave)
    wave = jnp.concatenate(halves, axis=1)
    wave_ref[...] = pltpu.roll(wave, (WIDE - shift) % WIDE, 1)[0, :points]
    copies[1].start()
    mean_ref[...] = jnp.sum(height_in[...], axis=1, keepdims=True) * (1.0 / sea_cells)
    copies[2].start()
    for copy in copies:
        copy.wait()


def fused_local(spectrum, sea_mask, wind_speed, wind_angle):
    count = lax.axis_size("spec")
    bins_dev, cells = spectrum.shape
    group = group_size(count, bins_dev, cells)
    freq_dev = bins_dev // ND
    freq_group = freq_dev * group
    sea_cells = SEA_DEV * count
    width = sea_cells // group
    points = cells // count
    parts = width // LANES
    f32, bf16 = jnp.float32, jnp.bfloat16
    dma = pltpu.SemaphoreType.DMA
    vmem = pl.BlockSpec(memory_space=pltpu.VMEM)
    handed = pl.pallas_call(
        functools.partial(fused_kernel, count, group),
        out_shape=(
            pltpu.VMEM((bins_dev, cells), f32),
            pltpu.VMEM((1, sea_cells), f32),
            pltpu.VMEM((1, WIDE), f32),
        ),
        in_specs=[pl.BlockSpec(memory_space=pl.ANY)] * 4,
        out_specs=(vmem,) * 3,
        scratch_shapes=[
            pltpu.VMEM((cells,), jnp.int32),
            pltpu.VMEM((cells,), f32),
            pltpu.VMEM((cells,), f32),
            pltpu.VMEM((1, cells), f32),
            pltpu.VMEM((1, cells), f32),
            pltpu.VMEM((sea_cells, cells), bf16),
            dma((3,)),
            pltpu.VMEM((bins_dev, cells), f32),
            pltpu.VMEM((bins_dev, cells), f32),
            pltpu.VMEM((3 * bins_dev, cells), bf16),
            pltpu.VMEM((ND // 2, cells), bf16),
            pltpu.VMEM((freq_dev, ND, sea_cells), f32),
            pltpu.VMEM((freq_group + 2 * HALO, ND, width), f32),
            pltpu.VMEM((freq_group, ND, width), f32),
            pltpu.VMEM((freq_dev, ND, sea_cells), f32),
            pltpu.VMEM((parts, 2, group * LANES), f32),
            pltpu.VMEM((count, parts, 2, LANES), f32),
            pltpu.VMEM((ND, width), f32),
            pltpu.VMEM((ND, width), f32),
            pltpu.VMEM((1, width), f32),
            pltpu.VMEM((count, 1, width), f32),
            pltpu.VMEM((parts, 2, LANES), f32),
            pltpu.VMEM((group, parts, 2, LANES), f32),
            dma((freq_dev,)),
            dma((group, freq_dev, parts)),
            dma((2, parts)),
            dma,
            dma((2,)),
            pltpu.SemaphoreType.REGULAR((2,)),
            dma,
            dma,
            dma,
            dma((parts,)),
            dma,
            dma,
            dma,
            dma,
        ],
        compiler_params=pltpu.CompilerParams(collective_id=0, has_side_effects=True),
    )(sea_mask, wind_speed, wind_angle, spectrum)
    out, wave, mean = pl.pallas_call(
        functools.partial(store_kernel, count),
        out_shape=(
            pltpu.HBM((bins_dev, cells), f32),
            pltpu.HBM((points,), f32),
            pltpu.HBM((1, 1), f32),
        ),
        in_specs=[vmem] * 3,
        out_specs=(pl.BlockSpec(memory_space=pltpu.HBM),) * 3,
        scratch_shapes=[pltpu.VMEM((points,), f32), pltpu.VMEM((1, 1), f32), dma((3,))],
    )(*[pltpu.with_memory_space_constraint(piece, pltpu.VMEM) for piece in handed])
    return (out, wave, mean.reshape(1))


def solution(mesh):
    in_specs = (P(("grp", "spec"), None), P(), P("grp"), P("grp"))
    out_specs = (P(("grp", "spec"), None), P(("grp", "spec")), P("grp"))

    def body(spectrum, sea_mask, wind_speed, wind_angle):
        fits = group_size(mesh.shape["spec"], *spectrum.shape)
        plan = fused_local if fits else local
        return plan(spectrum, sea_mask, wind_speed, wind_angle)

    return jax.shard_map(body, mesh=mesh, in_specs=in_specs, out_specs=out_specs, check_vma=False)
```

```python
import functools
import math

import jax
import jax.numpy as jnp
from jax import lax
from jax.experimental import pallas as pl
from jax.experimental.pallas import tpu as pltpu
from jax.sharding import PartitionSpec as P

NF = 48
ND = 32
NLON = 384
ADV_STEPS = 2
SEA_DEV = 64


def upwind_step(energy, courant_x, courant_y, sea_grid):
    west_cell = jnp.roll(energy, 1, axis=2)
    east_cell = jnp.roll(energy, -1, axis=2)
    edge_row = jnp.zeros_like(energy[:, :1])
    south_cell = jnp.concatenate([edge_row, energy[:, :-1]], axis=1)
    north_cell = jnp.concatenate([energy[:, 1:], edge_row], axis=1)
    updated = (
        energy
        - jnp.maximum(courant_x, 0.0) * (energy - west_cell)
        - jnp.minimum(courant_x, 0.0) * (east_cell - energy)
        - jnp.maximum(courant_y, 0.0) * (energy - south_cell)
        - jnp.minimum(courant_y, 0.0) * (north_cell - energy)
    )
    return updated * sea_grid


def courant_numbers(freq_index, dir_index, lat_count, dir_count):
    speed = 0.2 * jnp.exp(-math.log(1.1) * freq_index)
    heading = 2.0 * math.pi * (dir_index + 0.5) / dir_count
    rows = jnp.arange(lat_count, dtype=jnp.float32)
    latitude = (-75.0 + 150.0 * (rows + 0.5) / lat_count) * (math.pi / 180.0)
    courant_x = (speed * jnp.cos(heading))[:, None, None] / jnp.cos(latitude)[None, :, None]
    courant_y = (speed * jnp.sin(heading))[:, None, None]
    return (courant_x, courant_y)


def shift_freq(values, amount):
    if amount > 0:
        filler = jnp.zeros_like(values[:amount])
        return jnp.concatenate([filler, values[:-amount]], axis=0)
    filler = jnp.zeros_like(values[:-amount])
    return jnp.concatenate([values[-amount:], filler], axis=0)


def source_terms(energy, speed, angle):
    freq_count = energy.shape[0]
    dir_count = energy.shape[1]
    freq_ids = jnp.arange(freq_count, dtype=jnp.float32)
    frequency = jnp.exp(math.log(1.1) * (freq_ids - freq_count // 2))[:, None, None]
    heading = (2.0 * math.pi * (jnp.arange(dir_count, dtype=jnp.float32) + 0.5) / dir_count)[
        None, :, None
    ]
    energy_mean = jnp.mean(energy, axis=(0, 1))
    moment_one = jnp.mean(frequency * energy, axis=(0, 1))
    mean_freq = moment_one / (energy_mean + 1e-06)
    steepness = energy_mean * mean_freq * mean_freq
    breaking = steepness * steepness / (1.0 + steepness * steepness)
    wind_gain = (
        0.05
        * frequency
        * jnp.maximum(
            0.0, speed[None, None, :] * frequency * jnp.cos(heading - angle[None, None, :]) - 1.0
        )
    )
    damping = 0.03 * frequency * breaking[None, None, :]
    valid = ((freq_ids >= 3) & (freq_ids <= freq_count - 3)).astype(jnp.float32)[:, None, None]
    interaction = jnp.zeros_like(energy)
    for mirror in (1, -1):
        plus_bins = shift_freq(jnp.roll(energy, -mirror, axis=1), -2)
        minus_bins = shift_freq(jnp.roll(energy, 3 * mirror, axis=1), 3)
        transfer_rate = (
            0.001
            * valid
            * (energy * energy * (plus_bins + minus_bins) - 2.0 * energy * plus_bins * minus_bins)
        )
        interaction = interaction - 2.0 * transfer_rate
        interaction = interaction + jnp.roll(shift_freq(transfer_rate, 2), mirror, axis=1)
        interaction = interaction + jnp.roll(shift_freq(transfer_rate, -3), -3 * mirror, axis=1)
    updated = energy + (wind_gain - damping) * energy + interaction
    raw_height = 4.0 * jnp.sqrt(jnp.mean(updated, axis=(0, 1)) + 1e-06)
    return (updated, raw_height)


def local(spectrum, sea_mask, wind_speed, wind_angle):
    count = lax.axis_size("spec")
    position = lax.axis_index("spec")
    bins_dev = spectrum.shape[0]
    cells = spectrum.shape[1]
    points = cells // count
    lat_count = cells // NLON
    sea_float = sea_mask.astype(jnp.float32)
    bin_ids = position * bins_dev + jnp.arange(bins_dev, dtype=jnp.int32)
    freq_index = (bin_ids // ND).astype(jnp.float32)
    dir_index = (bin_ids % ND).astype(jnp.float32)
    courant_x, courant_y = courant_numbers(freq_index, dir_index, lat_count, ND)
    sea_grid = sea_float.reshape(1, lat_count, NLON)
    energy = (spectrum * sea_float[None, :]).reshape(bins_dev, lat_count, NLON)
    for substep in range(ADV_STEPS):
        energy = upwind_step(energy, courant_x, courant_y, sea_grid)
    advected = energy.reshape(bins_dev, cells)
    outgoing = advected.reshape(bins_dev, count, points)
    arrived = lax.all_to_all(outgoing, "spec", split_axis=1, concat_axis=0, tiled=True)
    start = position * points
    speed_own = lax.dynamic_slice_in_dim(wind_speed, start, points)
    angle_own = lax.dynamic_slice_in_dim(wind_angle, start, points)
    sea_own = lax.dynamic_slice_in_dim(sea_float, start, points)
    updated, raw_height = source_terms(arrived.reshape(NF, ND, points), speed_own, angle_own)
    wave_height = sea_own * raw_height
    own_total = jnp.zeros((count, 1), jnp.float32) + jnp.sum(wave_height)
    returned, totals = (
        lax.all_to_all(
            updated.reshape(NF * ND, 1, points), "spec", split_axis=0, concat_axis=1, tiled=True
        ),
        lax.all_to_all(own_total, "spec", split_axis=0, concat_axis=1, tiled=True),
    )
    new_spectrum = returned.reshape(bins_dev, cells)
    height_sum = jnp.sum(totals)
    mean_height = (height_sum / (SEA_DEV * count)).reshape(1)
    return (new_spectrum, wave_height, mean_height)


HALO = 5
LANES = 128
WIDE = 256
LAND = 4096.0


def group_size(count, bins_dev, cells):
    size = 4
    if count % size or bins_dev % ND or cells % (size * LANES) or cells % NLON:
        return 0
    if NLON % LANES or bins_dev // ND * size < 2 * HALO or cells % count:
        return 0
    sea = SEA_DEV * count
    if sea > min(cells, LAND) or sea % (size * LANES) or sea % WIDE or cells % WIDE:
        return 0
    if (cells - sea) % WIDE:
        return 0
    return size


def split_bf16(values):
    high = values.astype(jnp.bfloat16)
    left = values - high.astype(jnp.float32)
    mid = left.astype(jnp.bfloat16)
    low = (left - mid.astype(jnp.float32)).astype(jnp.bfloat16)
    return high, mid, low


def rows_of(parts, height, width):
    ids = lax.broadcasted_iota(jnp.int32, (height, width), 0)
    out = jnp.zeros((height, width), jnp.float32)
    for i, part in enumerate(parts):
        out = jnp.where(ids == i, jnp.broadcast_to(part.astype(jnp.float32), (height, width)), out)
    return out.astype(jnp.bfloat16)


def window_start(count, me, cells):
    return jnp.minimum(me * (cells // count) // LANES * LANES, cells - WIDE)


def fused_kernel(
    count, group, sea_in, wind_in, angle_in, spec_ref, full_ref, height_ref, near_ref,
    sea_raw, wind_raw, angle_raw, aux_ref, place_ref, spread_ref, aux_sem,
    raw, moved, split, wsplit, adv, held, done, back, mom_out, mom_in, wind, acc,
    sum_out, sum_in, damp_out, damp_in,
    load_sem, held_sem, halo_sem, y_sem, z_sem, chain_sem, mom_send, mom_recv,
    ret_send, ret_recv, sum_send, sum_recv, damp_send, damp_recv,
):
    f32, bf16 = jnp.float32, jnp.bfloat16
    freq_dev, _, sea_cells = adv.shape
    bins_dev, cells = moved.shape
    freq_group = freq_dev * group
    width = sea_cells // group
    zones = count // group
    lat_count = cells // NLON
    sides = group // 2
    parts = width // LANES
    cell_tiles = cells // LANES
    land = cells - sea_cells
    reach = land + WIDE
    me = lax.axis_index("spec")
    zone, rank = me // group, me % group
    side, core = rank // 2, rank % 2

    def remote(src, dst, send, recv, target):
        return pltpu.make_async_remote_copy(
            src_ref=src, dst_ref=dst, send_sem=send, recv_sem=recv,
            device_id={"spec": target}, device_id_type=pl.DeviceIdType.MESH,
        )

    loads = [
        pltpu.make_async_copy(
            spec_ref.at[pl.ds(f * ND, ND)], raw.at[pl.ds(f * ND, ND)], load_sem.at[f]
        )
        for f in range(freq_dev)
    ]
    small = [
        pltpu.make_async_copy(sea_in, sea_raw, aux_sem.at[0]),
        pltpu.make_async_copy(wind_in, wind_raw, aux_sem.at[1]),
        pltpu.make_async_copy(angle_in, angle_raw, aux_sem.at[2]),
    ]
    for load in small[:1] + loads + small[1:]:
        load.start()
    barrier = pltpu.get_barrier_semaphore()

    def signal(semaphore, target):
        pl.semaphore_signal(
            semaphore, inc=1, device_id={"spec": target}, device_id_type=pl.DeviceIdType.MESH
        )

    for step in range(1, group):
        signal(barrier, zone * group + (rank + step) % group)

    @pl.when(zone > 0)
    def _():
        for c in range(2):
            signal(barrier, (zone - 1) * group + side * 2 + c)

    @pl.when(zone < zones - 1)
    def _():
        for c in range(2):
            signal(barrier, (zone + 1) * group + side * 2 + c)

    @pl.when(zone == 0)
    def _():
        held[0:HALO] = jnp.zeros((HALO, ND, width), f32)

    @pl.when(zone == zones - 1)
    def _():
        held[HALO + freq_group :] = jnp.zeros((HALO, ND, width), f32)

    def block_of(index, t):
        return t * group + index

    def tile_of(index, t):
        return pl.ds(pl.multiple_of(block_of(index, t) * LANES, LANES), LANES)

    def lanes_of(t):
        return pl.ds(t * LANES, LANES)

    offsets = [(dy, dc) for dy in range(sides) for dc in range(2)]

    def rank_of(offset):
        return (side + offset[0]) % sides * 2 + (core + offset[1]) % 2

    def y_copy(f, peer, t):
        return remote(
            adv.at[f, :, tile_of(peer, t)],
            held.at[HALO + rank * freq_dev + f, :, lanes_of(t)],
            y_sem, held_sem.at[rank, f, t], zone * group + peer,
        )

    dirs = lax.broadcasted_iota(jnp.int32, (ND, LANES), 0).astype(f32)
    heading = 2.0 * math.pi * (dirs + 0.5) / ND
    cos_h, sin_h = jnp.cos(heading), jnp.sin(heading)
    log_step = math.log(1.1)
    lats = [math.radians(-75.0 + 150.0 * (r + 0.5) / lat_count) for r in range(lat_count)]

    def omega_of(freq, shape):
        return jnp.exp(jnp.full(shape, log_step, f32) * (freq.astype(f32) - NF // 2))

    square_rows = lax.broadcasted_iota(jnp.int32, (LANES, LANES), 0)
    square_cols = lax.broadcasted_iota(jnp.int32, (LANES, LANES), 1)
    small[0].wait()
    aux_ref[...] = sea_raw[...].astype(f32).reshape(1, cells)
    sea = [aux_ref[0:1, r * NLON : (r + 1) * NLON] for r in range(lat_count)]
    mask = [aux_ref[0:1, i * LANES : (i + 1) * LANES] for i in range(cell_tiles)]
    tri_up = jnp.where(square_rows < square_cols, 1.0, 0.0).astype(bf16)
    ranks = jnp.dot(rows_of(mask, ND // 2, LANES), tri_up, preferred_element_type=f32)
    before = jnp.zeros((1, 1), f32)
    for i in range(cell_tiles):
        place_ref[0:1, i * LANES : (i + 1) * LANES] = jnp.where(
            mask[i] > 0.0, ranks[i : i + 1] + before, LAND
        )
        before = before + jnp.sum(mask[i], axis=1, keepdims=True)
    pair_rows = lax.broadcasted_iota(jnp.int32, (WIDE, reach), 0).astype(f32)

    def build(pair):
        cols = pl.ds(pl.multiple_of(pair * WIDE, LANES), reach)
        first = (pair * WIDE).astype(f32)
        hit = jnp.where(place_ref[0:1, cols] - first == pair_rows, 1.0, 0.0)
        spread_ref[pl.ds(pl.multiple_of(pair * WIDE, LANES), WIDE), cols] = hit.astype(bf16)

    def packed(values, pair):
        cols = pl.ds(pl.multiple_of(pair * WIDE, LANES), reach)
        return lax.dot_general(
            values[:, cols],
            spread_ref[pl.ds(pl.multiple_of(pair * WIDE, LANES), WIDE), cols],
            (((1,), (1,)), ((), ())), preferred_element_type=f32,
        )

    quarter = ND // 4
    tiles = NLON // LANES
    def advect(f):
        loads[f].wait()
        freq = (me * freq_dev + f).astype(f32)
        speed = 0.2 * jnp.exp(jnp.full((quarter, LANES), -log_step, f32) * freq)
        for q in range(4):
            east, north = q in (0, 3), q in (0, 1)
            rows = slice(f * ND + q * quarter, f * ND + (q + 1) * quarter)
            part = slice(q * quarter, (q + 1) * quarter)
            cx0 = speed * jnp.abs(cos_h[part])
            cy = jnp.concatenate([speed * jnp.abs(sin_h[part])] * tiles, axis=1)
            cx = [jnp.concatenate([cx0 * (1.0 / math.cos(a))] * tiles, axis=1) for a in lats]
            energy = [raw[rows, r * NLON : (r + 1) * NLON] * sea[r] for r in range(lat_count)]
            for _ in range(ADV_STEPS):
                fresh = []
                for r in range(lat_count):
                    e = energy[r]
                    side_x = pltpu.roll(e, 1 if east else NLON - 1, 1)
                    other = r - 1 if north else r + 1
                    side_y = energy[other] if 0 <= other < lat_count else 0.0
                    fresh.append((e - cx[r] * (e - side_x) - cy * (e - side_y)) * sea[r])
                energy = fresh
            for r in range(lat_count):
                moved[rows, r * NLON : (r + 1) * NLON] = energy[r]
        for i, piece in enumerate(split_bf16(moved[f * ND : (f + 1) * ND])):
            split[(3 * f + i) * ND : (3 * f + i + 1) * ND, :] = piece

    def cols_of(index):
        return pl.ds(pl.multiple_of(index * LANES, LANES), LANES)

    def side_of(dy):
        return (side + dy) % sides

    def pack(t, dy, begin, end):
        pair = t * sides + side_of(dy)
        got = packed(split.at[begin * 3 * ND : end * 3 * ND], pair)
        cols = pl.ds(pl.multiple_of(pair * WIDE, LANES), WIDE)
        here = pl.ds(pl.multiple_of(side_of(dy) * WIDE, LANES), WIDE)
        mass, moment = None, None
        for f in range(begin, end):
            base = (f - begin) * 3 * ND
            piece = got[base : base + ND] + got[base + ND : base + 2 * ND] + (
                got[base + 2 * ND : base + 3 * ND]
            )
            adv[f, :, cols] = piece
            total = jnp.sum(piece, axis=0, keepdims=True)
            scaled = omega_of(me * freq_dev + f, (1, WIDE)) * total
            mass = total if mass is None else mass + total
            moment = scaled if moment is None else moment + scaled
        if begin:
            mass, moment = mass + mom_out[t, 0:1, here], moment + mom_out[t, 1:2, here]
        mom_out[t, 0:1, here] = mass
        mom_out[t, 1:2, here] = moment

    def send_far(t, dy, begin, end):
        for c in range(2):
            for f in range(begin, end):
                y_copy(f, side_of(dy) * 2 + c, t).start()

    def up_copy(slot, t):
        return remote(
            held.at[HALO + slot, :, lanes_of(t)],
            held.at[HALO + slot - freq_group, :, lanes_of(t)],
            z_sem.at[0], halo_sem.at[0, t], (zone + 1) % zones * group + rank,
        )

    def down_copy(slot, t):
        return remote(
            held.at[HALO + slot, :, lanes_of(t)],
            held.at[HALO + slot + freq_group, :, lanes_of(t)],
            z_sem.at[1], halo_sem.at[1, t], (zone + zones - 1) % zones * group + rank,
        )

    def early_up(f, c, t):
        slot = rank * freq_dev + f
        return remote(
            adv.at[f, :, tile_of(side * 2 + c, t)],
            held.at[HALO + slot - freq_group, :, lanes_of(t)],
            z_sem.at[0], halo_sem.at[0, t], (zone + 1) % zones * group + side * 2 + c,
        )

    def early_down(f, c, t):
        slot = rank * freq_dev + f
        return remote(
            adv.at[f, :, tile_of(side * 2 + c, t)],
            held.at[HALO + slot + freq_group, :, lanes_of(t)],
            z_sem.at[1], halo_sem.at[1, t], (zone + zones - 1) % zones * group + side * 2 + c,
        )

    def goes_up(slot):
        return (slot >= freq_group - HALO) & (zone < zones - 1)

    def goes_down(slot):
        return (slot < HALO) & (zone > 0)

    def forward(slot, t):
        @pl.when(goes_up(slot))
        def _():
            up_copy(slot, t).start()

        @pl.when(goes_down(slot))
        def _():
            down_copy(slot, t).start()

    def send_near(t):
        for c in range(2):
            for f in range(freq_dev):
                @pl.when(goes_up(rank * freq_dev + f))
                def _():
                    early_up(f, c, t).start()

                @pl.when(goes_down(rank * freq_dev + f))
                def _():
                    early_down(f, c, t).start()

        for f in range(freq_dev):
            y_copy(f, rank_of((0, 1)), t).start()
        for f in range(freq_dev):
            held[HALO + rank * freq_dev + f, :, lanes_of(t)] = adv[f, :, tile_of(rank, t)]

    def arrive_group(dy, t, begin, end):
        for f in range(begin, end):
            for dc in range(2):
                if (dy, dc) != (0, 0):
                    source = rank_of((dy, dc))
                    slot = source * freq_dev + f
                    block = held.at[HALO + slot, :, lanes_of(t)]
                    remote(
                        block, block, y_sem, held_sem.at[source, f, t], (me + 1) % count
                    ).wait_recv()
                    if dy:
                        forward(slot, t)

    def up_relay(level):
        @pl.when(zone == level)
        def _():
            pl.semaphore_wait(chain_sem.at[0], 1)
            if level < zones - 1:
                signal(chain_sem.at[0], (me + group) % count)

    def down_relay(level):
        @pl.when(zone == level)
        def _():
            pl.semaphore_wait(chain_sem.at[1], 1)
            if level > 0:
                signal(chain_sem.at[1], (me + count - group) % count)

    def send_moments():
        for step in range(1, count):
            target = (me + step) % count
            remote(
                mom_out.at[:, :, cols_of(target % group)], mom_in.at[me],
                mom_send, mom_recv, target,
            ).start()

    far = list(range(1, sides))
    for dy in far:
        build(side_of(dy))
    advect(0)
    for dy in far:
        pack(0, dy, 0, 1)
    advect(1)
    pl.semaphore_wait(
        barrier, group - 1 + jnp.where(zone > 0, 2, 0) + jnp.where(zone < zones - 1, 2, 0)
    )
    for dy in far:
        send_far(0, dy, 0, 1)

    @pl.when(zone == 0)
    def _():
        signal(chain_sem.at[0], (me + group) % count)

    @pl.when(zone == zones - 1)
    def _():
        signal(chain_sem.at[1], (me + count - group) % count)

    up_relay(1)
    for f in range(2, freq_dev):
        advect(f)
    for dy in far:
        pack(0, dy, 1, freq_dev)
        send_far(0, dy, 1, freq_dev)
    for level in range(2, zones - 1):
        up_relay(level)
    build(side)
    pack(0, 0, 0, freq_dev)
    send_near(0)
    for t in range(1, parts):
        for dy in far:
            build(t * sides + side_of(dy))
            pack(t, dy, 0, freq_dev)
            send_far(t, dy, 0, freq_dev)
        build(t * sides + side)
        pack(t, 0, 0, freq_dev)
        send_near(t)

    up_relay(zones - 1)
    down_relay(zones - 2)

    @pl.when(zone >= zones // 2)
    def _():
        send_moments()

    for dy in far:
        arrive_group(dy, 0, 0, 1)
    for level in range(zones - 3, 0, -1):
        down_relay(level)

    @pl.when((zone < zones // 2) & (zone > 0))
    def _():
        send_moments()

    small[1].wait()
    small[2].wait()
    speed_all = wind_raw[...].reshape(1, cells)
    angle_all = angle_raw[...].reshape(1, cells)
    wsplit[...] = rows_of(
        split_bf16(speed_all * jnp.cos(angle_all)) + split_bf16(speed_all * jnp.sin(angle_all)),
        2 * quarter, cells,
    )
    for t in range(parts):
        own = packed(wsplit, t * sides + side)
        own = jnp.where(core == 0, own[:, :LANES], own[:, LANES:])
        along = own[0:1] + own[1:2] + own[2:3]
        across = own[3:4] + own[4:5] + own[5:6]
        wind[:, t * LANES : (t + 1) * LANES] = cos_h * along + sin_h * across

    for dy in far:
        arrive_group(dy, 0, 1, freq_dev)
    down_relay(0)

    @pl.when(zone == 0)
    def _():
        send_moments()

    mom_in[me] = mom_out[:, :, cols_of(rank)]
    start = window_start(count, me, cells)
    near_ref[...] = place_ref[0:1, pl.ds(pl.multiple_of(start, LANES), WIDE)]
    for t in range(parts):
        arrive_group(0, t, 0, freq_dev)

    acc[...] = jnp.zeros_like(acc)
    ascending = side > 0

    def arrive_halo(at_top, t):
        block = held.at[0:HALO, :, lanes_of(t)]

        @pl.when(jnp.where(at_top, zone < zones - 1, zone > 0))
        def _():
            way = jnp.where(at_top, 1, 0)
            remote(
                block, block, z_sem.at[0], halo_sem.at[way, t], (me + 1) % count
            ).wait_recv()

    def ret_copy(owner, t):
        return remote(
            done.at[pl.ds(owner * freq_dev, freq_dev), :, lanes_of(t)],
            back.at[:, :, tile_of(rank, t)],
            ret_send, ret_recv.at[t], zone * group + owner,
        )

    def turn(values, amount):
        return pltpu.roll(values, amount % ND, 0)

    def rate(a, p, m):
        return a * (a * (p + m) - 2.0 * (p * m))

    def scale(index, factor):
        return jnp.where((index >= 3) & (index <= NF - 3), factor, 0.0).astype(f32)

    def slab(k, t):
        return held[HALO + k, :, t * LANES : (t + 1) * LANES]

    def rates(own, p2, m3):
        return rate(own, turn(p2, -1), turn(m3, 3)) + rate(own, turn(p2, 1), turn(m3, -3))

    def grown(own, freq, t):
        omega = omega_of(freq, (1, LANES))
        push = wind[:, t * LANES : (t + 1) * LANES] * omega - 1.0
        return own + (0.05 * omega) * jnp.maximum(0.0, push) * own

    def tally(energy, near, freq, t):
        flow = scale(freq, 0.001) * near
        acc[:, t * LANES : (t + 1) * LANES] += energy + (flow + flow - 2.0 * flow)

    def sources(t, begin, end):
        def source_step(i, carry):
            k = jnp.where(ascending, i, freq_group - 1 - i)
            freq = zone * freq_group + k
            own = slab(k, t)
            p2, m3, m2, m5, p3, p5 = (slab(k + shift, t) for shift in (2, -3, -2, -5, 3, 5))
            near = rates(own, p2, m3)
            low = rate(turn(m2, 1), own, turn(m5, 4)) + rate(turn(m2, -1), own, turn(m5, -4))
            high = rate(turn(p3, -3), turn(p5, -4), own) + rate(turn(p3, 3), turn(p5, 4), own)
            interaction = scale(freq, -0.002) * near + scale(freq - 2, 0.001) * low + (
                scale(freq + 3, 0.001) * high
            )
            energy = grown(own, freq, t)
            done[k, :, t * LANES : (t + 1) * LANES] = energy + interaction
            if begin == 0:
                tally(energy, near, freq, t)
            return carry

        lax.fori_loop(begin, end, source_step, 0)

    def tally_rest(t):
        def rest_step(i, carry):
            k = jnp.where(ascending, half + i, half - 1 - i)
            center = jnp.where(
                ascending,
                jnp.where(i < 2, i - 2, half + i - 2),
                jnp.where(i < 3, freq_group + i, half + 2 - i),
            )
            near = rates(slab(center, t), slab(center + 2, t), slab(center - 3, t))
            energy = grown(slab(k, t), zone * freq_group + k, t)
            tally(energy, near, zone * freq_group + center, t)
            return carry

        lax.fori_loop(0, half, rest_step, 0)

    half = freq_group // 2
    near_side = rank_of((0, 1))

    def first_half(t):
        arrive_halo(jnp.logical_not(ascending), t)
        sources(t, 0, half)
        if t == parts - 1:
            tally_rest(t)
            send_sums()
        for dy in range(1, sides):
            for dc in range(2):
                ret_copy(rank_of((dy, dc)), t).start()
        if t < parts - 1:
            tally_rest(t)

    def send_sums():
        sum_out[...] = jnp.sum(acc[...], axis=0, keepdims=True)
        for step in range(1, count):
            remote(sum_out, sum_in.at[me], sum_send, sum_recv, (me + step) % count).start()
        sum_in[me] = sum_out[...]

    def second_half(t):
        if t == parts - 1:
            damping_terms()
        arrive_halo(ascending, t)
        sources(t, half, freq_group)
        ret_copy(near_side, t).start()
        back[:, :, tile_of(rank, t)] = done[
            pl.ds(rank * freq_dev, freq_dev), :, lanes_of(t)
        ]

    def zone_copy(dst_rank, src, dst, send, recv):
        return remote(src, dst, send, recv, zone * group + dst_rank)

    def damping_terms():
        others = mom_in.at[0 : count - 1]
        remote(others, others, mom_send, mom_recv, (me + 1) % count).wait_recv()
        total = jnp.sum(mom_in[...], axis=0) * (1.0 / (NF * ND))
        for t in range(parts):
            energy_mean, moment_one = total[t, 0:1], total[t, 1:2]
            mean_freq = moment_one / (energy_mean + 1e-06)
            steepness = energy_mean * mean_freq * mean_freq
            breaking = steepness * steepness / (1.0 + steepness * steepness)
            damp_out[t, 0:1] = 0.03 * breaking
            damp_out[t, 1:2] = 0.03 * breaking * moment_one
        for i in range(1, group):
            zone_copy(
                rank_of(offsets[i]), damp_out, damp_in.at[rank], damp_send, damp_recv
            ).start()
        damp_in[rank] = damp_out[...]

    first_half(0)
    for t in range(1, parts):
        for dy in range(1, sides):
            arrive_group(dy, t, 0, freq_dev)
        first_half(t)
        second_half(t - 1)
    second_half(parts - 1)

    others = damp_in.at[0 : group - 1]
    remote(others, others, damp_send, damp_recv, (me + 1) % count).wait_recv()
    for t in range(parts):
        block = done.at[0 : (group - 1) * freq_dev, :, lanes_of(t)]
        remote(block, block, ret_send, ret_recv.at[t], (me + 1) % count).wait_recv()
    for f in range(freq_dev):
        omega = omega_of(me * freq_dev + f, (1, LANES))
        for t in range(parts):
            for g in range(group):
                cols = slice(block_of(g, t) * LANES, (block_of(g, t) + 1) * LANES)
                value = back[f, :, cols] - (omega * damp_in[g, t, 0:1]) * adv[f, :, cols]
                for i, piece in enumerate(split_bf16(value)):
                    split[(3 * f + i) * ND : (3 * f + i + 1) * ND, cols] = piece
    for j in range(cells // WIDE):
        low, high = max(0, j * WIDE - land), min(sea_cells, (j + 1) * WIDE)
        cols = slice(j * WIDE, (j + 1) * WIDE)
        got = jnp.dot(
            split[:, low:high], spread_ref[low:high, cols], preferred_element_type=f32
        )
        for f in range(freq_dev):
            base = 3 * f * ND
            full_ref[f * ND : (f + 1) * ND, cols] = got[base : base + ND] + (
                got[base + ND : base + 2 * ND]
            ) + got[base + 2 * ND : base + 3 * ND]

    block = held.at[0 : (group - 1) * freq_dev]
    remote(block, block, y_sem, held_sem.at[0, 0, 0], (me + 1) % count).wait_send()
    remote(block, block, ret_send, ret_recv.at[0], (me + 1) % count).wait_send()
    others = mom_in.at[0 : count - 1]
    remote(others, others, mom_send, mom_recv, (me + 1) % count).wait_send()
    others = damp_in.at[0 : group - 1]
    remote(others, others, damp_send, damp_recv, (me + 1) % count).wait_send()
    def drain(slots, way):
        block = held.at[0:slots]
        remote(
            block, block, z_sem.at[way], halo_sem.at[0, 0], (me + 1) % count
        ).wait_send()

    for f in range(freq_dev):
        @pl.when(goes_up(rank * freq_dev + f))
        def _():
            drain(2, 0)

        @pl.when(goes_down(rank * freq_dev + f))
        def _():
            drain(2, 1)

    for dy in far:
        for c in range(2):
            for f in range(freq_dev):
                slot = (side_of(dy) * 2 + c) * freq_dev + f

                @pl.when(goes_up(slot))
                def _():
                    drain(1, 0)

                @pl.when(goes_down(slot))
                def _():
                    drain(1, 1)

    others = sum_in.at[0 : count - 1]
    remote(others, others, sum_send, sum_recv, (me + 1) % count).wait()
    for g in range(group):
        mass = sum_in[g]
        for other in range(1, zones):
            mass = mass + sum_in[other * group + g]
        for t in range(parts):
            mean = mass[:, t * LANES : (t + 1) * LANES] * (1.0 / (NF * ND)) - damp_in[g, t, 1:2]
            cols = slice(block_of(g, t) * LANES, (block_of(g, t) + 1) * LANES)
            height_ref[0:1, cols] = 4.0 * jnp.sqrt(mean + 1e-06)


def store_kernel(
    count, full_in, height_in, near_in, new_out, wave_out, mean_out, wave_ref, mean_ref, sem
):
    cells = full_in.shape[1]
    sea_cells = height_in.shape[1]
    copies = [
        pltpu.make_async_copy(full_in, new_out, sem.at[0]),
        pltpu.make_async_copy(wave_ref, wave_out, sem.at[1]),
        pltpu.make_async_copy(mean_ref, mean_out, sem.at[2]),
    ]
    copies[0].start()
    me = lax.axis_index("spec")
    points = cells // count
    shift = me * points - window_start(count, me, cells)
    halves = []
    for h in range(WIDE // LANES):
        place = jnp.broadcast_to(near_in[:, h * LANES : (h + 1) * LANES], (8, LANES))
        place = place.astype(jnp.int32)
        wave = jnp.zeros((8, LANES), jnp.float32)
        for b in range(sea_cells // LANES):
            values = jnp.broadcast_to(height_in[:, b * LANES : (b + 1) * LANES], (8, LANES))
            found = jnp.take_along_axis(values, place % LANES, axis=1)
            wave = jnp.where(place // LANES == b, found, wave)
        halves.append(wave)
    wave = jnp.concatenate(halves, axis=1)
    wave_ref[...] = pltpu.roll(wave, (WIDE - shift) % WIDE, 1)[0, :points]
    copies[1].start()
    mean_ref[...] = jnp.sum(height_in[...], axis=1, keepdims=True) * (1.0 / sea_cells)
    copies[2].start()
    for copy in copies:
        copy.wait()


def fused_local(spectrum, sea_mask, wind_speed, wind_angle):
    count = lax.axis_size("spec")
    bins_dev, cells = spectrum.shape
    group = group_size(count, bins_dev, cells)
    freq_dev = bins_dev // ND
    freq_group = freq_dev * group
    sea_cells = SEA_DEV * count
    width = sea_cells // group
    points = cells // count
    parts = width // LANES
    f32, bf16 = jnp.float32, jnp.bfloat16
    dma = pltpu.SemaphoreType.DMA
    vmem = pl.BlockSpec(memory_space=pltpu.VMEM)
    handed = pl.pallas_call(
        functools.partial(fused_kernel, count, group),
        out_shape=(
            pltpu.VMEM((bins_dev, cells), f32),
            pltpu.VMEM((1, sea_cells), f32),
            pltpu.VMEM((1, WIDE), f32),
        ),
        in_specs=[pl.BlockSpec(memory_space=pl.ANY)] * 4,
        out_specs=(vmem,) * 3,
        scratch_shapes=[
            pltpu.VMEM((cells,), jnp.int32),
            pltpu.VMEM((cells,), f32),
            pltpu.VMEM((cells,), f32),
            pltpu.VMEM((1, cells), f32),
            pltpu.VMEM((1, cells), f32),
            pltpu.VMEM((sea_cells, cells), bf16),
            dma((3,)),
            pltpu.VMEM((bins_dev, cells), f32),
            pltpu.VMEM((bins_dev, cells), f32),
            pltpu.VMEM((3 * bins_dev, cells), bf16),
            pltpu.VMEM((ND // 2, cells), bf16),
            pltpu.VMEM((freq_dev, ND, sea_cells), f32),
            pltpu.VMEM((freq_group + 2 * HALO, ND, width), f32),
            pltpu.VMEM((freq_group, ND, width), f32),
            pltpu.VMEM((freq_dev, ND, sea_cells), f32),
            pltpu.VMEM((parts, 2, group * LANES), f32),
            pltpu.VMEM((count, parts, 2, LANES), f32),
            pltpu.VMEM((ND, width), f32),
            pltpu.VMEM((ND, width), f32),
            pltpu.VMEM((1, width), f32),
            pltpu.VMEM((count, 1, width), f32),
            pltpu.VMEM((parts, 2, LANES), f32),
            pltpu.VMEM((group, parts, 2, LANES), f32),
            dma((freq_dev,)),
            dma((group, freq_dev, parts)),
            dma((2, parts)),
            dma,
            dma((2,)),
            pltpu.SemaphoreType.REGULAR((2,)),
            dma,
            dma,
            dma,
            dma((parts,)),
            dma,
            dma,
            dma,
            dma,
        ],
        compiler_params=pltpu.CompilerParams(collective_id=0, has_side_effects=True),
    )(sea_mask, wind_speed, wind_angle, spectrum)
    out, wave, mean = pl.pallas_call(
        functools.partial(store_kernel, count),
        out_shape=(
            pltpu.HBM((bins_dev, cells), f32),
            pltpu.HBM((points,), f32),
            pltpu.HBM((1, 1), f32),
        ),
        in_specs=[vmem] * 3,
        out_specs=(pl.BlockSpec(memory_space=pltpu.HBM),) * 3,
        scratch_shapes=[pltpu.VMEM((points,), f32), pltpu.VMEM((1, 1), f32), dma((3,))],
    )(*[pltpu.with_memory_space_constraint(piece, pltpu.VMEM) for piece in handed])
    return (out, wave, mean.reshape(1))


def solution(mesh):
    in_specs = (P(("grp", "spec"), None), P(), P("grp"), P("grp"))
    out_specs = (P(("grp", "spec"), None), P(("grp", "spec")), P("grp"))

    def body(spectrum, sea_mask, wind_speed, wind_angle):
        fits = group_size(mesh.shape["spec"], *spectrum.shape)
        plan = fused_local if fits else local
        return plan(spectrum, sea_mask, wind_speed, wind_angle)

    return jax.shard_map(body, mesh=mesh, in_specs=in_specs, out_specs=out_specs, check_vma=False)
```

```python
import functools
import math

import jax
import jax.numpy as jnp
from jax import lax
from jax.experimental import pallas as pl
from jax.experimental.pallas import tpu as pltpu
from jax.sharding import PartitionSpec as P

NF = 48
ND = 32
NLON = 384
ADV_STEPS = 2
SEA_DEV = 64


def upwind_step(energy, courant_x, courant_y, sea_grid):
    west_cell = jnp.roll(energy, 1, axis=2)
    east_cell = jnp.roll(energy, -1, axis=2)
    edge_row = jnp.zeros_like(energy[:, :1])
    south_cell = jnp.concatenate([edge_row, energy[:, :-1]], axis=1)
    north_cell = jnp.concatenate([energy[:, 1:], edge_row], axis=1)
    updated = (
        energy
        - jnp.maximum(courant_x, 0.0) * (energy - west_cell)
        - jnp.minimum(courant_x, 0.0) * (east_cell - energy)
        - jnp.maximum(courant_y, 0.0) * (energy - south_cell)
        - jnp.minimum(courant_y, 0.0) * (north_cell - energy)
    )
    return updated * sea_grid


def courant_numbers(freq_index, dir_index, lat_count, dir_count):
    speed = 0.2 * jnp.exp(-math.log(1.1) * freq_index)
    heading = 2.0 * math.pi * (dir_index + 0.5) / dir_count
    rows = jnp.arange(lat_count, dtype=jnp.float32)
    latitude = (-75.0 + 150.0 * (rows + 0.5) / lat_count) * (math.pi / 180.0)
    courant_x = (speed * jnp.cos(heading))[:, None, None] / jnp.cos(latitude)[None, :, None]
    courant_y = (speed * jnp.sin(heading))[:, None, None]
    return (courant_x, courant_y)


def shift_freq(values, amount):
    if amount > 0:
        filler = jnp.zeros_like(values[:amount])
        return jnp.concatenate([filler, values[:-amount]], axis=0)
    filler = jnp.zeros_like(values[:-amount])
    return jnp.concatenate([values[-amount:], filler], axis=0)


def source_terms(energy, speed, angle):
    freq_count = energy.shape[0]
    dir_count = energy.shape[1]
    freq_ids = jnp.arange(freq_count, dtype=jnp.float32)
    frequency = jnp.exp(math.log(1.1) * (freq_ids - freq_count // 2))[:, None, None]
    heading = (2.0 * math.pi * (jnp.arange(dir_count, dtype=jnp.float32) + 0.5) / dir_count)[
        None, :, None
    ]
    energy_mean = jnp.mean(energy, axis=(0, 1))
    moment_one = jnp.mean(frequency * energy, axis=(0, 1))
    mean_freq = moment_one / (energy_mean + 1e-06)
    steepness = energy_mean * mean_freq * mean_freq
    breaking = steepness * steepness / (1.0 + steepness * steepness)
    wind_gain = (
        0.05
        * frequency
        * jnp.maximum(
            0.0, speed[None, None, :] * frequency * jnp.cos(heading - angle[None, None, :]) - 1.0
        )
    )
    damping = 0.03 * frequency * breaking[None, None, :]
    valid = ((freq_ids >= 3) & (freq_ids <= freq_count - 3)).astype(jnp.float32)[:, None, None]
    interaction = jnp.zeros_like(energy)
    for mirror in (1, -1):
        plus_bins = shift_freq(jnp.roll(energy, -mirror, axis=1), -2)
        minus_bins = shift_freq(jnp.roll(energy, 3 * mirror, axis=1), 3)
        transfer_rate = (
            0.001
            * valid
            * (energy * energy * (plus_bins + minus_bins) - 2.0 * energy * plus_bins * minus_bins)
        )
        interaction = interaction - 2.0 * transfer_rate
        interaction = interaction + jnp.roll(shift_freq(transfer_rate, 2), mirror, axis=1)
        interaction = interaction + jnp.roll(shift_freq(transfer_rate, -3), -3 * mirror, axis=1)
    updated = energy + (wind_gain - damping) * energy + interaction
    raw_height = 4.0 * jnp.sqrt(jnp.mean(updated, axis=(0, 1)) + 1e-06)
    return (updated, raw_height)


def local(spectrum, sea_mask, wind_speed, wind_angle):
    count = lax.axis_size("spec")
    position = lax.axis_index("spec")
    bins_dev = spectrum.shape[0]
    cells = spectrum.shape[1]
    points = cells // count
    lat_count = cells // NLON
    sea_float = sea_mask.astype(jnp.float32)
    bin_ids = position * bins_dev + jnp.arange(bins_dev, dtype=jnp.int32)
    freq_index = (bin_ids // ND).astype(jnp.float32)
    dir_index = (bin_ids % ND).astype(jnp.float32)
    courant_x, courant_y = courant_numbers(freq_index, dir_index, lat_count, ND)
    sea_grid = sea_float.reshape(1, lat_count, NLON)
    energy = (spectrum * sea_float[None, :]).reshape(bins_dev, lat_count, NLON)
    for substep in range(ADV_STEPS):
        energy = upwind_step(energy, courant_x, courant_y, sea_grid)
    advected = energy.reshape(bins_dev, cells)
    outgoing = advected.reshape(bins_dev, count, points)
    arrived = lax.all_to_all(outgoing, "spec", split_axis=1, concat_axis=0, tiled=True)
    start = position * points
    speed_own = lax.dynamic_slice_in_dim(wind_speed, start, points)
    angle_own = lax.dynamic_slice_in_dim(wind_angle, start, points)
    sea_own = lax.dynamic_slice_in_dim(sea_float, start, points)
    updated, raw_height = source_terms(arrived.reshape(NF, ND, points), speed_own, angle_own)
    wave_height = sea_own * raw_height
    own_total = jnp.zeros((count, 1), jnp.float32) + jnp.sum(wave_height)
    returned, totals = (
        lax.all_to_all(
            updated.reshape(NF * ND, 1, points), "spec", split_axis=0, concat_axis=1, tiled=True
        ),
        lax.all_to_all(own_total, "spec", split_axis=0, concat_axis=1, tiled=True),
    )
    new_spectrum = returned.reshape(bins_dev, cells)
    height_sum = jnp.sum(totals)
    mean_height = (height_sum / (SEA_DEV * count)).reshape(1)
    return (new_spectrum, wave_height, mean_height)


HALO = 5
LANES = 128
WIDE = 256
LAND = 4096.0


def group_size(count, bins_dev, cells):
    size = 4
    if count % size or bins_dev % ND or cells % (size * LANES) or cells % NLON:
        return 0
    if NLON % LANES or bins_dev // ND * size < 2 * HALO or cells % count:
        return 0
    sea = SEA_DEV * count
    if sea > min(cells, LAND) or sea % (size * LANES) or sea % WIDE or cells % WIDE:
        return 0
    if (cells - sea) % WIDE:
        return 0
    return size


def split_bf16(values):
    high = values.astype(jnp.bfloat16)
    left = values - high.astype(jnp.float32)
    mid = left.astype(jnp.bfloat16)
    low = (left - mid.astype(jnp.float32)).astype(jnp.bfloat16)
    return high, mid, low


def rows_of(parts, height, width):
    ids = lax.broadcasted_iota(jnp.int32, (height, width), 0)
    out = jnp.zeros((height, width), jnp.float32)
    for i, part in enumerate(parts):
        out = jnp.where(ids == i, jnp.broadcast_to(part.astype(jnp.float32), (height, width)), out)
    return out.astype(jnp.bfloat16)


def window_start(count, me, cells):
    return jnp.minimum(me * (cells // count) // LANES * LANES, cells - WIDE)


def fused_kernel(
    count, group, sea_in, wind_in, angle_in, spec_ref, full_ref, height_ref, near_ref,
    sea_raw, wind_raw, angle_raw, aux_ref, place_ref, spread_ref, aux_sem,
    raw, moved, split, wsplit, adv, held, done, back, mom_out, mom_in, wind, acc,
    sum_out, sum_in, damp_out, damp_in,
    load_sem, held_sem, halo_sem, y_sem, z_sem, chain_sem, mom_send, mom_recv,
    ret_send, ret_recv, sum_send, sum_recv, damp_send, damp_recv,
):
    f32, bf16 = jnp.float32, jnp.bfloat16
    freq_dev, _, sea_cells = adv.shape
    bins_dev, cells = moved.shape
    freq_group = freq_dev * group
    width = sea_cells // group
    zones = count // group
    lat_count = cells // NLON
    sides = group // 2
    parts = width // LANES
    cell_tiles = cells // LANES
    land = cells - sea_cells
    reach = land + WIDE
    me = lax.axis_index("spec")
    zone, rank = me // group, me % group
    side, core = rank // 2, rank % 2

    def remote(src, dst, send, recv, target):
        return pltpu.make_async_remote_copy(
            src_ref=src, dst_ref=dst, send_sem=send, recv_sem=recv,
            device_id={"spec": target}, device_id_type=pl.DeviceIdType.MESH,
        )

    loads = [
        pltpu.make_async_copy(
            spec_ref.at[pl.ds(f * ND, ND)], raw.at[pl.ds(f * ND, ND)], load_sem.at[f]
        )
        for f in range(freq_dev)
    ]
    small = [
        pltpu.make_async_copy(sea_in, sea_raw, aux_sem.at[0]),
        pltpu.make_async_copy(wind_in, wind_raw, aux_sem.at[1]),
        pltpu.make_async_copy(angle_in, angle_raw, aux_sem.at[2]),
    ]
    for load in small[:1] + loads + small[1:]:
        load.start()
    barrier = pltpu.get_barrier_semaphore()

    def signal(semaphore, target):
        pl.semaphore_signal(
            semaphore, inc=1, device_id={"spec": target}, device_id_type=pl.DeviceIdType.MESH
        )

    for step in range(1, group):
        signal(barrier, zone * group + (rank + step) % group)

    @pl.when(zone > 0)
    def _():
        for c in range(2):
            signal(barrier, (zone - 1) * group + side * 2 + c)

    @pl.when(zone < zones - 1)
    def _():
        for c in range(2):
            signal(barrier, (zone + 1) * group + side * 2 + c)

    @pl.when(zone == 0)
    def _():
        held[0:HALO] = jnp.zeros((HALO, ND, width), f32)

    @pl.when(zone == zones - 1)
    def _():
        held[HALO + freq_group :] = jnp.zeros((HALO, ND, width), f32)

    def block_of(index, t):
        return t * group + index

    def tile_of(index, t):
        return pl.ds(pl.multiple_of(block_of(index, t) * LANES, LANES), LANES)

    def lanes_of(t):
        return pl.ds(t * LANES, LANES)

    offsets = [(dy, dc) for dy in range(sides) for dc in range(2)]

    def rank_of(offset):
        return (side + offset[0]) % sides * 2 + (core + offset[1]) % 2

    def y_copy(f, peer, t):
        return remote(
            adv.at[f, :, tile_of(peer, t)],
            held.at[HALO + rank * freq_dev + f, :, lanes_of(t)],
            y_sem, held_sem.at[rank, f, t], zone * group + peer,
        )

    dirs = lax.broadcasted_iota(jnp.int32, (ND, LANES), 0).astype(f32)
    heading = 2.0 * math.pi * (dirs + 0.5) / ND
    cos_h, sin_h = jnp.cos(heading), jnp.sin(heading)
    log_step = math.log(1.1)
    lats = [math.radians(-75.0 + 150.0 * (r + 0.5) / lat_count) for r in range(lat_count)]

    def omega_of(freq, shape):
        return jnp.exp(jnp.full(shape, log_step, f32) * (freq.astype(f32) - NF // 2))

    square_rows = lax.broadcasted_iota(jnp.int32, (LANES, LANES), 0)
    square_cols = lax.broadcasted_iota(jnp.int32, (LANES, LANES), 1)
    small[0].wait()
    aux_ref[...] = sea_raw[...].astype(f32).reshape(1, cells)
    sea = [aux_ref[0:1, r * NLON : (r + 1) * NLON] for r in range(lat_count)]
    mask = [aux_ref[0:1, i * LANES : (i + 1) * LANES] for i in range(cell_tiles)]
    tri_up = jnp.where(square_rows < square_cols, 1.0, 0.0).astype(bf16)
    ranks = jnp.dot(rows_of(mask, ND // 2, LANES), tri_up, preferred_element_type=f32)
    before = jnp.zeros((1, 1), f32)
    for i in range(cell_tiles):
        place_ref[0:1, i * LANES : (i + 1) * LANES] = jnp.where(
            mask[i] > 0.0, ranks[i : i + 1] + before, LAND
        )
        before = before + jnp.sum(mask[i], axis=1, keepdims=True)
    pair_rows = lax.broadcasted_iota(jnp.int32, (WIDE, reach), 0).astype(f32)

    def build(pair):
        cols = pl.ds(pl.multiple_of(pair * WIDE, LANES), reach)
        first = (pair * WIDE).astype(f32)
        hit = jnp.where(place_ref[0:1, cols] - first == pair_rows, 1.0, 0.0)
        spread_ref[pl.ds(pl.multiple_of(pair * WIDE, LANES), WIDE), cols] = hit.astype(
            spread_ref.dtype
        )

    def packed(values, pair):
        cols = pl.ds(pl.multiple_of(pair * WIDE, LANES), reach)
        return lax.dot_general(
            values[:, cols],
            spread_ref[pl.ds(pl.multiple_of(pair * WIDE, LANES), WIDE), cols],
            (((1,), (1,)), ((), ())), preferred_element_type=f32,
        )

    quarter = ND // 4
    tiles = NLON // LANES
    def advect(f):
        loads[f].wait()
        freq = (me * freq_dev + f).astype(f32)
        speed = 0.2 * jnp.exp(jnp.full((quarter, LANES), -log_step, f32) * freq)
        for q in range(4):
            east, north = q in (0, 3), q in (0, 1)
            rows = slice(f * ND + q * quarter, f * ND + (q + 1) * quarter)
            part = slice(q * quarter, (q + 1) * quarter)
            cx0 = speed * jnp.abs(cos_h[part])
            cy = jnp.concatenate([speed * jnp.abs(sin_h[part])] * tiles, axis=1)
            cx = [jnp.concatenate([cx0 * (1.0 / math.cos(a))] * tiles, axis=1) for a in lats]
            rest = [1.0 - (cx[r] + cy) for r in range(lat_count)]
            energy = [raw[rows, r * NLON : (r + 1) * NLON] * sea[r] for r in range(lat_count)]
            for step in range(ADV_STEPS):
                fresh = []
                for r in range(lat_count):
                    e = energy[r]
                    side_x = pltpu.roll(e, 1 if east else NLON - 1, 1)
                    other = r - 1 if north else r + 1
                    value = rest[r] * e + cx[r] * side_x
                    if 0 <= other < lat_count:
                        value = value + cy * energy[other]
                    fresh.append(value if step == ADV_STEPS - 1 else value * sea[r])
                energy = fresh
            for r in range(lat_count):
                moved[rows, r * NLON : (r + 1) * NLON] = energy[r]
        for i, piece in enumerate(split_bf16(moved[f * ND : (f + 1) * ND])):
            split[(3 * f + i) * ND : (3 * f + i + 1) * ND, :] = piece

    def cols_of(index):
        return pl.ds(pl.multiple_of(index * LANES, LANES), LANES)

    def side_of(dy):
        return (side + dy) % sides

    def pack(t, dy, begin, end):
        pair = t * sides + side_of(dy)
        got = packed(split.at[begin * 3 * ND : end * 3 * ND], pair)
        cols = pl.ds(pl.multiple_of(pair * WIDE, LANES), WIDE)
        here = pl.ds(pl.multiple_of(side_of(dy) * WIDE, LANES), WIDE)
        mass, moment = None, None
        for f in range(begin, end):
            base = (f - begin) * 3 * ND
            piece = got[base : base + ND] + got[base + ND : base + 2 * ND] + (
                got[base + 2 * ND : base + 3 * ND]
            )
            adv[f, :, cols] = piece
            total = jnp.sum(piece, axis=0, keepdims=True)
            scaled = omega_of(me * freq_dev + f, (1, WIDE)) * total
            mass = total if mass is None else mass + total
            moment = scaled if moment is None else moment + scaled
        if begin:
            mass, moment = mass + mom_out[t, 0:1, here], moment + mom_out[t, 1:2, here]
        mom_out[t, 0:1, here] = mass
        mom_out[t, 1:2, here] = moment

    def send_far(t, dy, begin, end):
        for c in range(2):
            for f in range(begin, end):
                y_copy(f, side_of(dy) * 2 + c, t).start()

    top = side > 0
    early_way, late_way = jnp.where(top, 0, 1), jnp.where(top, 1, 0)
    early_ok = jnp.where(top, zone < zones - 1, zone > 0)
    late_ok = jnp.where(top, zone > 0, zone < zones - 1)
    early_zone = jnp.where(top, zone + 1, zone + zones - 1) % zones
    late_zone = jnp.where(top, zone + zones - 1, zone + 1) % zones
    early_shift = HALO + jnp.where(top, -freq_group, freq_group)
    late_shift = HALO + jnp.where(top, freq_group, -freq_group)

    def early_slot(slot):
        return early_ok & jnp.where(top, slot >= freq_group - HALO, slot < HALO)

    def late_slot(slot):
        return late_ok & jnp.where(top, slot < HALO, slot >= freq_group - HALO)

    def early_copy(f, c, t):
        return remote(
            adv.at[f, :, tile_of(side * 2 + c, t)],
            held.at[early_shift + rank * freq_dev + f, :, lanes_of(t)],
            z_sem.at[0], halo_sem.at[early_way, t], early_zone * group + side * 2 + c,
        )

    def forward(slot, t):
        @pl.when(late_slot(slot))
        def _():
            remote(
                held.at[HALO + slot, :, lanes_of(t)],
                held.at[late_shift + slot, :, lanes_of(t)],
                z_sem.at[1], halo_sem.at[late_way, t], late_zone * group + rank,
            ).start()

    def send_near(t):
        for c in range(2):
            for f in range(freq_dev):
                @pl.when(early_slot(rank * freq_dev + f))
                def _():
                    early_copy(f, c, t).start()

        for f in range(freq_dev):
            y_copy(f, rank_of((0, 1)), t).start()
        for f in range(freq_dev):
            held[HALO + rank * freq_dev + f, :, lanes_of(t)] = adv[f, :, tile_of(rank, t)]

    def arrive_group(dy, t, begin, end):
        for f in range(begin, end):
            for dc in range(2):
                if (dy, dc) != (0, 0):
                    source = rank_of((dy, dc))
                    slot = source * freq_dev + f
                    block = held.at[HALO + slot, :, lanes_of(t)]
                    remote(
                        block, block, y_sem, held_sem.at[source, f, t], (me + 1) % count
                    ).wait_recv()
                    if dy:
                        forward(slot, t)

    def up_relay(level):
        @pl.when(zone == level)
        def _():
            pl.semaphore_wait(chain_sem.at[0], 1)
            if level < zones - 1:
                signal(chain_sem.at[0], (me + group) % count)

    def down_relay(level):
        @pl.when(zone == level)
        def _():
            pl.semaphore_wait(chain_sem.at[1], 1)
            if level > 0:
                signal(chain_sem.at[1], (me + count - group) % count)

    def moment_copy(target_zone, target_rank):
        return remote(
            mom_out.at[:, :, cols_of(target_rank)], mom_in.at[me],
            mom_send, mom_recv, target_zone * group + target_rank,
        )

    def send_zone_moments():
        for step in range(1, group):
            moment_copy(zone, (rank + step) % group).start()

    def send_moments():
        for away in range(1, zones):
            for other in range(group):
                moment_copy((zone + away) % zones, other).start()

    far = list(range(1, sides))
    for dy in far:
        build(side_of(dy))
    advect(0)
    for dy in far:
        pack(0, dy, 0, 1)
    advect(1)
    pl.semaphore_wait(
        barrier, group - 1 + jnp.where(zone > 0, 2, 0) + jnp.where(zone < zones - 1, 2, 0)
    )
    for dy in far:
        send_far(0, dy, 0, 1)

    @pl.when(zone == 0)
    def _():
        signal(chain_sem.at[0], (me + group) % count)

    @pl.when(zone == zones - 1)
    def _():
        signal(chain_sem.at[1], (me + count - group) % count)

    up_relay(1)
    for f in range(2, freq_dev):
        advect(f)
    for dy in far:
        pack(0, dy, 1, freq_dev)
        send_far(0, dy, 1, freq_dev)
    for level in range(2, zones - 1):
        up_relay(level)
    build(side)
    pack(0, 0, 0, freq_dev)
    send_near(0)
    upper = zone >= zones // 2
    for t in range(1, parts):
        last = t == parts - 1
        for dy in far:
            build(t * sides + side_of(dy))
            pack(t, dy, 0, freq_dev)

            @pl.when(jnp.logical_not(upper) if last else zone >= 0)
            def _():
                send_far(t, dy, 0, freq_dev)
        build(t * sides + side)
        pack(t, 0, 0, freq_dev)
        if last:
            up_relay(zones - 1)
            down_relay(zones - 2)

            send_zone_moments()

            @pl.when(upper)
            def _():
                send_moments()
                for dy in far:
                    send_far(t, dy, 0, freq_dev)

        send_near(t)

    for dy in far:
        arrive_group(dy, 0, 0, 1)
    for level in range(zones - 3, 0, -1):
        down_relay(level)

    @pl.when(jnp.logical_not(upper) & (zone > 0))
    def _():
        send_moments()

    small[1].wait()
    small[2].wait()
    speed_all = wind_raw[...].reshape(1, cells)
    angle_all = angle_raw[...].reshape(1, cells)
    wsplit[...] = rows_of(
        split_bf16(speed_all * jnp.cos(angle_all)) + split_bf16(speed_all * jnp.sin(angle_all)),
        2 * quarter, cells,
    )
    for t in range(parts):
        own = packed(wsplit, t * sides + side)
        own = jnp.where(core == 0, own[:, :LANES], own[:, LANES:])
        along = own[0:1] + own[1:2] + own[2:3]
        across = own[3:4] + own[4:5] + own[5:6]
        wind[:, t * LANES : (t + 1) * LANES] = cos_h * along + sin_h * across

    for dy in far:
        arrive_group(dy, 0, 1, freq_dev)
    mom_in[me] = mom_out[:, :, cols_of(rank)]
    start = window_start(count, me, cells)
    near_ref[...] = place_ref[0:1, pl.ds(pl.multiple_of(start, LANES), WIDE)]
    for t in range(parts):
        arrive_group(0, t, 0, freq_dev)

    acc[...] = jnp.zeros_like(acc)
    ascending = side > 0

    def arrive_halo(at_top, t):
        block = held.at[0:HALO, :, lanes_of(t)]

        @pl.when(jnp.where(at_top, zone < zones - 1, zone > 0))
        def _():
            way = jnp.where(at_top, 1, 0)
            remote(
                block, block, z_sem.at[0], halo_sem.at[way, t], (me + 1) % count
            ).wait_recv()

    def ret_copy(owner, t):
        return remote(
            done.at[pl.ds(owner * freq_dev, freq_dev), :, lanes_of(t)],
            back.at[:, :, tile_of(rank, t)],
            ret_send, ret_recv.at[t], zone * group + owner,
        )

    def turn(values, amount):
        return pltpu.roll(values, amount % ND, 0)

    def rate(a, p, m):
        return a * (a * (p + m) - 2.0 * (p * m))

    def scale(index, factor):
        return jnp.where((index >= 3) & (index <= NF - 3), factor, 0.0).astype(f32)

    def slab(k, t):
        return held[HALO + k, :, t * LANES : (t + 1) * LANES]

    def rates(own, p2, m3):
        return rate(own, turn(p2, -1), turn(m3, 3)) + rate(own, turn(p2, 1), turn(m3, -3))

    def grown(own, freq, t):
        omega = omega_of(freq, (1, LANES))
        push = wind[:, t * LANES : (t + 1) * LANES] * omega - 1.0
        return own + (0.05 * omega) * jnp.maximum(0.0, push) * own

    def tally(energy, near, freq, t):
        flow = scale(freq, 0.001) * near
        acc[:, t * LANES : (t + 1) * LANES] += energy + (flow + flow - 2.0 * flow)

    def sources(t, begin, end):
        def source_step(i, carry):
            k = jnp.where(ascending, i, freq_group - 1 - i)
            freq = zone * freq_group + k
            own = slab(k, t)
            p2, m3, m2, m5, p3, p5 = (slab(k + shift, t) for shift in (2, -3, -2, -5, 3, 5))
            near = rates(own, p2, m3)
            low = rate(turn(m2, 1), own, turn(m5, 4)) + rate(turn(m2, -1), own, turn(m5, -4))
            high = rate(turn(p3, -3), turn(p5, -4), own) + rate(turn(p3, 3), turn(p5, 4), own)
            interaction = scale(freq, -0.002) * near + scale(freq - 2, 0.001) * low + (
                scale(freq + 3, 0.001) * high
            )
            energy = grown(own, freq, t)
            done[k, :, t * LANES : (t + 1) * LANES] = energy + interaction
            if begin == 0:
                tally(energy, near, freq, t)
            return carry

        lax.fori_loop(begin, end, source_step, 0)

    def tally_rest(t):
        def rest_step(i, carry):
            k = jnp.where(ascending, half + i, half - 1 - i)
            center = jnp.where(
                ascending,
                jnp.where(i < 2, i - 2, half + i - 2),
                jnp.where(i < 3, freq_group + i, half + 2 - i),
            )
            near = rates(slab(center, t), slab(center + 2, t), slab(center - 3, t))
            energy = grown(slab(k, t), zone * freq_group + k, t)
            tally(energy, near, zone * freq_group + center, t)
            return carry

        lax.fori_loop(0, half, rest_step, 0)

    half = freq_group // 2
    near_side = rank_of((0, 1))

    def first_half(t):
        arrive_halo(jnp.logical_not(ascending), t)
        sources(t, 0, half)
        if t == parts - 1:
            tally_rest(t)
            send_sums()
        for dy in range(1, sides):
            for dc in range(2):
                ret_copy(rank_of((dy, dc)), t).start()
        if t == 0:
            down_relay(0)

            @pl.when(zone == 0)
            def _():
                send_moments()

        if t < parts - 1:
            tally_rest(t)

    def send_sums():
        sum_out[...] = jnp.sum(acc[...], axis=0, keepdims=True)
        for step in range(1, count):
            remote(sum_out, sum_in.at[me], sum_send, sum_recv, (me + step) % count).start()
        sum_in[me] = sum_out[...]

    def second_half(t):
        if t == parts - 1:
            damping_terms()
        arrive_halo(ascending, t)
        sources(t, half, freq_group)
        ret_copy(near_side, t).start()
        back[:, :, tile_of(rank, t)] = done[
            pl.ds(rank * freq_dev, freq_dev), :, lanes_of(t)
        ]

    def zone_copy(dst_rank, src, dst, send, recv):
        return remote(src, dst, send, recv, zone * group + dst_rank)

    def damping_terms():
        others = mom_in.at[0 : count - 1]
        remote(others, others, mom_send, mom_recv, (me + 1) % count).wait_recv()
        total = jnp.sum(mom_in[...], axis=0) * (1.0 / (NF * ND))
        for t in range(parts):
            energy_mean, moment_one = total[t, 0:1], total[t, 1:2]
            mean_freq = moment_one / (energy_mean + 1e-06)
            steepness = energy_mean * mean_freq * mean_freq
            breaking = steepness * steepness / (1.0 + steepness * steepness)
            damp_out[t, 0:1] = 0.03 * breaking
            damp_out[t, 1:2] = 0.03 * breaking * moment_one
        for i in range(1, group):
            zone_copy(
                rank_of(offsets[i]), damp_out, damp_in.at[rank], damp_send, damp_recv
            ).start()
        damp_in[rank] = damp_out[...]

    first_half(0)
    for t in range(1, parts):
        for dy in range(1, sides):
            arrive_group(dy, t, 0, freq_dev)
        first_half(t)
        second_half(t - 1)
    second_half(parts - 1)

    others = damp_in.at[0 : group - 1]
    remote(others, others, damp_send, damp_recv, (me + 1) % count).wait_recv()

    def finish(t):
        block = done.at[0 : (group - 1) * freq_dev, :, lanes_of(t)]
        remote(block, block, ret_send, ret_recv.at[t], (me + 1) % count).wait_recv()
        for f in range(freq_dev):
            omega = omega_of(me * freq_dev + f, (1, LANES))
            for g in range(group):
                cols = slice(block_of(g, t) * LANES, (block_of(g, t) + 1) * LANES)
                value = back[f, :, cols] - (omega * damp_in[g, t, 0:1]) * adv[f, :, cols]
                for i, piece in enumerate(split_bf16(value)):
                    split[(3 * f + i) * ND : (3 * f + i + 1) * ND, cols] = piece
        ready = (t + 1) * group * LANES
        for j in range(cells // WIDE):
            low, high = max(0, j * WIDE - land), min(sea_cells, (j + 1) * WIDE)
            if high > ready or high <= t * group * LANES:
                continue
            cols = slice(j * WIDE, (j + 1) * WIDE)
            got = jnp.dot(
                split[:, low:high], spread_ref[low:high, cols], preferred_element_type=f32
            )
            for f in range(freq_dev):
                base = 3 * f * ND
                full_ref[f * ND : (f + 1) * ND, cols] = got[base : base + ND] + (
                    got[base + ND : base + 2 * ND]
                ) + got[base + 2 * ND : base + 3 * ND]

    for t in range(parts):
        finish(t)

    block = held.at[0 : (group - 1) * freq_dev]
    remote(block, block, y_sem, held_sem.at[0, 0, 0], (me + 1) % count).wait_send()
    remote(block, block, ret_send, ret_recv.at[0], (me + 1) % count).wait_send()
    others = mom_in.at[0 : count - 1]
    remote(others, others, mom_send, mom_recv, (me + 1) % count).wait_send()
    others = damp_in.at[0 : group - 1]
    remote(others, others, damp_send, damp_recv, (me + 1) % count).wait_send()
    def drain(slots, way):
        block = held.at[0:slots]
        remote(
            block, block, z_sem.at[way], halo_sem.at[0, 0], (me + 1) % count
        ).wait_send()

    for f in range(freq_dev):
        @pl.when(early_slot(rank * freq_dev + f))
        def _():
            drain(2, 0)

    @pl.when(late_ok)
    def _():
        drain(HALO, 1)

    others = sum_in.at[0 : count - 1]
    remote(others, others, sum_send, sum_recv, (me + 1) % count).wait()
    for g in range(group):
        mass = sum_in[g]
        for other in range(1, zones):
            mass = mass + sum_in[other * group + g]
        for t in range(parts):
            mean = mass[:, t * LANES : (t + 1) * LANES] * (1.0 / (NF * ND)) - damp_in[g, t, 1:2]
            cols = slice(block_of(g, t) * LANES, (block_of(g, t) + 1) * LANES)
            height_ref[0:1, cols] = 4.0 * jnp.sqrt(mean + 1e-06)


def store_kernel(
    count, full_in, height_in, near_in, new_out, wave_out, mean_out, wave_ref, mean_ref, sem
):
    cells = full_in.shape[1]
    sea_cells = height_in.shape[1]
    copies = [
        pltpu.make_async_copy(full_in, new_out, sem.at[0]),
        pltpu.make_async_copy(wave_ref, wave_out, sem.at[1]),
        pltpu.make_async_copy(mean_ref, mean_out, sem.at[2]),
    ]
    copies[0].start()
    me = lax.axis_index("spec")
    points = cells // count
    shift = me * points - window_start(count, me, cells)
    halves = []
    for h in range(WIDE // LANES):
        place = jnp.broadcast_to(near_in[:, h * LANES : (h + 1) * LANES], (8, LANES))
        place = place.astype(jnp.int32)
        wave = jnp.zeros((8, LANES), jnp.float32)
        for b in range(sea_cells // LANES):
            values = jnp.broadcast_to(height_in[:, b * LANES : (b + 1) * LANES], (8, LANES))
            found = jnp.take_along_axis(values, place % LANES, axis=1)
            wave = jnp.where(place // LANES == b, found, wave)
        halves.append(wave)
    wave = jnp.concatenate(halves, axis=1)
    wave_ref[...] = pltpu.roll(wave, (WIDE - shift) % WIDE, 1)[0, :points]
    copies[1].start()
    mean_ref[...] = jnp.sum(height_in[...], axis=1, keepdims=True) * (1.0 / sea_cells)
    copies[2].start()
    for copy in copies:
        copy.wait()


def fused_local(spectrum, sea_mask, wind_speed, wind_angle):
    count = lax.axis_size("spec")
    bins_dev, cells = spectrum.shape
    group = group_size(count, bins_dev, cells)
    freq_dev = bins_dev // ND
    freq_group = freq_dev * group
    sea_cells = SEA_DEV * count
    width = sea_cells // group
    points = cells // count
    parts = width // LANES
    f32, bf16 = jnp.float32, jnp.bfloat16
    dma = pltpu.SemaphoreType.DMA
    vmem = pl.BlockSpec(memory_space=pltpu.VMEM)
    handed = pl.pallas_call(
        functools.partial(fused_kernel, count, group),
        out_shape=(
            pltpu.VMEM((bins_dev, cells), f32),
            pltpu.VMEM((1, sea_cells), f32),
            pltpu.VMEM((1, WIDE), f32),
        ),
        in_specs=[pl.BlockSpec(memory_space=pl.ANY)] * 4,
        out_specs=(vmem,) * 3,
        scratch_shapes=[
            pltpu.VMEM((cells,), jnp.int32),
            pltpu.VMEM((cells,), f32),
            pltpu.VMEM((cells,), f32),
            pltpu.VMEM((1, cells), f32),
            pltpu.VMEM((1, cells), f32),
            pltpu.VMEM((sea_cells, cells), jnp.float8_e4m3fn),
            dma((3,)),
            pltpu.VMEM((bins_dev, cells), f32),
            pltpu.VMEM((bins_dev, cells), f32),
            pltpu.VMEM((3 * bins_dev, cells), bf16),
            pltpu.VMEM((ND // 2, cells), bf16),
            pltpu.VMEM((freq_dev, ND, sea_cells), f32),
            pltpu.VMEM((freq_group + 2 * HALO, ND, width), f32),
            pltpu.VMEM((freq_group, ND, width), f32),
            pltpu.VMEM((freq_dev, ND, sea_cells), f32),
            pltpu.VMEM((parts, 2, group * LANES), f32),
            pltpu.VMEM((count, parts, 2, LANES), f32),
            pltpu.VMEM((ND, width), f32),
            pltpu.VMEM((ND, width), f32),
            pltpu.VMEM((1, width), f32),
            pltpu.VMEM((count, 1, width), f32),
            pltpu.VMEM((parts, 2, LANES), f32),
            pltpu.VMEM((group, parts, 2, LANES), f32),
            dma((freq_dev,)),
            dma((group, freq_dev, parts)),
            dma((2, parts)),
            dma,
            dma((2,)),
            pltpu.SemaphoreType.REGULAR((2,)),
            dma,
            dma,
            dma,
            dma((parts,)),
            dma,
            dma,
            dma,
            dma,
        ],
        compiler_params=pltpu.CompilerParams(collective_id=0, has_side_effects=True),
    )(sea_mask, wind_speed, wind_angle, spectrum)
    out, wave, mean = pl.pallas_call(
        functools.partial(store_kernel, count),
        out_shape=(
            pltpu.HBM((bins_dev, cells), f32),
            pltpu.HBM((points,), f32),
            pltpu.HBM((1, 1), f32),
        ),
        in_specs=[vmem] * 3,
        out_specs=(pl.BlockSpec(memory_space=pltpu.HBM),) * 3,
        scratch_shapes=[pltpu.VMEM((points,), f32), pltpu.VMEM((1, 1), f32), dma((3,))],
    )(*[pltpu.with_memory_space_constraint(piece, pltpu.VMEM) for piece in handed])
    return (out, wave, mean.reshape(1))


def solution(mesh):
    in_specs = (P(("grp", "spec"), None), P(), P("grp"), P("grp"))
    out_specs = (P(("grp", "spec"), None), P(("grp", "spec")), P("grp"))

    def body(spectrum, sea_mask, wind_speed, wind_angle):
        fits = group_size(mesh.shape["spec"], *spectrum.shape)
        plan = fused_local if fits else local
        return plan(spectrum, sea_mask, wind_speed, wind_angle)

    return jax.shard_map(body, mesh=mesh, in_specs=in_specs, out_specs=out_specs, check_vma=False)
```

```python
import functools
import math

import jax
import jax.numpy as jnp
from jax import lax
from jax.experimental import pallas as pl
from jax.experimental.pallas import tpu as pltpu
from jax.sharding import PartitionSpec as P

NF = 48
ND = 32
NLON = 384
ADV_STEPS = 2
SEA_DEV = 64


def upwind_step(energy, courant_x, courant_y, sea_grid):
    west_cell = jnp.roll(energy, 1, axis=2)
    east_cell = jnp.roll(energy, -1, axis=2)
    edge_row = jnp.zeros_like(energy[:, :1])
    south_cell = jnp.concatenate([edge_row, energy[:, :-1]], axis=1)
    north_cell = jnp.concatenate([energy[:, 1:], edge_row], axis=1)
    updated = (
        energy
        - jnp.maximum(courant_x, 0.0) * (energy - west_cell)
        - jnp.minimum(courant_x, 0.0) * (east_cell - energy)
        - jnp.maximum(courant_y, 0.0) * (energy - south_cell)
        - jnp.minimum(courant_y, 0.0) * (north_cell - energy)
    )
    return updated * sea_grid


def courant_numbers(freq_index, dir_index, lat_count, dir_count):
    speed = 0.2 * jnp.exp(-math.log(1.1) * freq_index)
    heading = 2.0 * math.pi * (dir_index + 0.5) / dir_count
    rows = jnp.arange(lat_count, dtype=jnp.float32)
    latitude = (-75.0 + 150.0 * (rows + 0.5) / lat_count) * (math.pi / 180.0)
    courant_x = (speed * jnp.cos(heading))[:, None, None] / jnp.cos(latitude)[None, :, None]
    courant_y = (speed * jnp.sin(heading))[:, None, None]
    return (courant_x, courant_y)


def shift_freq(values, amount):
    if amount > 0:
        filler = jnp.zeros_like(values[:amount])
        return jnp.concatenate([filler, values[:-amount]], axis=0)
    filler = jnp.zeros_like(values[:-amount])
    return jnp.concatenate([values[-amount:], filler], axis=0)


def source_terms(energy, speed, angle):
    freq_count = energy.shape[0]
    dir_count = energy.shape[1]
    freq_ids = jnp.arange(freq_count, dtype=jnp.float32)
    frequency = jnp.exp(math.log(1.1) * (freq_ids - freq_count // 2))[:, None, None]
    heading = (2.0 * math.pi * (jnp.arange(dir_count, dtype=jnp.float32) + 0.5) / dir_count)[
        None, :, None
    ]
    energy_mean = jnp.mean(energy, axis=(0, 1))
    moment_one = jnp.mean(frequency * energy, axis=(0, 1))
    mean_freq = moment_one / (energy_mean + 1e-06)
    steepness = energy_mean * mean_freq * mean_freq
    breaking = steepness * steepness / (1.0 + steepness * steepness)
    wind_gain = (
        0.05
        * frequency
        * jnp.maximum(
            0.0, speed[None, None, :] * frequency * jnp.cos(heading - angle[None, None, :]) - 1.0
        )
    )
    damping = 0.03 * frequency * breaking[None, None, :]
    valid = ((freq_ids >= 3) & (freq_ids <= freq_count - 3)).astype(jnp.float32)[:, None, None]
    interaction = jnp.zeros_like(energy)
    for mirror in (1, -1):
        plus_bins = shift_freq(jnp.roll(energy, -mirror, axis=1), -2)
        minus_bins = shift_freq(jnp.roll(energy, 3 * mirror, axis=1), 3)
        transfer_rate = (
            0.001
            * valid
            * (energy * energy * (plus_bins + minus_bins) - 2.0 * energy * plus_bins * minus_bins)
        )
        interaction = interaction - 2.0 * transfer_rate
        interaction = interaction + jnp.roll(shift_freq(transfer_rate, 2), mirror, axis=1)
        interaction = interaction + jnp.roll(shift_freq(transfer_rate, -3), -3 * mirror, axis=1)
    updated = energy + (wind_gain - damping) * energy + interaction
    raw_height = 4.0 * jnp.sqrt(jnp.mean(updated, axis=(0, 1)) + 1e-06)
    return (updated, raw_height)


def local(spectrum, sea_mask, wind_speed, wind_angle):
    count = lax.axis_size("spec")
    position = lax.axis_index("spec")
    bins_dev = spectrum.shape[0]
    cells = spectrum.shape[1]
    points = cells // count
    lat_count = cells // NLON
    sea_float = sea_mask.astype(jnp.float32)
    bin_ids = position * bins_dev + jnp.arange(bins_dev, dtype=jnp.int32)
    freq_index = (bin_ids // ND).astype(jnp.float32)
    dir_index = (bin_ids % ND).astype(jnp.float32)
    courant_x, courant_y = courant_numbers(freq_index, dir_index, lat_count, ND)
    sea_grid = sea_float.reshape(1, lat_count, NLON)
    energy = (spectrum * sea_float[None, :]).reshape(bins_dev, lat_count, NLON)
    for substep in range(ADV_STEPS):
        energy = upwind_step(energy, courant_x, courant_y, sea_grid)
    advected = energy.reshape(bins_dev, cells)
    outgoing = advected.reshape(bins_dev, count, points)
    arrived = lax.all_to_all(outgoing, "spec", split_axis=1, concat_axis=0, tiled=True)
    start = position * points
    speed_own = lax.dynamic_slice_in_dim(wind_speed, start, points)
    angle_own = lax.dynamic_slice_in_dim(wind_angle, start, points)
    sea_own = lax.dynamic_slice_in_dim(sea_float, start, points)
    updated, raw_height = source_terms(arrived.reshape(NF, ND, points), speed_own, angle_own)
    wave_height = sea_own * raw_height
    own_total = jnp.zeros((count, 1), jnp.float32) + jnp.sum(wave_height)
    returned, totals = (
        lax.all_to_all(
            updated.reshape(NF * ND, 1, points), "spec", split_axis=0, concat_axis=1, tiled=True
        ),
        lax.all_to_all(own_total, "spec", split_axis=0, concat_axis=1, tiled=True),
    )
    new_spectrum = returned.reshape(bins_dev, cells)
    height_sum = jnp.sum(totals)
    mean_height = (height_sum / (SEA_DEV * count)).reshape(1)
    return (new_spectrum, wave_height, mean_height)


HALO = 5
LANES = 128
WIDE = 256
LAND = 4096.0


def group_size(count, bins_dev, cells):
    size = 4
    if count % size or bins_dev % ND or cells % (size * LANES) or cells % NLON:
        return 0
    if NLON % LANES or bins_dev // ND * size < 2 * HALO or cells % count:
        return 0
    sea = SEA_DEV * count
    if sea > min(cells, LAND) or sea % (size * LANES) or sea % WIDE or cells % WIDE:
        return 0
    if (cells - sea) % WIDE:
        return 0
    return size


def split_bf16(values):
    high = values.astype(jnp.bfloat16)
    left = values - high.astype(jnp.float32)
    mid = left.astype(jnp.bfloat16)
    low = (left - mid.astype(jnp.float32)).astype(jnp.bfloat16)
    return high, mid, low


def rows_of(parts, height, width):
    ids = lax.broadcasted_iota(jnp.int32, (height, width), 0)
    out = jnp.zeros((height, width), jnp.float32)
    for i, part in enumerate(parts):
        out = jnp.where(ids == i, jnp.broadcast_to(part.astype(jnp.float32), (height, width)), out)
    return out.astype(jnp.bfloat16)


def window_start(count, me, cells):
    return jnp.minimum(me * (cells // count) // LANES * LANES, cells - WIDE)


def fused_kernel(
    count, group, sea_in, wind_in, angle_in, spec_ref, full_ref, height_ref, near_ref,
    sea_raw, wind_raw, angle_raw, aux_ref, place_ref, spread_ref, aux_sem,
    raw, moved, split, wsplit, adv, held, done, back, mom_out, mom_in, wind, acc,
    sum_out, sum_in, damp_out, damp_in,
    load_sem, held_sem, halo_sem, y_sem, z_sem, chain_sem, mom_send, mom_recv,
    ret_send, ret_recv, sum_send, sum_recv, damp_send, damp_recv,
):
    f32, bf16 = jnp.float32, jnp.bfloat16
    freq_dev, _, sea_cells = adv.shape
    bins_dev, cells = moved.shape
    freq_group = freq_dev * group
    width = sea_cells // group
    zones = count // group
    lat_count = cells // NLON
    sides = group // 2
    parts = width // LANES
    cell_tiles = cells // LANES
    land = cells - sea_cells
    reach = land + WIDE
    me = lax.axis_index("spec")
    zone, rank = me // group, me % group
    side, core = rank // 2, rank % 2

    def remote(src, dst, send, recv, target):
        return pltpu.make_async_remote_copy(
            src_ref=src, dst_ref=dst, send_sem=send, recv_sem=recv,
            device_id={"spec": target}, device_id_type=pl.DeviceIdType.MESH,
        )

    loads = [
        pltpu.make_async_copy(
            spec_ref.at[pl.ds(f * ND, ND)], raw.at[pl.ds(f * ND, ND)], load_sem.at[f]
        )
        for f in range(freq_dev)
    ]
    small = [
        pltpu.make_async_copy(sea_in, sea_raw, aux_sem.at[0]),
        pltpu.make_async_copy(wind_in, wind_raw, aux_sem.at[1]),
        pltpu.make_async_copy(angle_in, angle_raw, aux_sem.at[2]),
    ]
    for load in small[:1] + loads + small[1:]:
        load.start()
    barrier = pltpu.get_barrier_semaphore()

    def signal(semaphore, target):
        pl.semaphore_signal(
            semaphore, inc=1, device_id={"spec": target}, device_id_type=pl.DeviceIdType.MESH
        )

    for step in range(1, group):
        signal(barrier, zone * group + (rank + step) % group)

    @pl.when(zone > 0)
    def _():
        for c in range(2):
            signal(barrier, (zone - 1) * group + side * 2 + c)

    @pl.when(zone < zones - 1)
    def _():
        for c in range(2):
            signal(barrier, (zone + 1) * group + side * 2 + c)

    @pl.when(zone == 0)
    def _():
        held[0:HALO] = jnp.zeros((HALO, ND, width), f32)

    @pl.when(zone == zones - 1)
    def _():
        held[HALO + freq_group :] = jnp.zeros((HALO, ND, width), f32)

    def block_of(index, t):
        return t * group + index

    def tile_of(index, t):
        return pl.ds(pl.multiple_of(block_of(index, t) * LANES, LANES), LANES)

    def lanes_of(t):
        return pl.ds(t * LANES, LANES)

    offsets = [(dy, dc) for dy in range(sides) for dc in range(2)]

    def rank_of(offset):
        return (side + offset[0]) % sides * 2 + (core + offset[1]) % 2

    def y_copy(f, peer, t):
        return remote(
            adv.at[f, :, tile_of(peer, t)],
            held.at[HALO + rank * freq_dev + f, :, lanes_of(t)],
            y_sem, held_sem.at[rank, f, t], zone * group + peer,
        )

    dirs = lax.broadcasted_iota(jnp.int32, (ND, LANES), 0).astype(f32)
    heading = 2.0 * math.pi * (dirs + 0.5) / ND
    cos_h, sin_h = jnp.cos(heading), jnp.sin(heading)
    log_step = math.log(1.1)
    lats = [math.radians(-75.0 + 150.0 * (r + 0.5) / lat_count) for r in range(lat_count)]

    def omega_of(freq, shape):
        return jnp.exp(jnp.full(shape, log_step, f32) * (freq.astype(f32) - NF // 2))

    square_rows = lax.broadcasted_iota(jnp.int32, (LANES, LANES), 0)
    square_cols = lax.broadcasted_iota(jnp.int32, (LANES, LANES), 1)
    small[0].wait()
    aux_ref[...] = sea_raw[...].astype(f32).reshape(1, cells)
    sea = [aux_ref[0:1, r * NLON : (r + 1) * NLON] for r in range(lat_count)]
    mask = [aux_ref[0:1, i * LANES : (i + 1) * LANES] for i in range(cell_tiles)]
    tri_up = jnp.where(square_rows < square_cols, 1.0, 0.0).astype(bf16)
    ranks = jnp.dot(rows_of(mask, ND // 2, LANES), tri_up, preferred_element_type=f32)
    before = jnp.zeros((1, 1), f32)
    for i in range(cell_tiles):
        place_ref[0:1, i * LANES : (i + 1) * LANES] = jnp.where(
            mask[i] > 0.0, ranks[i : i + 1] + before, LAND
        )
        before = before + jnp.sum(mask[i], axis=1, keepdims=True)
    pair_rows = lax.broadcasted_iota(jnp.int32, (WIDE, reach), 0).astype(f32)

    def build(pair):
        cols = pl.ds(pl.multiple_of(pair * WIDE, LANES), reach)
        first = (pair * WIDE).astype(f32)
        hit = jnp.where(place_ref[0:1, cols] - first == pair_rows, 1.0, 0.0)
        spread_ref[pl.ds(pl.multiple_of(pair * WIDE, LANES), WIDE), cols] = hit.astype(
            spread_ref.dtype
        )

    def packed(values, pair):
        cols = pl.ds(pl.multiple_of(pair * WIDE, LANES), reach)
        return lax.dot_general(
            values[:, cols],
            spread_ref[pl.ds(pl.multiple_of(pair * WIDE, LANES), WIDE), cols],
            (((1,), (1,)), ((), ())), preferred_element_type=f32,
        )

    quarter = ND // 4
    tiles = NLON // LANES
    def advect(f):
        loads[f].wait()
        freq = (me * freq_dev + f).astype(f32)
        speed = 0.2 * jnp.exp(jnp.full((quarter, LANES), -log_step, f32) * freq)
        for q in range(4):
            east, north = q in (0, 3), q in (0, 1)
            rows = slice(f * ND + q * quarter, f * ND + (q + 1) * quarter)
            part = slice(q * quarter, (q + 1) * quarter)
            cx0 = speed * jnp.abs(cos_h[part])
            cy = jnp.concatenate([speed * jnp.abs(sin_h[part])] * tiles, axis=1)
            cx = [jnp.concatenate([cx0 * (1.0 / math.cos(a))] * tiles, axis=1) for a in lats]
            rest = [1.0 - (cx[r] + cy) for r in range(lat_count)]
            energy = [raw[rows, r * NLON : (r + 1) * NLON] * sea[r] for r in range(lat_count)]
            for step in range(ADV_STEPS):
                fresh = []
                for r in range(lat_count):
                    e = energy[r]
                    side_x = pltpu.roll(e, 1 if east else NLON - 1, 1)
                    other = r - 1 if north else r + 1
                    value = rest[r] * e + cx[r] * side_x
                    if 0 <= other < lat_count:
                        value = value + cy * energy[other]
                    fresh.append(value if step == ADV_STEPS - 1 else value * sea[r])
                energy = fresh
            for r in range(lat_count):
                moved[rows, r * NLON : (r + 1) * NLON] = energy[r]
        for i, piece in enumerate(split_bf16(moved[f * ND : (f + 1) * ND])):
            split[(3 * f + i) * ND : (3 * f + i + 1) * ND, :] = piece

    def cols_of(index):
        return pl.ds(pl.multiple_of(index * LANES, LANES), LANES)

    def side_of(dy):
        return (side + dy) % sides

    def pack(t, dy, begin, end):
        return packed(split.at[begin * 3 * ND : end * 3 * ND], t * sides + side_of(dy))

    def unload(t, dy, begin, end, got):
        pair = t * sides + side_of(dy)
        cols = pl.ds(pl.multiple_of(pair * WIDE, LANES), WIDE)
        here = pl.ds(pl.multiple_of(side_of(dy) * WIDE, LANES), WIDE)
        mass, moment = None, None
        for f in range(begin, end):
            base = (f - begin) * 3 * ND
            piece = got[base : base + ND] + got[base + ND : base + 2 * ND] + (
                got[base + 2 * ND : base + 3 * ND]
            )
            adv[f, :, cols] = piece
            total = jnp.sum(piece, axis=0, keepdims=True)
            scaled = omega_of(me * freq_dev + f, (1, WIDE)) * total
            mass = total if mass is None else mass + total
            moment = scaled if moment is None else moment + scaled
        if begin:
            mass, moment = mass + mom_out[t, 0:1, here], moment + mom_out[t, 1:2, here]
        mom_out[t, 0:1, here] = mass
        mom_out[t, 1:2, here] = moment

    def send_far(t, dy, begin, end):
        for c in range(2):
            for f in range(begin, end):
                y_copy(f, side_of(dy) * 2 + c, t).start()

    top = side > 0
    early_way, late_way = jnp.where(top, 0, 1), jnp.where(top, 1, 0)
    early_ok = jnp.where(top, zone < zones - 1, zone > 0)
    late_ok = jnp.where(top, zone > 0, zone < zones - 1)
    early_zone = jnp.where(top, zone + 1, zone + zones - 1) % zones
    late_zone = jnp.where(top, zone + zones - 1, zone + 1) % zones
    early_shift = HALO + jnp.where(top, -freq_group, freq_group)
    late_shift = HALO + jnp.where(top, freq_group, -freq_group)

    def early_slot(slot):
        return early_ok & jnp.where(top, slot >= freq_group - HALO, slot < HALO)

    def late_slot(slot):
        return late_ok & jnp.where(top, slot < HALO, slot >= freq_group - HALO)

    def early_copy(f, c, t):
        return remote(
            adv.at[f, :, tile_of(side * 2 + c, t)],
            held.at[early_shift + rank * freq_dev + f, :, lanes_of(t)],
            z_sem.at[0], halo_sem.at[early_way, t], early_zone * group + side * 2 + c,
        )

    def forward(slot, t):
        @pl.when(late_slot(slot))
        def _():
            remote(
                held.at[HALO + slot, :, lanes_of(t)],
                held.at[late_shift + slot, :, lanes_of(t)],
                z_sem.at[1], halo_sem.at[late_way, t], late_zone * group + rank,
            ).start()

    def send_near(t):
        for c in range(2):
            for f in range(freq_dev):
                @pl.when(early_slot(rank * freq_dev + f))
                def _():
                    early_copy(f, c, t).start()

        for f in range(freq_dev):
            y_copy(f, rank_of((0, 1)), t).start()
        for f in range(freq_dev):
            held[HALO + rank * freq_dev + f, :, lanes_of(t)] = adv[f, :, tile_of(rank, t)]

    def arrive_group(dy, t, begin, end):
        for f in range(begin, end):
            for dc in range(2):
                if (dy, dc) != (0, 0):
                    source = rank_of((dy, dc))
                    slot = source * freq_dev + f
                    block = held.at[HALO + slot, :, lanes_of(t)]
                    remote(
                        block, block, y_sem, held_sem.at[source, f, t], (me + 1) % count
                    ).wait_recv()
                    if dy:
                        forward(slot, t)

    def up_relay(level):
        @pl.when(zone == level)
        def _():
            pl.semaphore_wait(chain_sem.at[0], 1)
            if level < zones - 1:
                signal(chain_sem.at[0], (me + group) % count)

    def down_relay(level):
        @pl.when(zone == level)
        def _():
            pl.semaphore_wait(chain_sem.at[1], 1)
            if level > 0:
                signal(chain_sem.at[1], (me + count - group) % count)

    def moment_copy(target_zone, target_rank):
        return remote(
            mom_out.at[:, :, cols_of(target_rank)], mom_in.at[me],
            mom_send, mom_recv, target_zone * group + target_rank,
        )

    def send_zone_moments():
        for step in range(1, group):
            moment_copy(zone, (rank + step) % group).start()

    def send_moments():
        for away in range(1, zones):
            for other in range(group):
                moment_copy((zone + away) % zones, other).start()

    far = list(range(1, sides))
    for dy in far:
        build(side_of(dy))
    advect(0)
    for dy in far:
        unload(0, dy, 0, 1, pack(0, dy, 0, 1))
    advect(1)
    pl.semaphore_wait(
        barrier, group - 1 + jnp.where(zone > 0, 2, 0) + jnp.where(zone < zones - 1, 2, 0)
    )
    for dy in far:
        send_far(0, dy, 0, 1)

    @pl.when(zone == 0)
    def _():
        signal(chain_sem.at[0], (me + group) % count)

    @pl.when(zone == zones - 1)
    def _():
        signal(chain_sem.at[1], (me + count - group) % count)

    up_relay(1)
    for f in range(2, freq_dev):
        advect(f)
    for level in range(2, zones - 1):
        up_relay(level)
    got = [pack(0, dy, 1, freq_dev) for dy in far]
    build(side)
    got_near = pack(0, 0, 0, freq_dev)
    for dy in far:
        unload(0, dy, 1, freq_dev, got[dy - 1])
        send_far(0, dy, 1, freq_dev)
    unload(0, 0, 0, freq_dev, got_near)
    send_near(0)
    down_relay(zones - 2)
    upper = zone >= zones // 2
    for t in range(1, parts):
        last = t == parts - 1
        for dy in far:
            build(t * sides + side_of(dy))
        got = [pack(t, dy, 0, freq_dev) for dy in far]
        build(t * sides + side)
        got_near = pack(t, 0, 0, freq_dev)
        for dy in far:
            unload(t, dy, 0, freq_dev, got[dy - 1])

            @pl.when(jnp.logical_not(upper) if last else zone >= 0)
            def _():
                send_far(t, dy, 0, freq_dev)

        unload(t, 0, 0, freq_dev, got_near)
        if last:
            up_relay(zones - 1)
            send_zone_moments()

            @pl.when(upper)
            def _():
                send_moments()
                for dy in far:
                    send_far(t, dy, 0, freq_dev)

        send_near(t)

    for dy in far:
        arrive_group(dy, 0, 0, 1)
    for level in range(zones - 3, 0, -1):
        down_relay(level)

    @pl.when(jnp.logical_not(upper) & (zone > 0))
    def _():
        send_moments()

    small[1].wait()
    small[2].wait()
    speed_all = wind_raw[...].reshape(1, cells)
    angle_all = angle_raw[...].reshape(1, cells)
    wsplit[...] = rows_of(
        split_bf16(speed_all * jnp.cos(angle_all)) + split_bf16(speed_all * jnp.sin(angle_all)),
        2 * quarter, cells,
    )
    for t in range(parts):
        own = packed(wsplit, t * sides + side)
        own = jnp.where(core == 0, own[:, :LANES], own[:, LANES:])
        along = own[0:1] + own[1:2] + own[2:3]
        across = own[3:4] + own[4:5] + own[5:6]
        wind[:, t * LANES : (t + 1) * LANES] = cos_h * along + sin_h * across

    for dy in far:
        arrive_group(dy, 0, 1, freq_dev)
    mom_in[me] = mom_out[:, :, cols_of(rank)]
    start = window_start(count, me, cells)
    near_ref[...] = place_ref[0:1, pl.ds(pl.multiple_of(start, LANES), WIDE)]
    for t in range(parts):
        arrive_group(0, t, 0, freq_dev)

    acc[...] = jnp.zeros_like(acc)
    ascending = side > 0

    def arrive_halo(at_top, t):
        block = held.at[0:HALO, :, lanes_of(t)]

        @pl.when(jnp.where(at_top, zone < zones - 1, zone > 0))
        def _():
            way = jnp.where(at_top, 1, 0)
            remote(
                block, block, z_sem.at[0], halo_sem.at[way, t], (me + 1) % count
            ).wait_recv()

    def ret_copy(owner, t):
        return remote(
            done.at[pl.ds(owner * freq_dev, freq_dev), :, lanes_of(t)],
            back.at[:, :, tile_of(rank, t)],
            ret_send, ret_recv.at[t], zone * group + owner,
        )

    def turn(values, amount):
        return pltpu.roll(values, amount % ND, 0)

    def rate(a, p, m):
        return a * (a * (p + m) - 2.0 * (p * m))

    def scale(index, factor):
        return jnp.where((index >= 3) & (index <= NF - 3), factor, 0.0).astype(f32)

    def slab(k, t):
        return held[HALO + k, :, t * LANES : (t + 1) * LANES]

    def rates(own, p2, m3):
        return rate(own, turn(p2, -1), turn(m3, 3)) + rate(own, turn(p2, 1), turn(m3, -3))

    def grown(own, freq, t):
        omega = omega_of(freq, (1, LANES))
        push = wind[:, t * LANES : (t + 1) * LANES] * omega - 1.0
        return own + (0.05 * omega) * jnp.maximum(0.0, push) * own

    def tally(energy, near, freq, t):
        flow = scale(freq, 0.001) * near
        acc[:, t * LANES : (t + 1) * LANES] += energy + (flow + flow - 2.0 * flow)

    def sources(t, begin, end):
        def source_step(i, carry):
            k = jnp.where(ascending, i, freq_group - 1 - i)
            freq = zone * freq_group + k
            own = slab(k, t)
            p2, m3, m2, m5, p3, p5 = (slab(k + shift, t) for shift in (2, -3, -2, -5, 3, 5))
            near = rates(own, p2, m3)
            low = rate(turn(m2, 1), own, turn(m5, 4)) + rate(turn(m2, -1), own, turn(m5, -4))
            high = rate(turn(p3, -3), turn(p5, -4), own) + rate(turn(p3, 3), turn(p5, 4), own)
            interaction = scale(freq, -0.002) * near + scale(freq - 2, 0.001) * low + (
                scale(freq + 3, 0.001) * high
            )
            energy = grown(own, freq, t)
            done[k, :, t * LANES : (t + 1) * LANES] = energy + interaction
            if begin == 0:
                tally(energy, near, freq, t)
            return carry

        lax.fori_loop(begin, end, source_step, 0)

    def tally_rest(t):
        def rest_step(i, carry):
            k = jnp.where(ascending, half + i, half - 1 - i)
            center = jnp.where(
                ascending,
                jnp.where(i < 2, i - 2, half + i - 2),
                jnp.where(i < 3, freq_group + i, half + 2 - i),
            )
            near = rates(slab(center, t), slab(center + 2, t), slab(center - 3, t))
            energy = grown(slab(k, t), zone * freq_group + k, t)
            tally(energy, near, zone * freq_group + center, t)
            return carry

        lax.fori_loop(0, half, rest_step, 0)

    half = freq_group // 2
    near_side = rank_of((0, 1))

    def first_half(t):
        arrive_halo(jnp.logical_not(ascending), t)
        sources(t, 0, half)
        if t == parts - 1:
            tally_rest(t)
            send_sums()
        for dy in range(1, sides):
            for dc in range(2):
                ret_copy(rank_of((dy, dc)), t).start()
        if t == 0:
            down_relay(0)

            @pl.when(zone == 0)
            def _():
                send_moments()

        if t < parts - 1:
            tally_rest(t)

    def send_sums():
        sum_out[...] = jnp.sum(acc[...], axis=0, keepdims=True)
        for step in range(1, count):
            remote(sum_out, sum_in.at[me], sum_send, sum_recv, (me + step) % count).start()
        sum_in[me] = sum_out[...]

    def second_half(t):
        if t == parts - 1:
            damping_terms()
        arrive_halo(ascending, t)
        sources(t, half, freq_group)
        ret_copy(near_side, t).start()
        back[:, :, tile_of(rank, t)] = done[
            pl.ds(rank * freq_dev, freq_dev), :, lanes_of(t)
        ]

    def zone_copy(dst_rank, src, dst, send, recv):
        return remote(src, dst, send, recv, zone * group + dst_rank)

    def damping_terms():
        others = mom_in.at[0 : count - 1]
        remote(others, others, mom_send, mom_recv, (me + 1) % count).wait_recv()
        total = jnp.sum(mom_in[...], axis=0) * (1.0 / (NF * ND))
        for t in range(parts):
            energy_mean, moment_one = total[t, 0:1], total[t, 1:2]
            mean_freq = moment_one / (energy_mean + 1e-06)
            steepness = energy_mean * mean_freq * mean_freq
            breaking = steepness * steepness / (1.0 + steepness * steepness)
            damp_out[t, 0:1] = 0.03 * breaking
            damp_out[t, 1:2] = 0.03 * breaking * moment_one
        for i in range(1, group):
            zone_copy(
                rank_of(offsets[i]), damp_out, damp_in.at[rank], damp_send, damp_recv
            ).start()
        damp_in[rank] = damp_out[...]

    first_half(0)
    for t in range(1, parts):
        for dy in range(1, sides):
            arrive_group(dy, t, 0, freq_dev)
        first_half(t)
        second_half(t - 1)
    second_half(parts - 1)

    others = damp_in.at[0 : group - 1]
    remote(others, others, damp_send, damp_recv, (me + 1) % count).wait_recv()

    def finish(t):
        block = done.at[0 : (group - 1) * freq_dev, :, lanes_of(t)]
        remote(block, block, ret_send, ret_recv.at[t], (me + 1) % count).wait_recv()
        for f in range(freq_dev):
            omega = omega_of(me * freq_dev + f, (1, LANES))
            for g in range(group):
                cols = slice(block_of(g, t) * LANES, (block_of(g, t) + 1) * LANES)
                value = back[f, :, cols] - (omega * damp_in[g, t, 0:1]) * adv[f, :, cols]
                for i, piece in enumerate(split_bf16(value)):
                    split[(3 * f + i) * ND : (3 * f + i + 1) * ND, cols] = piece
        ready = (t + 1) * group * LANES
        for j in range(cells // WIDE):
            low, high = max(0, j * WIDE - land), min(sea_cells, (j + 1) * WIDE)
            if high > ready or high <= t * group * LANES:
                continue
            cols = slice(j * WIDE, (j + 1) * WIDE)
            got = jnp.dot(
                split[:, low:high], spread_ref[low:high, cols], preferred_element_type=f32
            )
            for f in range(freq_dev):
                base = 3 * f * ND
                full_ref[f * ND : (f + 1) * ND, cols] = got[base : base + ND] + (
                    got[base + ND : base + 2 * ND]
                ) + got[base + 2 * ND : base + 3 * ND]

    for t in range(parts):
        finish(t)

    block = held.at[0 : (group - 1) * freq_dev]
    remote(block, block, y_sem, held_sem.at[0, 0, 0], (me + 1) % count).wait_send()
    remote(block, block, ret_send, ret_recv.at[0], (me + 1) % count).wait_send()
    others = mom_in.at[0 : count - 1]
    remote(others, others, mom_send, mom_recv, (me + 1) % count).wait_send()
    others = damp_in.at[0 : group - 1]
    remote(others, others, damp_send, damp_recv, (me + 1) % count).wait_send()
    def drain(slots, way):
        block = held.at[0:slots]
        remote(
            block, block, z_sem.at[way], halo_sem.at[0, 0], (me + 1) % count
        ).wait_send()

    for f in range(freq_dev):
        @pl.when(early_slot(rank * freq_dev + f))
        def _():
            drain(2, 0)

    @pl.when(late_ok)
    def _():
        drain(HALO, 1)

    others = sum_in.at[0 : count - 1]
    remote(others, others, sum_send, sum_recv, (me + 1) % count).wait()
    for g in range(group):
        mass = sum_in[g]
        for other in range(1, zones):
            mass = mass + sum_in[other * group + g]
        for t in range(parts):
            mean = mass[:, t * LANES : (t + 1) * LANES] * (1.0 / (NF * ND)) - damp_in[g, t, 1:2]
            cols = slice(block_of(g, t) * LANES, (block_of(g, t) + 1) * LANES)
            height_ref[0:1, cols] = 4.0 * jnp.sqrt(mean + 1e-06)


def store_kernel(
    count, full_in, height_in, near_in, new_out, wave_out, mean_out, wave_ref, mean_ref, sem
):
    cells = full_in.shape[1]
    sea_cells = height_in.shape[1]
    copies = [
        pltpu.make_async_copy(full_in, new_out, sem.at[0]),
        pltpu.make_async_copy(wave_ref, wave_out, sem.at[1]),
        pltpu.make_async_copy(mean_ref, mean_out, sem.at[2]),
    ]
    copies[0].start()
    me = lax.axis_index("spec")
    points = cells // count
    shift = me * points - window_start(count, me, cells)
    halves = []
    for h in range(WIDE // LANES):
        place = jnp.broadcast_to(near_in[:, h * LANES : (h + 1) * LANES], (8, LANES))
        place = place.astype(jnp.int32)
        wave = jnp.zeros((8, LANES), jnp.float32)
        for b in range(sea_cells // LANES):
            values = jnp.broadcast_to(height_in[:, b * LANES : (b + 1) * LANES], (8, LANES))
            found = jnp.take_along_axis(values, place % LANES, axis=1)
            wave = jnp.where(place // LANES == b, found, wave)
        halves.append(wave)
    wave = jnp.concatenate(halves, axis=1)
    wave_ref[...] = pltpu.roll(wave, (WIDE - shift) % WIDE, 1)[0, :points]
    copies[1].start()
    mean_ref[...] = jnp.sum(height_in[...], axis=1, keepdims=True) * (1.0 / sea_cells)
    copies[2].start()
    for copy in copies:
        copy.wait()


def fused_local(spectrum, sea_mask, wind_speed, wind_angle):
    count = lax.axis_size("spec")
    bins_dev, cells = spectrum.shape
    group = group_size(count, bins_dev, cells)
    freq_dev = bins_dev // ND
    freq_group = freq_dev * group
    sea_cells = SEA_DEV * count
    width = sea_cells // group
    points = cells // count
    parts = width // LANES
    f32, bf16 = jnp.float32, jnp.bfloat16
    dma = pltpu.SemaphoreType.DMA
    vmem = pl.BlockSpec(memory_space=pltpu.VMEM)
    handed = pl.pallas_call(
        functools.partial(fused_kernel, count, group),
        out_shape=(
            pltpu.VMEM((bins_dev, cells), f32),
            pltpu.VMEM((1, sea_cells), f32),
            pltpu.VMEM((1, WIDE), f32),
        ),
        in_specs=[pl.BlockSpec(memory_space=pl.ANY)] * 4,
        out_specs=(vmem,) * 3,
        scratch_shapes=[
            pltpu.VMEM((cells,), jnp.int32),
            pltpu.VMEM((cells,), f32),
            pltpu.VMEM((cells,), f32),
            pltpu.VMEM((1, cells), f32),
            pltpu.VMEM((1, cells), f32),
            pltpu.VMEM((sea_cells, cells), jnp.float8_e4m3fn),
            dma((3,)),
            pltpu.VMEM((bins_dev, cells), f32),
            pltpu.VMEM((bins_dev, cells), f32),
            pltpu.VMEM((3 * bins_dev, cells), bf16),
            pltpu.VMEM((ND // 2, cells), bf16),
            pltpu.VMEM((freq_dev, ND, sea_cells), f32),
            pltpu.VMEM((freq_group + 2 * HALO, ND, width), f32),
            pltpu.VMEM((freq_group, ND, width), f32),
            pltpu.VMEM((freq_dev, ND, sea_cells), f32),
            pltpu.VMEM((parts, 2, group * LANES), f32),
            pltpu.VMEM((count, parts, 2, LANES), f32),
            pltpu.VMEM((ND, width), f32),
            pltpu.VMEM((ND, width), f32),
            pltpu.VMEM((1, width), f32),
            pltpu.VMEM((count, 1, width), f32),
            pltpu.VMEM((parts, 2, LANES), f32),
            pltpu.VMEM((group, parts, 2, LANES), f32),
            dma((freq_dev,)),
            dma((group, freq_dev, parts)),
            dma((2, parts)),
            dma,
            dma((2,)),
            pltpu.SemaphoreType.REGULAR((2,)),
            dma,
            dma,
            dma,
            dma((parts,)),
            dma,
            dma,
            dma,
            dma,
        ],
        compiler_params=pltpu.CompilerParams(collective_id=0, has_side_effects=True),
    )(sea_mask, wind_speed, wind_angle, spectrum)
    out, wave, mean = pl.pallas_call(
        functools.partial(store_kernel, count),
        out_shape=(
            pltpu.HBM((bins_dev, cells), f32),
            pltpu.HBM((points,), f32),
            pltpu.HBM((1, 1), f32),
        ),
        in_specs=[vmem] * 3,
        out_specs=(pl.BlockSpec(memory_space=pltpu.HBM),) * 3,
        scratch_shapes=[pltpu.VMEM((points,), f32), pltpu.VMEM((1, 1), f32), dma((3,))],
    )(*[pltpu.with_memory_space_constraint(piece, pltpu.VMEM) for piece in handed])
    return (out, wave, mean.reshape(1))


def solution(mesh):
    in_specs = (P(("grp", "spec"), None), P(), P("grp"), P("grp"))
    out_specs = (P(("grp", "spec"), None), P(("grp", "spec")), P("grp"))

    def body(spectrum, sea_mask, wind_speed, wind_angle):
        fits = group_size(mesh.shape["spec"], *spectrum.shape)
        plan = fused_local if fits else local
        return plan(spectrum, sea_mask, wind_speed, wind_angle)

    return jax.shard_map(body, mesh=mesh, in_specs=in_specs, out_specs=out_specs, check_vma=False)
```

```python
import functools
import math

import jax
import jax.numpy as jnp
from jax import lax
from jax.experimental import pallas as pl
from jax.experimental.pallas import tpu as pltpu
from jax.sharding import PartitionSpec as P

NF = 48
ND = 32
NLON = 384
ADV_STEPS = 2
SEA_DEV = 64


def upwind_step(energy, courant_x, courant_y, sea_grid):
    west_cell = jnp.roll(energy, 1, axis=2)
    east_cell = jnp.roll(energy, -1, axis=2)
    edge_row = jnp.zeros_like(energy[:, :1])
    south_cell = jnp.concatenate([edge_row, energy[:, :-1]], axis=1)
    north_cell = jnp.concatenate([energy[:, 1:], edge_row], axis=1)
    updated = (
        energy
        - jnp.maximum(courant_x, 0.0) * (energy - west_cell)
        - jnp.minimum(courant_x, 0.0) * (east_cell - energy)
        - jnp.maximum(courant_y, 0.0) * (energy - south_cell)
        - jnp.minimum(courant_y, 0.0) * (north_cell - energy)
    )
    return updated * sea_grid


def courant_numbers(freq_index, dir_index, lat_count, dir_count):
    speed = 0.2 * jnp.exp(-math.log(1.1) * freq_index)
    heading = 2.0 * math.pi * (dir_index + 0.5) / dir_count
    rows = jnp.arange(lat_count, dtype=jnp.float32)
    latitude = (-75.0 + 150.0 * (rows + 0.5) / lat_count) * (math.pi / 180.0)
    courant_x = (speed * jnp.cos(heading))[:, None, None] / jnp.cos(latitude)[None, :, None]
    courant_y = (speed * jnp.sin(heading))[:, None, None]
    return (courant_x, courant_y)


def shift_freq(values, amount):
    if amount > 0:
        filler = jnp.zeros_like(values[:amount])
        return jnp.concatenate([filler, values[:-amount]], axis=0)
    filler = jnp.zeros_like(values[:-amount])
    return jnp.concatenate([values[-amount:], filler], axis=0)


def source_terms(energy, speed, angle):
    freq_count = energy.shape[0]
    dir_count = energy.shape[1]
    freq_ids = jnp.arange(freq_count, dtype=jnp.float32)
    frequency = jnp.exp(math.log(1.1) * (freq_ids - freq_count // 2))[:, None, None]
    heading = (2.0 * math.pi * (jnp.arange(dir_count, dtype=jnp.float32) + 0.5) / dir_count)[
        None, :, None
    ]
    energy_mean = jnp.mean(energy, axis=(0, 1))
    moment_one = jnp.mean(frequency * energy, axis=(0, 1))
    mean_freq = moment_one / (energy_mean + 1e-06)
    steepness = energy_mean * mean_freq * mean_freq
    breaking = steepness * steepness / (1.0 + steepness * steepness)
    wind_gain = (
        0.05
        * frequency
        * jnp.maximum(
            0.0, speed[None, None, :] * frequency * jnp.cos(heading - angle[None, None, :]) - 1.0
        )
    )
    damping = 0.03 * frequency * breaking[None, None, :]
    valid = ((freq_ids >= 3) & (freq_ids <= freq_count - 3)).astype(jnp.float32)[:, None, None]
    interaction = jnp.zeros_like(energy)
    for mirror in (1, -1):
        plus_bins = shift_freq(jnp.roll(energy, -mirror, axis=1), -2)
        minus_bins = shift_freq(jnp.roll(energy, 3 * mirror, axis=1), 3)
        transfer_rate = (
            0.001
            * valid
            * (energy * energy * (plus_bins + minus_bins) - 2.0 * energy * plus_bins * minus_bins)
        )
        interaction = interaction - 2.0 * transfer_rate
        interaction = interaction + jnp.roll(shift_freq(transfer_rate, 2), mirror, axis=1)
        interaction = interaction + jnp.roll(shift_freq(transfer_rate, -3), -3 * mirror, axis=1)
    updated = energy + (wind_gain - damping) * energy + interaction
    raw_height = 4.0 * jnp.sqrt(jnp.mean(updated, axis=(0, 1)) + 1e-06)
    return (updated, raw_height)


def local(spectrum, sea_mask, wind_speed, wind_angle):
    count = lax.axis_size("spec")
    position = lax.axis_index("spec")
    bins_dev = spectrum.shape[0]
    cells = spectrum.shape[1]
    points = cells // count
    lat_count = cells // NLON
    sea_float = sea_mask.astype(jnp.float32)
    bin_ids = position * bins_dev + jnp.arange(bins_dev, dtype=jnp.int32)
    freq_index = (bin_ids // ND).astype(jnp.float32)
    dir_index = (bin_ids % ND).astype(jnp.float32)
    courant_x, courant_y = courant_numbers(freq_index, dir_index, lat_count, ND)
    sea_grid = sea_float.reshape(1, lat_count, NLON)
    energy = (spectrum * sea_float[None, :]).reshape(bins_dev, lat_count, NLON)
    for substep in range(ADV_STEPS):
        energy = upwind_step(energy, courant_x, courant_y, sea_grid)
    advected = energy.reshape(bins_dev, cells)
    outgoing = advected.reshape(bins_dev, count, points)
    arrived = lax.all_to_all(outgoing, "spec", split_axis=1, concat_axis=0, tiled=True)
    start = position * points
    speed_own = lax.dynamic_slice_in_dim(wind_speed, start, points)
    angle_own = lax.dynamic_slice_in_dim(wind_angle, start, points)
    sea_own = lax.dynamic_slice_in_dim(sea_float, start, points)
    updated, raw_height = source_terms(arrived.reshape(NF, ND, points), speed_own, angle_own)
    wave_height = sea_own * raw_height
    own_total = jnp.zeros((count, 1), jnp.float32) + jnp.sum(wave_height)
    returned, totals = (
        lax.all_to_all(
            updated.reshape(NF * ND, 1, points), "spec", split_axis=0, concat_axis=1, tiled=True
        ),
        lax.all_to_all(own_total, "spec", split_axis=0, concat_axis=1, tiled=True),
    )
    new_spectrum = returned.reshape(bins_dev, cells)
    height_sum = jnp.sum(totals)
    mean_height = (height_sum / (SEA_DEV * count)).reshape(1)
    return (new_spectrum, wave_height, mean_height)


HALO = 5
LANES = 128
WIDE = 256
LAND = 4096.0
UNROLL = 3


def group_size(count, bins_dev, cells):
    size = 4
    if count % size or bins_dev % ND or cells % (size * LANES) or cells % NLON:
        return 0
    if NLON % LANES or bins_dev // ND * size < 2 * HALO or cells % count:
        return 0
    sea = SEA_DEV * count
    if sea > min(cells, LAND) or sea % (size * LANES) or sea % WIDE or cells % WIDE:
        return 0
    if (cells - sea) % WIDE:
        return 0
    return size


def split_bf16(values):
    high = values.astype(jnp.bfloat16)
    left = values - high.astype(jnp.float32)
    mid = left.astype(jnp.bfloat16)
    low = (left - mid.astype(jnp.float32)).astype(jnp.bfloat16)
    return high, mid, low


def rows_of(parts, height, width):
    ids = lax.broadcasted_iota(jnp.int32, (height, width), 0)
    out = jnp.zeros((height, width), jnp.float32)
    for i, part in enumerate(parts):
        out = jnp.where(ids == i, jnp.broadcast_to(part.astype(jnp.float32), (height, width)), out)
    return out.astype(jnp.bfloat16)


def window_start(count, me, cells):
    return jnp.minimum(me * (cells // count) // LANES * LANES, cells - WIDE)


def fused_kernel(
    count, group, sea_in, wind_in, angle_in, spec_ref, full_ref, height_ref, near_ref,
    sea_raw, wind_raw, angle_raw, aux_ref, place_ref, spread_ref, aux_sem,
    raw, moved, split, wsplit, adv, held, done, back, mom_out, mom_in, wind, acc,
    sum_out, sum_in, damp_out, damp_in,
    load_sem, held_sem, halo_sem, y_sem, z_sem, chain_sem, mom_send, mom_recv,
    ret_send, ret_recv, sum_send, sum_recv, damp_send, damp_recv,
):
    f32, bf16 = jnp.float32, jnp.bfloat16
    freq_dev, _, sea_cells = adv.shape
    bins_dev, cells = moved.shape
    freq_group = freq_dev * group
    width = sea_cells // group
    zones = count // group
    lat_count = cells // NLON
    sides = group // 2
    parts = width // LANES
    cell_tiles = cells // LANES
    land = cells - sea_cells
    reach = land + WIDE
    me = lax.axis_index("spec")
    zone, rank = me // group, me % group
    side, core = rank // 2, rank % 2

    def remote(src, dst, send, recv, target):
        return pltpu.make_async_remote_copy(
            src_ref=src, dst_ref=dst, send_sem=send, recv_sem=recv,
            device_id={"spec": target}, device_id_type=pl.DeviceIdType.MESH,
        )

    loads = [
        pltpu.make_async_copy(
            spec_ref.at[pl.ds(f * ND, ND)], raw.at[pl.ds(f * ND, ND)], load_sem.at[f]
        )
        for f in range(freq_dev)
    ]
    small = [
        pltpu.make_async_copy(sea_in, sea_raw, aux_sem.at[0]),
        pltpu.make_async_copy(wind_in, wind_raw, aux_sem.at[1]),
        pltpu.make_async_copy(angle_in, angle_raw, aux_sem.at[2]),
    ]
    for load in small[:1] + loads + small[1:]:
        load.start()
    barrier = pltpu.get_barrier_semaphore()

    def signal(semaphore, target):
        pl.semaphore_signal(
            semaphore, inc=1, device_id={"spec": target}, device_id_type=pl.DeviceIdType.MESH
        )

    for step in range(1, group):
        signal(barrier, zone * group + (rank + step) % group)

    @pl.when(zone > 0)
    def _():
        for c in range(2):
            signal(barrier, (zone - 1) * group + side * 2 + c)

    @pl.when(zone < zones - 1)
    def _():
        for c in range(2):
            signal(barrier, (zone + 1) * group + side * 2 + c)

    @pl.when(zone == 0)
    def _():
        held[0:HALO] = jnp.zeros((HALO, ND, width), f32)

    @pl.when(zone == zones - 1)
    def _():
        held[HALO + freq_group :] = jnp.zeros((HALO, ND, width), f32)

    def block_of(index, t):
        return t * group + index

    def tile_of(index, t):
        return pl.ds(pl.multiple_of(block_of(index, t) * LANES, LANES), LANES)

    def lanes_of(t):
        return pl.ds(t * LANES, LANES)

    offsets = [(dy, dc) for dy in range(sides) for dc in range(2)]

    def rank_of(offset):
        return (side + offset[0]) % sides * 2 + (core + offset[1]) % 2

    def y_copy(begin, end, peer, t):
        return remote(
            adv.at[begin:end, :, tile_of(peer, t)],
            held.at[pl.ds(HALO + rank * freq_dev + begin, end - begin), :, lanes_of(t)],
            y_sem, held_sem.at[rank, t], zone * group + peer,
        )

    dirs = lax.broadcasted_iota(jnp.int32, (ND, LANES), 0).astype(f32)
    heading = 2.0 * math.pi * (dirs + 0.5) / ND
    cos_h, sin_h = jnp.cos(heading), jnp.sin(heading)
    log_step = math.log(1.1)
    lats = [math.radians(-75.0 + 150.0 * (r + 0.5) / lat_count) for r in range(lat_count)]

    def omega_of(freq, shape):
        return jnp.exp(jnp.full(shape, log_step, f32) * (freq.astype(f32) - NF // 2))

    square_rows = lax.broadcasted_iota(jnp.int32, (LANES, LANES), 0)
    square_cols = lax.broadcasted_iota(jnp.int32, (LANES, LANES), 1)
    small[0].wait()
    aux_ref[...] = sea_raw[...].astype(f32).reshape(1, cells)
    sea = [aux_ref[0:1, r * NLON : (r + 1) * NLON] for r in range(lat_count)]
    mask = [aux_ref[0:1, i * LANES : (i + 1) * LANES] for i in range(cell_tiles)]
    tri_up = jnp.where(square_rows < square_cols, 1.0, 0.0).astype(bf16)
    ranks = jnp.dot(rows_of(mask, ND // 2, LANES), tri_up, preferred_element_type=f32)
    before = jnp.zeros((1, 1), f32)
    for i in range(cell_tiles):
        place_ref[0:1, i * LANES : (i + 1) * LANES] = jnp.where(
            mask[i] > 0.0, ranks[i : i + 1] + before, LAND
        )
        before = before + jnp.sum(mask[i], axis=1, keepdims=True)
    pair_rows = lax.broadcasted_iota(jnp.int32, (WIDE, reach), 0).astype(f32)

    def build(pair):
        cols = pl.ds(pl.multiple_of(pair * WIDE, LANES), reach)
        first = (pair * WIDE).astype(f32)
        hit = jnp.where(place_ref[0:1, cols] - first == pair_rows, 1.0, 0.0)
        spread_ref[pl.ds(pl.multiple_of(pair * WIDE, LANES), WIDE), cols] = hit.astype(
            spread_ref.dtype
        )

    def packed(values, pair):
        cols = pl.ds(pl.multiple_of(pair * WIDE, LANES), reach)
        return lax.dot_general(
            values[:, cols],
            spread_ref[pl.ds(pl.multiple_of(pair * WIDE, LANES), WIDE), cols],
            (((1,), (1,)), ((), ())), preferred_element_type=f32,
        )

    quarter = ND // 4
    tiles = NLON // LANES
    def advect(f):
        loads[f].wait()
        freq = (me * freq_dev + f).astype(f32)
        speed = 0.2 * jnp.exp(jnp.full((quarter, LANES), -log_step, f32) * freq)
        for q in range(4):
            east, north = q in (0, 3), q in (0, 1)
            rows = slice(f * ND + q * quarter, f * ND + (q + 1) * quarter)
            part = slice(q * quarter, (q + 1) * quarter)
            cx0 = speed * jnp.abs(cos_h[part])
            cy = jnp.concatenate([speed * jnp.abs(sin_h[part])] * tiles, axis=1)
            cx = [jnp.concatenate([cx0 * (1.0 / math.cos(a))] * tiles, axis=1) for a in lats]
            rest = [1.0 - (cx[r] + cy) for r in range(lat_count)]
            energy = [raw[rows, r * NLON : (r + 1) * NLON] * sea[r] for r in range(lat_count)]
            for step in range(ADV_STEPS):
                fresh = []
                for r in range(lat_count):
                    e = energy[r]
                    side_x = pltpu.roll(e, 1 if east else NLON - 1, 1)
                    other = r - 1 if north else r + 1
                    value = rest[r] * e + cx[r] * side_x
                    if 0 <= other < lat_count:
                        value = value + cy * energy[other]
                    fresh.append(value if step == ADV_STEPS - 1 else value * sea[r])
                energy = fresh
            for r in range(lat_count):
                moved[rows, r * NLON : (r + 1) * NLON] = energy[r]
        for i, piece in enumerate(split_bf16(moved[f * ND : (f + 1) * ND])):
            split[(3 * f + i) * ND : (3 * f + i + 1) * ND, :] = piece

    def cols_of(index):
        return pl.ds(pl.multiple_of(index * LANES, LANES), LANES)

    def side_of(dy):
        return (side + dy) % sides

    def pack(t, dy, begin, end):
        return packed(split.at[begin * 3 * ND : end * 3 * ND], t * sides + side_of(dy))

    def unload(t, dy, begin, end, got):
        pair = t * sides + side_of(dy)
        cols = pl.ds(pl.multiple_of(pair * WIDE, LANES), WIDE)
        here = pl.ds(pl.multiple_of(side_of(dy) * WIDE, LANES), WIDE)
        mass, moment = None, None
        for f in range(begin, end):
            base = (f - begin) * 3 * ND
            piece = got[base : base + ND] + got[base + ND : base + 2 * ND] + (
                got[base + 2 * ND : base + 3 * ND]
            )
            adv[f, :, cols] = piece
            total = jnp.sum(piece, axis=0, keepdims=True)
            scaled = omega_of(me * freq_dev + f, (1, WIDE)) * total
            mass = total if mass is None else mass + total
            moment = scaled if moment is None else moment + scaled
        if begin:
            mass, moment = mass + mom_out[t, 0:1, here], moment + mom_out[t, 1:2, here]
        mom_out[t, 0:1, here] = mass
        mom_out[t, 1:2, here] = moment

    def send_far(t, dy, begin, end):
        for c in range(2):
            y_copy(begin, end, side_of(dy) * 2 + c, t).start()

    top = side > 0
    early_way, late_way = jnp.where(top, 0, 1), jnp.where(top, 1, 0)
    early_ok = jnp.where(top, zone < zones - 1, zone > 0)
    late_ok = jnp.where(top, zone > 0, zone < zones - 1)
    early_zone = jnp.where(top, zone + 1, zone + zones - 1) % zones
    late_zone = jnp.where(top, zone + zones - 1, zone + 1) % zones
    early_shift = HALO + jnp.where(top, -freq_group, freq_group)
    late_shift = HALO + jnp.where(top, freq_group, -freq_group)

    def early_slot(slot):
        return early_ok & jnp.where(top, slot >= freq_group - HALO, slot < HALO)

    def late_slot(slot):
        return late_ok & jnp.where(top, slot < HALO, slot >= freq_group - HALO)

    def early_copy(f, c, t):
        return remote(
            adv.at[f, :, tile_of(side * 2 + c, t)],
            held.at[early_shift + rank * freq_dev + f, :, lanes_of(t)],
            z_sem.at[0], halo_sem.at[early_way, t], early_zone * group + side * 2 + c,
        )

    def forward(slot, t):
        @pl.when(late_slot(slot))
        def _():
            remote(
                held.at[HALO + slot, :, lanes_of(t)],
                held.at[late_shift + slot, :, lanes_of(t)],
                z_sem.at[1], halo_sem.at[late_way, t], late_zone * group + rank,
            ).start()

    def send_near(t):
        for c in range(2):
            for f in range(freq_dev):
                @pl.when(early_slot(rank * freq_dev + f))
                def _():
                    early_copy(f, c, t).start()

        y_copy(0, freq_dev, rank_of((0, 1)), t).start()
        for f in range(freq_dev):
            held[HALO + rank * freq_dev + f, :, lanes_of(t)] = adv[f, :, tile_of(rank, t)]

    def arrive_group(dy, t):
        for dc in range(2):
            if (dy, dc) != (0, 0):
                source = rank_of((dy, dc))
                slots = held.at[
                    pl.ds(HALO + source * freq_dev, freq_dev), :, lanes_of(t)
                ]
                remote(
                    slots, slots, y_sem, held_sem.at[source, t], (me + 1) % count
                ).wait_recv()
                if dy and t < parts - 1:
                    for f in range(freq_dev):
                        forward(source * freq_dev + f, t)

    def up_relay(level):
        @pl.when(zone == level)
        def _():
            pl.semaphore_wait(chain_sem.at[0], 1)
            if level < zones - 1:
                signal(chain_sem.at[0], (me + group) % count)

    def down_relay(level):
        @pl.when(zone == level)
        def _():
            pl.semaphore_wait(chain_sem.at[1], 1)
            if level > 0:
                signal(chain_sem.at[1], (me + count - group) % count)

    def moment_copy(target_zone, target_rank):
        return remote(
            mom_out.at[:, :, cols_of(target_rank)], mom_in.at[me],
            mom_send, mom_recv, target_zone * group + target_rank,
        )

    def send_zone_moments():
        for step in range(1, group):
            moment_copy(zone, (rank + step) % group).start()

    def send_moments():
        for away in range(1, zones):
            for other in range(group):
                moment_copy((zone + away) % zones, other).start()

    far = list(range(1, sides))
    for dy in far:
        build(side_of(dy))
    advect(0)
    for dy in far:
        unload(0, dy, 0, 1, pack(0, dy, 0, 1))
    advect(1)
    pl.semaphore_wait(
        barrier, group - 1 + jnp.where(zone > 0, 2, 0) + jnp.where(zone < zones - 1, 2, 0)
    )
    for dy in far:
        send_far(0, dy, 0, 1)

    @pl.when(zone == 0)
    def _():
        signal(chain_sem.at[0], (me + group) % count)

    @pl.when(zone == zones - 1)
    def _():
        signal(chain_sem.at[1], (me + count - group) % count)

    up_relay(1)
    for f in range(2, freq_dev):
        advect(f)
    for level in range(2, zones - 1):
        up_relay(level)
    got = [pack(0, dy, 1, freq_dev) for dy in far]
    build(side)
    got_near = pack(0, 0, 0, freq_dev)
    for dy in far:
        unload(0, dy, 1, freq_dev, got[dy - 1])
        send_far(0, dy, 1, freq_dev)
    unload(0, 0, 0, freq_dev, got_near)
    send_near(0)
    down_relay(zones - 2)
    upper = zone >= zones // 2
    for t in range(1, parts):
        last = t == parts - 1
        for dy in far:
            build(t * sides + side_of(dy))
        got = [pack(t, dy, 0, freq_dev) for dy in far]
        build(t * sides + side)
        got_near = pack(t, 0, 0, freq_dev)
        for dy in far:
            unload(t, dy, 0, freq_dev, got[dy - 1])

            @pl.when(jnp.logical_not(upper) if last else zone >= 0)
            def _():
                send_far(t, dy, 0, freq_dev)

        unload(t, 0, 0, freq_dev, got_near)
        if last:
            up_relay(zones - 1)
            send_zone_moments()

            @pl.when(upper)
            def _():
                send_moments()
                for dy in far:
                    send_far(t, dy, 0, freq_dev)

        send_near(t)

    small[1].wait()
    small[2].wait()
    speed_all = wind_raw[...].reshape(1, cells)
    angle_all = angle_raw[...].reshape(1, cells)
    wsplit[...] = rows_of(
        split_bf16(speed_all * jnp.cos(angle_all)) + split_bf16(speed_all * jnp.sin(angle_all)),
        2 * quarter, cells,
    )
    for t in range(parts):
        own = packed(wsplit, t * sides + side)
        own = jnp.where(core == 0, own[:, :LANES], own[:, LANES:])
        along = own[0:1] + own[1:2] + own[2:3]
        across = own[3:4] + own[4:5] + own[5:6]
        wind[:, t * LANES : (t + 1) * LANES] = cos_h * along + sin_h * across

    for level in range(zones - 3, 0, -1):
        down_relay(level)

    @pl.when(jnp.logical_not(upper) & (zone > 0))
    def _():
        send_moments()

    for dy in far:
        arrive_group(dy, 0)
    mom_in[me] = mom_out[:, :, cols_of(rank)]
    start = window_start(count, me, cells)
    near_ref[...] = place_ref[0:1, pl.ds(pl.multiple_of(start, LANES), WIDE)]
    for t in range(parts):
        arrive_group(0, t)

    acc[...] = jnp.zeros_like(acc)
    ascending = side > 0

    def arrive_halo(at_top, t):
        block = held.at[0:HALO, :, lanes_of(t)]

        @pl.when(jnp.where(at_top, zone < zones - 1, zone > 0))
        def _():
            way = jnp.where(at_top, 1, 0)
            remote(
                block, block, z_sem.at[0], halo_sem.at[way, t], (me + 1) % count
            ).wait_recv()

    def ret_copy(owner, t):
        return remote(
            done.at[pl.ds(owner * freq_dev, freq_dev), :, lanes_of(t)],
            back.at[:, :, tile_of(rank, t)],
            ret_send, ret_recv.at[t], zone * group + owner,
        )

    def turn(values, amount):
        return pltpu.roll(values, amount % ND, 0)

    def rate(a, p, m):
        return a * (a * (p + m) - 2.0 * (p * m))

    def scale(index, factor):
        return jnp.where((index >= 3) & (index <= NF - 3), factor, 0.0).astype(f32)

    def slab(k, t):
        return held[HALO + k, :, t * LANES : (t + 1) * LANES]

    def rates(own, p2, m3):
        return rate(own, turn(p2, -1), turn(m3, 3)) + rate(own, turn(p2, 1), turn(m3, -3))

    def grown(own, freq, t):
        omega = omega_of(freq, (1, LANES))
        push = wind[:, t * LANES : (t + 1) * LANES] * omega - 1.0
        return own + (0.05 * omega) * jnp.maximum(0.0, push) * own

    def tally(energy, near, freq, t):
        flow = scale(freq, 0.001) * near
        acc[:, t * LANES : (t + 1) * LANES] += energy + (flow + flow - 2.0 * flow)

    def sources(t, begin, end):
        def source_step(i, carry):
            k = jnp.where(ascending, i, freq_group - 1 - i)
            freq = zone * freq_group + k
            own = slab(k, t)
            p2, m3, m2, m5, p3, p5 = (slab(k + shift, t) for shift in (2, -3, -2, -5, 3, 5))
            near = rates(own, p2, m3)
            low = rate(turn(m2, 1), own, turn(m5, 4)) + rate(turn(m2, -1), own, turn(m5, -4))
            high = rate(turn(p3, -3), turn(p5, -4), own) + rate(turn(p3, 3), turn(p5, 4), own)
            interaction = scale(freq, -0.002) * near + scale(freq - 2, 0.001) * low + (
                scale(freq + 3, 0.001) * high
            )
            energy = grown(own, freq, t)
            done[k, :, t * LANES : (t + 1) * LANES] = energy + interaction
            if begin == 0:
                tally(energy, near, freq, t)
            return carry

        lax.fori_loop(begin, end, source_step, 0, unroll=UNROLL)

    def tally_rest(t):
        def rest_step(i, carry):
            k = jnp.where(ascending, half + i, half - 1 - i)
            center = jnp.where(
                ascending,
                jnp.where(i < 2, i - 2, half + i - 2),
                jnp.where(i < 3, freq_group + i, half + 2 - i),
            )
            near = rates(slab(center, t), slab(center + 2, t), slab(center - 3, t))
            energy = grown(slab(k, t), zone * freq_group + k, t)
            tally(energy, near, zone * freq_group + center, t)
            return carry

        lax.fori_loop(0, half, rest_step, 0, unroll=UNROLL)

    half = freq_group // 2
    near_side = rank_of((0, 1))

    def first_half(t):
        arrive_halo(jnp.logical_not(ascending), t)
        sources(t, 0, half)
        if t == parts - 1:
            tally_rest(t)
            send_sums()
        for dy in range(1, sides):
            for dc in range(2):
                ret_copy(rank_of((dy, dc)), t).start()
        if t == parts - 1:
            for slot_rank in range(group):
                for f in range(freq_dev):
                    @pl.when(side != slot_rank // 2)
                    def _():
                        forward(slot_rank * freq_dev + f, t)

        if t == 0:
            down_relay(0)

            @pl.when(zone == 0)
            def _():
                send_moments()

        if t < parts - 1:
            tally_rest(t)

    def send_sums():
        sum_out[...] = jnp.sum(acc[...], axis=0, keepdims=True)
        for step in range(1, count):
            remote(sum_out, sum_in.at[me], sum_send, sum_recv, (me + step) % count).start()
        sum_in[me] = sum_out[...]

    def second_half(t):
        if t == parts - 1:
            damping_terms()
        arrive_halo(ascending, t)
        sources(t, half, freq_group)
        ret_copy(near_side, t).start()
        back[:, :, tile_of(rank, t)] = done[
            pl.ds(rank * freq_dev, freq_dev), :, lanes_of(t)
        ]

    def zone_copy(dst_rank, src, dst, send, recv):
        return remote(src, dst, send, recv, zone * group + dst_rank)

    def damping_terms():
        others = mom_in.at[0 : count - 1]
        remote(others, others, mom_send, mom_recv, (me + 1) % count).wait_recv()
        total = jnp.sum(mom_in[...], axis=0) * (1.0 / (NF * ND))
        for t in range(parts):
            energy_mean, moment_one = total[t, 0:1], total[t, 1:2]
            mean_freq = moment_one / (energy_mean + 1e-06)
            steepness = energy_mean * mean_freq * mean_freq
            breaking = steepness * steepness / (1.0 + steepness * steepness)
            damp_out[t, 0:1] = 0.03 * breaking
            damp_out[t, 1:2] = 0.03 * breaking * moment_one
        for i in range(1, group):
            zone_copy(
                rank_of(offsets[i]), damp_out, damp_in.at[rank], damp_send, damp_recv
            ).start()
        damp_in[rank] = damp_out[...]

    first_half(0)
    for t in range(1, parts):
        for dy in range(1, sides):
            arrive_group(dy, t)
        first_half(t)
        second_half(t - 1)
    second_half(parts - 1)

    others = damp_in.at[0 : group - 1]
    remote(others, others, damp_send, damp_recv, (me + 1) % count).wait_recv()

    def finish(t):
        block = done.at[0 : (group - 1) * freq_dev, :, lanes_of(t)]
        remote(block, block, ret_send, ret_recv.at[t], (me + 1) % count).wait_recv()
        for f in range(freq_dev):
            omega = omega_of(me * freq_dev + f, (1, LANES))
            for g in range(group):
                cols = slice(block_of(g, t) * LANES, (block_of(g, t) + 1) * LANES)
                value = back[f, :, cols] - (omega * damp_in[g, t, 0:1]) * adv[f, :, cols]
                for i, piece in enumerate(split_bf16(value)):
                    split[(3 * f + i) * ND : (3 * f + i + 1) * ND, cols] = piece
        ready = (t + 1) * group * LANES
        for j in range(cells // WIDE):
            low, high = max(0, j * WIDE - land), min(sea_cells, (j + 1) * WIDE)
            if high > ready or high <= t * group * LANES:
                continue
            cols = slice(j * WIDE, (j + 1) * WIDE)
            got = jnp.dot(
                split[:, low:high], spread_ref[low:high, cols], preferred_element_type=f32
            )
            for f in range(freq_dev):
                base = 3 * f * ND
                full_ref[f * ND : (f + 1) * ND, cols] = got[base : base + ND] + (
                    got[base + ND : base + 2 * ND]
                ) + got[base + 2 * ND : base + 3 * ND]

    for t in range(parts):
        finish(t)

    block = held.at[0 : (group - 1) * freq_dev]
    remote(block, block, y_sem, held_sem.at[0, 0], (me + 1) % count).wait_send()
    remote(block, block, ret_send, ret_recv.at[0], (me + 1) % count).wait_send()
    others = mom_in.at[0 : count - 1]
    remote(others, others, mom_send, mom_recv, (me + 1) % count).wait_send()
    others = damp_in.at[0 : group - 1]
    remote(others, others, damp_send, damp_recv, (me + 1) % count).wait_send()
    def drain(slots, way):
        block = held.at[0:slots]
        remote(
            block, block, z_sem.at[way], halo_sem.at[0, 0], (me + 1) % count
        ).wait_send()

    for f in range(freq_dev):
        @pl.when(early_slot(rank * freq_dev + f))
        def _():
            drain(2, 0)

    @pl.when(late_ok)
    def _():
        drain(HALO, 1)

    others = sum_in.at[0 : count - 1]
    remote(others, others, sum_send, sum_recv, (me + 1) % count).wait()
    for g in range(group):
        mass = sum_in[g]
        for other in range(1, zones):
            mass = mass + sum_in[other * group + g]
        for t in range(parts):
            mean = mass[:, t * LANES : (t + 1) * LANES] * (1.0 / (NF * ND)) - damp_in[g, t, 1:2]
            cols = slice(block_of(g, t) * LANES, (block_of(g, t) + 1) * LANES)
            height_ref[0:1, cols] = 4.0 * jnp.sqrt(mean + 1e-06)


def store_kernel(
    count, full_in, height_in, near_in, new_out, wave_out, mean_out, wave_ref, mean_ref, sem
):
    cells = full_in.shape[1]
    sea_cells = height_in.shape[1]
    copies = [
        pltpu.make_async_copy(full_in, new_out, sem.at[0]),
        pltpu.make_async_copy(wave_ref, wave_out, sem.at[1]),
        pltpu.make_async_copy(mean_ref, mean_out, sem.at[2]),
    ]
    copies[0].start()
    me = lax.axis_index("spec")
    points = cells // count
    shift = me * points - window_start(count, me, cells)
    halves = []
    for h in range(WIDE // LANES):
        place = jnp.broadcast_to(near_in[:, h * LANES : (h + 1) * LANES], (8, LANES))
        place = place.astype(jnp.int32)
        wave = jnp.zeros((8, LANES), jnp.float32)
        for b in range(sea_cells // LANES):
            values = jnp.broadcast_to(height_in[:, b * LANES : (b + 1) * LANES], (8, LANES))
            found = jnp.take_along_axis(values, place % LANES, axis=1)
            wave = jnp.where(place // LANES == b, found, wave)
        halves.append(wave)
    wave = jnp.concatenate(halves, axis=1)
    wave_ref[...] = pltpu.roll(wave, (WIDE - shift) % WIDE, 1)[0, :points]
    copies[1].start()
    mean_ref[...] = jnp.sum(height_in[...], axis=1, keepdims=True) * (1.0 / sea_cells)
    copies[2].start()
    for copy in copies:
        copy.wait()


def fused_local(spectrum, sea_mask, wind_speed, wind_angle):
    count = lax.axis_size("spec")
    bins_dev, cells = spectrum.shape
    group = group_size(count, bins_dev, cells)
    freq_dev = bins_dev // ND
    freq_group = freq_dev * group
    sea_cells = SEA_DEV * count
    width = sea_cells // group
    points = cells // count
    parts = width // LANES
    f32, bf16 = jnp.float32, jnp.bfloat16
    dma = pltpu.SemaphoreType.DMA
    vmem = pl.BlockSpec(memory_space=pltpu.VMEM)
    handed = pl.pallas_call(
        functools.partial(fused_kernel, count, group),
        out_shape=(
            pltpu.VMEM((bins_dev, cells), f32),
            pltpu.VMEM((1, sea_cells), f32),
            pltpu.VMEM((1, WIDE), f32),
        ),
        in_specs=[pl.BlockSpec(memory_space=pl.ANY)] * 4,
        out_specs=(vmem,) * 3,
        scratch_shapes=[
            pltpu.VMEM((cells,), jnp.int32),
            pltpu.VMEM((cells,), f32),
            pltpu.VMEM((cells,), f32),
            pltpu.VMEM((1, cells), f32),
            pltpu.VMEM((1, cells), f32),
            pltpu.VMEM((sea_cells, cells), jnp.float8_e4m3fn),
            dma((3,)),
            pltpu.VMEM((bins_dev, cells), f32),
            pltpu.VMEM((bins_dev, cells), f32),
            pltpu.VMEM((3 * bins_dev, cells), bf16),
            pltpu.VMEM((ND // 2, cells), bf16),
            pltpu.VMEM((freq_dev, ND, sea_cells), f32),
            pltpu.VMEM((freq_group + 2 * HALO, ND, width), f32),
            pltpu.VMEM((freq_group, ND, width), f32),
            pltpu.VMEM((freq_dev, ND, sea_cells), f32),
            pltpu.VMEM((parts, 2, group * LANES), f32),
            pltpu.VMEM((count, parts, 2, LANES), f32),
            pltpu.VMEM((ND, width), f32),
            pltpu.VMEM((ND, width), f32),
            pltpu.VMEM((1, width), f32),
            pltpu.VMEM((count, 1, width), f32),
            pltpu.VMEM((parts, 2, LANES), f32),
            pltpu.VMEM((group, parts, 2, LANES), f32),
            dma((freq_dev,)),
            dma((group, parts)),
            dma((2, parts)),
            dma,
            dma((2,)),
            pltpu.SemaphoreType.REGULAR((2,)),
            dma,
            dma,
            dma,
            dma((parts,)),
            dma,
            dma,
            dma,
            dma,
        ],
        compiler_params=pltpu.CompilerParams(collective_id=0, has_side_effects=True),
    )(sea_mask, wind_speed, wind_angle, spectrum)
    out, wave, mean = pl.pallas_call(
        functools.partial(store_kernel, count),
        out_shape=(
            pltpu.HBM((bins_dev, cells), f32),
            pltpu.HBM((points,), f32),
            pltpu.HBM((1, 1), f32),
        ),
        in_specs=[vmem] * 3,
        out_specs=(pl.BlockSpec(memory_space=pltpu.HBM),) * 3,
        scratch_shapes=[pltpu.VMEM((points,), f32), pltpu.VMEM((1, 1), f32), dma((3,))],
    )(*[pltpu.with_memory_space_constraint(piece, pltpu.VMEM) for piece in handed])
    return (out, wave, mean.reshape(1))


def solution(mesh):
    in_specs = (P(("grp", "spec"), None), P(), P("grp"), P("grp"))
    out_specs = (P(("grp", "spec"), None), P(("grp", "spec")), P("grp"))

    def body(spectrum, sea_mask, wind_speed, wind_angle):
        fits = group_size(mesh.shape["spec"], *spectrum.shape)
        plan = fused_local if fits else local
        return plan(spectrum, sea_mask, wind_speed, wind_angle)

    return jax.shard_map(body, mesh=mesh, in_specs=in_specs, out_specs=out_specs, check_vma=False)
```

```python
import functools
import math

import jax
import jax.numpy as jnp
from jax import lax
from jax.experimental import pallas as pl
from jax.experimental.pallas import tpu as pltpu
from jax.sharding import PartitionSpec as P

NF = 48
ND = 32
NLON = 384
ADV_STEPS = 2
SEA_DEV = 64


def upwind_step(energy, courant_x, courant_y, sea_grid):
    west_cell = jnp.roll(energy, 1, axis=2)
    east_cell = jnp.roll(energy, -1, axis=2)
    edge_row = jnp.zeros_like(energy[:, :1])
    south_cell = jnp.concatenate([edge_row, energy[:, :-1]], axis=1)
    north_cell = jnp.concatenate([energy[:, 1:], edge_row], axis=1)
    updated = (
        energy
        - jnp.maximum(courant_x, 0.0) * (energy - west_cell)
        - jnp.minimum(courant_x, 0.0) * (east_cell - energy)
        - jnp.maximum(courant_y, 0.0) * (energy - south_cell)
        - jnp.minimum(courant_y, 0.0) * (north_cell - energy)
    )
    return updated * sea_grid


def courant_numbers(freq_index, dir_index, lat_count, dir_count):
    speed = 0.2 * jnp.exp(-math.log(1.1) * freq_index)
    heading = 2.0 * math.pi * (dir_index + 0.5) / dir_count
    rows = jnp.arange(lat_count, dtype=jnp.float32)
    latitude = (-75.0 + 150.0 * (rows + 0.5) / lat_count) * (math.pi / 180.0)
    courant_x = (speed * jnp.cos(heading))[:, None, None] / jnp.cos(latitude)[None, :, None]
    courant_y = (speed * jnp.sin(heading))[:, None, None]
    return (courant_x, courant_y)


def shift_freq(values, amount):
    if amount > 0:
        filler = jnp.zeros_like(values[:amount])
        return jnp.concatenate([filler, values[:-amount]], axis=0)
    filler = jnp.zeros_like(values[:-amount])
    return jnp.concatenate([values[-amount:], filler], axis=0)


def source_terms(energy, speed, angle):
    freq_count = energy.shape[0]
    dir_count = energy.shape[1]
    freq_ids = jnp.arange(freq_count, dtype=jnp.float32)
    frequency = jnp.exp(math.log(1.1) * (freq_ids - freq_count // 2))[:, None, None]
    heading = (2.0 * math.pi * (jnp.arange(dir_count, dtype=jnp.float32) + 0.5) / dir_count)[
        None, :, None
    ]
    energy_mean = jnp.mean(energy, axis=(0, 1))
    moment_one = jnp.mean(frequency * energy, axis=(0, 1))
    mean_freq = moment_one / (energy_mean + 1e-06)
    steepness = energy_mean * mean_freq * mean_freq
    breaking = steepness * steepness / (1.0 + steepness * steepness)
    wind_gain = (
        0.05
        * frequency
        * jnp.maximum(
            0.0, speed[None, None, :] * frequency * jnp.cos(heading - angle[None, None, :]) - 1.0
        )
    )
    damping = 0.03 * frequency * breaking[None, None, :]
    valid = ((freq_ids >= 3) & (freq_ids <= freq_count - 3)).astype(jnp.float32)[:, None, None]
    interaction = jnp.zeros_like(energy)
    for mirror in (1, -1):
        plus_bins = shift_freq(jnp.roll(energy, -mirror, axis=1), -2)
        minus_bins = shift_freq(jnp.roll(energy, 3 * mirror, axis=1), 3)
        transfer_rate = (
            0.001
            * valid
            * (energy * energy * (plus_bins + minus_bins) - 2.0 * energy * plus_bins * minus_bins)
        )
        interaction = interaction - 2.0 * transfer_rate
        interaction = interaction + jnp.roll(shift_freq(transfer_rate, 2), mirror, axis=1)
        interaction = interaction + jnp.roll(shift_freq(transfer_rate, -3), -3 * mirror, axis=1)
    updated = energy + (wind_gain - damping) * energy + interaction
    raw_height = 4.0 * jnp.sqrt(jnp.mean(updated, axis=(0, 1)) + 1e-06)
    return (updated, raw_height)


def local(spectrum, sea_mask, wind_speed, wind_angle):
    count = lax.axis_size("spec")
    position = lax.axis_index("spec")
    bins_dev = spectrum.shape[0]
    cells = spectrum.shape[1]
    points = cells // count
    lat_count = cells // NLON
    sea_float = sea_mask.astype(jnp.float32)
    bin_ids = position * bins_dev + jnp.arange(bins_dev, dtype=jnp.int32)
    freq_index = (bin_ids // ND).astype(jnp.float32)
    dir_index = (bin_ids % ND).astype(jnp.float32)
    courant_x, courant_y = courant_numbers(freq_index, dir_index, lat_count, ND)
    sea_grid = sea_float.reshape(1, lat_count, NLON)
    energy = (spectrum * sea_float[None, :]).reshape(bins_dev, lat_count, NLON)
    for substep in range(ADV_STEPS):
        energy = upwind_step(energy, courant_x, courant_y, sea_grid)
    advected = energy.reshape(bins_dev, cells)
    outgoing = advected.reshape(bins_dev, count, points)
    arrived = lax.all_to_all(outgoing, "spec", split_axis=1, concat_axis=0, tiled=True)
    start = position * points
    speed_own = lax.dynamic_slice_in_dim(wind_speed, start, points)
    angle_own = lax.dynamic_slice_in_dim(wind_angle, start, points)
    sea_own = lax.dynamic_slice_in_dim(sea_float, start, points)
    updated, raw_height = source_terms(arrived.reshape(NF, ND, points), speed_own, angle_own)
    wave_height = sea_own * raw_height
    own_total = jnp.zeros((count, 1), jnp.float32) + jnp.sum(wave_height)
    returned, totals = (
        lax.all_to_all(
            updated.reshape(NF * ND, 1, points), "spec", split_axis=0, concat_axis=1, tiled=True
        ),
        lax.all_to_all(own_total, "spec", split_axis=0, concat_axis=1, tiled=True),
    )
    new_spectrum = returned.reshape(bins_dev, cells)
    height_sum = jnp.sum(totals)
    mean_height = (height_sum / (SEA_DEV * count)).reshape(1)
    return (new_spectrum, wave_height, mean_height)


HALO = 5
LANES = 128
WIDE = 256
LAND = 4096.0
UNROLL = 3


def group_size(count, bins_dev, cells):
    size = 4
    if count % size or bins_dev % ND or cells % (size * LANES) or cells % NLON:
        return 0
    if NLON % LANES or bins_dev // ND * size < 2 * HALO or cells % count:
        return 0
    sea = SEA_DEV * count
    if sea > min(cells, LAND) or sea % (size * LANES) or sea % WIDE or cells % WIDE:
        return 0
    if (cells - sea) % WIDE:
        return 0
    return size


def split_bf16(values):
    high = values.astype(jnp.bfloat16)
    left = values - high.astype(jnp.float32)
    mid = left.astype(jnp.bfloat16)
    low = (left - mid.astype(jnp.float32)).astype(jnp.bfloat16)
    return high, mid, low


def rows_of(parts, height, width):
    ids = lax.broadcasted_iota(jnp.int32, (height, width), 0)
    out = jnp.zeros((height, width), jnp.float32)
    for i, part in enumerate(parts):
        out = jnp.where(ids == i, jnp.broadcast_to(part.astype(jnp.float32), (height, width)), out)
    return out.astype(jnp.bfloat16)


def window_start(count, me, cells):
    return jnp.minimum(me * (cells // count) // LANES * LANES, cells - WIDE)


def fused_kernel(
    count, group, sea_in, wind_in, angle_in, spec_ref, full_ref, height_ref, near_ref,
    sea_raw, wind_raw, angle_raw, aux_ref, place_ref, spread_ref, aux_sem,
    raw, moved, split, wsplit, adv, held, done, back, mom_out, mom_in, wind, acc,
    sum_out, sum_in, damp_out, damp_in,
    load_sem, held_sem, halo_sem, y_sem, z_sem, chain_sem, mom_send, mom_recv,
    ret_send, ret_recv, sum_send, sum_recv, damp_send, damp_recv,
):
    f32, bf16 = jnp.float32, jnp.bfloat16
    freq_dev, _, sea_cells = adv.shape
    bins_dev, cells = moved.shape
    freq_group = freq_dev * group
    width = sea_cells // group
    zones = count // group
    lat_count = cells // NLON
    sides = group // 2
    parts = width // LANES
    cell_tiles = cells // LANES
    land = cells - sea_cells
    reach = land + WIDE
    me = lax.axis_index("spec")
    zone, rank = me // group, me % group
    side, core = rank // 2, rank % 2

    def remote(src, dst, send, recv, target):
        return pltpu.make_async_remote_copy(
            src_ref=src, dst_ref=dst, send_sem=send, recv_sem=recv,
            device_id={"spec": target}, device_id_type=pl.DeviceIdType.MESH,
        )

    loads = [
        pltpu.make_async_copy(
            spec_ref.at[pl.ds(f * ND, ND)], raw.at[pl.ds(f * ND, ND)], load_sem.at[f]
        )
        for f in range(freq_dev)
    ]
    small = [
        pltpu.make_async_copy(sea_in, sea_raw, aux_sem.at[0]),
        pltpu.make_async_copy(wind_in, wind_raw, aux_sem.at[1]),
        pltpu.make_async_copy(angle_in, angle_raw, aux_sem.at[2]),
    ]
    for load in small[:1] + loads + small[1:]:
        load.start()
    barrier = pltpu.get_barrier_semaphore()

    def signal(semaphore, target):
        pl.semaphore_signal(
            semaphore, inc=1, device_id={"spec": target}, device_id_type=pl.DeviceIdType.MESH
        )

    for step in range(1, group):
        signal(barrier, zone * group + (rank + step) % group)

    @pl.when(zone > 0)
    def _():
        for c in range(2):
            signal(barrier, (zone - 1) * group + side * 2 + c)

    @pl.when(zone < zones - 1)
    def _():
        for c in range(2):
            signal(barrier, (zone + 1) * group + side * 2 + c)

    @pl.when(zone == 0)
    def _():
        held[0:HALO] = jnp.zeros((HALO, ND, width), f32)

    @pl.when(zone == zones - 1)
    def _():
        held[HALO + freq_group :] = jnp.zeros((HALO, ND, width), f32)

    def block_of(index, t):
        return t * group + index

    def tile_of(index, t):
        return pl.ds(pl.multiple_of(block_of(index, t) * LANES, LANES), LANES)

    def lanes_of(t):
        return pl.ds(t * LANES, LANES)

    offsets = [(dy, dc) for dy in range(sides) for dc in range(2)]

    def rank_of(offset):
        return (side + offset[0]) % sides * 2 + (core + offset[1]) % 2

    def y_copy(begin, end, peer, t):
        return remote(
            adv.at[begin:end, :, tile_of(peer, t)],
            held.at[pl.ds(HALO + rank * freq_dev + begin, end - begin), :, lanes_of(t)],
            y_sem, held_sem.at[rank, t], zone * group + peer,
        )

    dirs = lax.broadcasted_iota(jnp.int32, (ND, LANES), 0).astype(f32)
    heading = 2.0 * math.pi * (dirs + 0.5) / ND
    cos_h, sin_h = jnp.cos(heading), jnp.sin(heading)
    log_step = math.log(1.1)
    lats = [math.radians(-75.0 + 150.0 * (r + 0.5) / lat_count) for r in range(lat_count)]

    def omega_of(freq, shape):
        return jnp.exp(jnp.full(shape, log_step, f32) * (freq.astype(f32) - NF // 2))

    square_rows = lax.broadcasted_iota(jnp.int32, (LANES, LANES), 0)
    square_cols = lax.broadcasted_iota(jnp.int32, (LANES, LANES), 1)
    small[0].wait()
    aux_ref[...] = sea_raw[...].astype(f32).reshape(1, cells)
    sea = [aux_ref[0:1, r * NLON : (r + 1) * NLON] for r in range(lat_count)]
    mask = [aux_ref[0:1, i * LANES : (i + 1) * LANES] for i in range(cell_tiles)]
    tri_up = jnp.where(square_rows < square_cols, 1.0, 0.0).astype(bf16)
    ranks = jnp.dot(rows_of(mask, ND // 2, LANES), tri_up, preferred_element_type=f32)
    before = jnp.zeros((1, 1), f32)
    for i in range(cell_tiles):
        place_ref[0:1, i * LANES : (i + 1) * LANES] = jnp.where(
            mask[i] > 0.0, ranks[i : i + 1] + before, LAND
        )
        before = before + jnp.sum(mask[i], axis=1, keepdims=True)
    pair_rows = lax.broadcasted_iota(jnp.int32, (WIDE, reach), 0).astype(f32)

    def build(pair):
        cols = pl.ds(pl.multiple_of(pair * WIDE, LANES), reach)
        first = (pair * WIDE).astype(f32)
        hit = jnp.where(place_ref[0:1, cols] - first == pair_rows, 1.0, 0.0)
        spread_ref[pl.ds(pl.multiple_of(pair * WIDE, LANES), WIDE), cols] = hit.astype(
            spread_ref.dtype
        )

    def packed(values, pair):
        cols = pl.ds(pl.multiple_of(pair * WIDE, LANES), reach)
        return lax.dot_general(
            values[:, cols],
            spread_ref[pl.ds(pl.multiple_of(pair * WIDE, LANES), WIDE), cols],
            (((1,), (1,)), ((), ())), preferred_element_type=f32,
        )

    quarter = ND // 4
    tiles = NLON // LANES
    def advect(f):
        loads[f].wait()
        freq = (me * freq_dev + f).astype(f32)
        speed = 0.2 * jnp.exp(jnp.full((quarter, LANES), -log_step, f32) * freq)
        for q in range(4):
            east, north = q in (0, 3), q in (0, 1)
            rows = slice(f * ND + q * quarter, f * ND + (q + 1) * quarter)
            part = slice(q * quarter, (q + 1) * quarter)
            cx0 = speed * jnp.abs(cos_h[part])
            cy = jnp.concatenate([speed * jnp.abs(sin_h[part])] * tiles, axis=1)
            cx = [jnp.concatenate([cx0 * (1.0 / math.cos(a))] * tiles, axis=1) for a in lats]
            rest = [1.0 - (cx[r] + cy) for r in range(lat_count)]
            energy = [raw[rows, r * NLON : (r + 1) * NLON] * sea[r] for r in range(lat_count)]
            for step in range(ADV_STEPS):
                fresh = []
                for r in range(lat_count):
                    e = energy[r]
                    side_x = pltpu.roll(e, 1 if east else NLON - 1, 1)
                    other = r - 1 if north else r + 1
                    value = rest[r] * e + cx[r] * side_x
                    if 0 <= other < lat_count:
                        value = value + cy * energy[other]
                    fresh.append(value if step == ADV_STEPS - 1 else value * sea[r])
                energy = fresh
            for r in range(lat_count):
                moved[rows, r * NLON : (r + 1) * NLON] = energy[r]
        for i, piece in enumerate(split_bf16(moved[f * ND : (f + 1) * ND])):
            split[(3 * f + i) * ND : (3 * f + i + 1) * ND, :] = piece

    def cols_of(index):
        return pl.ds(pl.multiple_of(index * LANES, LANES), LANES)

    def side_of(dy):
        return (side + dy) % sides

    def pack(t, dy, begin, end):
        return packed(split.at[begin * 3 * ND : end * 3 * ND], t * sides + side_of(dy))

    def unload(t, dy, begin, end, got):
        pair = t * sides + side_of(dy)
        cols = pl.ds(pl.multiple_of(pair * WIDE, LANES), WIDE)
        here = pl.ds(pl.multiple_of(side_of(dy) * WIDE, LANES), WIDE)
        mass, moment = None, None
        for f in range(begin, end):
            base = (f - begin) * 3 * ND
            piece = got[base : base + ND] + got[base + ND : base + 2 * ND] + (
                got[base + 2 * ND : base + 3 * ND]
            )
            adv[f, :, cols] = piece
            total = jnp.sum(piece, axis=0, keepdims=True)
            scaled = omega_of(me * freq_dev + f, (1, WIDE)) * total
            mass = total if mass is None else mass + total
            moment = scaled if moment is None else moment + scaled
        if begin:
            mass, moment = mass + mom_out[t, 0:1, here], moment + mom_out[t, 1:2, here]
        mom_out[t, 0:1, here] = mass
        mom_out[t, 1:2, here] = moment

    def send_far(t, dy, begin, end):
        for c in range(2):
            y_copy(begin, end, side_of(dy) * 2 + c, t).start()

    top = side > 0
    early_way, late_way = jnp.where(top, 0, 1), jnp.where(top, 1, 0)
    early_ok = jnp.where(top, zone < zones - 1, zone > 0)
    late_ok = jnp.where(top, zone > 0, zone < zones - 1)
    early_zone = jnp.where(top, zone + 1, zone + zones - 1) % zones
    late_zone = jnp.where(top, zone + zones - 1, zone + 1) % zones
    early_shift = HALO + jnp.where(top, -freq_group, freq_group)
    late_shift = HALO + jnp.where(top, freq_group, -freq_group)

    def early_slot(slot):
        return early_ok & jnp.where(top, slot >= freq_group - HALO, slot < HALO)

    def late_slot(slot):
        return late_ok & jnp.where(top, slot < HALO, slot >= freq_group - HALO)

    def early_copy(f, c, t):
        return remote(
            adv.at[f, :, tile_of(side * 2 + c, t)],
            held.at[early_shift + rank * freq_dev + f, :, lanes_of(t)],
            z_sem.at[0], halo_sem.at[early_way, t], early_zone * group + side * 2 + c,
        )

    def forward(slot, t, now):
        @pl.when(late_slot(slot) & now)
        def _():
            remote(
                held.at[HALO + slot, :, lanes_of(t)],
                held.at[late_shift + slot, :, lanes_of(t)],
                z_sem.at[1], halo_sem.at[late_way, t], late_zone * group + rank,
            ).start()

    def send_near(t):
        for c in range(2):
            for f in range(freq_dev):
                @pl.when(early_slot(rank * freq_dev + f))
                def _():
                    early_copy(f, c, t).start()

        y_copy(0, freq_dev, rank_of((0, 1)), t).start()
        for f in range(freq_dev):
            held[HALO + rank * freq_dev + f, :, lanes_of(t)] = adv[f, :, tile_of(rank, t)]

    def arrive_group(dy, t):
        for dc in range(2):
            if (dy, dc) != (0, 0):
                source = rank_of((dy, dc))
                slots = held.at[
                    pl.ds(HALO + source * freq_dev, freq_dev), :, lanes_of(t)
                ]
                remote(
                    slots, slots, y_sem, held_sem.at[source, t], (me + 1) % count
                ).wait_recv()
                if dy:
                    for f in range(freq_dev):
                        forward(source * freq_dev + f, t, t < parts - 1 or side == 0)

    def up_relay(level):
        @pl.when(zone == level)
        def _():
            pl.semaphore_wait(chain_sem.at[0], 1)
            if level < zones - 1:
                signal(chain_sem.at[0], (me + group) % count)

    def down_relay(level):
        @pl.when(zone == level)
        def _():
            pl.semaphore_wait(chain_sem.at[1], 1)
            if level > 0:
                signal(chain_sem.at[1], (me + count - group) % count)

    def moment_copy(target_zone, target_rank):
        return remote(
            mom_out.at[:, :, cols_of(target_rank)], mom_in.at[me],
            mom_send, mom_recv, target_zone * group + target_rank,
        )

    def send_zone_moments():
        for step in range(1, group):
            moment_copy(zone, (rank + step) % group).start()

    def send_moments():
        for away in range(1, zones):
            for other in range(group):
                moment_copy((zone + away) % zones, other).start()

    far = list(range(1, sides))
    for dy in far:
        build(side_of(dy))
    advect(0)
    for dy in far:
        unload(0, dy, 0, 1, pack(0, dy, 0, 1))
    advect(1)
    pl.semaphore_wait(
        barrier, group - 1 + jnp.where(zone > 0, 2, 0) + jnp.where(zone < zones - 1, 2, 0)
    )
    for dy in far:
        send_far(0, dy, 0, 1)

    @pl.when(zone == 0)
    def _():
        signal(chain_sem.at[0], (me + group) % count)

    @pl.when(zone == zones - 1)
    def _():
        signal(chain_sem.at[1], (me + count - group) % count)

    up_relay(1)
    for f in range(2, freq_dev):
        advect(f)
    for level in range(2, zones - 1):
        up_relay(level)
    got = [pack(0, dy, 1, freq_dev) for dy in far]
    build(side)
    got_near = pack(0, 0, 0, freq_dev)
    for dy in far:
        unload(0, dy, 1, freq_dev, got[dy - 1])
        send_far(0, dy, 1, freq_dev)
    unload(0, 0, 0, freq_dev, got_near)
    send_near(0)
    down_relay(zones - 2)
    upper = zone >= zones // 2
    for t in range(1, parts):
        last = t == parts - 1
        for dy in far:
            build(t * sides + side_of(dy))
        got = [pack(t, dy, 0, freq_dev) for dy in far]
        build(t * sides + side)
        got_near = pack(t, 0, 0, freq_dev)
        for dy in far:
            unload(t, dy, 0, freq_dev, got[dy - 1])

            @pl.when(jnp.logical_not(upper) if last else zone >= 0)
            def _():
                send_far(t, dy, 0, freq_dev)

        unload(t, 0, 0, freq_dev, got_near)
        if last:
            up_relay(zones - 1)
            send_zone_moments()

            @pl.when(upper)
            def _():
                send_moments()
                for dy in far:
                    send_far(t, dy, 0, freq_dev)

        send_near(t)

    small[1].wait()
    small[2].wait()
    speed_all = wind_raw[...].reshape(1, cells)
    angle_all = angle_raw[...].reshape(1, cells)
    wsplit[...] = rows_of(
        split_bf16(speed_all * jnp.cos(angle_all)) + split_bf16(speed_all * jnp.sin(angle_all)),
        2 * quarter, cells,
    )
    for t in range(parts):
        own = packed(wsplit, t * sides + side)
        own = jnp.where(core == 0, own[:, :LANES], own[:, LANES:])
        along = own[0:1] + own[1:2] + own[2:3]
        across = own[3:4] + own[4:5] + own[5:6]
        wind[:, t * LANES : (t + 1) * LANES] = cos_h * along + sin_h * across

    for level in range(zones - 3, 0, -1):
        down_relay(level)

    @pl.when(jnp.logical_not(upper) & (zone > 0))
    def _():
        send_moments()

    for dy in far:
        arrive_group(dy, 0)
    mom_in[me] = mom_out[:, :, cols_of(rank)]
    start = window_start(count, me, cells)
    near_ref[...] = place_ref[0:1, pl.ds(pl.multiple_of(start, LANES), WIDE)]
    for t in range(parts):
        arrive_group(0, t)

    acc[...] = jnp.zeros_like(acc)
    ascending = side > 0

    def arrive_halo(at_top, t):
        block = held.at[0:HALO, :, lanes_of(t)]

        @pl.when(jnp.where(at_top, zone < zones - 1, zone > 0))
        def _():
            way = jnp.where(at_top, 1, 0)
            remote(
                block, block, z_sem.at[0], halo_sem.at[way, t], (me + 1) % count
            ).wait_recv()

    def ret_copy(owner, t):
        return remote(
            done.at[pl.ds(owner * freq_dev, freq_dev), :, lanes_of(t)],
            back.at[:, :, tile_of(rank, t)],
            ret_send, ret_recv.at[t], zone * group + owner,
        )

    def turn(values, amount):
        return pltpu.roll(values, amount % ND, 0)

    def rate(a, p, m):
        return a * (a * (p + m) - 2.0 * (p * m))

    def scale(index, factor):
        return jnp.where((index >= 3) & (index <= NF - 3), factor, 0.0).astype(f32)

    def slab(k, t):
        return held[HALO + k, :, t * LANES : (t + 1) * LANES]

    def rates(own, p2, m3):
        return rate(own, turn(p2, -1), turn(m3, 3)) + rate(own, turn(p2, 1), turn(m3, -3))

    def grown(own, freq, t):
        omega = omega_of(freq, (1, LANES))
        push = wind[:, t * LANES : (t + 1) * LANES] * omega - 1.0
        return own + (0.05 * omega) * jnp.maximum(0.0, push) * own

    def tally(energy, near, freq, t):
        flow = scale(freq, 0.001) * near
        acc[:, t * LANES : (t + 1) * LANES] += energy + (flow + flow - 2.0 * flow)

    def sources(t, begin, end):
        def source_step(i, carry):
            k = jnp.where(ascending, i, freq_group - 1 - i)
            freq = zone * freq_group + k
            own = slab(k, t)
            p2, m3, m2, m5, p3, p5 = (slab(k + shift, t) for shift in (2, -3, -2, -5, 3, 5))
            near = rates(own, p2, m3)
            low = rate(turn(m2, 1), own, turn(m5, 4)) + rate(turn(m2, -1), own, turn(m5, -4))
            high = rate(turn(p3, -3), turn(p5, -4), own) + rate(turn(p3, 3), turn(p5, 4), own)
            interaction = scale(freq, -0.002) * near + scale(freq - 2, 0.001) * low + (
                scale(freq + 3, 0.001) * high
            )
            energy = grown(own, freq, t)
            done[k, :, t * LANES : (t + 1) * LANES] = energy + interaction
            if begin == 0:
                tally(energy, near, freq, t)
            return carry

        lax.fori_loop(begin, end, source_step, 0, unroll=UNROLL)

    def tally_rest(t):
        def rest_step(i, carry):
            k = jnp.where(ascending, half + i, half - 1 - i)
            center = jnp.where(
                ascending,
                jnp.where(i < 2, i - 2, half + i - 2),
                jnp.where(i < 3, freq_group + i, half + 2 - i),
            )
            near = rates(slab(center, t), slab(center + 2, t), slab(center - 3, t))
            energy = grown(slab(k, t), zone * freq_group + k, t)
            tally(energy, near, zone * freq_group + center, t)
            return carry

        lax.fori_loop(0, half, rest_step, 0, unroll=UNROLL)

    half = freq_group // 2
    near_side = rank_of((0, 1))

    def first_half(t):
        arrive_halo(jnp.logical_not(ascending), t)
        sources(t, 0, half)
        if t == parts - 1:
            tally_rest(t)
            send_sums()
        for dy in range(1, sides):
            for dc in range(2):
                ret_copy(rank_of((dy, dc)), t).start()
        if t == parts - 1:
            for slot in range(HALO):
                forward(slot, t, side > 0)

        if t == 0:
            down_relay(0)

            @pl.when(zone == 0)
            def _():
                send_moments()

        if t < parts - 1:
            tally_rest(t)

    def send_sums():
        sum_out[...] = jnp.sum(acc[...], axis=0, keepdims=True)
        for step in range(1, count):
            remote(sum_out, sum_in.at[me], sum_send, sum_recv, (me + step) % count).start()
        sum_in[me] = sum_out[...]

    def second_half(t):
        if t == parts - 1:
            damping_terms()
        arrive_halo(ascending, t)
        sources(t, half, freq_group)
        ret_copy(near_side, t).start()
        back[:, :, tile_of(rank, t)] = done[
            pl.ds(rank * freq_dev, freq_dev), :, lanes_of(t)
        ]

    def zone_copy(dst_rank, src, dst, send, recv):
        return remote(src, dst, send, recv, zone * group + dst_rank)

    def damping_terms():
        others = mom_in.at[0 : count - 1]
        remote(others, others, mom_send, mom_recv, (me + 1) % count).wait_recv()
        total = jnp.sum(mom_in[...], axis=0) * (1.0 / (NF * ND))
        for t in range(parts):
            energy_mean, moment_one = total[t, 0:1], total[t, 1:2]
            mean_freq = moment_one / (energy_mean + 1e-06)
            steepness = energy_mean * mean_freq * mean_freq
            breaking = steepness * steepness / (1.0 + steepness * steepness)
            damp_out[t, 0:1] = 0.03 * breaking
            damp_out[t, 1:2] = 0.03 * breaking * moment_one
        for i in range(1, group):
            zone_copy(
                rank_of(offsets[i]), damp_out, damp_in.at[rank], damp_send, damp_recv
            ).start()
        damp_in[rank] = damp_out[...]

    first_half(0)
    for t in range(1, parts):
        for dy in range(1, sides):
            arrive_group(dy, t)
        first_half(t)
        second_half(t - 1)
    second_half(parts - 1)

    def gather_back(t):
        block = done.at[0 : (group - 1) * freq_dev, :, lanes_of(t)]
        remote(block, block, ret_send, ret_recv.at[t], (me + 1) % count).wait_recv()
        cols = slice(t * group * LANES, (t + 1) * group * LANES)
        for f in range(freq_dev):
            for i, piece in enumerate(split_bf16(back[f, :, cols])):
                split[(3 * f + i) * ND : (3 * f + i + 1) * ND, cols] = piece

    def spread(j, begin, end):
        low, high = max(0, j * WIDE - land), min(sea_cells, (j + 1) * WIDE)
        return jnp.dot(
            split[begin:end, low:high],
            spread_ref[low:high, j * WIDE : (j + 1) * WIDE],
            preferred_element_type=f32,
        )

    def joined(got, f):
        base = 3 * f * ND
        return got[base : base + ND] + got[base + ND : base + 2 * ND] + (
            got[base + 2 * ND : base + 3 * ND]
        )

    values = 3 * bins_dev
    early_tiles = [
        j for j in range(cells // WIDE) if (j + 1) * WIDE <= (parts - 1) * group * LANES
    ]
    for t in range(parts - 1):
        gather_back(t)
    for j in early_tiles:
        got = spread(j, 0, values)
        for f in range(freq_dev):
            full_ref[f * ND : (f + 1) * ND, j * WIDE : (j + 1) * WIDE] = joined(got, f)
    gather_back(parts - 1)
    others = damp_in.at[0 : group - 1]
    remote(others, others, damp_send, damp_recv, (me + 1) % count).wait_recv()
    for g in range(group):
        for t in range(parts):
            split[values:, block_of(g, t) * LANES : (block_of(g, t) + 1) * LANES] = rows_of(
                split_bf16(damp_in[g, t, 0:1]), ND // 2, LANES
            )
    for j in range(cells // WIDE):
        cols = slice(j * WIDE, (j + 1) * WIDE)
        got = spread(j, values if j in early_tiles else 0, values + ND // 2)
        rows = got[got.shape[0] - ND // 2 :]
        row = rows[0:1] + rows[1:2] + rows[2:3]
        for f in range(freq_dev):
            bins = slice(f * ND, (f + 1) * ND)
            value = full_ref[bins, cols] if j in early_tiles else joined(got, f)
            loss = omega_of(me * freq_dev + f, (1, WIDE)) * row
            full_ref[bins, cols] = value - loss * moved[bins, cols]

    block = held.at[0 : (group - 1) * freq_dev]
    remote(block, block, y_sem, held_sem.at[0, 0], (me + 1) % count).wait_send()
    remote(block, block, ret_send, ret_recv.at[0], (me + 1) % count).wait_send()
    others = mom_in.at[0 : count - 1]
    remote(others, others, mom_send, mom_recv, (me + 1) % count).wait_send()
    others = damp_in.at[0 : group - 1]
    remote(others, others, damp_send, damp_recv, (me + 1) % count).wait_send()
    def drain(slots, way):
        block = held.at[0:slots]
        remote(
            block, block, z_sem.at[way], halo_sem.at[0, 0], (me + 1) % count
        ).wait_send()

    for f in range(freq_dev):
        @pl.when(early_slot(rank * freq_dev + f))
        def _():
            drain(2, 0)

    @pl.when(late_ok)
    def _():
        drain(HALO, 1)

    others = sum_in.at[0 : count - 1]
    remote(others, others, sum_send, sum_recv, (me + 1) % count).wait()
    for g in range(group):
        mass = sum_in[g]
        for other in range(1, zones):
            mass = mass + sum_in[other * group + g]
        for t in range(parts):
            mean = mass[:, t * LANES : (t + 1) * LANES] * (1.0 / (NF * ND)) - damp_in[g, t, 1:2]
            cols = slice(block_of(g, t) * LANES, (block_of(g, t) + 1) * LANES)
            height_ref[0:1, cols] = 4.0 * jnp.sqrt(mean + 1e-06)


def store_kernel(
    count, full_in, height_in, near_in, new_out, wave_out, mean_out, wave_ref, mean_ref, sem
):
    cells = full_in.shape[1]
    sea_cells = height_in.shape[1]
    copies = [
        pltpu.make_async_copy(full_in, new_out, sem.at[0]),
        pltpu.make_async_copy(wave_ref, wave_out, sem.at[1]),
        pltpu.make_async_copy(mean_ref, mean_out, sem.at[2]),
    ]
    copies[0].start()
    me = lax.axis_index("spec")
    points = cells // count
    shift = me * points - window_start(count, me, cells)
    halves = []
    for h in range(WIDE // LANES):
        place = jnp.broadcast_to(near_in[:, h * LANES : (h + 1) * LANES], (8, LANES))
        place = place.astype(jnp.int32)
        wave = jnp.zeros((8, LANES), jnp.float32)
        for b in range(sea_cells // LANES):
            values = jnp.broadcast_to(height_in[:, b * LANES : (b + 1) * LANES], (8, LANES))
            found = jnp.take_along_axis(values, place % LANES, axis=1)
            wave = jnp.where(place // LANES == b, found, wave)
        halves.append(wave)
    wave = jnp.concatenate(halves, axis=1)
    wave_ref[...] = pltpu.roll(wave, (WIDE - shift) % WIDE, 1)[0, :points]
    copies[1].start()
    mean_ref[...] = jnp.sum(height_in[...], axis=1, keepdims=True) * (1.0 / sea_cells)
    copies[2].start()
    for copy in copies:
        copy.wait()


def fused_local(spectrum, sea_mask, wind_speed, wind_angle):
    count = lax.axis_size("spec")
    bins_dev, cells = spectrum.shape
    group = group_size(count, bins_dev, cells)
    freq_dev = bins_dev // ND
    freq_group = freq_dev * group
    sea_cells = SEA_DEV * count
    width = sea_cells // group
    points = cells // count
    parts = width // LANES
    f32, bf16 = jnp.float32, jnp.bfloat16
    dma = pltpu.SemaphoreType.DMA
    vmem = pl.BlockSpec(memory_space=pltpu.VMEM)
    handed = pl.pallas_call(
        functools.partial(fused_kernel, count, group),
        out_shape=(
            pltpu.VMEM((bins_dev, cells), f32),
            pltpu.VMEM((1, sea_cells), f32),
            pltpu.VMEM((1, WIDE), f32),
        ),
        in_specs=[pl.BlockSpec(memory_space=pl.ANY)] * 4,
        out_specs=(vmem,) * 3,
        scratch_shapes=[
            pltpu.VMEM((cells,), jnp.int32),
            pltpu.VMEM((cells,), f32),
            pltpu.VMEM((cells,), f32),
            pltpu.VMEM((1, cells), f32),
            pltpu.VMEM((1, cells), f32),
            pltpu.VMEM((sea_cells, cells), jnp.float8_e4m3fn),
            dma((3,)),
            pltpu.VMEM((bins_dev, cells), f32),
            pltpu.VMEM((bins_dev, cells), f32),
            pltpu.VMEM((3 * bins_dev + ND // 2, cells), bf16),
            pltpu.VMEM((ND // 2, cells), bf16),
            pltpu.VMEM((freq_dev, ND, sea_cells), f32),
            pltpu.VMEM((freq_group + 2 * HALO, ND, width), f32),
            pltpu.VMEM((freq_group, ND, width), f32),
            pltpu.VMEM((freq_dev, ND, sea_cells), f32),
            pltpu.VMEM((parts, 2, group * LANES), f32),
            pltpu.VMEM((count, parts, 2, LANES), f32),
            pltpu.VMEM((ND, width), f32),
            pltpu.VMEM((ND, width), f32),
            pltpu.VMEM((1, width), f32),
            pltpu.VMEM((count, 1, width), f32),
            pltpu.VMEM((parts, 2, LANES), f32),
            pltpu.VMEM((group, parts, 2, LANES), f32),
            dma((freq_dev,)),
            dma((group, parts)),
            dma((2, parts)),
            dma,
            dma((2,)),
            pltpu.SemaphoreType.REGULAR((2,)),
            dma,
            dma,
            dma,
            dma((parts,)),
            dma,
            dma,
            dma,
            dma,
        ],
        compiler_params=pltpu.CompilerParams(collective_id=0, has_side_effects=True),
    )(sea_mask, wind_speed, wind_angle, spectrum)
    out, wave, mean = pl.pallas_call(
        functools.partial(store_kernel, count),
        out_shape=(
            pltpu.HBM((bins_dev, cells), f32),
            pltpu.HBM((points,), f32),
            pltpu.HBM((1, 1), f32),
        ),
        in_specs=[vmem] * 3,
        out_specs=(pl.BlockSpec(memory_space=pltpu.HBM),) * 3,
        scratch_shapes=[pltpu.VMEM((points,), f32), pltpu.VMEM((1, 1), f32), dma((3,))],
    )(*[pltpu.with_memory_space_constraint(piece, pltpu.VMEM) for piece in handed])
    return (out, wave, mean.reshape(1))


def solution(mesh):
    in_specs = (P(("grp", "spec"), None), P(), P("grp"), P("grp"))
    out_specs = (P(("grp", "spec"), None), P(("grp", "spec")), P("grp"))

    def body(spectrum, sea_mask, wind_speed, wind_angle):
        fits = group_size(mesh.shape["spec"], *spectrum.shape)
        plan = fused_local if fits else local
        return plan(spectrum, sea_mask, wind_speed, wind_angle)

    return jax.shard_map(body, mesh=mesh, in_specs=in_specs, out_specs=out_specs, check_vma=False)
```

```python
import functools
import math

import jax
import jax.numpy as jnp
from jax import lax
from jax.experimental import pallas as pl
from jax.experimental.pallas import tpu as pltpu
from jax.sharding import PartitionSpec as P

NF = 48
ND = 32
NLON = 384
ADV_STEPS = 2
SEA_DEV = 64


def upwind_step(energy, courant_x, courant_y, sea_grid):
    west_cell = jnp.roll(energy, 1, axis=2)
    east_cell = jnp.roll(energy, -1, axis=2)
    edge_row = jnp.zeros_like(energy[:, :1])
    south_cell = jnp.concatenate([edge_row, energy[:, :-1]], axis=1)
    north_cell = jnp.concatenate([energy[:, 1:], edge_row], axis=1)
    updated = (
        energy
        - jnp.maximum(courant_x, 0.0) * (energy - west_cell)
        - jnp.minimum(courant_x, 0.0) * (east_cell - energy)
        - jnp.maximum(courant_y, 0.0) * (energy - south_cell)
        - jnp.minimum(courant_y, 0.0) * (north_cell - energy)
    )
    return updated * sea_grid


def courant_numbers(freq_index, dir_index, lat_count, dir_count):
    speed = 0.2 * jnp.exp(-math.log(1.1) * freq_index)
    heading = 2.0 * math.pi * (dir_index + 0.5) / dir_count
    rows = jnp.arange(lat_count, dtype=jnp.float32)
    latitude = (-75.0 + 150.0 * (rows + 0.5) / lat_count) * (math.pi / 180.0)
    courant_x = (speed * jnp.cos(heading))[:, None, None] / jnp.cos(latitude)[None, :, None]
    courant_y = (speed * jnp.sin(heading))[:, None, None]
    return (courant_x, courant_y)


def shift_freq(values, amount):
    if amount > 0:
        filler = jnp.zeros_like(values[:amount])
        return jnp.concatenate([filler, values[:-amount]], axis=0)
    filler = jnp.zeros_like(values[:-amount])
    return jnp.concatenate([values[-amount:], filler], axis=0)


def source_terms(energy, speed, angle):
    freq_count = energy.shape[0]
    dir_count = energy.shape[1]
    freq_ids = jnp.arange(freq_count, dtype=jnp.float32)
    frequency = jnp.exp(math.log(1.1) * (freq_ids - freq_count // 2))[:, None, None]
    heading = (2.0 * math.pi * (jnp.arange(dir_count, dtype=jnp.float32) + 0.5) / dir_count)[
        None, :, None
    ]
    energy_mean = jnp.mean(energy, axis=(0, 1))
    moment_one = jnp.mean(frequency * energy, axis=(0, 1))
    mean_freq = moment_one / (energy_mean + 1e-06)
    steepness = energy_mean * mean_freq * mean_freq
    breaking = steepness * steepness / (1.0 + steepness * steepness)
    wind_gain = (
        0.05
        * frequency
        * jnp.maximum(
            0.0, speed[None, None, :] * frequency * jnp.cos(heading - angle[None, None, :]) - 1.0
        )
    )
    damping = 0.03 * frequency * breaking[None, None, :]
    valid = ((freq_ids >= 3) & (freq_ids <= freq_count - 3)).astype(jnp.float32)[:, None, None]
    interaction = jnp.zeros_like(energy)
    for mirror in (1, -1):
        plus_bins = shift_freq(jnp.roll(energy, -mirror, axis=1), -2)
        minus_bins = shift_freq(jnp.roll(energy, 3 * mirror, axis=1), 3)
        transfer_rate = (
            0.001
            * valid
            * (energy * energy * (plus_bins + minus_bins) - 2.0 * energy * plus_bins * minus_bins)
        )
        interaction = interaction - 2.0 * transfer_rate
        interaction = interaction + jnp.roll(shift_freq(transfer_rate, 2), mirror, axis=1)
        interaction = interaction + jnp.roll(shift_freq(transfer_rate, -3), -3 * mirror, axis=1)
    updated = energy + (wind_gain - damping) * energy + interaction
    raw_height = 4.0 * jnp.sqrt(jnp.mean(updated, axis=(0, 1)) + 1e-06)
    return (updated, raw_height)


def local(spectrum, sea_mask, wind_speed, wind_angle):
    count = lax.axis_size("spec")
    position = lax.axis_index("spec")
    bins_dev = spectrum.shape[0]
    cells = spectrum.shape[1]
    points = cells // count
    lat_count = cells // NLON
    sea_float = sea_mask.astype(jnp.float32)
    bin_ids = position * bins_dev + jnp.arange(bins_dev, dtype=jnp.int32)
    freq_index = (bin_ids // ND).astype(jnp.float32)
    dir_index = (bin_ids % ND).astype(jnp.float32)
    courant_x, courant_y = courant_numbers(freq_index, dir_index, lat_count, ND)
    sea_grid = sea_float.reshape(1, lat_count, NLON)
    energy = (spectrum * sea_float[None, :]).reshape(bins_dev, lat_count, NLON)
    for substep in range(ADV_STEPS):
        energy = upwind_step(energy, courant_x, courant_y, sea_grid)
    advected = energy.reshape(bins_dev, cells)
    outgoing = advected.reshape(bins_dev, count, points)
    arrived = lax.all_to_all(outgoing, "spec", split_axis=1, concat_axis=0, tiled=True)
    start = position * points
    speed_own = lax.dynamic_slice_in_dim(wind_speed, start, points)
    angle_own = lax.dynamic_slice_in_dim(wind_angle, start, points)
    sea_own = lax.dynamic_slice_in_dim(sea_float, start, points)
    updated, raw_height = source_terms(arrived.reshape(NF, ND, points), speed_own, angle_own)
    wave_height = sea_own * raw_height
    own_total = jnp.zeros((count, 1), jnp.float32) + jnp.sum(wave_height)
    returned, totals = (
        lax.all_to_all(
            updated.reshape(NF * ND, 1, points), "spec", split_axis=0, concat_axis=1, tiled=True
        ),
        lax.all_to_all(own_total, "spec", split_axis=0, concat_axis=1, tiled=True),
    )
    new_spectrum = returned.reshape(bins_dev, cells)
    height_sum = jnp.sum(totals)
    mean_height = (height_sum / (SEA_DEV * count)).reshape(1)
    return (new_spectrum, wave_height, mean_height)


HALO = 5
LANES = 128
WIDE = 256
LAND = 4096.0
UNROLL = 3


def group_size(count, bins_dev, cells):
    size = 4
    if count % size or bins_dev % ND or cells % (size * LANES) or cells % NLON:
        return 0
    if NLON % LANES or bins_dev // ND * size < 2 * HALO or cells % count:
        return 0
    sea = SEA_DEV * count
    if sea > min(cells, LAND) or sea % (size * LANES) or sea % WIDE or cells % WIDE:
        return 0
    if (cells - sea) % WIDE:
        return 0
    return size


def split_bf16(values):
    high = values.astype(jnp.bfloat16)
    left = values - high.astype(jnp.float32)
    mid = left.astype(jnp.bfloat16)
    low = (left - mid.astype(jnp.float32)).astype(jnp.bfloat16)
    return high, mid, low


def rows_of(parts, height, width):
    ids = lax.broadcasted_iota(jnp.int32, (height, width), 0)
    out = jnp.zeros((height, width), jnp.float32)
    for i, part in enumerate(parts):
        out = jnp.where(ids == i, jnp.broadcast_to(part.astype(jnp.float32), (height, width)), out)
    return out.astype(jnp.bfloat16)


def window_start(count, me, cells):
    return jnp.minimum(me * (cells // count) // LANES * LANES, cells - WIDE)


def fused_kernel(
    count, group, sea_in, wind_in, angle_in, spec_ref, full_ref, mean_out, near_ref, loss_ref,
    sea_raw, wind_raw, angle_raw, aux_ref, place_ref, spread_ref, aux_sem,
    raw, moved, split, wsplit, adv, held, done, back, mom_out, mom_in, wind, acc,
    sum_out, sum_in, damp_out, damp_in,
    load_sem, held_sem, halo_sem, y_sem, z_sem, chain_sem, mom_send, mom_recv,
    ret_send, ret_recv, sum_send, sum_recv, damp_send, damp_recv,
):
    f32, bf16 = jnp.float32, jnp.bfloat16
    freq_dev, _, sea_cells = adv.shape
    bins_dev, cells = moved.shape
    freq_group = freq_dev * group
    width = sea_cells // group
    zones = count // group
    lat_count = cells // NLON
    sides = group // 2
    parts = width // LANES
    cell_tiles = cells // LANES
    land = cells - sea_cells
    reach = land + WIDE
    me = lax.axis_index("spec")
    zone, rank = me // group, me % group
    side, core = rank // 2, rank % 2

    def remote(src, dst, send, recv, target):
        return pltpu.make_async_remote_copy(
            src_ref=src, dst_ref=dst, send_sem=send, recv_sem=recv,
            device_id={"spec": target}, device_id_type=pl.DeviceIdType.MESH,
        )

    loads = [
        pltpu.make_async_copy(
            spec_ref.at[pl.ds(f * ND, ND)], raw.at[pl.ds(f * ND, ND)], load_sem.at[f]
        )
        for f in range(freq_dev)
    ]
    small = [
        pltpu.make_async_copy(sea_in, sea_raw, aux_sem.at[0]),
        pltpu.make_async_copy(wind_in, wind_raw, aux_sem.at[1]),
        pltpu.make_async_copy(angle_in, angle_raw, aux_sem.at[2]),
    ]
    for load in small[:1] + loads + small[1:]:
        load.start()
    barrier = pltpu.get_barrier_semaphore()

    def signal(semaphore, target):
        pl.semaphore_signal(
            semaphore, inc=1, device_id={"spec": target}, device_id_type=pl.DeviceIdType.MESH
        )

    for step in range(1, group):
        signal(barrier, zone * group + (rank + step) % group)

    @pl.when(zone > 0)
    def _():
        for c in range(2):
            signal(barrier, (zone - 1) * group + side * 2 + c)

    @pl.when(zone < zones - 1)
    def _():
        for c in range(2):
            signal(barrier, (zone + 1) * group + side * 2 + c)

    @pl.when(zone == 0)
    def _():
        held[0:HALO] = jnp.zeros((HALO, ND, width), f32)

    @pl.when(zone == zones - 1)
    def _():
        held[HALO + freq_group :] = jnp.zeros((HALO, ND, width), f32)

    def block_of(index, t):
        return t * group + index

    def tile_of(index, t):
        return pl.ds(pl.multiple_of(block_of(index, t) * LANES, LANES), LANES)

    def lanes_of(t):
        return pl.ds(t * LANES, LANES)

    offsets = [(dy, dc) for dy in range(sides) for dc in range(2)]

    def rank_of(offset):
        return (side + offset[0]) % sides * 2 + (core + offset[1]) % 2

    def y_copy(begin, end, peer, t):
        return remote(
            adv.at[begin:end, :, tile_of(peer, t)],
            held.at[pl.ds(HALO + rank * freq_dev + begin, end - begin), :, lanes_of(t)],
            y_sem, held_sem.at[rank, t], zone * group + peer,
        )

    dirs = lax.broadcasted_iota(jnp.int32, (ND, LANES), 0).astype(f32)
    heading = 2.0 * math.pi * (dirs + 0.5) / ND
    cos_h, sin_h = jnp.cos(heading), jnp.sin(heading)
    log_step = math.log(1.1)
    lats = [math.radians(-75.0 + 150.0 * (r + 0.5) / lat_count) for r in range(lat_count)]

    def omega_of(freq, shape):
        return jnp.exp(jnp.full(shape, log_step, f32) * (freq.astype(f32) - NF // 2))

    square_rows = lax.broadcasted_iota(jnp.int32, (LANES, LANES), 0)
    square_cols = lax.broadcasted_iota(jnp.int32, (LANES, LANES), 1)
    small[0].wait()
    aux_ref[...] = sea_raw[...].astype(f32).reshape(1, cells)
    sea = [aux_ref[0:1, r * NLON : (r + 1) * NLON] for r in range(lat_count)]
    mask = [aux_ref[0:1, i * LANES : (i + 1) * LANES] for i in range(cell_tiles)]
    tri_up = jnp.where(square_rows < square_cols, 1.0, 0.0).astype(bf16)
    ranks = jnp.dot(rows_of(mask, ND // 2, LANES), tri_up, preferred_element_type=f32)
    before = jnp.zeros((1, 1), f32)
    for i in range(cell_tiles):
        place_ref[0:1, i * LANES : (i + 1) * LANES] = jnp.where(
            mask[i] > 0.0, ranks[i : i + 1] + before, LAND
        )
        before = before + jnp.sum(mask[i], axis=1, keepdims=True)
    pair_rows = lax.broadcasted_iota(jnp.int32, (WIDE, reach), 0).astype(f32)

    def build(pair):
        cols = pl.ds(pl.multiple_of(pair * WIDE, LANES), reach)
        first = (pair * WIDE).astype(f32)
        hit = jnp.where(place_ref[0:1, cols] - first == pair_rows, 1.0, 0.0)
        spread_ref[pl.ds(pl.multiple_of(pair * WIDE, LANES), WIDE), cols] = hit.astype(
            spread_ref.dtype
        )

    def packed(values, pair):
        cols = pl.ds(pl.multiple_of(pair * WIDE, LANES), reach)
        return lax.dot_general(
            values[:, cols],
            spread_ref[pl.ds(pl.multiple_of(pair * WIDE, LANES), WIDE), cols],
            (((1,), (1,)), ((), ())), preferred_element_type=f32,
        )

    quarter = ND // 4
    tiles = NLON // LANES
    def advect(f):
        loads[f].wait()
        freq = (me * freq_dev + f).astype(f32)
        speed = 0.2 * jnp.exp(jnp.full((quarter, LANES), -log_step, f32) * freq)
        for q in range(4):
            east, north = q in (0, 3), q in (0, 1)
            rows = slice(f * ND + q * quarter, f * ND + (q + 1) * quarter)
            part = slice(q * quarter, (q + 1) * quarter)
            cx0 = speed * jnp.abs(cos_h[part])
            cy = jnp.concatenate([speed * jnp.abs(sin_h[part])] * tiles, axis=1)
            cx = [jnp.concatenate([cx0 * (1.0 / math.cos(a))] * tiles, axis=1) for a in lats]
            rest = [1.0 - (cx[r] + cy) for r in range(lat_count)]
            energy = [raw[rows, r * NLON : (r + 1) * NLON] * sea[r] for r in range(lat_count)]
            for step in range(ADV_STEPS):
                fresh = []
                for r in range(lat_count):
                    e = energy[r]
                    side_x = pltpu.roll(e, 1 if east else NLON - 1, 1)
                    other = r - 1 if north else r + 1
                    value = rest[r] * e + cx[r] * side_x
                    if 0 <= other < lat_count:
                        value = value + cy * energy[other]
                    fresh.append(value if step == ADV_STEPS - 1 else value * sea[r])
                energy = fresh
            for r in range(lat_count):
                moved[rows, r * NLON : (r + 1) * NLON] = energy[r]
        for i, piece in enumerate(split_bf16(moved[f * ND : (f + 1) * ND])):
            split[(3 * f + i) * ND : (3 * f + i + 1) * ND, :] = piece

    def cols_of(index):
        return pl.ds(pl.multiple_of(index * LANES, LANES), LANES)

    def side_of(dy):
        return (side + dy) % sides

    def pack(t, dy, begin, end):
        return packed(split.at[begin * 3 * ND : end * 3 * ND], t * sides + side_of(dy))

    def unload(t, dy, begin, end, got):
        pair = t * sides + side_of(dy)
        cols = pl.ds(pl.multiple_of(pair * WIDE, LANES), WIDE)
        here = pl.ds(pl.multiple_of(side_of(dy) * WIDE, LANES), WIDE)
        mass, moment = None, None
        for f in range(begin, end):
            base = (f - begin) * 3 * ND
            piece = got[base : base + ND] + got[base + ND : base + 2 * ND] + (
                got[base + 2 * ND : base + 3 * ND]
            )
            adv[f, :, cols] = piece
            total = jnp.sum(piece, axis=0, keepdims=True)
            scaled = omega_of(me * freq_dev + f, (1, WIDE)) * total
            mass = total if mass is None else mass + total
            moment = scaled if moment is None else moment + scaled
        if begin:
            mass, moment = mass + mom_out[t, 0:1, here], moment + mom_out[t, 1:2, here]
        mom_out[t, 0:1, here] = mass
        mom_out[t, 1:2, here] = moment

    def send_far(t, dy, begin, end):
        for c in range(2):
            y_copy(begin, end, side_of(dy) * 2 + c, t).start()

    top = side > 0
    early_way, late_way = jnp.where(top, 0, 1), jnp.where(top, 1, 0)
    early_ok = jnp.where(top, zone < zones - 1, zone > 0)
    late_ok = jnp.where(top, zone > 0, zone < zones - 1)
    early_zone = jnp.where(top, zone + 1, zone + zones - 1) % zones
    late_zone = jnp.where(top, zone + zones - 1, zone + 1) % zones
    early_shift = HALO + jnp.where(top, -freq_group, freq_group)
    late_shift = HALO + jnp.where(top, freq_group, -freq_group)

    def early_slot(slot):
        return early_ok & jnp.where(top, slot >= freq_group - HALO, slot < HALO)

    def late_slot(slot):
        return late_ok & jnp.where(top, slot < HALO, slot >= freq_group - HALO)

    def early_copy(f, c, t):
        return remote(
            adv.at[f, :, tile_of(side * 2 + c, t)],
            held.at[early_shift + rank * freq_dev + f, :, lanes_of(t)],
            z_sem.at[0], halo_sem.at[early_way, t], early_zone * group + side * 2 + c,
        )

    def forward(slot, t, now):
        @pl.when(late_slot(slot) & now)
        def _():
            remote(
                held.at[HALO + slot, :, lanes_of(t)],
                held.at[late_shift + slot, :, lanes_of(t)],
                z_sem.at[1], halo_sem.at[late_way, t], late_zone * group + rank,
            ).start()

    def send_near(t):
        for c in range(2):
            for f in range(freq_dev):
                @pl.when(early_slot(rank * freq_dev + f))
                def _():
                    early_copy(f, c, t).start()

        y_copy(0, freq_dev, rank_of((0, 1)), t).start()
        for f in range(freq_dev):
            held[HALO + rank * freq_dev + f, :, lanes_of(t)] = adv[f, :, tile_of(rank, t)]

    def arrive_group(dy, t):
        for dc in range(2):
            if (dy, dc) != (0, 0):
                source = rank_of((dy, dc))
                slots = held.at[
                    pl.ds(HALO + source * freq_dev, freq_dev), :, lanes_of(t)
                ]
                remote(
                    slots, slots, y_sem, held_sem.at[source, t], (me + 1) % count
                ).wait_recv()
                if dy:
                    for f in range(freq_dev):
                        forward(source * freq_dev + f, t, t < parts - 1 or side == 0)

    def up_relay(level):
        @pl.when(zone == level)
        def _():
            pl.semaphore_wait(chain_sem.at[0], 1)
            if level < zones - 1:
                signal(chain_sem.at[0], (me + group) % count)

    def down_relay(level):
        @pl.when(zone == level)
        def _():
            pl.semaphore_wait(chain_sem.at[1], 1)
            if level > 0:
                signal(chain_sem.at[1], (me + count - group) % count)

    def moment_copy(target_zone, target_rank):
        return remote(
            mom_out.at[:, :, cols_of(target_rank)], mom_in.at[me],
            mom_send, mom_recv, target_zone * group + target_rank,
        )

    def send_zone_moments():
        for step in range(1, group):
            moment_copy(zone, (rank + step) % group).start()

    def send_moments():
        for away in range(1, zones):
            for other in range(group):
                moment_copy((zone + away) % zones, other).start()

    far = list(range(1, sides))
    for dy in far:
        build(side_of(dy))
    advect(0)
    for dy in far:
        unload(0, dy, 0, 1, pack(0, dy, 0, 1))
    advect(1)
    pl.semaphore_wait(
        barrier, group - 1 + jnp.where(zone > 0, 2, 0) + jnp.where(zone < zones - 1, 2, 0)
    )
    for dy in far:
        send_far(0, dy, 0, 1)

    @pl.when(zone == 0)
    def _():
        signal(chain_sem.at[0], (me + group) % count)

    @pl.when(zone == zones - 1)
    def _():
        signal(chain_sem.at[1], (me + count - group) % count)

    up_relay(1)
    for f in range(2, freq_dev):
        advect(f)
    for level in range(2, zones - 1):
        up_relay(level)
    got = [pack(0, dy, 1, freq_dev) for dy in far]
    build(side)
    got_near = pack(0, 0, 0, freq_dev)
    for dy in far:
        unload(0, dy, 1, freq_dev, got[dy - 1])
        send_far(0, dy, 1, freq_dev)
    unload(0, 0, 0, freq_dev, got_near)
    send_near(0)
    down_relay(zones - 2)
    upper = zone >= zones // 2
    for t in range(1, parts):
        last = t == parts - 1
        for dy in far:
            build(t * sides + side_of(dy))
        got = [pack(t, dy, 0, freq_dev) for dy in far]
        build(t * sides + side)
        got_near = pack(t, 0, 0, freq_dev)
        for dy in far:
            unload(t, dy, 0, freq_dev, got[dy - 1])

            @pl.when(jnp.logical_not(upper) if last else zone >= 0)
            def _():
                send_far(t, dy, 0, freq_dev)

        unload(t, 0, 0, freq_dev, got_near)
        if last:
            up_relay(zones - 1)
            send_zone_moments()

            @pl.when(upper)
            def _():
                send_moments()
                for dy in far:
                    send_far(t, dy, 0, freq_dev)

        send_near(t)

    small[1].wait()
    small[2].wait()
    speed_all = wind_raw[...].reshape(1, cells)
    angle_all = angle_raw[...].reshape(1, cells)
    wsplit[...] = rows_of(
        split_bf16(speed_all * jnp.cos(angle_all)) + split_bf16(speed_all * jnp.sin(angle_all)),
        2 * quarter, cells,
    )
    for t in range(parts):
        own = packed(wsplit, t * sides + side)
        own = jnp.where(core == 0, own[:, :LANES], own[:, LANES:])
        along = own[0:1] + own[1:2] + own[2:3]
        across = own[3:4] + own[4:5] + own[5:6]
        wind[:, t * LANES : (t + 1) * LANES] = cos_h * along + sin_h * across

    for level in range(zones - 3, 0, -1):
        down_relay(level)

    @pl.when(jnp.logical_not(upper) & (zone > 0))
    def _():
        send_moments()

    for dy in far:
        arrive_group(dy, 0)
    mom_in[me] = mom_out[:, :, cols_of(rank)]
    start = window_start(count, me, cells)
    near_ref[...] = place_ref[0:1, pl.ds(pl.multiple_of(start, LANES), WIDE)]
    for t in range(parts):
        arrive_group(0, t)

    acc[...] = jnp.zeros_like(acc)
    ascending = side > 0

    def arrive_halo(at_top, t):
        block = held.at[0:HALO, :, lanes_of(t)]

        @pl.when(jnp.where(at_top, zone < zones - 1, zone > 0))
        def _():
            way = jnp.where(at_top, 1, 0)
            remote(
                block, block, z_sem.at[0], halo_sem.at[way, t], (me + 1) % count
            ).wait_recv()

    def ret_copy(owner, t):
        return remote(
            done.at[pl.ds(owner * freq_dev, freq_dev), :, lanes_of(t)],
            back.at[:, :, tile_of(rank, t)],
            ret_send, ret_recv.at[t], zone * group + owner,
        )

    def turn(values, amount):
        return pltpu.roll(values, amount % ND, 0)

    def rate(a, p, m):
        return a * (a * (p + m) - 2.0 * (p * m))

    def scale(index, factor):
        return jnp.where((index >= 3) & (index <= NF - 3), factor, 0.0).astype(f32)

    def slab(k, t):
        return held[HALO + k, :, t * LANES : (t + 1) * LANES]

    def rates(own, p2, m3):
        return rate(own, turn(p2, -1), turn(m3, 3)) + rate(own, turn(p2, 1), turn(m3, -3))

    def grown(own, freq, t):
        omega = omega_of(freq, (1, LANES))
        push = wind[:, t * LANES : (t + 1) * LANES] * omega - 1.0
        return own + (0.05 * omega) * jnp.maximum(0.0, push) * own

    def tally(energy, near, freq, t):
        flow = scale(freq, 0.001) * near
        acc[:, t * LANES : (t + 1) * LANES] += energy + (flow + flow - 2.0 * flow)

    def sources(t, begin, end):
        def source_step(i, carry):
            k = jnp.where(ascending, i, freq_group - 1 - i)
            freq = zone * freq_group + k
            own = slab(k, t)
            p2, m3, m2, m5, p3, p5 = (slab(k + shift, t) for shift in (2, -3, -2, -5, 3, 5))
            near = rates(own, p2, m3)
            low = rate(turn(m2, 1), own, turn(m5, 4)) + rate(turn(m2, -1), own, turn(m5, -4))
            high = rate(turn(p3, -3), turn(p5, -4), own) + rate(turn(p3, 3), turn(p5, 4), own)
            interaction = scale(freq, -0.002) * near + scale(freq - 2, 0.001) * low + (
                scale(freq + 3, 0.001) * high
            )
            energy = grown(own, freq, t)
            done[k, :, t * LANES : (t + 1) * LANES] = energy + interaction
            if begin == 0:
                tally(energy, near, freq, t)
            return carry

        lax.fori_loop(begin, end, source_step, 0, unroll=UNROLL)

    def tally_rest(t):
        def rest_step(i, carry):
            k = jnp.where(ascending, half + i, half - 1 - i)
            center = jnp.where(
                ascending,
                jnp.where(i < 2, i - 2, half + i - 2),
                jnp.where(i < 3, freq_group + i, half + 2 - i),
            )
            near = rates(slab(center, t), slab(center + 2, t), slab(center - 3, t))
            energy = grown(slab(k, t), zone * freq_group + k, t)
            tally(energy, near, zone * freq_group + center, t)
            return carry

        lax.fori_loop(0, half, rest_step, 0, unroll=UNROLL)

    half = freq_group // 2
    near_side = rank_of((0, 1))

    def first_half(t):
        arrive_halo(jnp.logical_not(ascending), t)
        sources(t, 0, half)
        if t == parts - 1:
            tally_rest(t)
            send_sums()
        for dy in range(1, sides):
            for dc in range(2):
                ret_copy(rank_of((dy, dc)), t).start()
        if t == parts - 1:
            for slot in range(HALO):
                forward(slot, t, side > 0)

        if t == 0:
            down_relay(0)

            @pl.when(zone == 0)
            def _():
                send_moments()

        if t < parts - 1:
            tally_rest(t)

    def send_sums():
        sum_out[...] = jnp.sum(acc[...], axis=0, keepdims=True)
        for step in range(1, count):
            remote(sum_out, sum_in.at[me], sum_send, sum_recv, (me + step) % count).start()
        sum_in[me] = sum_out[...]

    def second_half(t):
        if t == parts - 1:
            damping_terms()
        arrive_halo(ascending, t)
        sources(t, half, freq_group)
        ret_copy(near_side, t).start()
        back[:, :, tile_of(rank, t)] = done[
            pl.ds(rank * freq_dev, freq_dev), :, lanes_of(t)
        ]

    def zone_copy(dst_rank, src, dst, send, recv):
        return remote(src, dst, send, recv, zone * group + dst_rank)

    def damping_terms():
        others = mom_in.at[0 : count - 1]
        remote(others, others, mom_send, mom_recv, (me + 1) % count).wait_recv()
        total = jnp.sum(mom_in[...], axis=0) * (1.0 / (NF * ND))
        for t in range(parts):
            energy_mean, moment_one = total[t, 0:1], total[t, 1:2]
            mean_freq = moment_one / (energy_mean + 1e-06)
            steepness = energy_mean * mean_freq * mean_freq
            breaking = steepness * steepness / (1.0 + steepness * steepness)
            damp_out[t, 0:1] = 0.03 * breaking
            damp_out[t, 1:2] = 0.03 * breaking * moment_one
        for i in range(1, group):
            zone_copy(
                rank_of(offsets[i]), damp_out, damp_in.at[rank], damp_send, damp_recv
            ).start()
        damp_in[rank] = damp_out[...]

    first_half(0)
    for t in range(1, parts):
        for dy in range(1, sides):
            arrive_group(dy, t)
        first_half(t)
        second_half(t - 1)
    second_half(parts - 1)

    def gather_back(t):
        block = done.at[0 : (group - 1) * freq_dev, :, lanes_of(t)]
        remote(block, block, ret_send, ret_recv.at[t], (me + 1) % count).wait_recv()
        cols = slice(t * group * LANES, (t + 1) * group * LANES)
        for f in range(freq_dev):
            for i, piece in enumerate(split_bf16(back[f, :, cols])[:2]):
                split[(2 * f + i) * ND : (2 * f + i + 1) * ND, cols] = piece

    def spread(j, begin, end):
        low, high = max(0, j * WIDE - land), min(sea_cells, (j + 1) * WIDE)
        return jnp.dot(
            split[begin:end, low:high],
            spread_ref[low:high, j * WIDE : (j + 1) * WIDE],
            preferred_element_type=f32,
        )

    def joined(got, f):
        base = 2 * f * ND
        return got[base : base + ND] + got[base + ND : base + 2 * ND]

    values = 2 * bins_dev
    early_tiles = [
        j for j in range(cells // WIDE) if (j + 1) * WIDE <= (parts - 1) * group * LANES
    ]
    for t in range(parts - 1):
        gather_back(t)
    for j in early_tiles:
        got = spread(j, 0, values)
        for f in range(freq_dev):
            full_ref[f * ND : (f + 1) * ND, j * WIDE : (j + 1) * WIDE] = joined(got, f)
    gather_back(parts - 1)
    others = damp_in.at[0 : group - 1]
    remote(others, others, damp_send, damp_recv, (me + 1) % count).wait_recv()
    for g in range(group):
        for t in range(parts):
            loss_ref[0:1, block_of(g, t) * LANES : (block_of(g, t) + 1) * LANES] = damp_in[
                g, t, 1:2
            ]
            split[values : values + ND // 2, block_of(g, t) * LANES : (block_of(g, t) + 1) * LANES] = rows_of(
                split_bf16(damp_in[g, t, 0:1]), ND // 2, LANES
            )
    for j in range(cells // WIDE):
        cols = slice(j * WIDE, (j + 1) * WIDE)
        got = spread(j, values if j in early_tiles else 0, values + ND // 2)
        rows = got[got.shape[0] - ND // 2 :]
        row = rows[0:1] + rows[1:2] + rows[2:3]
        for f in range(freq_dev):
            bins = slice(f * ND, (f + 1) * ND)
            value = full_ref[bins, cols] if j in early_tiles else joined(got, f)
            loss = omega_of(me * freq_dev + f, (1, WIDE)) * row
            full_ref[bins, cols] = value - loss * moved[bins, cols]

    block = held.at[0 : (group - 1) * freq_dev]
    remote(block, block, y_sem, held_sem.at[0, 0], (me + 1) % count).wait_send()
    remote(block, block, ret_send, ret_recv.at[0], (me + 1) % count).wait_send()
    others = mom_in.at[0 : count - 1]
    remote(others, others, mom_send, mom_recv, (me + 1) % count).wait_send()
    others = damp_in.at[0 : group - 1]
    remote(others, others, damp_send, damp_recv, (me + 1) % count).wait_send()
    def drain(slots, way):
        block = held.at[0:slots]
        remote(
            block, block, z_sem.at[way], halo_sem.at[0, 0], (me + 1) % count
        ).wait_send()

    for f in range(freq_dev):
        @pl.when(early_slot(rank * freq_dev + f))
        def _():
            drain(2, 0)

    @pl.when(late_ok)
    def _():
        drain(HALO, 1)

    others = sum_in.at[0 : count - 1]
    remote(others, others, sum_send, sum_recv, (me + 1) % count).wait()
    for g in range(group):
        mass = sum_in[g]
        for other in range(1, zones):
            mass = mass + sum_in[other * group + g]
        for t in range(parts):
            cols = slice(block_of(g, t) * LANES, (block_of(g, t) + 1) * LANES)
            mean_out[0:1, cols] = mass[:, t * LANES : (t + 1) * LANES]


def store_kernel(
    count, full_in, mass_in, near_in, loss_in, new_out, wave_out, mean_out,
    height, wave_ref, mean_ref, sem,
):
    cells = full_in.shape[1]
    sea_cells = mass_in.shape[1]
    copies = [
        pltpu.make_async_copy(full_in, new_out, sem.at[0]),
        pltpu.make_async_copy(wave_ref, wave_out, sem.at[1]),
        pltpu.make_async_copy(mean_ref, mean_out, sem.at[2]),
    ]
    copies[0].start()
    mean = mass_in[...] * (1.0 / (NF * ND)) - loss_in[...]
    height[...] = 4.0 * jnp.sqrt(mean + 1e-06)
    me = lax.axis_index("spec")
    points = cells // count
    shift = me * points - window_start(count, me, cells)
    halves = []
    for h in range(WIDE // LANES):
        place = jnp.broadcast_to(near_in[:, h * LANES : (h + 1) * LANES], (8, LANES))
        place = place.astype(jnp.int32)
        wave = jnp.zeros((8, LANES), jnp.float32)
        for b in range(sea_cells // LANES):
            values = jnp.broadcast_to(height[:, b * LANES : (b + 1) * LANES], (8, LANES))
            found = jnp.take_along_axis(values, place % LANES, axis=1)
            wave = jnp.where(place // LANES == b, found, wave)
        halves.append(wave)
    wave = jnp.concatenate(halves, axis=1)
    wave_ref[...] = pltpu.roll(wave, (WIDE - shift) % WIDE, 1)[0, :points]
    copies[1].start()
    mean_ref[...] = jnp.sum(height[...], axis=1, keepdims=True) * (1.0 / sea_cells)
    copies[2].start()
    for copy in copies:
        copy.wait()


def fused_local(spectrum, sea_mask, wind_speed, wind_angle):
    count = lax.axis_size("spec")
    bins_dev, cells = spectrum.shape
    group = group_size(count, bins_dev, cells)
    freq_dev = bins_dev // ND
    freq_group = freq_dev * group
    sea_cells = SEA_DEV * count
    width = sea_cells // group
    points = cells // count
    parts = width // LANES
    f32, bf16 = jnp.float32, jnp.bfloat16
    dma = pltpu.SemaphoreType.DMA
    vmem = pl.BlockSpec(memory_space=pltpu.VMEM)
    handed = pl.pallas_call(
        functools.partial(fused_kernel, count, group),
        out_shape=(
            pltpu.VMEM((bins_dev, cells), f32),
            pltpu.VMEM((1, sea_cells), f32),
            pltpu.VMEM((1, WIDE), f32),
            pltpu.VMEM((1, sea_cells), f32),
        ),
        in_specs=[pl.BlockSpec(memory_space=pl.ANY)] * 4,
        out_specs=(vmem,) * 4,
        scratch_shapes=[
            pltpu.VMEM((cells,), jnp.int32),
            pltpu.VMEM((cells,), f32),
            pltpu.VMEM((cells,), f32),
            pltpu.VMEM((1, cells), f32),
            pltpu.VMEM((1, cells), f32),
            pltpu.VMEM((sea_cells, cells), jnp.float8_e4m3fn),
            dma((3,)),
            pltpu.VMEM((bins_dev, cells), f32),
            pltpu.VMEM((bins_dev, cells), f32),
            pltpu.VMEM((3 * bins_dev + ND // 2, cells), bf16),
            pltpu.VMEM((ND // 2, cells), bf16),
            pltpu.VMEM((freq_dev, ND, sea_cells), f32),
            pltpu.VMEM((freq_group + 2 * HALO, ND, width), f32),
            pltpu.VMEM((freq_group, ND, width), f32),
            pltpu.VMEM((freq_dev, ND, sea_cells), f32),
            pltpu.VMEM((parts, 2, group * LANES), f32),
            pltpu.VMEM((count, parts, 2, LANES), f32),
            pltpu.VMEM((ND, width), f32),
            pltpu.VMEM((ND, width), f32),
            pltpu.VMEM((1, width), f32),
            pltpu.VMEM((count, 1, width), f32),
            pltpu.VMEM((parts, 2, LANES), f32),
            pltpu.VMEM((group, parts, 2, LANES), f32),
            dma((freq_dev,)),
            dma((group, parts)),
            dma((2, parts)),
            dma,
            dma((2,)),
            pltpu.SemaphoreType.REGULAR((2,)),
            dma,
            dma,
            dma,
            dma((parts,)),
            dma,
            dma,
            dma,
            dma,
        ],
        compiler_params=pltpu.CompilerParams(collective_id=0, has_side_effects=True),
    )(sea_mask, wind_speed, wind_angle, spectrum)
    out, wave, mean = pl.pallas_call(
        functools.partial(store_kernel, count),
        out_shape=(
            pltpu.HBM((bins_dev, cells), f32),
            pltpu.HBM((points,), f32),
            pltpu.HBM((1, 1), f32),
        ),
        in_specs=[vmem] * 4,
        out_specs=(pl.BlockSpec(memory_space=pltpu.HBM),) * 3,
        scratch_shapes=[
            pltpu.VMEM((1, sea_cells), f32), pltpu.VMEM((points,), f32),
            pltpu.VMEM((1, 1), f32), dma((3,)),
        ],
    )(*[pltpu.with_memory_space_constraint(piece, pltpu.VMEM) for piece in handed])
    return (out, wave, mean.reshape(1))


def solution(mesh):
    in_specs = (P(("grp", "spec"), None), P(), P("grp"), P("grp"))
    out_specs = (P(("grp", "spec"), None), P(("grp", "spec")), P("grp"))

    def body(spectrum, sea_mask, wind_speed, wind_angle):
        fits = group_size(mesh.shape["spec"], *spectrum.shape)
        plan = fused_local if fits else local
        return plan(spectrum, sea_mask, wind_speed, wind_angle)

    return jax.shard_map(body, mesh=mesh, in_specs=in_specs, out_specs=out_specs, check_vma=False)
```

```python
import functools
import math

import jax
import jax.numpy as jnp
from jax import lax
from jax.experimental import pallas as pl
from jax.experimental.pallas import tpu as pltpu
from jax.sharding import PartitionSpec as P

NF = 48
ND = 32
NLON = 384
ADV_STEPS = 2
SEA_DEV = 64


def upwind_step(energy, courant_x, courant_y, sea_grid):
    west_cell = jnp.roll(energy, 1, axis=2)
    east_cell = jnp.roll(energy, -1, axis=2)
    edge_row = jnp.zeros_like(energy[:, :1])
    south_cell = jnp.concatenate([edge_row, energy[:, :-1]], axis=1)
    north_cell = jnp.concatenate([energy[:, 1:], edge_row], axis=1)
    updated = (
        energy
        - jnp.maximum(courant_x, 0.0) * (energy - west_cell)
        - jnp.minimum(courant_x, 0.0) * (east_cell - energy)
        - jnp.maximum(courant_y, 0.0) * (energy - south_cell)
        - jnp.minimum(courant_y, 0.0) * (north_cell - energy)
    )
    return updated * sea_grid


def courant_numbers(freq_index, dir_index, lat_count, dir_count):
    speed = 0.2 * jnp.exp(-math.log(1.1) * freq_index)
    heading = 2.0 * math.pi * (dir_index + 0.5) / dir_count
    rows = jnp.arange(lat_count, dtype=jnp.float32)
    latitude = (-75.0 + 150.0 * (rows + 0.5) / lat_count) * (math.pi / 180.0)
    courant_x = (speed * jnp.cos(heading))[:, None, None] / jnp.cos(latitude)[None, :, None]
    courant_y = (speed * jnp.sin(heading))[:, None, None]
    return (courant_x, courant_y)


def shift_freq(values, amount):
    if amount > 0:
        filler = jnp.zeros_like(values[:amount])
        return jnp.concatenate([filler, values[:-amount]], axis=0)
    filler = jnp.zeros_like(values[:-amount])
    return jnp.concatenate([values[-amount:], filler], axis=0)


def source_terms(energy, speed, angle):
    freq_count = energy.shape[0]
    dir_count = energy.shape[1]
    freq_ids = jnp.arange(freq_count, dtype=jnp.float32)
    frequency = jnp.exp(math.log(1.1) * (freq_ids - freq_count // 2))[:, None, None]
    heading = (2.0 * math.pi * (jnp.arange(dir_count, dtype=jnp.float32) + 0.5) / dir_count)[
        None, :, None
    ]
    energy_mean = jnp.mean(energy, axis=(0, 1))
    moment_one = jnp.mean(frequency * energy, axis=(0, 1))
    mean_freq = moment_one / (energy_mean + 1e-06)
    steepness = energy_mean * mean_freq * mean_freq
    breaking = steepness * steepness / (1.0 + steepness * steepness)
    wind_gain = (
        0.05
        * frequency
        * jnp.maximum(
            0.0, speed[None, None, :] * frequency * jnp.cos(heading - angle[None, None, :]) - 1.0
        )
    )
    damping = 0.03 * frequency * breaking[None, None, :]
    valid = ((freq_ids >= 3) & (freq_ids <= freq_count - 3)).astype(jnp.float32)[:, None, None]
    interaction = jnp.zeros_like(energy)
    for mirror in (1, -1):
        plus_bins = shift_freq(jnp.roll(energy, -mirror, axis=1), -2)
        minus_bins = shift_freq(jnp.roll(energy, 3 * mirror, axis=1), 3)
        transfer_rate = (
            0.001
            * valid
            * (energy * energy * (plus_bins + minus_bins) - 2.0 * energy * plus_bins * minus_bins)
        )
        interaction = interaction - 2.0 * transfer_rate
        interaction = interaction + jnp.roll(shift_freq(transfer_rate, 2), mirror, axis=1)
        interaction = interaction + jnp.roll(shift_freq(transfer_rate, -3), -3 * mirror, axis=1)
    updated = energy + (wind_gain - damping) * energy + interaction
    raw_height = 4.0 * jnp.sqrt(jnp.mean(updated, axis=(0, 1)) + 1e-06)
    return (updated, raw_height)


def local(spectrum, sea_mask, wind_speed, wind_angle):
    count = lax.axis_size("spec")
    position = lax.axis_index("spec")
    bins_dev = spectrum.shape[0]
    cells = spectrum.shape[1]
    points = cells // count
    lat_count = cells // NLON
    sea_float = sea_mask.astype(jnp.float32)
    bin_ids = position * bins_dev + jnp.arange(bins_dev, dtype=jnp.int32)
    freq_index = (bin_ids // ND).astype(jnp.float32)
    dir_index = (bin_ids % ND).astype(jnp.float32)
    courant_x, courant_y = courant_numbers(freq_index, dir_index, lat_count, ND)
    sea_grid = sea_float.reshape(1, lat_count, NLON)
    energy = (spectrum * sea_float[None, :]).reshape(bins_dev, lat_count, NLON)
    for substep in range(ADV_STEPS):
        energy = upwind_step(energy, courant_x, courant_y, sea_grid)
    advected = energy.reshape(bins_dev, cells)
    outgoing = advected.reshape(bins_dev, count, points)
    arrived = lax.all_to_all(outgoing, "spec", split_axis=1, concat_axis=0, tiled=True)
    start = position * points
    speed_own = lax.dynamic_slice_in_dim(wind_speed, start, points)
    angle_own = lax.dynamic_slice_in_dim(wind_angle, start, points)
    sea_own = lax.dynamic_slice_in_dim(sea_float, start, points)
    updated, raw_height = source_terms(arrived.reshape(NF, ND, points), speed_own, angle_own)
    wave_height = sea_own * raw_height
    own_total = jnp.zeros((count, 1), jnp.float32) + jnp.sum(wave_height)
    returned, totals = (
        lax.all_to_all(
            updated.reshape(NF * ND, 1, points), "spec", split_axis=0, concat_axis=1, tiled=True
        ),
        lax.all_to_all(own_total, "spec", split_axis=0, concat_axis=1, tiled=True),
    )
    new_spectrum = returned.reshape(bins_dev, cells)
    height_sum = jnp.sum(totals)
    mean_height = (height_sum / (SEA_DEV * count)).reshape(1)
    return (new_spectrum, wave_height, mean_height)


HALO = 5
LANES = 128
WIDE = 256
LAND = 4096.0
UNROLL = 3


def group_size(count, bins_dev, cells):
    size = 4
    if count % size or bins_dev % ND or cells % (size * LANES) or cells % NLON:
        return 0
    if NLON % LANES or bins_dev // ND * size < 2 * HALO or cells % count:
        return 0
    sea = SEA_DEV * count
    if sea > min(cells, LAND) or sea % (size * LANES) or sea % WIDE or cells % WIDE:
        return 0
    if (cells - sea) % WIDE:
        return 0
    return size


def split_bf16(values):
    high = values.astype(jnp.bfloat16)
    left = values - high.astype(jnp.float32)
    mid = left.astype(jnp.bfloat16)
    low = (left - mid.astype(jnp.float32)).astype(jnp.bfloat16)
    return high, mid, low


def rows_of(parts, height, width):
    ids = lax.broadcasted_iota(jnp.int32, (height, width), 0)
    out = jnp.zeros((height, width), jnp.float32)
    for i, part in enumerate(parts):
        out = jnp.where(ids == i, jnp.broadcast_to(part.astype(jnp.float32), (height, width)), out)
    return out.astype(jnp.bfloat16)


def window_start(count, me, cells):
    return jnp.minimum(me * (cells // count) // LANES * LANES, cells - WIDE)


def fused_kernel(
    count, group, sea_in, wind_in, angle_in, spec_ref, full_ref, mean_out, near_ref, loss_ref,
    sea_raw, wind_raw, angle_raw, aux_ref, place_ref, spread_ref, aux_sem,
    raw, moved, split, wsplit, adv, held, done, back, mom_out, mom_in, wind, acc,
    sum_out, sum_in, damp_out, damp_in,
    load_sem, held_sem, halo_sem, y_sem, z_sem, chain_sem, mom_send, mom_recv,
    ret_send, ret_recv, sum_send, sum_recv, damp_send, damp_recv,
):
    f32, bf16 = jnp.float32, jnp.bfloat16
    freq_dev, _, sea_cells = adv.shape
    bins_dev, cells = moved.shape
    freq_group = freq_dev * group
    width = sea_cells // group
    zones = count // group
    lat_count = cells // NLON
    sides = group // 2
    parts = width // LANES
    cell_tiles = cells // LANES
    land = cells - sea_cells
    reach = land + WIDE
    me = lax.axis_index("spec")
    zone, rank = me // group, me % group
    side, core = rank // 2, rank % 2

    def remote(src, dst, send, recv, target):
        return pltpu.make_async_remote_copy(
            src_ref=src, dst_ref=dst, send_sem=send, recv_sem=recv,
            device_id={"spec": target}, device_id_type=pl.DeviceIdType.MESH,
        )

    loads = [
        pltpu.make_async_copy(
            spec_ref.at[pl.ds(f * ND, ND)], raw.at[pl.ds(f * ND, ND)], load_sem.at[f]
        )
        for f in range(freq_dev)
    ]
    small = [
        pltpu.make_async_copy(sea_in, sea_raw, aux_sem.at[0]),
        pltpu.make_async_copy(wind_in, wind_raw, aux_sem.at[1]),
        pltpu.make_async_copy(angle_in, angle_raw, aux_sem.at[2]),
    ]
    for load in small[:1] + loads + small[1:]:
        load.start()
    barrier = pltpu.get_barrier_semaphore()

    def signal(semaphore, target):
        pl.semaphore_signal(
            semaphore, inc=1, device_id={"spec": target}, device_id_type=pl.DeviceIdType.MESH
        )

    for step in range(1, group):
        signal(barrier, zone * group + (rank + step) % group)

    @pl.when(zone > 0)
    def _():
        for c in range(2):
            signal(barrier, (zone - 1) * group + side * 2 + c)

    @pl.when(zone < zones - 1)
    def _():
        for c in range(2):
            signal(barrier, (zone + 1) * group + side * 2 + c)

    @pl.when(zone == 0)
    def _():
        held[0:HALO] = jnp.zeros((HALO, ND, width), f32)

    @pl.when(zone == zones - 1)
    def _():
        held[HALO + freq_group :] = jnp.zeros((HALO, ND, width), f32)

    def block_of(index, t):
        return t * group + index

    def tile_of(index, t):
        return pl.ds(pl.multiple_of(block_of(index, t) * LANES, LANES), LANES)

    def lanes_of(t):
        return pl.ds(t * LANES, LANES)

    offsets = [(dy, dc) for dy in range(sides) for dc in range(2)]

    def rank_of(offset):
        return (side + offset[0]) % sides * 2 + (core + offset[1]) % 2

    def y_copy(begin, end, peer, t):
        return remote(
            adv.at[begin:end, :, tile_of(peer, t)],
            held.at[pl.ds(HALO + rank * freq_dev + begin, end - begin), :, lanes_of(t)],
            y_sem, held_sem.at[rank, t], zone * group + peer,
        )

    dirs = lax.broadcasted_iota(jnp.int32, (ND, LANES), 0).astype(f32)
    heading = 2.0 * math.pi * (dirs + 0.5) / ND
    cos_h, sin_h = jnp.cos(heading), jnp.sin(heading)
    log_step = math.log(1.1)
    lats = [math.radians(-75.0 + 150.0 * (r + 0.5) / lat_count) for r in range(lat_count)]

    def omega_of(freq, shape):
        return jnp.exp(jnp.full(shape, log_step, f32) * (freq.astype(f32) - NF // 2))

    square_rows = lax.broadcasted_iota(jnp.int32, (LANES, LANES), 0)
    square_cols = lax.broadcasted_iota(jnp.int32, (LANES, LANES), 1)
    small[0].wait()
    aux_ref[...] = sea_raw[...].astype(f32).reshape(1, cells)
    sea = [aux_ref[0:1, r * NLON : (r + 1) * NLON] for r in range(lat_count)]
    mask = [aux_ref[0:1, i * LANES : (i + 1) * LANES] for i in range(cell_tiles)]
    tri_up = jnp.where(square_rows < square_cols, 1.0, 0.0).astype(bf16)
    ranks = jnp.dot(rows_of(mask, ND // 2, LANES), tri_up, preferred_element_type=f32)
    before = jnp.zeros((1, 1), f32)
    for i in range(cell_tiles):
        place_ref[0:1, i * LANES : (i + 1) * LANES] = jnp.where(
            mask[i] > 0.0, ranks[i : i + 1] + before, LAND
        )
        before = before + jnp.sum(mask[i], axis=1, keepdims=True)
    pair_rows = lax.broadcasted_iota(jnp.int32, (WIDE, reach), 0).astype(f32)

    def build(pair):
        cols = pl.ds(pl.multiple_of(pair * WIDE, LANES), reach)
        first = (pair * WIDE).astype(f32)
        hit = jnp.where(place_ref[0:1, cols] - first == pair_rows, 1.0, 0.0)
        spread_ref[pl.ds(pl.multiple_of(pair * WIDE, LANES), WIDE), cols] = hit.astype(
            spread_ref.dtype
        )

    def packed(values, pair):
        cols = pl.ds(pl.multiple_of(pair * WIDE, LANES), reach)
        return lax.dot_general(
            values[:, cols],
            spread_ref[pl.ds(pl.multiple_of(pair * WIDE, LANES), WIDE), cols],
            (((1,), (1,)), ((), ())), preferred_element_type=f32,
        )

    quarter = ND // 4
    tiles = NLON // LANES
    def advect(f):
        loads[f].wait()
        freq = (me * freq_dev + f).astype(f32)
        speed = 0.2 * jnp.exp(jnp.full((quarter, LANES), -log_step, f32) * freq)
        for q in range(4):
            east, north = q in (0, 3), q in (0, 1)
            rows = slice(f * ND + q * quarter, f * ND + (q + 1) * quarter)
            part = slice(q * quarter, (q + 1) * quarter)
            cx0 = speed * jnp.abs(cos_h[part])
            cy = jnp.concatenate([speed * jnp.abs(sin_h[part])] * tiles, axis=1)
            cx = [jnp.concatenate([cx0 * (1.0 / math.cos(a))] * tiles, axis=1) for a in lats]
            rest = [1.0 - (cx[r] + cy) for r in range(lat_count)]
            energy = [raw[rows, r * NLON : (r + 1) * NLON] * sea[r] for r in range(lat_count)]
            for step in range(ADV_STEPS):
                fresh = []
                for r in range(lat_count):
                    e = energy[r]
                    side_x = pltpu.roll(e, 1 if east else NLON - 1, 1)
                    other = r - 1 if north else r + 1
                    value = rest[r] * e + cx[r] * side_x
                    if 0 <= other < lat_count:
                        value = value + cy * energy[other]
                    fresh.append(value if step == ADV_STEPS - 1 else value * sea[r])
                energy = fresh
            for r in range(lat_count):
                moved[rows, r * NLON : (r + 1) * NLON] = energy[r]
        for i, piece in enumerate(split_bf16(moved[f * ND : (f + 1) * ND])):
            split[(3 * f + i) * ND : (3 * f + i + 1) * ND, :] = piece

    def cols_of(index):
        return pl.ds(pl.multiple_of(index * LANES, LANES), LANES)

    def side_of(dy):
        return (side + dy) % sides

    def pack(t, dy, begin, end):
        return packed(split.at[begin * 3 * ND : end * 3 * ND], t * sides + side_of(dy))

    def unload(t, dy, begin, end, got):
        pair = t * sides + side_of(dy)
        cols = pl.ds(pl.multiple_of(pair * WIDE, LANES), WIDE)
        here = pl.ds(pl.multiple_of(side_of(dy) * WIDE, LANES), WIDE)
        mass, moment = None, None
        for f in range(begin, end):
            base = (f - begin) * 3 * ND
            piece = got[base : base + ND] + got[base + ND : base + 2 * ND] + (
                got[base + 2 * ND : base + 3 * ND]
            )
            adv[f, :, cols] = piece
            total = jnp.sum(piece, axis=0, keepdims=True)
            scaled = omega_of(me * freq_dev + f, (1, WIDE)) * total
            mass = total if mass is None else mass + total
            moment = scaled if moment is None else moment + scaled
        if begin:
            mass, moment = mass + mom_out[t, 0:1, here], moment + mom_out[t, 1:2, here]
        mom_out[t, 0:1, here] = mass
        mom_out[t, 1:2, here] = moment

    def send_far(t, dy, begin, end):
        for c in range(2):
            y_copy(begin, end, side_of(dy) * 2 + c, t).start()

    top = side > 0
    early_way, late_way = jnp.where(top, 0, 1), jnp.where(top, 1, 0)
    early_ok = jnp.where(top, zone < zones - 1, zone > 0)
    late_ok = jnp.where(top, zone > 0, zone < zones - 1)
    early_zone = jnp.where(top, zone + 1, zone + zones - 1) % zones
    late_zone = jnp.where(top, zone + zones - 1, zone + 1) % zones
    early_shift = HALO + jnp.where(top, -freq_group, freq_group)
    late_shift = HALO + jnp.where(top, freq_group, -freq_group)

    def early_slot(slot):
        return early_ok & jnp.where(top, slot >= freq_group - HALO, slot < HALO)

    def late_slot(slot):
        return late_ok & jnp.where(top, slot < HALO, slot >= freq_group - HALO)

    def early_copy(f, c, t):
        return remote(
            adv.at[f, :, tile_of(side * 2 + c, t)],
            held.at[early_shift + rank * freq_dev + f, :, lanes_of(t)],
            z_sem.at[0], halo_sem.at[early_way, t], early_zone * group + side * 2 + c,
        )

    def forward(slot, t, now):
        @pl.when(late_slot(slot) & now)
        def _():
            remote(
                held.at[HALO + slot, :, lanes_of(t)],
                held.at[late_shift + slot, :, lanes_of(t)],
                z_sem.at[1], halo_sem.at[late_way, t], late_zone * group + rank,
            ).start()

    def send_near(t):
        for c in range(2):
            for f in range(freq_dev):
                @pl.when(early_slot(rank * freq_dev + f))
                def _():
                    early_copy(f, c, t).start()

        y_copy(0, freq_dev, rank_of((0, 1)), t).start()
        for f in range(freq_dev):
            held[HALO + rank * freq_dev + f, :, lanes_of(t)] = adv[f, :, tile_of(rank, t)]

    def arrive_group(dy, t):
        for dc in range(2):
            if (dy, dc) != (0, 0):
                source = rank_of((dy, dc))
                slots = held.at[
                    pl.ds(HALO + source * freq_dev, freq_dev), :, lanes_of(t)
                ]
                remote(
                    slots, slots, y_sem, held_sem.at[source, t], (me + 1) % count
                ).wait_recv()
                if dy:
                    for f in range(freq_dev):
                        forward(source * freq_dev + f, t, t < parts - 1 or side == 0)

    def up_relay(level):
        @pl.when(zone == level)
        def _():
            pl.semaphore_wait(chain_sem.at[0], 1)
            if level < zones - 1:
                signal(chain_sem.at[0], (me + group) % count)

    def down_relay(level):
        @pl.when(zone == level)
        def _():
            pl.semaphore_wait(chain_sem.at[1], 1)
            if level > 0:
                signal(chain_sem.at[1], (me + count - group) % count)

    def moment_copy(target_zone, target_rank):
        return remote(
            mom_out.at[:, :, cols_of(target_rank)], mom_in.at[me],
            mom_send, mom_recv, target_zone * group + target_rank,
        )

    def send_zone_moments():
        for step in range(1, group):
            moment_copy(zone, (rank + step) % group).start()

    def send_moments():
        for away in range(1, zones):
            for other in range(group):
                moment_copy((zone + away) % zones, other).start()

    far = list(range(1, sides))
    for dy in far:
        build(side_of(dy))
    advect(0)
    for dy in far:
        unload(0, dy, 0, 1, pack(0, dy, 0, 1))
    advect(1)
    pl.semaphore_wait(
        barrier, group - 1 + jnp.where(zone > 0, 2, 0) + jnp.where(zone < zones - 1, 2, 0)
    )
    for dy in far:
        send_far(0, dy, 0, 1)

    @pl.when(zone == 0)
    def _():
        signal(chain_sem.at[0], (me + group) % count)

    @pl.when(zone == zones - 1)
    def _():
        signal(chain_sem.at[1], (me + count - group) % count)

    up_relay(1)
    for f in range(2, freq_dev):
        advect(f)
    for level in range(2, zones - 1):
        up_relay(level)
    got = [pack(0, dy, 1, freq_dev) for dy in far]
    build(side)
    got_near = pack(0, 0, 0, freq_dev)
    for dy in far:
        unload(0, dy, 1, freq_dev, got[dy - 1])
        send_far(0, dy, 1, freq_dev)
    unload(0, 0, 0, freq_dev, got_near)
    send_near(0)
    down_relay(zones - 2)
    upper = zone >= zones // 2
    for t in range(1, parts):
        last = t == parts - 1
        for dy in far:
            build(t * sides + side_of(dy))
        got = [pack(t, dy, 0, freq_dev) for dy in far]
        build(t * sides + side)
        got_near = pack(t, 0, 0, freq_dev)
        for dy in far:
            unload(t, dy, 0, freq_dev, got[dy - 1])

            @pl.when(jnp.logical_not(upper) if last else zone >= 0)
            def _():
                send_far(t, dy, 0, freq_dev)

        unload(t, 0, 0, freq_dev, got_near)
        if last:
            up_relay(zones - 1)
            send_zone_moments()

            @pl.when(upper)
            def _():
                send_moments()
                for dy in far:
                    send_far(t, dy, 0, freq_dev)

        send_near(t)

    small[1].wait()
    small[2].wait()
    speed_all = wind_raw[...].reshape(1, cells)
    angle_all = angle_raw[...].reshape(1, cells)
    wsplit[...] = rows_of(
        split_bf16(speed_all * jnp.cos(angle_all)) + split_bf16(speed_all * jnp.sin(angle_all)),
        2 * quarter, cells,
    )
    for t in range(parts):
        own = packed(wsplit, t * sides + side)
        own = jnp.where(core == 0, own[:, :LANES], own[:, LANES:])
        along = own[0:1] + own[1:2] + own[2:3]
        across = own[3:4] + own[4:5] + own[5:6]
        wind[:, t * LANES : (t + 1) * LANES] = cos_h * along + sin_h * across

    for level in range(zones - 3, 0, -1):
        down_relay(level)

    @pl.when(jnp.logical_not(upper) & (zone > 0))
    def _():
        send_moments()

    for dy in far:
        arrive_group(dy, 0)
    mom_in[me] = mom_out[:, :, cols_of(rank)]
    start = window_start(count, me, cells)
    near_ref[...] = place_ref[0:1, pl.ds(pl.multiple_of(start, LANES), WIDE)]
    for t in range(parts):
        arrive_group(0, t)

    acc[...] = jnp.zeros_like(acc)
    ascending = side > 0

    def arrive_halo(at_top, t):
        block = held.at[0:HALO, :, lanes_of(t)]

        @pl.when(jnp.where(at_top, zone < zones - 1, zone > 0))
        def _():
            way = jnp.where(at_top, 1, 0)
            remote(
                block, block, z_sem.at[0], halo_sem.at[way, t], (me + 1) % count
            ).wait_recv()

    def ret_copy(owner, t):
        return remote(
            done.at[pl.ds(owner * freq_dev, freq_dev), :, lanes_of(t)],
            back.at[:, :, tile_of(rank, t)],
            ret_send, ret_recv.at[t], zone * group + owner,
        )

    def turn(values, amount):
        return pltpu.roll(values, amount % ND, 0)

    def rate(a, p, m):
        return a * (a * (p + m) - 2.0 * (p * m))

    def scale(index, factor):
        return jnp.where((index >= 3) & (index <= NF - 3), factor, 0.0).astype(f32)

    def slab(k, t):
        return held[HALO + k, :, t * LANES : (t + 1) * LANES]

    def rates(own, p2, m3):
        return rate(own, turn(p2, -1), turn(m3, 3)) + rate(own, turn(p2, 1), turn(m3, -3))

    def grown(own, freq, t):
        omega = omega_of(freq, (1, LANES))
        push = wind[:, t * LANES : (t + 1) * LANES] * omega - 1.0
        return own + (0.05 * omega) * jnp.maximum(0.0, push) * own

    def tally(energy, near, freq, t):
        flow = scale(freq, 0.001) * near
        acc[:, t * LANES : (t + 1) * LANES] += energy + (flow + flow - 2.0 * flow)

    def sources(t, begin, end):
        def source_step(i, carry):
            k = jnp.where(ascending, i, freq_group - 1 - i)
            freq = zone * freq_group + k
            own = slab(k, t)
            p2, m3, m2, m5, p3, p5 = (slab(k + shift, t) for shift in (2, -3, -2, -5, 3, 5))
            near = rates(own, p2, m3)
            low = rate(turn(m2, 1), own, turn(m5, 4)) + rate(turn(m2, -1), own, turn(m5, -4))
            high = rate(turn(p3, -3), turn(p5, -4), own) + rate(turn(p3, 3), turn(p5, 4), own)
            interaction = scale(freq, -0.002) * near + scale(freq - 2, 0.001) * low + (
                scale(freq + 3, 0.001) * high
            )
            energy = grown(own, freq, t)
            done[k, :, t * LANES : (t + 1) * LANES] = energy + interaction
            if begin == 0:
                tally(energy, near, freq, t)
            return carry

        lax.fori_loop(begin, end, source_step, 0, unroll=UNROLL)

    def tally_rest(t):
        def rest_step(i, carry):
            k = jnp.where(ascending, half + i, half - 1 - i)
            center = jnp.where(
                ascending,
                jnp.where(i < 2, i - 2, half + i - 2),
                jnp.where(i < 3, freq_group + i, half + 2 - i),
            )
            near = rates(slab(center, t), slab(center + 2, t), slab(center - 3, t))
            energy = grown(slab(k, t), zone * freq_group + k, t)
            tally(energy, near, zone * freq_group + center, t)
            return carry

        lax.fori_loop(0, half, rest_step, 0, unroll=UNROLL)

    half = freq_group // 2
    near_side = rank_of((0, 1))

    def first_half(t):
        arrive_halo(jnp.logical_not(ascending), t)
        sources(t, 0, half)
        if t == parts - 1:
            tally_rest(t)
            send_sums()
        for dy in range(1, sides):
            for dc in range(2):
                ret_copy(rank_of((dy, dc)), t).start()
        if t == parts - 1:
            for slot in range(HALO):
                forward(slot, t, side > 0)

        if t == 0:
            down_relay(0)

            @pl.when(zone == 0)
            def _():
                send_moments()

        if t < parts - 1:
            tally_rest(t)

    def send_sums():
        sum_out[...] = jnp.sum(acc[...], axis=0, keepdims=True)
        for step in range(1, count):
            remote(sum_out, sum_in.at[me], sum_send, sum_recv, (me + step) % count).start()
        sum_in[me] = sum_out[...]

    def second_half(t):
        if t == parts - 1:
            damping_terms()
        arrive_halo(ascending, t)
        sources(t, half, freq_group)
        ret_copy(near_side, t).start()
        back[:, :, tile_of(rank, t)] = done[
            pl.ds(rank * freq_dev, freq_dev), :, lanes_of(t)
        ]

    def zone_copy(dst_rank, src, dst, send, recv):
        return remote(src, dst, send, recv, zone * group + dst_rank)

    def damping_terms():
        others = mom_in.at[0 : count - 1]
        remote(others, others, mom_send, mom_recv, (me + 1) % count).wait_recv()
        total = jnp.sum(mom_in[...], axis=0) * (1.0 / (NF * ND))
        for t in range(parts):
            energy_mean, moment_one = total[t, 0:1], total[t, 1:2]
            mean_freq = moment_one / (energy_mean + 1e-06)
            steepness = energy_mean * mean_freq * mean_freq
            breaking = steepness * steepness / (1.0 + steepness * steepness)
            damp_out[t, 0:1] = 0.03 * breaking
            damp_out[t, 1:2] = 0.03 * breaking * moment_one
        for i in range(1, group):
            zone_copy(
                rank_of(offsets[i]), damp_out, damp_in.at[rank], damp_send, damp_recv
            ).start()
        damp_in[rank] = damp_out[...]

    first_half(0)
    for t in range(1, parts):
        for dy in range(1, sides):
            arrive_group(dy, t)
        first_half(t)
        second_half(t - 1)
    second_half(parts - 1)

    def gather_back(t):
        block = done.at[0 : (group - 1) * freq_dev, :, lanes_of(t)]
        remote(block, block, ret_send, ret_recv.at[t], (me + 1) % count).wait_recv()
        cols = slice(t * group * LANES, (t + 1) * group * LANES)
        for f in range(freq_dev):
            for i, piece in enumerate(split_bf16(back[f, :, cols])):
                split[(3 * f + i) * ND : (3 * f + i + 1) * ND, cols] = piece

    def spread(j, begin, end):
        low, high = max(0, j * WIDE - land), min(sea_cells, (j + 1) * WIDE)
        return jnp.dot(
            split[begin:end, low:high],
            spread_ref[low:high, j * WIDE : (j + 1) * WIDE],
            preferred_element_type=f32,
        )

    def joined(got, f):
        base = 3 * f * ND
        return got[base : base + ND] + got[base + ND : base + 2 * ND] + (
            got[base + 2 * ND : base + 3 * ND]
        )

    values = 3 * bins_dev
    early_tiles = [
        j for j in range(cells // WIDE) if (j + 1) * WIDE <= (parts - 1) * group * LANES
    ]
    for t in range(parts - 1):
        gather_back(t)
    for j in early_tiles:
        got = spread(j, 0, values)
        for f in range(freq_dev):
            full_ref[f * ND : (f + 1) * ND, j * WIDE : (j + 1) * WIDE] = joined(got, f)
    gather_back(parts - 1)
    others = damp_in.at[0 : group - 1]
    remote(others, others, damp_send, damp_recv, (me + 1) % count).wait_recv()
    for g in range(group):
        for t in range(parts):
            loss_ref[0:1, block_of(g, t) * LANES : (block_of(g, t) + 1) * LANES] = damp_in[
                g, t, 1:2
            ]
            split[values:, block_of(g, t) * LANES : (block_of(g, t) + 1) * LANES] = rows_of(
                split_bf16(damp_in[g, t, 0:1]), ND // 2, LANES
            )
    for j in range(cells // WIDE):
        cols = slice(j * WIDE, (j + 1) * WIDE)
        got = spread(j, values if j in early_tiles else 0, values + ND // 2)
        rows = got[got.shape[0] - ND // 2 :]
        row = rows[0:1] + rows[1:2] + rows[2:3]
        for f in range(freq_dev):
            bins = slice(f * ND, (f + 1) * ND)
            value = full_ref[bins, cols] if j in early_tiles else joined(got, f)
            loss = omega_of(me * freq_dev + f, (1, WIDE)) * row
            full_ref[bins, cols] = value - loss * moved[bins, cols]

    block = held.at[0 : (group - 1) * freq_dev]
    remote(block, block, y_sem, held_sem.at[0, 0], (me + 1) % count).wait_send()
    remote(block, block, ret_send, ret_recv.at[0], (me + 1) % count).wait_send()
    others = mom_in.at[0 : count - 1]
    remote(others, others, mom_send, mom_recv, (me + 1) % count).wait_send()
    others = damp_in.at[0 : group - 1]
    remote(others, others, damp_send, damp_recv, (me + 1) % count).wait_send()
    def drain(slots, way):
        block = held.at[0:slots]
        remote(
            block, block, z_sem.at[way], halo_sem.at[0, 0], (me + 1) % count
        ).wait_send()

    for f in range(freq_dev):
        @pl.when(early_slot(rank * freq_dev + f))
        def _():
            drain(2, 0)

    @pl.when(late_ok)
    def _():
        drain(HALO, 1)

    others = sum_in.at[0 : count - 1]
    remote(others, others, sum_send, sum_recv, (me + 1) % count).wait()
    for g in range(group):
        mass = sum_in[g]
        for other in range(1, zones):
            mass = mass + sum_in[other * group + g]
        for t in range(parts):
            cols = slice(block_of(g, t) * LANES, (block_of(g, t) + 1) * LANES)
            mean_out[0:1, cols] = mass[:, t * LANES : (t + 1) * LANES]


def store_kernel(
    count, full_in, mass_in, near_in, loss_in, new_out, wave_out, mean_out,
    height, wave_ref, mean_ref, sem,
):
    cells = full_in.shape[1]
    sea_cells = mass_in.shape[1]
    copies = [
        pltpu.make_async_copy(full_in, new_out, sem.at[0]),
        pltpu.make_async_copy(wave_ref, wave_out, sem.at[1]),
        pltpu.make_async_copy(mean_ref, mean_out, sem.at[2]),
    ]
    copies[0].start()
    mean = mass_in[...] * (1.0 / (NF * ND)) - loss_in[...]
    height[...] = 4.0 * jnp.sqrt(mean + 1e-06)
    me = lax.axis_index("spec")
    points = cells // count
    shift = me * points - window_start(count, me, cells)
    halves = []
    for h in range(WIDE // LANES):
        place = jnp.broadcast_to(near_in[:, h * LANES : (h + 1) * LANES], (8, LANES))
        place = place.astype(jnp.int32)
        wave = jnp.zeros((8, LANES), jnp.float32)
        for b in range(sea_cells // LANES):
            values = jnp.broadcast_to(height[:, b * LANES : (b + 1) * LANES], (8, LANES))
            found = jnp.take_along_axis(values, place % LANES, axis=1)
            wave = jnp.where(place // LANES == b, found, wave)
        halves.append(wave)
    wave = jnp.concatenate(halves, axis=1)
    wave_ref[...] = pltpu.roll(wave, (WIDE - shift) % WIDE, 1)[0, :points]
    copies[1].start()
    mean_ref[...] = jnp.sum(height[...], axis=1, keepdims=True) * (1.0 / sea_cells)
    copies[2].start()
    for copy in copies:
        copy.wait()


def fused_local(spectrum, sea_mask, wind_speed, wind_angle):
    count = lax.axis_size("spec")
    bins_dev, cells = spectrum.shape
    group = group_size(count, bins_dev, cells)
    freq_dev = bins_dev // ND
    freq_group = freq_dev * group
    sea_cells = SEA_DEV * count
    width = sea_cells // group
    points = cells // count
    parts = width // LANES
    f32, bf16 = jnp.float32, jnp.bfloat16
    dma = pltpu.SemaphoreType.DMA
    vmem = pl.BlockSpec(memory_space=pltpu.VMEM)
    handed = pl.pallas_call(
        functools.partial(fused_kernel, count, group),
        out_shape=(
            pltpu.VMEM((bins_dev, cells), f32),
            pltpu.VMEM((1, sea_cells), f32),
            pltpu.VMEM((1, WIDE), f32),
            pltpu.VMEM((1, sea_cells), f32),
        ),
        in_specs=[pl.BlockSpec(memory_space=pl.ANY)] * 4,
        out_specs=(vmem,) * 4,
        scratch_shapes=[
            pltpu.VMEM((cells,), jnp.int32),
            pltpu.VMEM((cells,), f32),
            pltpu.VMEM((cells,), f32),
            pltpu.VMEM((1, cells), f32),
            pltpu.VMEM((1, cells), f32),
            pltpu.VMEM((sea_cells, cells), jnp.float8_e4m3fn),
            dma((3,)),
            pltpu.VMEM((bins_dev, cells), f32),
            pltpu.VMEM((bins_dev, cells), f32),
            pltpu.VMEM((3 * bins_dev + ND // 2, cells), bf16),
            pltpu.VMEM((ND // 2, cells), bf16),
            pltpu.VMEM((freq_dev, ND, sea_cells), f32),
            pltpu.VMEM((freq_group + 2 * HALO, ND, width), f32),
            pltpu.VMEM((freq_group, ND, width), f32),
            pltpu.VMEM((freq_dev, ND, sea_cells), f32),
            pltpu.VMEM((parts, 2, group * LANES), f32),
            pltpu.VMEM((count, parts, 2, LANES), f32),
            pltpu.VMEM((ND, width), f32),
            pltpu.VMEM((ND, width), f32),
            pltpu.VMEM((1, width), f32),
            pltpu.VMEM((count, 1, width), f32),
            pltpu.VMEM((parts, 2, LANES), f32),
            pltpu.VMEM((group, parts, 2, LANES), f32),
            dma((freq_dev,)),
            dma((group, parts)),
            dma((2, parts)),
            dma,
            dma((2,)),
            pltpu.SemaphoreType.REGULAR((2,)),
            dma,
            dma,
            dma,
            dma((parts,)),
            dma,
            dma,
            dma,
            dma,
        ],
        compiler_params=pltpu.CompilerParams(collective_id=0, has_side_effects=True),
    )(sea_mask, wind_speed, wind_angle, spectrum)
    out, wave, mean = pl.pallas_call(
        functools.partial(store_kernel, count),
        out_shape=(
            pltpu.HBM((bins_dev, cells), f32),
            pltpu.HBM((points,), f32),
            pltpu.HBM((1, 1), f32),
        ),
        in_specs=[vmem] * 4,
        out_specs=(pl.BlockSpec(memory_space=pltpu.HBM),) * 3,
        scratch_shapes=[
            pltpu.VMEM((1, sea_cells), f32), pltpu.VMEM((points,), f32),
            pltpu.VMEM((1, 1), f32), dma((3,)),
        ],
    )(*[pltpu.with_memory_space_constraint(piece, pltpu.VMEM) for piece in handed])
    return (out, wave, mean.reshape(1))


def solution(mesh):
    in_specs = (P(("grp", "spec"), None), P(), P("grp"), P("grp"))
    out_specs = (P(("grp", "spec"), None), P(("grp", "spec")), P("grp"))

    def body(spectrum, sea_mask, wind_speed, wind_angle):
        fits = group_size(mesh.shape["spec"], *spectrum.shape)
        plan = fused_local if fits else local
        return plan(spectrum, sea_mask, wind_speed, wind_angle)

    return jax.shard_map(body, mesh=mesh, in_specs=in_specs, out_specs=out_specs, check_vma=False)
```
